32 devices in a mesh: fsdp: 4 (over y, x), ctx: 2 (over core), tp: 4 (over z).
Axes of the slice: x: 2, y: 2, z: 4, core: 2. Of those that a mesh axis runs over, the one named last changes fastest.
Arguments:
- tokens: bfloat16 [24576, 768], P(('fsdp', 'ctx')), may hold values from -6 to 6
- grad_out: bfloat16 [24576, 768], P(('fsdp', 'ctx')), may hold values from -6 to 6
- lengths: int32 [4, 4], P('fsdp'), may hold values from 256 to 3072, as said below
- norm_gain: float32 [768], replicated, may hold values from 0.25 to 1.75
- w_z: bfloat16 [768, 1536], P('fsdp', 'tp'), may hold values from -0.21875 to 0.21875
- w_x: bfloat16 [768, 1536], P('fsdp', 'tp'), may hold values from -0.21875 to 0.21875
- w_bc: bfloat16 [768, 256], P('fsdp'), may hold values from -0.21875 to 0.21875
- w_dt: bfloat16 [768, 24], P('fsdp', 'tp'), may hold values from -0.21875 to 0.21875
- conv_x_w: float32 [4, 1536], P(None, 'tp'), may hold values from -3 to 3
- conv_x_b: float32 [1536], P('tp'), may hold values from -3 to 3
- conv_bc_w: float32 [4, 256], replicated, may hold values from -3 to 3
- conv_bc_b: float32 [256], replicated, may hold values from -3 to 3
- dt_bias: float32 [24], P('tp')
- a_log: float32 [24], P('tp'), may hold values from -3 to 1
- d_skip: float32 [24], P('tp'), may hold values from 0.5 to 1.5
- gate_gain: float32 [1536], P('tp'), may hold values from 0.25 to 1.75
- w_out: bfloat16 [1536, 768], P('tp', 'fsdp'), may hold values from -0.15625 to 0.15625
Outputs:
- layer_out: bfloat16 [24576, 768], P(('fsdp', 'ctx'), 'tp')
- grad_tokens: bfloat16 [24576, 768], P(('fsdp', 'ctx'), 'tp')
- grad_norm_gain: float32 [768], P('tp')
- grad_w_z: float32 [768, 1536], P('fsdp', 'tp')
- grad_w_x: float32 [768, 1536], P('fsdp', 'tp')
- grad_w_bc: float32 [768, 256], P('fsdp')
- grad_w_dt: float32 [768, 24], P('fsdp', 'tp')
- grad_conv_x_w: float32 [4, 1536], P(None, 'tp')
- grad_conv_x_b: float32 [1536], P('tp')
- grad_conv_bc_w: float32 [4, 256], replicated
- grad_conv_bc_b: float32 [256], replicated
- grad_dt_bias: float32 [24], P('tp')
- grad_a_log: float32 [24], P('tp')
- grad_d_skip: float32 [24], P('tp')
- grad_gate_gain: float32 [1536], P('tp')
- grad_w_out: float32 [1536, 768], P('tp', 'fsdp')
The draws below stay inside these ranges and needn't reach their ends.
Inputs may be any that keep to these rules, and one draw needn't show every extreme that they name: Row g gives the lengths of the 4 sequences of group g in the order they stand; they sum to 6144, and one of them is exactly 3072.
All inputs are finite; a program needn't handle non-finite values.
Results may differ from the reference program's by a relative error of at most 0.017.
Values may be sent and summed in bfloat16 or wider, within the bound.
A program may use at most 256 MiB of HBM per device.

```python
from functools import partial
import jax
import jax.numpy as jnp
from jax import lax

D = 768
HEADS = 24
HEADDIM = 64
STATE = 128
CONV = 4
STRETCH = 256
MINLEN = 256
SEQS = 4
INNER = 1536
GROUP = 6144
TOKENS = 24576
LONGEST = 3072


def draw_lengths(key, part):
    groups = TOKENS // GROUP
    others = SEQS - 1
    remain = GROUP - LONGEST
    base_len = remain // others
    extra_len = remain - base_len * others
    spread = min(base_len - MINLEN, LONGEST - base_len - extra_len)
    pair_count = max(others // 2, 1)
    key_delta, key_order = jax.random.split(key, 2)
    deltas = jax.random.randint(key_delta, (groups, pair_count), 0, spread + 1, dtype=jnp.int32)
    position = jnp.arange(others, dtype=jnp.int32)
    pair_of = jnp.minimum(position // 2, pair_count - 1)
    pair_sign = jnp.where(position >= 2 * (others // 2), 0, 1 - 2 * (position % 2)).astype(jnp.int32)
    middle = base_len + pair_sign[None, :] * deltas[:, pair_of]
    middle = middle + jnp.where(position == others - 1, extra_len, 0).astype(jnp.int32)[None, :]
    joined = jnp.concatenate([jnp.full((groups, 1), LONGEST, jnp.int32), middle.astype(jnp.int32)], axis=1)
    shuffle = jax.vmap(lambda sub_key: jax.random.permutation(sub_key, SEQS))(jax.random.split(key_order, groups))
    return jnp.take_along_axis(joined, shuffle.astype(jnp.int32), axis=1).astype(jnp.int32)


def lasting_heads(key):
    order = jax.random.permutation(jax.random.fold_in(key, 101), HEADS)
    count = HEADS // 2
    return order < count


def lasting_log_rate(key):
    return jax.random.uniform(jax.random.fold_in(key, 103), (HEADS,), jnp.float32, -2.0, -0.5)


def draw_a_log(key, part):
    lasting = lasting_heads(key)
    quick = jax.random.uniform(jax.random.fold_in(key, 107), (HEADS,), jnp.float32, -3.0, 1.0)
    return jnp.where(lasting, lasting_log_rate(key), quick).astype(jnp.float32)


def draw_dt_bias(key, part):
    lasting = lasting_heads(key)
    quick = jax.random.uniform(jax.random.fold_in(key, 109), (HEADS,), jnp.float32, -4.5, -1.5)
    total_loss = jnp.exp(jax.random.uniform(jax.random.fold_in(key, 113), (HEADS,), jnp.float32, jnp.log(0.2), jnp.log(1.5)))
    step_target = total_loss / (jnp.exp(lasting_log_rate(key)) * LONGEST)
    slow_bias = jnp.log(jnp.expm1(step_target)) - 0.5
    return jnp.where(lasting, slow_bias, quick).astype(jnp.float32)


def levels(rng, shape, cuts, smallest, largest):
    def one(axis_at, blocks):
        draws = jax.random.uniform(jax.random.fold_in(jax.random.fold_in(rng, 6), axis_at), (blocks,), jnp.float32, smallest / len(cuts), largest / len(cuts))
        return jnp.repeat(jnp.exp(draws), shape[axis_at] // blocks).reshape((-1,) + (1,) * (len(shape) - axis_at - 1))

    loudness = one(*cuts[0])
    for cut in cuts[1:]:
        loudness = loudness * one(*cut)
    return loudness


def gaussian(stream_key, extent, scale, reach, cuts=(), kind=jnp.bfloat16):
    values = jax.random.normal(stream_key, extent, jnp.float32) * scale
    if len(cuts) > 0:
        values = levels(stream_key, extent, cuts, -0.22, 0.18) * values
    return jnp.clip(values, min=-reach, max=reach).astype(kind)


def setup_inputs(seed: int = 0) -> dict:
    seeds = jax.random.split(jax.random.key(seed), 18)
    return {
        "tokens": gaussian(seeds[0], (TOKENS, D), 1.0, 6.0, ((0, 8),)),
        "grad_out": gaussian(seeds[1], (TOKENS, D), 1.0, 6.0, ((0, 8),)),
        "lengths": draw_lengths(jax.random.fold_in(seeds[17], 71), 0),
        "norm_gain": jnp.clip(1.0 + 0.15 * jax.random.normal(seeds[3], (D,), jnp.float32), 0.25, 1.75),
        "w_z": gaussian(seeds[4], (D, INNER), D ** -0.5, 0.21875, ((0, 4), (1, 4))),
        "w_x": gaussian(seeds[5], (D, INNER), D ** -0.5, 0.21875, ((0, 4), (1, 4))),
        "w_bc": gaussian(seeds[6], (D, 2 * STATE), D ** -0.5, 0.21875, ((0, 4),)),
        "w_dt": gaussian(seeds[7], (D, HEADS), D ** -0.5, 0.21875, ((0, 4), (1, 4))),
        "conv_x_w": gaussian(seeds[8], (CONV, INNER), 0.5, 3.0, ((1, 4),), jnp.float32),
        "conv_x_b": gaussian(seeds[9], (INNER,), 0.3, 3.0, ((0, 4),), jnp.float32),
        "conv_bc_w": gaussian(seeds[10], (CONV, 2 * STATE), 0.5, 3.0, (), jnp.float32),
        "conv_bc_b": gaussian(seeds[11], (2 * STATE,), 0.3, 3.0, (), jnp.float32),
        "dt_bias": draw_dt_bias(jax.random.fold_in(seeds[17], 71), 0),
        "a_log": draw_a_log(jax.random.fold_in(seeds[17], 71), 0),
        "d_skip": jnp.clip(0.5 + 1.0 * jax.random.uniform(seeds[14], (HEADS,), jnp.float32) ** levels(seeds[14], (HEADS,), ((0, 4),), -0.2, 0.2), 0.5, 1.5),
        "gate_gain": jnp.clip(1.0 + 0.15 * jax.random.normal(seeds[15], (INNER,), jnp.float32), 0.25, 1.75),
        "w_out": gaussian(seeds[16], (INNER, D), INNER ** -0.5, 0.15625, ((0, 4), (1, 4))),
    }


epsilon = 1e-05
highest = lax.Precision.HIGHEST

@jax.custom_vjp
def low(v):
    return lax.optimization_barrier(v.astype(jnp.bfloat16)).astype(jnp.float32)

@jax.custom_vjp
def low_back(v):
    return v

def low_keep(v):
    return (low(v), None)

def low_pass(kept, grad):
    return (grad,)

def back_keep(v):
    return (v, None)

def back_low(kept, grad):
    return (low(grad),)
low.defvjp(low_keep, low_pass)
low_back.defvjp(back_keep, back_low)

def matmul_hi(left, right):
    return jnp.dot(left, right, precision=highest)

def stretch_layer(params, carry_in, inputs):
    norm_gain, w_z, w_x, w_bc, w_dt, conv_w, conv_b, dt_bias, a_log, d_skip, gate_gain, w_out = params
    rim_vals, rim_segs, state_now, last_seg = carry_in
    residual, segment = inputs
    rim_width = CONV - 1
    inverse = lax.rsqrt(lax.optimization_barrier(jnp.mean(residual * residual, axis=1, keepdims=True)) + epsilon)
    normed = low(residual * inverse * norm_gain)
    z_part = low_back(matmul_hi(normed, w_z))
    joined = low_back(low(matmul_hi(normed, jnp.concatenate([w_x, w_bc], axis=1))))
    dt_raw = low_back(matmul_hi(normed, w_dt))
    extended = jnp.concatenate([rim_vals, joined], axis=0)
    ext_segs = jnp.concatenate([rim_segs, segment])
    preact = jnp.zeros(joined.shape, jnp.float32) + conv_b[None, :]
    for offset in range(CONV):
        tap_valid = (ext_segs[offset:offset + STRETCH] == segment).astype(jnp.float32)
        preact = preact + conv_w[offset][None, :] * extended[offset:offset + STRETCH] * tap_valid[:, None]
    activated = jax.nn.silu(preact)
    values = low(activated[:, :INNER]).reshape(STRETCH, HEADS, HEADDIM)
    b_mat = low(activated[:, INNER:INNER + STATE])
    c_mat = low(activated[:, INNER + STATE:])
    step_size = jax.nn.softplus(dt_raw + dt_bias)
    log_decay = -step_size * jnp.exp(a_log)
    cum_log = jnp.cumsum(log_decay, axis=0)
    positions = jnp.arange(STRETCH, dtype=jnp.int32)
    same_seq = (segment[:, None] == segment[None, :]) & (positions[:, None] >= positions[None, :])
    head_cum = cum_log.T
    log_gap = head_cum[:, :, None] - head_cum[:, None, :]
    decay_mat = jnp.where(same_seq[None], jnp.exp(jnp.where(same_seq[None], log_gap, 0.0)), 0.0)
    gram_mat = low_back(matmul_hi(c_mat, b_mat.T))
    mixing = low(gram_mat[None] * decay_mat * step_size.T[:, None, :])
    inner_out = low_back(jnp.einsum('hts,shp->thp', mixing, values, precision=highest))
    enter_mask = (segment == last_seg).astype(jnp.float32)
    scale_in = jnp.exp(cum_log) * enter_mask[:, None]
    carried = low_back(jnp.einsum('tn,hpn->thp', c_mat, low(state_now), precision=highest))
    output = inner_out + carried * scale_in[:, :, None] + d_skip[None, :, None] * values
    keep_end = (segment == segment[STRETCH - 1]).astype(jnp.float32)
    end_weight = jnp.exp(cum_log[STRETCH - 1][None, :] - cum_log) * step_size * keep_end[:, None]
    weighted = low(b_mat[:, None, :] * end_weight[:, :, None])
    stretch_state = low_back(jnp.einsum('shp,shn->hpn', values, weighted, precision=highest))
    through = jnp.exp(cum_log[STRETCH - 1]) * (segment[STRETCH - 1] == last_seg).astype(jnp.float32)
    next_state = through[:, None, None] * state_now + stretch_state
    gated_rows = output.reshape(STRETCH, INNER) * jax.nn.silu(z_part)
    inverse_two = lax.rsqrt(lax.optimization_barrier(jnp.mean(gated_rows * gated_rows, axis=1, keepdims=True)) + epsilon)
    normed_two = low(gated_rows * inverse_two * gate_gain)
    result = residual + matmul_hi(normed_two, w_out)
    carry_out = (joined[STRETCH - rim_width:], segment[STRETCH - rim_width:], next_state, segment[STRETCH - 1])
    return (carry_out, result)

def segment_ids(lengths):
    row_ids = jnp.arange(TOKENS, dtype=jnp.int32)
    group_ids = (row_ids // GROUP).astype(jnp.int32)
    place_in = row_ids - group_ids * GROUP
    starts = (jnp.cumsum(lengths, axis=1) - lengths).astype(jnp.int32)
    counted = lax.optimization_barrier(jnp.sum((place_in[:, None] >= starts[group_ids]).astype(jnp.int32), axis=1)).astype(jnp.int32)
    return (group_ids * SEQS + counted).astype(jnp.int32)

def layer_forward(segments, tokens_f, norm_gain, w_z, w_x, w_bc, w_dt, conv_x_w, conv_x_b, conv_bc_w, conv_bc_b, dt_bias, a_log, d_skip, gate_gain, w_out):
    params = (norm_gain, w_z, w_x, w_bc, w_dt, jnp.concatenate([conv_x_w, conv_bc_w], axis=1), jnp.concatenate([conv_x_b, conv_bc_b]), dt_bias, a_log, d_skip, gate_gain, w_out)
    step_fn = jax.checkpoint(partial(stretch_layer, params))
    start_carry = (jnp.zeros((CONV - 1, INNER + 2 * STATE), jnp.float32), jnp.full((CONV - 1,), -1, jnp.int32), jnp.zeros((HEADS, HEADDIM, STATE), jnp.float32), jnp.array(-1, jnp.int32))
    block_count = TOKENS // STRETCH
    final_carry, results = lax.scan(step_fn, start_carry, (tokens_f.reshape(block_count, STRETCH, D), segments.reshape(block_count, STRETCH)))
    return results.reshape(TOKENS, D)

def reference(tokens, grad_out, lengths, norm_gain, w_z, w_x, w_bc, w_dt, conv_x_w, conv_x_b, conv_bc_w, conv_bc_b, dt_bias, a_log, d_skip, gate_gain, w_out):
    segments = segment_ids(lengths)
    floats = [array_in.astype(jnp.float32) for array_in in (tokens, norm_gain, w_z, w_x, w_bc, w_dt, conv_x_w, conv_x_b, conv_bc_w, conv_bc_b, dt_bias, a_log, d_skip, gate_gain, w_out)]
    forward_out, pull_back = jax.vjp(partial(layer_forward, segments), *floats)
    gradients = pull_back(grad_out.astype(jnp.float32))
    return (forward_out.astype(jnp.bfloat16), gradients[0].astype(jnp.bfloat16), gradients[1], gradients[2], gradients[3], gradients[4], gradients[5], gradients[6], gradients[7], gradients[8], gradients[9], gradients[10], gradients[11], gradients[12], gradients[13], gradients[14])
```

```python
import functools

import jax
import jax.numpy as jnp
import numpy as np
from jax import lax
from jax.experimental import pallas as pl
from jax.experimental.pallas import tpu as pltpu
from jax.sharding import PartitionSpec as P

STRETCH = 256
INNER = 1536
HEAD_ROWS = 8
LOG2E = 1.4426950408889634

epsilon = 1e-05
f32 = jnp.float32
bf16 = jnp.bfloat16


def nn(left, right):
    return lax.dot_general(left, right, (((1,), (0,)), ((), ())), preferred_element_type=f32)


def nt(left, right):
    return lax.dot_general(left, right, (((1,), (1,)), ((), ())), preferred_element_type=f32)


def tn(left, right):
    return lax.dot_general(left, right, (((0,), (0,)), ((), ())), preferred_element_type=f32)


def halves(x):
    high = x.astype(bf16)
    return high, (x - high.astype(f32)).astype(bf16)


def thirds(x):
    high = x.astype(bf16)
    rest = x - high.astype(f32)
    mid = rest.astype(bf16)
    return high, mid, (rest - mid.astype(f32)).astype(bf16)


def exact_rows(x, ones_matrix):
    high, mid, low = thirds(x)
    r = HEAD_ROWS
    out = nn(jnp.concatenate([high, mid, low, jnp.zeros_like(low)], axis=0), ones_matrix)
    return out[:r] + out[r : 2 * r] + out[2 * r : 3 * r]


def columns_of(rows):
    have = sum(r.shape[0] for r in rows)
    pad = jnp.zeros((128 - have, rows[0].shape[1]), f32)
    cols = jnp.transpose(jnp.concatenate(list(rows) + [pad], axis=0))
    high, low = halves(cols)
    return cols, jnp.concatenate([high, low], axis=1)


def segment_start(pos, starts):
    found = jnp.zeros_like(pos)
    for s in starts:
        found = jnp.where(pos >= s, s, found)
    return found


def joined_ok(u, distance, starts):
    ok = jnp.ones(u.shape, jnp.bool_)
    for s in starts[1:]:
        ok = ok & jnp.logical_not((u < s) & (u + distance >= s))
    return ok


def iota(shape, axis):
    return lax.broadcasted_iota(jnp.int32, shape, axis)


def read_info(info, block):
    first = info[0]
    starts = [info[1 + k] for k in range(info.shape[0] - 1)]
    base = first + block * STRETCH
    end_start = segment_start(base + STRETCH - 1, starts)
    flag = jnp.where(end_start < base, 1.0, 0.0).astype(f32)
    return starts, base, end_start, flag


def norm_rows(tok):
    x = tok.astype(f32)
    inverse = lax.rsqrt(jnp.mean(x * x, axis=1, keepdims=True) + epsilon)
    return x * inverse, inverse


def lanes_of(column, e8):
    return jnp.sum(column * e8, axis=0, keepdims=True)


def entry_kernel(
    info, tok, halo, gain, wj, cw, cb, bias, rate, tri, ew, e8,
    nrm_o, jx_o, jb_o, vbc_o, sx_o, sb_o, pre_o, step_o, cum_o, s_o, end_o, dec_o,
    ext, run, dec,
):
    i = pl.program_id(0)
    starts, base, end_start, flag = read_info(info, i)
    width = cw.shape[1]
    inner = jx_o.shape[1]
    taps = cw.shape[0]

    @pl.when(i == 0)
    def _():
        unit, _inv = norm_rows(halo[...])
        before = nn((unit * gain[...]).astype(bf16), wj[:, :width])
        ext[0:8, :] = before.astype(bf16).astype(f32)[8:16]
        run[...] = jnp.zeros_like(run)
        dec[...] = jnp.ones_like(dec)

    unit, _inv = norm_rows(tok[...])
    normed = (unit * gain[...]).astype(bf16)
    nrm_o[...] = normed
    product = nn(normed, wj[...])
    joined = product[:, :width].astype(bf16)
    jx_o[...] = joined[:, :inner]
    jb_o[...] = joined[:, inner:]
    ext[8 : 8 + STRETCH, :] = joined.astype(f32)
    pos = base + iota((STRETCH, 128), 0)
    first_of = segment_start(pos, starts)
    valid = [
        jnp.where(pos - (taps - 1 - k) >= first_of, 1.0, 0.0).astype(f32) for k in range(taps - 1)
    ]
    for g in range(width // 128):
        at = slice(128 * g, 128 * (g + 1))
        acc = cb[:, at] + cw[taps - 1 : taps, at] * ext[8 : 8 + STRETCH, at]
        for k in range(taps - 1):
            low = 8 - (taps - 1) + k
            acc = acc + cw[k : k + 1, at] * (ext[low : low + STRETCH, at] * valid[k])
        sig = jax.nn.sigmoid(acc)
        act = acc * sig
        vbc_o[:, at] = act.astype(bf16)
        slope = sig + act * (1.0 - sig)
        if 128 * g < inner:
            sx_o[:, at] = slope.astype(bf16)
        else:
            sb_o[:, 128 * g - inner : 128 * (g + 1) - inner] = slope
    ext[0:8, :] = ext[STRETCH : STRETCH + 8, :]
    pre = jnp.transpose(product[:, width:])[:HEAD_ROWS] + bias[...]
    step = jax.nn.softplus(pre)
    logd = -step * rate[...]
    cum = exact_rows(logd, tri[...])
    pre_o[...] = pre
    step_o[...] = step
    cum_o[...] = cum
    cum_e = cum[:, STRETCH - 1 : STRETCH]
    where_s = base + iota((1, STRETCH), 1)
    keep = jnp.where(where_s >= end_start, 1.0, 0.0).astype(f32)
    weight = jnp.exp(cum_e - cum) * step * keep
    _cols, both = columns_of([weight])
    spread = nn(both, ew[...])
    v = vbc_o[:, :inner].astype(f32)
    b = vbc_o[:, inner : inner + 128]
    state = tn(b, (v * spread).astype(bf16))
    s_o[0] = state
    through = lanes_of(jnp.exp(cum_e) * flag, e8[...])
    run[...] = through * run[...] + state
    dec[...] = dec[...] * through
    end_o[...] = run[...].astype(bf16)
    dec_o[...] = dec[...]


def mix_kernel(
    info, vbc, step, cum, s_in, inc, normed, gout, wz_out, dskip, gain, e_step, e_scale, e8,
    z_o, out_o, gn_o, br_o, sum_o, st_o,
    run, gram,
):
    i = pl.program_id(0)
    starts, base, _end_start, flag = read_info(info, i)
    inner = gain.shape[1]

    @pl.when(i == 0)
    def _():
        run[...] = inc[...].astype(f32)

    st = run[...].astype(bf16)
    st_o[0] = st
    cum_v = cum[...]
    cum_e = cum_v[:, STRETCH - 1 : STRETCH]
    through = lanes_of(jnp.exp(cum_e) * flag, e8[...])
    run[...] = through * run[...] + s_in[0]

    row_first = segment_start(base + iota((1, STRETCH), 1), starts)
    scale = jnp.exp(cum_v) * jnp.where(row_first < base, 1.0, 0.0).astype(f32)
    cum2 = cum_v * LOG2E
    cols, both = columns_of([cum2, step[...], scale])
    step_x = nn(both, e_step[...])
    scale_x = nn(both, e_scale[...])
    b = vbc[:, inner : inner + 128]
    c = vbc[:, inner + 128 : inner + 256]
    t_at = iota((STRETCH, STRETCH), 0)
    s_at = iota((STRETCH, STRETCH), 1)
    t_first = segment_start(t_at + base, starts)
    mask = (s_at <= t_at) & (s_at + base >= t_first)
    gram[...] = jnp.where(mask, nt(c, b), 0.0)
    carried = nn(c, st) * scale_x
    lane = iota((STRETCH, 128), 1)
    pieces = []
    for p in range(inner // 128):
        at = slice(128 * p, 128 * (p + 1))
        v = vbc[:, at].astype(f32)
        sv = v * step_x[:, at]
        acc = carried[:, at] + dskip[:, at] * v
        for j in range(2):
            h = 2 * p + j
            half = jnp.where((lane < 64) if j == 0 else (lane >= 64), sv, 0.0).astype(bf16)
            gap = cols[:, h : h + 1] - cum2[h : h + 1, :]
            m = (gram[...] * jnp.exp2(jnp.minimum(gap, 0.0))).astype(bf16)
            acc = acc + nn(m, half)
        pieces.append(acc)
    out = jnp.concatenate(pieces, axis=1)
    out_o[...] = out
    zf = nn(normed[...], wz_out[:, :inner])
    z_o[...] = zf
    gated = out * (zf * jax.nn.sigmoid(zf))
    gn = nn(gout[...], wz_out[:, inner:])
    gn_o[...] = gn
    gg = gated * gain[...]
    br_o[...] = nt(wz_out[:, inner:], gg.astype(bf16)).astype(bf16)
    ss = jnp.sum(gated * gated, axis=1, keepdims=True)
    dq = jnp.sum(gn * gg, axis=1, keepdims=True)
    sum_o[...] = jnp.transpose(jnp.where(lane == 0, ss, dq))[0:2]


def gate_kernel(
    info, sums, cum, out, z, gn, vc, st, dskip, gain, e_scale, e8, f_sum,
    gz_o, gb_o, gc_o, n2_o, a_o, gs_o, start_o, misc_o,
    run,
):
    step_id = pl.program_id(0)
    blocks = pl.num_programs(0)
    i = blocks - 1 - step_id
    starts, base, _end_start, flag = read_info(info, i)
    inner = z.shape[1]

    @pl.when(step_id == 0)
    def _():
        run[...] = jnp.zeros_like(run)
        misc_o[...] = jnp.zeros_like(misc_o)

    alpha = lax.rsqrt(sums[0:1, :] / INNER + epsilon)
    beta = alpha * alpha * alpha * sums[1:2, :] / INNER
    cum_v = cum[...]
    row_first = segment_start(base + iota((1, STRETCH), 1), starts)
    scale = jnp.exp(cum_v) * jnp.where(row_first < base, 1.0, 0.0).astype(f32)
    cols, both = columns_of([alpha, beta, jnp.zeros((14, STRETCH), f32), scale])
    alpha_c = cols[:, 0:1]
    beta_c = cols[:, 1:2]
    scale_x = nn(both, e_scale[...])
    v = vc[:, :inner].astype(f32)
    c = vc[:, inner + 128 : inner + 256]
    zf = z[...]
    sig = jax.nn.sigmoid(zf)
    act = zf * sig
    o = out[...]
    gated = o * act
    g_n = gn[...]
    unit = gated * alpha_c
    g_gated = alpha_c * (g_n * gain[...]) - beta_c * gated
    g_out = g_gated * act
    gz_o[...] = (g_gated * o * (sig + act * (1.0 - sig))).astype(bf16)
    gb = g_out.astype(bf16)
    gb_o[...] = gb
    n2_o[...] = (unit * gain[...]).astype(bf16)
    misc_o[0:1, :] += jnp.sum(g_n * unit, axis=0, keepdims=True)
    misc_o[1:2, :] += jnp.sum(g_out * v, axis=0, keepdims=True)
    gf = gb.astype(f32)
    carried = nn(c, st[0]) * scale_x
    prod = gf * (o - dskip[...] * v) + (g_out - gf) * carried
    high, low = halves(prod)
    sums_c = nn(jnp.concatenate([high, low], axis=1), f_sum[...])
    a_o[...] = jnp.transpose(sums_c)[0:HEAD_ROWS]
    gc = (g_out * scale_x).astype(bf16)
    gc_o[...] = gc
    gs = tn(c, gc)
    gs_o[0] = gs
    through = lanes_of(jnp.exp(cum_v[:, STRETCH - 1 : STRETCH]) * flag, e8[...])
    run[...] = through * run[...] + gs
    start_o[...] = run[...].astype(bf16)


def scan_kernel(
    info, vbc, gb, gc, step, cum, pre, a_sum, st, gs_in, outg, sx, sb, jx, jb, cw, dskip, rate,
    e_step, e_w, e8, f_one, f_two, f_three, tril,
    gcat_o, tail_o, head_o, misc_o, dt_o,
    run, ext, gram, acc,
):
    step_id = pl.program_id(0)
    blocks = pl.num_programs(0)
    i = blocks - 1 - step_id
    starts, base, end_start, flag = read_info(info, i)
    inner = gb.shape[1]
    taps, width = cw.shape

    @pl.when(step_id == 0)
    def _():
        run[...] = outg[...].astype(f32)
        ext[STRETCH : STRETCH + 8, :] = jnp.zeros((8, width), f32)
        misc_o[...] = jnp.zeros_like(misc_o)
        dt_o[...] = jnp.zeros_like(dt_o)

    cum_v = cum[...]
    step_v = step[...]
    cum_e = cum_v[:, STRETCH - 1 : STRETCH]
    after = run[...]
    low_after = after.astype(bf16)
    state = st[0]
    through = lanes_of(jnp.exp(cum_e) * flag, e8[...])
    g_through = jnp.sum(after * state.astype(f32), axis=0, keepdims=True) * through
    end_more = jnp.sum(e8[...] * g_through, axis=1, keepdims=True)
    run[...] = through * after + gs_in[0]

    where_s = base + iota((1, STRETCH), 1)
    row_first = segment_start(where_s, starts)
    end_decay = jnp.exp(cum_e - cum_v) * jnp.where(where_s >= end_start, 1.0, 0.0).astype(f32)
    weight = end_decay * step_v
    cum2 = cum_v * LOG2E
    cols, both = columns_of([cum2, step_v, weight])
    step_x = nn(both, e_step[...])
    w_x = nn(both, e_w[...])
    b = vbc[:, inner : inner + 128]
    c = vbc[:, inner + 128 : inner + 256]
    s_at = iota((STRETCH, STRETCH), 0)
    t_at = iota((STRETCH, STRETCH), 1)
    mask = (s_at <= t_at) & (s_at + base >= row_first)
    gram[...] = jnp.where(mask, nt(b, c), 0.0)
    acc[...] = jnp.zeros_like(acc)
    y = nn(b, low_after)
    lane = iota((STRETCH, 128), 1)
    us = []
    svs = []
    for p in range(inner // 128):
        at = slice(128 * p, 128 * (p + 1))
        sv = (vbc[:, at].astype(f32) * step_x[:, at]).astype(bf16).astype(f32)
        svs.append(sv)
        g_pair = gb[:, at]
        g_wide = g_pair.astype(f32)
        u = jnp.zeros((STRETCH, 128), f32)
        for j in range(2):
            h = 2 * p + j
            side = (lane < 64) if j == 0 else (lane >= 64)
            gap = cum2[h : h + 1, :] - cols[:, h : h + 1]
            decay = jnp.exp2(jnp.minimum(gap, 0.0))
            m = (gram[...] * decay).astype(bf16)
            u = u + nn(m, jnp.where(side, g_wide, 0.0).astype(bf16))
            g_m = nt(jnp.where(side, sv, 0.0).astype(bf16), g_pair)
            acc[...] += g_m * decay
        us.append(u)
    u = jnp.concatenate(us, axis=1)
    g_gram = jnp.where(mask, acc[...], 0.0).astype(bf16)
    v = vbc[:, :inner].astype(f32)
    gf = gb[...].astype(f32)
    wv = (v * w_x).astype(bf16)
    ext[0:STRETCH, inner : inner + 128] = (nn(g_gram, c) + nt(wv, low_after)) * sb[:, :128]
    ext[0:STRETCH, inner + 128 :] = (tn(g_gram, b) + nt(gc[...], state)) * sb[:, 128:]
    gv = dskip[...] * gf + step_x * u + w_x * y
    h1, l1 = halves(v * u)
    h2, l2 = halves(v * y)
    h3, l3 = halves(jnp.concatenate(svs, axis=1) * u)
    sums_c = (
        nn(jnp.concatenate([h1, l1], axis=1), f_one[...])
        + nn(jnp.concatenate([h2, l2], axis=1), f_two[...])
        + nn(jnp.concatenate([h3, l3], axis=1), f_three[...])
    )
    sums_r = jnp.transpose(sums_c)
    g_step0 = sums_r[0:HEAD_ROWS]
    g_end = sums_r[HEAD_ROWS : 2 * HEAD_ROWS]
    ends = g_end * weight
    g_cum = a_sum[...] - sums_r[2 * HEAD_ROWS : 3 * HEAD_ROWS] - ends
    end_add = jnp.sum(ends, axis=1, keepdims=True) + end_more
    g_log = exact_rows(g_cum, tril[...]) + end_add
    g_step = g_step0 + g_end * end_decay - g_log * rate[...]
    g_pre_dt = g_step * jax.nn.sigmoid(pre[...])
    dt_o[0:HEAD_ROWS, :] += g_log * (-step_v * rate[...])
    dt_o[HEAD_ROWS:, :] += g_pre_dt
    pad = jnp.zeros((128 - HEAD_ROWS, STRETCH), f32)
    gcat_o[:, width:] = jnp.transpose(jnp.concatenate([g_pre_dt, pad], axis=0)).astype(bf16)

    ext[0:STRETCH, :inner] = gv * sx[...].astype(f32)
    pos = base + iota((STRETCH, 128), 0)
    ok = [
        jnp.where(joined_ok(pos, d, starts), 1.0, 0.0).astype(f32) for d in range(taps - 1, 0, -1)
    ]
    for g in range(width // 128):
        at = slice(128 * g, 128 * (g + 1))
        if 128 * g < inner:
            j_f = jx[:, at].astype(f32)
        else:
            j_f = jb[:, 128 * g - inner : 128 * (g + 1) - inner].astype(f32)
        own = ext[0:STRETCH, at]
        misc_o[taps : taps + 1, at] += jnp.sum(own, axis=0, keepdims=True)
        misc_o[taps - 1 : taps, at] += jnp.sum(own * j_f, axis=0, keepdims=True)
        total = own * cw[taps - 1 : taps, at]
        for k in range(taps - 1):
            d = taps - 1 - k
            term = ext[d : d + STRETCH, at] * ok[k]
            misc_o[k : k + 1, at] += jnp.sum(term * j_f, axis=0, keepdims=True)
            total = total + term * cw[k : k + 1, at]
        gcat_o[:, at] = total.astype(bf16)

        @pl.when(step_id == 0)
        def _():
            tail_o[:, at] = total[STRETCH - 8 :]

    head_o[...] = ext[0:8, :]
    ext[STRETCH : STRETCH + 8, :] = ext[0:8, :]


def exit_kernel(
    info, tok, gz, gcat, tail, nxt, last_j, cw, gain, wz_out, wj,
    gr_o, rim_o, rim_w_o, gain_o,
    fix,
):
    step_id = pl.program_id(0)
    blocks = pl.num_programs(0)
    i = blocks - 1 - step_id
    starts, base, _end_start, _flag = read_info(info, i)
    taps, width = cw.shape
    inner = gz.shape[1]

    @pl.when(step_id == 0)
    def _():
        gain_o[...] = jnp.zeros_like(gain_o)
        fix[0:8, :] = jnp.zeros((8, width), f32)
        fix[8:16, :] = nxt[...]
        places = base + STRETCH - 8 + iota((8, 128), 0)
        wide = last_j[8:16, :].astype(f32)
        total = tail[...]
        for k in range(taps - 1):
            d = taps - 1 - k
            ok = jnp.where(joined_ok(places, d, starts), 1.0, 0.0).astype(f32)
            inside = jnp.where(iota((8, width), 0) >= 8 - d, fix[d : d + 8, :], 0.0)
            term = inside * jnp.concatenate([ok] * (width // 128), axis=1)
            total = total + term * cw[k : k + 1, :]
            rim_w_o[k : k + 1, :] = jnp.sum(term * wide, axis=0, keepdims=True)
        rim_w_o[taps - 1 : 8, :] = jnp.zeros((9 - taps, width), f32)
        fix[0:8, :] = jnp.zeros((8, width), f32)
        fix[8:16, :] = total.astype(bf16).astype(f32) - tail[...].astype(bf16).astype(f32)
        rim_o[...] = fix[...].astype(bf16)

    g_normed = nt(gz[...], wz_out[:, :inner]) + nt(gcat[...], wj[...])

    def finish(g_normed):
        unit, inverse = norm_rows(tok[...])
        scaled = g_normed * gain[...]
        mean = jnp.mean(scaled * unit, axis=1, keepdims=True)
        gr_o[...] = jnp.transpose(inverse * (scaled - unit * mean)).astype(bf16)
        gain_o[...] += jnp.sum(g_normed * unit, axis=0, keepdims=True)

    @pl.when(step_id == 0)
    def _():
        more = nt(rim_o[...], wj[:, :width])
        finish(g_normed + jnp.concatenate([jnp.zeros((STRETCH - 16, more.shape[1]), f32), more]))

    @pl.when(step_id > 0)
    def _():
        finish(g_normed)


def finish_kernel(parts, scaled, place, part, base, *rest):
    out = rest[-1]
    wide = part[...].astype(f32)
    if scaled:
        wide = wide * lax.rsqrt(rest[0][0:1, :] / INNER + epsilon)
    add = jnp.transpose(wide)
    size = out.shape[1]
    for k in range(parts):

        @pl.when(place[0] == k)
        def _():
            out[...] = (base[:, size * k : size * (k + 1)].astype(f32) + add).astype(bf16)


def constants(inner, heads):
    lane_head = np.arange(inner) // (inner // heads)
    e8 = (np.arange(HEAD_ROWS)[:, None] == lane_head[None, :]).astype(np.float32)

    def spread(kind):
        m = np.zeros((128, inner), np.float32)
        m[HEAD_ROWS * kind : HEAD_ROWS * (kind + 1)] = e8
        return jnp.asarray(np.concatenate([m, m], axis=0), bf16)

    def gather(kind):
        m = np.zeros((inner, 128), np.float32)
        m[:, HEAD_ROWS * kind : HEAD_ROWS * (kind + 1)] = e8.T
        return jnp.asarray(np.concatenate([m, m], axis=0), bf16)

    at = np.arange(STRETCH)
    upper = jnp.asarray((at[:, None] <= at[None, :]).astype(np.float32), bf16)
    lower = jnp.asarray((at[:, None] >= at[None, :]).astype(np.float32), bf16)
    return jnp.asarray(e8), spread, gather, upper, lower


def passed_along(block, axis, distance):
    devices = range(lax.axis_size(axis))
    route = [(i - distance, i) for i in devices if i - distance in devices]
    return lax.ppermute(block, axis, route)


def entering(decay, state, axis, reverse):
    size = lax.axis_size(axis)
    if size == 2:
        return passed_along(state, axis, -1 if reverse else 1)
    index = lax.axis_index(axis)
    decays = lax.all_gather(decay.astype(bf16), axis)
    states = lax.all_gather(state, axis)

    def lap(k, before):
        at = size - 1 - k if reverse else k
        reached = at > index if reverse else at < index
        new = decays[at].astype(f32) * before + states[at].astype(f32)
        return jnp.where(reached, new, before)

    return lax.fori_loop(0, size, lap, jnp.zeros(state.shape, f32)).astype(bf16)


def call(kernel, blocks, ins, outs, scratch, micros=0):
    def spec(shape, how):
        if how == "smem":
            return pl.BlockSpec(memory_space=pltpu.SMEM)
        return pl.BlockSpec(shape, how)

    return pl.pallas_call(
        kernel,
        grid=(blocks,),
        in_specs=[spec(shape, how) for _a, shape, how in ins],
        out_specs=[spec(shape, how) for _s, shape, how in outs],
        out_shape=[s for s, _sh, _h in outs],
        scratch_shapes=scratch,
        cost_estimate=pl.CostEstimate(
            flops=0, transcendentals=0, bytes_accessed=3_000_000 * micros
        )
        if micros
        else None,
        compiler_params=pltpu.CompilerParams(
            dimension_semantics=("arbitrary",), vmem_limit_bytes=56 * 1024 * 1024
        ),
    )(*[a for a, _s, _h in ins])


def local(
    tokens, grad_out, lengths, norm_gain, w_z, w_x, w_bc, w_dt, conv_x_w, conv_x_b,
    conv_bc_w, conv_bc_b, dt_bias, a_log, d_skip, gate_gain, w_out,
):
    rows, model = tokens.shape
    inner = w_z.shape[1]
    heads = dt_bias.shape[0]
    states = w_bc.shape[1] // 2
    taps = conv_x_w.shape[0]
    blocks = rows // STRETCH
    width = inner + 2 * states
    tp_size = lax.axis_size("tp")
    slice_width = model // tp_size
    tp_index = lax.axis_index("tp")
    ctx_index = lax.axis_index("ctx")
    e8, spread, gather, upper, lower = constants(inner, heads)

    w_joined = lax.all_gather(
        jnp.concatenate([w_x, w_bc, jnp.pad(w_dt, ((0, 0), (0, 128 - heads)))], axis=1),
        "fsdp",
        axis=0,
        tiled=True,
    )
    wz_out = lax.all_gather(jnp.concatenate([w_z, w_out.T], axis=1), "fsdp", axis=0, tiled=True)

    starts = jnp.cumsum(lengths[0]) - lengths[0]
    info = jnp.concatenate([(ctx_index * rows).astype(jnp.int32)[None], starts.astype(jnp.int32)])
    halo = passed_along(tokens[rows - 16 :], "ctx", 1)
    gain = norm_gain[None, :]
    conv_w = jnp.concatenate([conv_x_w, conv_bc_w], axis=1)
    conv_b = jnp.concatenate([conv_x_b, conv_bc_b])[None, :]

    def head_rows(x):
        return jnp.broadcast_to(jnp.pad(x, (0, HEAD_ROWS - heads))[:, None], (HEAD_ROWS, STRETCH))

    bias = head_rows(dt_bias)
    rate = head_rows(jnp.exp(a_log))
    per_head = inner // heads
    dskip = jnp.repeat(d_skip, per_head)[None, :]
    ggain = gate_gain[None, :]

    def shape(dims, kind):
        return jax.ShapeDtypeStruct(dims, kind)

    def whole(x):
        return (x, x.shape, lambda i: (0,) * x.ndim)

    def by_rows(x, flip=False):
        if flip:
            return (x, (STRETCH, x.shape[1]), lambda i: (blocks - 1 - i, 0))
        return (x, (STRETCH, x.shape[1]), lambda i: (i, 0))

    def by_lanes(x, flip=False):
        if flip:
            return (x, (x.shape[0], STRETCH), lambda i: (0, blocks - 1 - i))
        return (x, (x.shape[0], STRETCH), lambda i: (0, i))

    def by_block(x, flip=False):
        if flip:
            return (x, (1,) + x.shape[1:], lambda i: (blocks - 1 - i, 0, 0))
        return (x, (1,) + x.shape[1:], lambda i: (i, 0, 0))

    def fixed(x):
        return (x, x.shape, lambda i: (0,) * len(x.shape))

    info_in = (info, None, "smem")
    state_dims = (blocks, states, inner)
    normed, joined_x, joined_bc, vbc, slope_x, slope_bc, pre, step, cum, s_part, end_state, decay = call(
        entry_kernel,
        blocks,
        [
            info_in, by_rows(tokens), whole(halo), whole(gain), whole(w_joined),
            whole(conv_w), whole(conv_b), whole(bias), whole(rate), whole(upper),
            whole(spread(0)), whole(e8),
        ],
        [
            by_rows(shape((rows, model), bf16)),
            by_rows(shape((rows, inner), bf16)),
            by_rows(shape((rows, 2 * states), bf16)),
            by_rows(shape((rows, width), bf16)),
            by_rows(shape((rows, inner), bf16)),
            by_rows(shape((rows, 2 * states), f32)),
            by_lanes(shape((HEAD_ROWS, rows), f32)),
            by_lanes(shape((HEAD_ROWS, rows), f32)),
            by_lanes(shape((HEAD_ROWS, rows), f32)),
            by_block(shape(state_dims, f32)),
            fixed(shape((states, inner), bf16)),
            fixed(shape((1, inner), f32)),
        ],
        [
            pltpu.VMEM((STRETCH + 8, width), f32),
            pltpu.VMEM((states, inner), f32),
            pltpu.VMEM((1, inner), f32),
        ],
    )
    incoming = entering(decay, end_state, "ctx", False)
    z_part, out, gn, branch, sums, state_in = call(
        mix_kernel,
        blocks,
        [
            info_in, by_rows(vbc), by_lanes(step), by_lanes(cum), by_block(s_part),
            whole(incoming), by_rows(normed), by_rows(grad_out), whole(wz_out), whole(dskip),
            whole(ggain), whole(spread(1)), whole(spread(2)), whole(e8),
        ],
        [
            by_rows(shape((rows, inner), f32)),
            by_rows(shape((rows, inner), f32)),
            by_rows(shape((rows, inner), f32)),
            by_lanes(shape((model, rows), bf16)),
            by_lanes(shape((2, rows), f32)),
            by_block(shape(state_dims, bf16)),
        ],
        [pltpu.VMEM((states, inner), f32), pltpu.VMEM((STRETCH, STRETCH), f32)],
    )
    sums = lax.psum(sums, "tp")
    branch = lax.psum_scatter(branch, "tp", scatter_dimension=0, tiled=True)
    g_z, g_b, g_c, normed_two, a_sum, gs_part, start_state, misc_gate = call(
        gate_kernel,
        blocks,
        [
            info_in, by_lanes(sums, True), by_lanes(cum, True), by_rows(out, True),
            by_rows(z_part, True), by_rows(gn, True), by_rows(vbc, True), by_block(state_in, True),
            whole(dskip), whole(ggain), whole(spread(2)), whole(e8), whole(gather(0)),
        ],
        [
            by_rows(shape((rows, inner), bf16), True),
            by_rows(shape((rows, inner), bf16), True),
            by_rows(shape((rows, inner), bf16), True),
            by_rows(shape((rows, inner), bf16), True),
            by_lanes(shape((HEAD_ROWS, rows), f32), True),
            by_block(shape(state_dims, f32), True),
            fixed(shape((states, inner), bf16)),
            fixed(shape((8, inner), f32)),
        ],
        [pltpu.VMEM((states, inner), f32)],
    )
    outgoing = entering(decay, start_state, "ctx", True)
    g_cat, tail, head, misc_scan, misc_dt = call(
        scan_kernel,
        blocks,
        [
            info_in, by_rows(vbc, True), by_rows(g_b, True), by_rows(g_c, True),
            by_lanes(step, True), by_lanes(cum, True), by_lanes(pre, True), by_lanes(a_sum, True),
            by_block(state_in, True), by_block(gs_part, True), whole(outgoing),
            by_rows(slope_x, True), by_rows(slope_bc, True), by_rows(joined_x, True),
            by_rows(joined_bc, True), whole(conv_w), whole(dskip), whole(rate), whole(spread(1)),
            whole(spread(2)), whole(e8), whole(gather(0)), whole(gather(1)),
            whole(gather(2)), whole(lower),
        ],
        [
            by_rows(shape((rows, width + 128), bf16), True),
            fixed(shape((8, width), f32)),
            fixed(shape((8, width), f32)),
            fixed(shape((8, width), f32)),
            fixed(shape((2 * HEAD_ROWS, STRETCH), f32)),
        ],
        [
            pltpu.VMEM((states, inner), f32),
            pltpu.VMEM((STRETCH + 8, width), f32),
            pltpu.VMEM((STRETCH, STRETCH), f32),
            pltpu.VMEM((STRETCH, STRETCH), f32),
        ],
    )
    next_rows = passed_along(head, "ctx", -1)
    last_joined = jnp.concatenate([joined_x[rows - 16 :], joined_bc[rows - 16 :]], axis=1)
    g_resid, rim, rim_w, gain_part = call(
        exit_kernel,
        blocks,
        [
            info_in, by_rows(tokens, True), by_rows(g_z, True), by_rows(g_cat, True),
            whole(tail), whole(next_rows), whole(last_joined), whole(conv_w), whole(gain),
            whole(wz_out), whole(w_joined),
        ],
        [
            by_lanes(shape((model, rows), bf16), True),
            fixed(shape((16, width), bf16)),
            fixed(shape((8, width), f32)),
            fixed(shape((1, model), f32)),
        ],
        [pltpu.VMEM((16, width), f32)],
    )
    g_resid = lax.psum_scatter(g_resid, "tp", scatter_dimension=0, tiled=True)

    part_out = tn(grad_out, normed_two)
    part_z = tn(normed, g_z)
    part_cat = tn(normed, g_cat)
    part_rim = tn(normed[rows - 16 :], rim)
    part_cat = part_cat + jnp.pad(part_rim, ((0, 0), (0, 128)))
    parts = jnp.concatenate([part_out, part_z, part_cat], axis=1).astype(bf16)
    shard = lax.psum_scatter(parts, "fsdp", scatter_dimension=0, tiled=True)
    shard = lax.psum(shard, "ctx").astype(f32)
    grad_w_out = shard[:, :inner].T
    grad_w_z = shard[:, inner : 2 * inner]
    grad_w_x = shard[:, 2 * inner : 3 * inner]
    grad_w_bc = lax.psum(shard[:, 3 * inner : 3 * inner + 2 * states], "tp")
    grad_w_dt = shard[:, 3 * inner + 2 * states : 3 * inner + 2 * states + heads]

    misc_scan = misc_scan + rim_w
    over_all = (gain_part[0], misc_scan[:taps, inner:], misc_scan[taps, inner:])
    sum_gain, grad_conv_bc_w, grad_conv_bc_b = lax.psum(over_all, ("fsdp", "ctx", "tp"))
    small = (
        misc_scan[:taps, :inner],
        misc_scan[taps, :inner],
        jnp.sum(misc_dt[HEAD_ROWS : HEAD_ROWS + heads], axis=1),
        jnp.sum(misc_dt[:heads], axis=1),
        jnp.sum(misc_gate[1].reshape(heads, per_head), axis=1),
        misc_gate[0],
    )
    (
        grad_conv_x_w, grad_conv_x_b, grad_dt_bias, grad_a_log, grad_d_skip, grad_gate_gain,
    ) = lax.psum(small, ("fsdp", "ctx"))
    here = tp_index * slice_width
    grad_norm_gain = lax.dynamic_slice_in_dim(sum_gain, here, slice_width, 0)

    place = tp_index.astype(jnp.int32)[None]

    def finish(part, base, scaled):
        extra = [by_lanes(sums)] if scaled else []
        return call(
            functools.partial(finish_kernel, tp_size, scaled),
            blocks,
            [(place, None, "smem"), by_lanes(part), by_rows(base)] + extra,
            [by_rows(shape((rows, slice_width), bf16))],
            [],
        )[0]

    layer_out = finish(branch, tokens, True)
    grad_tokens = finish(g_resid, grad_out, False)
    return (
        layer_out, grad_tokens, grad_norm_gain, grad_w_z, grad_w_x, grad_w_bc, grad_w_dt,
        grad_conv_x_w, grad_conv_x_b, grad_conv_bc_w, grad_conv_bc_b, grad_dt_bias, grad_a_log,
        grad_d_skip, grad_gate_gain, grad_w_out,
    )


def solution(mesh):
    both = ("fsdp", "ctx")
    in_specs = (
        P(both, None), P(both, None), P("fsdp", None), P(), P("fsdp", "tp"), P("fsdp", "tp"),
        P("fsdp", None), P("fsdp", "tp"), P(None, "tp"), P("tp"), P(), P(), P("tp"), P("tp"),
        P("tp"), P("tp"), P("tp", "fsdp"),
    )
    out_specs = (
        P(both, "tp"), P(both, "tp"), P("tp"), P("fsdp", "tp"), P("fsdp", "tp"), P("fsdp", None),
        P("fsdp", "tp"), P(None, "tp"), P("tp"), P(), P(), P("tp"), P("tp"), P("tp"), P("tp"),
        P("tp", "fsdp"),
    )
    return jax.shard_map(local, mesh=mesh, in_specs=in_specs, out_specs=out_specs, check_vma=False)
```

```python
import functools

import jax
import jax.numpy as jnp
import numpy as np
from jax import lax
from jax.experimental import pallas as pl
from jax.experimental.pallas import tpu as pltpu
from jax.sharding import PartitionSpec as P

STRETCH = 256
INNER = 1536
HEAD_ROWS = 8
LOG2E = 1.4426950408889634

epsilon = 1e-05
f32 = jnp.float32
bf16 = jnp.bfloat16


def nn(left, right):
    return lax.dot_general(left, right, (((1,), (0,)), ((), ())), preferred_element_type=f32)


def nt(left, right):
    return lax.dot_general(left, right, (((1,), (1,)), ((), ())), preferred_element_type=f32)


def tn(left, right):
    return lax.dot_general(left, right, (((0,), (0,)), ((), ())), preferred_element_type=f32)


def halves(x):
    high = x.astype(bf16)
    return high, (x - high.astype(f32)).astype(bf16)


def thirds(x):
    high = x.astype(bf16)
    rest = x - high.astype(f32)
    mid = rest.astype(bf16)
    return high, mid, (rest - mid.astype(f32)).astype(bf16)


def exact_rows(x, ones_matrix):
    high, mid, low = thirds(x)
    r = HEAD_ROWS
    out = nn(jnp.concatenate([high, mid, low, jnp.zeros_like(low)], axis=0), ones_matrix)
    return out[:r] + out[r : 2 * r] + out[2 * r : 3 * r]


def columns_of(rows):
    have = sum(r.shape[0] for r in rows)
    pad = jnp.zeros((128 - have, rows[0].shape[1]), f32)
    cols = jnp.transpose(jnp.concatenate(list(rows) + [pad], axis=0))
    high, low = halves(cols)
    return cols, jnp.concatenate([high, low], axis=1)


def segment_start(pos, starts):
    found = jnp.zeros_like(pos)
    for s in starts:
        found = jnp.where(pos >= s, s, found)
    return found


def joined_ok(u, distance, starts):
    ok = jnp.ones(u.shape, jnp.bool_)
    for s in starts[1:]:
        ok = ok & jnp.logical_not((u < s) & (u + distance >= s))
    return ok


def iota(shape, axis):
    return lax.broadcasted_iota(jnp.int32, shape, axis)


def read_info(info, block):
    first = info[0]
    starts = [info[1 + k] for k in range(info.shape[0] - 1)]
    base = first + block * STRETCH
    end_start = segment_start(base + STRETCH - 1, starts)
    flag = jnp.where(end_start < base, 1.0, 0.0).astype(f32)
    return starts, base, end_start, flag


def norm_rows(tok):
    x = tok.astype(f32)
    inverse = lax.rsqrt(jnp.mean(x * x, axis=1, keepdims=True) + epsilon)
    return x * inverse, inverse


def lanes_of(column, e8):
    return jnp.sum(column * e8, axis=0, keepdims=True)


def entry_kernel(
    info, tok, halo, gain, wj, cw, cb, bias, rate, tri, ew, e8,
    nrm_o, jx_o, jb_o, vbc_o, sx_o, sb_o, pre_o, step_o, cum_o, s_o, end_o, dec_o,
    ext, run, dec,
):
    i = pl.program_id(0)
    starts, base, end_start, flag = read_info(info, i)
    width = cw.shape[1]
    inner = jx_o.shape[1]
    taps = cw.shape[0]

    @pl.when(i == 0)
    def _():
        unit, _inv = norm_rows(halo[...])
        before = nn((unit * gain[...]).astype(bf16), wj[:, :width])
        ext[0:8, :] = before.astype(bf16).astype(f32)[8:16]
        run[...] = jnp.zeros_like(run)
        dec[...] = jnp.ones_like(dec)

    unit, _inv = norm_rows(tok[...])
    normed = (unit * gain[...]).astype(bf16)
    nrm_o[...] = normed
    product = nn(normed, wj[...])
    joined = product[:, :width].astype(bf16)
    jx_o[...] = joined[:, :inner]
    jb_o[...] = joined[:, inner:]
    ext[8 : 8 + STRETCH, :] = joined.astype(f32)
    pos = base + iota((STRETCH, 128), 0)
    first_of = segment_start(pos, starts)
    valid = [
        jnp.where(pos - (taps - 1 - k) >= first_of, 1.0, 0.0).astype(f32) for k in range(taps - 1)
    ]
    for g in range(width // 128):
        at = slice(128 * g, 128 * (g + 1))
        acc = cb[:, at] + cw[taps - 1 : taps, at] * ext[8 : 8 + STRETCH, at]
        for k in range(taps - 1):
            low = 8 - (taps - 1) + k
            acc = acc + cw[k : k + 1, at] * (ext[low : low + STRETCH, at] * valid[k])
        sig = jax.nn.sigmoid(acc)
        act = acc * sig
        vbc_o[:, at] = act.astype(bf16)
        slope = sig + act * (1.0 - sig)
        if 128 * g < inner:
            sx_o[:, at] = slope.astype(bf16)
        else:
            sb_o[:, 128 * g - inner : 128 * (g + 1) - inner] = slope
    ext[0:8, :] = ext[STRETCH : STRETCH + 8, :]
    pre = jnp.transpose(product[:, width:])[:HEAD_ROWS] + bias[...]
    step = jax.nn.softplus(pre)
    logd = -step * rate[...]
    cum = exact_rows(logd, tri[...])
    pre_o[...] = pre
    step_o[...] = step
    cum_o[...] = cum
    cum_e = cum[:, STRETCH - 1 : STRETCH]
    where_s = base + iota((1, STRETCH), 1)
    keep = jnp.where(where_s >= end_start, 1.0, 0.0).astype(f32)
    weight = jnp.exp(cum_e - cum) * step * keep
    _cols, both = columns_of([weight])
    spread = nn(both, ew[...])
    v = vbc_o[:, :inner].astype(f32)
    b = vbc_o[:, inner : inner + 128]
    state = tn(b, (v * spread).astype(bf16))
    s_o[0] = state
    through = lanes_of(jnp.exp(cum_e) * flag, e8[...])
    run[...] = through * run[...] + state
    dec[...] = dec[...] * through
    end_o[...] = run[...].astype(bf16)
    dec_o[...] = dec[...]


def mix_kernel(
    info, vbc, step, cum, s_in, inc, normed, gout, wz_out, dskip, gain, e_step, e_scale, e8,
    z_o, out_o, gn_o, br_o, sum_o, st_o,
    run, gram,
):
    i = pl.program_id(0)
    starts, base, _end_start, flag = read_info(info, i)
    inner = gain.shape[1]

    @pl.when(i == 0)
    def _():
        run[...] = inc[...].astype(f32)

    st = run[...].astype(bf16)
    st_o[0] = st
    cum_v = cum[...]
    cum_e = cum_v[:, STRETCH - 1 : STRETCH]
    through = lanes_of(jnp.exp(cum_e) * flag, e8[...])
    run[...] = through * run[...] + s_in[0]

    row_first = segment_start(base + iota((1, STRETCH), 1), starts)
    scale = jnp.exp(cum_v) * jnp.where(row_first < base, 1.0, 0.0).astype(f32)
    cum2 = cum_v * LOG2E
    cols, both = columns_of([cum2, step[...], scale])
    step_x = nn(both, e_step[...])
    scale_x = nn(both, e_scale[...])
    b = vbc[:, inner : inner + 128]
    c = vbc[:, inner + 128 : inner + 256]
    t_at = iota((STRETCH, STRETCH), 0)
    s_at = iota((STRETCH, STRETCH), 1)
    t_first = segment_start(t_at + base, starts)
    mask = (s_at <= t_at) & (s_at + base >= t_first)
    gram[...] = jnp.where(mask, nt(c, b), 0.0)
    carried = nn(c, st) * scale_x
    lane = iota((STRETCH, 128), 1)
    pieces = []
    for p in range(inner // 128):
        at = slice(128 * p, 128 * (p + 1))
        v = vbc[:, at].astype(f32)
        sv = v * step_x[:, at]
        acc = carried[:, at] + dskip[:, at] * v
        for j in range(2):
            h = 2 * p + j
            half = jnp.where((lane < 64) if j == 0 else (lane >= 64), sv, 0.0).astype(bf16)
            gap = cols[:, h : h + 1] - cum2[h : h + 1, :]
            m = (gram[...] * jnp.exp2(jnp.minimum(gap, 0.0))).astype(bf16)
            acc = acc + nn(m, half)
        pieces.append(acc)
    out = jnp.concatenate(pieces, axis=1)
    out_o[...] = out
    zf = nn(normed[...], wz_out[:, :inner])
    z_o[...] = zf
    gated = out * (zf * jax.nn.sigmoid(zf))
    gn = nn(gout[...], wz_out[:, inner:])
    gn_o[...] = gn
    gg = gated * gain[...]
    br_o[...] = nt(wz_out[:, inner:], gg.astype(bf16)).astype(bf16)
    ss = jnp.sum(gated * gated, axis=1, keepdims=True)
    dq = jnp.sum(gn * gg, axis=1, keepdims=True)
    sum_o[...] = jnp.transpose(jnp.where(lane == 0, ss, dq))[0:2]


def gate_kernel(
    info, sums, cum, out, z, gn, vc, st, dskip, gain, e_scale, e8, f_sum,
    gz_o, gb_o, gc_o, n2_o, a_o, gs_o, start_o, misc_o,
    run,
):
    step_id = pl.program_id(0)
    blocks = pl.num_programs(0)
    i = blocks - 1 - step_id
    starts, base, _end_start, flag = read_info(info, i)
    inner = z.shape[1]

    @pl.when(step_id == 0)
    def _():
        run[...] = jnp.zeros_like(run)
        misc_o[...] = jnp.zeros_like(misc_o)

    alpha = lax.rsqrt(sums[0:1, :] / INNER + epsilon)
    beta = alpha * alpha * alpha * sums[1:2, :] / INNER
    cum_v = cum[...]
    row_first = segment_start(base + iota((1, STRETCH), 1), starts)
    scale = jnp.exp(cum_v) * jnp.where(row_first < base, 1.0, 0.0).astype(f32)
    cols, both = columns_of([alpha, beta, jnp.zeros((14, STRETCH), f32), scale])
    alpha_c = cols[:, 0:1]
    beta_c = cols[:, 1:2]
    scale_x = nn(both, e_scale[...])
    v = vc[:, :inner].astype(f32)
    c = vc[:, inner + 128 : inner + 256]
    zf = z[...]
    sig = jax.nn.sigmoid(zf)
    act = zf * sig
    o = out[...]
    gated = o * act
    g_n = gn[...]
    unit = gated * alpha_c
    g_gated = alpha_c * (g_n * gain[...]) - beta_c * gated
    g_out = g_gated * act
    gz_o[...] = (g_gated * o * (sig + act * (1.0 - sig))).astype(bf16)
    gb = g_out.astype(bf16)
    gb_o[...] = gb
    n2_o[...] = (unit * gain[...]).astype(bf16)
    misc_o[0:1, :] += jnp.sum(g_n * unit, axis=0, keepdims=True)
    misc_o[1:2, :] += jnp.sum(g_out * v, axis=0, keepdims=True)
    gf = gb.astype(f32)
    carried = nn(c, st[0]) * scale_x
    prod = gf * (o - dskip[...] * v) + (g_out - gf) * carried
    high, low = halves(prod)
    sums_c = nn(jnp.concatenate([high, low], axis=1), f_sum[...])
    a_o[...] = jnp.transpose(sums_c)[0:HEAD_ROWS]
    gc = (g_out * scale_x).astype(bf16)
    gc_o[...] = gc
    gs = tn(c, gc)
    gs_o[0] = gs
    through = lanes_of(jnp.exp(cum_v[:, STRETCH - 1 : STRETCH]) * flag, e8[...])
    run[...] = through * run[...] + gs
    start_o[...] = run[...].astype(bf16)


def scan_kernel(
    info, vbc, gb, gc, step, cum, pre, a_sum, st, gs_in, outg, sx, sb, jx, jb, cw, dskip, rate,
    e_step, e_w, e8, f_one, f_two, f_three, tril,
    gcat_o, tail_o, head_o, misc_o, dt_o,
    run, ext, gram, acc,
):
    step_id = pl.program_id(0)
    blocks = pl.num_programs(0)
    i = blocks - 1 - step_id
    starts, base, end_start, flag = read_info(info, i)
    inner = gb.shape[1]
    taps, width = cw.shape

    @pl.when(step_id == 0)
    def _():
        run[...] = outg[...].astype(f32)
        ext[STRETCH : STRETCH + 8, :] = jnp.zeros((8, width), f32)
        misc_o[...] = jnp.zeros_like(misc_o)
        dt_o[...] = jnp.zeros_like(dt_o)

    cum_v = cum[...]
    step_v = step[...]
    cum_e = cum_v[:, STRETCH - 1 : STRETCH]
    after = run[...]
    low_after = after.astype(bf16)
    state = st[0]
    through = lanes_of(jnp.exp(cum_e) * flag, e8[...])
    g_through = jnp.sum(after * state.astype(f32), axis=0, keepdims=True) * through
    end_more = jnp.sum(e8[...] * g_through, axis=1, keepdims=True)
    run[...] = through * after + gs_in[0]

    where_s = base + iota((1, STRETCH), 1)
    row_first = segment_start(where_s, starts)
    end_decay = jnp.exp(cum_e - cum_v) * jnp.where(where_s >= end_start, 1.0, 0.0).astype(f32)
    weight = end_decay * step_v
    cum2 = cum_v * LOG2E
    cols, both = columns_of([cum2, step_v, weight])
    step_x = nn(both, e_step[...])
    w_x = nn(both, e_w[...])
    b = vbc[:, inner : inner + 128]
    c = vbc[:, inner + 128 : inner + 256]
    s_at = iota((STRETCH, STRETCH), 0)
    t_at = iota((STRETCH, STRETCH), 1)
    mask = (s_at <= t_at) & (s_at + base >= row_first)
    gram[...] = jnp.where(mask, nt(b, c), 0.0)
    acc[...] = jnp.zeros_like(acc)
    y = nn(b, low_after)
    lane = iota((STRETCH, 128), 1)
    us = []
    svs = []
    for p in range(inner // 128):
        at = slice(128 * p, 128 * (p + 1))
        sv = (vbc[:, at].astype(f32) * step_x[:, at]).astype(bf16).astype(f32)
        svs.append(sv)
        g_pair = gb[:, at]
        g_wide = g_pair.astype(f32)
        u = jnp.zeros((STRETCH, 128), f32)
        for j in range(2):
            h = 2 * p + j
            side = (lane < 64) if j == 0 else (lane >= 64)
            gap = cum2[h : h + 1, :] - cols[:, h : h + 1]
            decay = jnp.exp2(jnp.minimum(gap, 0.0))
            m = (gram[...] * decay).astype(bf16)
            u = u + nn(m, jnp.where(side, g_wide, 0.0).astype(bf16))
            g_m = nt(jnp.where(side, sv, 0.0).astype(bf16), g_pair)
            acc[...] += g_m * decay
        us.append(u)
    u = jnp.concatenate(us, axis=1)
    g_gram = jnp.where(mask, acc[...], 0.0).astype(bf16)
    v = vbc[:, :inner].astype(f32)
    gf = gb[...].astype(f32)
    wv = (v * w_x).astype(bf16)
    ext[0:STRETCH, inner : inner + 128] = (nn(g_gram, c) + nt(wv, low_after)) * sb[:, :128]
    ext[0:STRETCH, inner + 128 :] = (tn(g_gram, b) + nt(gc[...], state)) * sb[:, 128:]
    gv = dskip[...] * gf + step_x * u + w_x * y
    h1, l1 = halves(v * u)
    h2, l2 = halves(v * y)
    h3, l3 = halves(jnp.concatenate(svs, axis=1) * u)
    sums_c = (
        nn(jnp.concatenate([h1, l1], axis=1), f_one[...])
        + nn(jnp.concatenate([h2, l2], axis=1), f_two[...])
        + nn(jnp.concatenate([h3, l3], axis=1), f_three[...])
    )
    sums_r = jnp.transpose(sums_c)
    g_step0 = sums_r[0:HEAD_ROWS]
    g_end = sums_r[HEAD_ROWS : 2 * HEAD_ROWS]
    ends = g_end * weight
    g_cum = a_sum[...] - sums_r[2 * HEAD_ROWS : 3 * HEAD_ROWS] - ends
    end_add = jnp.sum(ends, axis=1, keepdims=True) + end_more
    g_log = exact_rows(g_cum, tril[...]) + end_add
    g_step = g_step0 + g_end * end_decay - g_log * rate[...]
    g_pre_dt = g_step * jax.nn.sigmoid(pre[...])
    dt_o[0:HEAD_ROWS, :] += g_log * (-step_v * rate[...])
    dt_o[HEAD_ROWS:, :] += g_pre_dt
    pad = jnp.zeros((128 - HEAD_ROWS, STRETCH), f32)
    gcat_o[:, width:] = jnp.transpose(jnp.concatenate([g_pre_dt, pad], axis=0)).astype(bf16)

    ext[0:STRETCH, :inner] = gv * sx[...].astype(f32)
    pos = base + iota((STRETCH, 128), 0)
    ok = [
        jnp.where(joined_ok(pos, d, starts), 1.0, 0.0).astype(f32) for d in range(taps - 1, 0, -1)
    ]
    for g in range(width // 128):
        at = slice(128 * g, 128 * (g + 1))
        if 128 * g < inner:
            j_f = jx[:, at].astype(f32)
        else:
            j_f = jb[:, 128 * g - inner : 128 * (g + 1) - inner].astype(f32)
        own = ext[0:STRETCH, at]
        misc_o[taps : taps + 1, at] += jnp.sum(own, axis=0, keepdims=True)
        misc_o[taps - 1 : taps, at] += jnp.sum(own * j_f, axis=0, keepdims=True)
        total = own * cw[taps - 1 : taps, at]
        for k in range(taps - 1):
            d = taps - 1 - k
            term = ext[d : d + STRETCH, at] * ok[k]
            misc_o[k : k + 1, at] += jnp.sum(term * j_f, axis=0, keepdims=True)
            total = total + term * cw[k : k + 1, at]
        gcat_o[:, at] = total.astype(bf16)

        @pl.when(step_id == 0)
        def _():
            tail_o[:, at] = total[STRETCH - 8 :]

    head_o[...] = ext[0:8, :]
    ext[STRETCH : STRETCH + 8, :] = ext[0:8, :]


def exit_kernel(
    info, tok, gout, mine, gz, gcat, tail, nxt, last_j, cw, gain, wz_out, wj,
    gr_o, rim_o, rim_w_o, gain_o,
    fix,
):
    step_id = pl.program_id(0)
    blocks = pl.num_programs(0)
    i = blocks - 1 - step_id
    starts, base, _end_start, _flag = read_info(info, i)
    taps, width = cw.shape
    inner = gz.shape[1]

    @pl.when(step_id == 0)
    def _():
        gain_o[...] = jnp.zeros_like(gain_o)
        fix[0:8, :] = jnp.zeros((8, width), f32)
        fix[8:16, :] = nxt[...]
        places = base + STRETCH - 8 + iota((8, 128), 0)
        wide = last_j[8:16, :].astype(f32)
        total = tail[...]
        for k in range(taps - 1):
            d = taps - 1 - k
            ok = jnp.where(joined_ok(places, d, starts), 1.0, 0.0).astype(f32)
            inside = jnp.where(iota((8, width), 0) >= 8 - d, fix[d : d + 8, :], 0.0)
            term = inside * jnp.concatenate([ok] * (width // 128), axis=1)
            total = total + term * cw[k : k + 1, :]
            rim_w_o[k : k + 1, :] = jnp.sum(term * wide, axis=0, keepdims=True)
        rim_w_o[taps - 1 : 8, :] = jnp.zeros((9 - taps, width), f32)
        fix[0:8, :] = jnp.zeros((8, width), f32)
        fix[8:16, :] = total.astype(bf16).astype(f32) - tail[...].astype(bf16).astype(f32)
        rim_o[...] = fix[...].astype(bf16)

    g_normed = nt(gz[...], wz_out[:, :inner]) + nt(gcat[...], wj[...])

    def finish(g_normed):
        unit, inverse = norm_rows(tok[...])
        scaled = g_normed * gain[...]
        mean = jnp.mean(scaled * unit, axis=1, keepdims=True)
        own = gout[...].astype(f32) * mine[...]
        gr_o[...] = jnp.transpose(own + inverse * (scaled - unit * mean)).astype(bf16)
        gain_o[...] += jnp.sum(g_normed * unit, axis=0, keepdims=True)

    @pl.when(step_id == 0)
    def _():
        more = nt(rim_o[...], wj[:, :width])
        finish(g_normed + jnp.concatenate([jnp.zeros((STRETCH - 16, more.shape[1]), f32), more]))

    @pl.when(step_id > 0)
    def _():
        finish(g_normed)


def finish_kernel(parts, place, part, base, sums, out):
    wide = part[...].astype(f32) * lax.rsqrt(sums[0:1, :] / INNER + epsilon)
    size = out.shape[0]
    for k in range(parts):

        @pl.when(place[0] == k)
        def _():
            add = jnp.transpose(base[:, size * k : size * (k + 1)].astype(f32))
            out[...] = (wide + add).astype(bf16)


MESH = pl.DeviceIdType.MESH


def start_together(peers):
    barrier = pltpu.get_barrier_semaphore()
    for peer in peers:
        pl.semaphore_signal(barrier, inc=1, device_id=peer, device_id_type=MESH)
    pl.semaphore_wait(barrier, len(peers))


def remote(src, dst, sent, came, peer):
    return pltpu.make_async_remote_copy(
        src_ref=src, dst_ref=dst, send_sem=sent, recv_sem=came, device_id=peer, device_id_type=MESH
    )


def turned(index, distance, size):
    return lax.rem(index + distance + size, size)


def twin_of(index):
    parity = lax.rem(index, 2)
    return parity, index + 1 - 2 * parity


def gather_kernel(n, x, bc, dt, out, sent, came, passed, relayed, own):
    f = lax.axis_index("fsdp")
    parity, twin = twin_of(lax.axis_index("ctx"))
    rows = x.shape[0]
    half = rows // 2
    start_together([{"fsdp": turned(f, d, n)} for d in range(1, n)] + [{"ctx": twin}])
    pieces = []
    at = 0
    for ref in (x, bc, dt):
        pieces.append((ref, slice(at, at + ref.shape[1])))
        at += ref.shape[1]

    def place(source, side):
        return pl.ds(pl.multiple_of(source * rows + side * half, 16), half)

    mine = pl.ds(pl.multiple_of(parity * half, 16), half)
    copies = []
    for d in range(1, n):
        for p, (ref, cols) in enumerate(pieces):
            copy = remote(
                ref.at[mine, :], out.at[place(f, parity), cols],
                sent.at[d - 1, p], came.at[d - 1, p], {"fsdp": turned(f, d, n)},
            )
            copy.start()
            copies.append(copy)
    locals_ = []
    for p, (ref, cols) in enumerate(pieces):
        copy = pltpu.make_async_copy(
            ref, out.at[pl.ds(pl.multiple_of(f * rows, 16), rows), cols], own.at[p]
        )
        copy.start()
        locals_.append(copy)
    relays = []
    for d in range(1, n):
        source = turned(f, -d, n)
        for p, (ref, cols) in enumerate(pieces):
            copies[(d - 1) * len(pieces) + p].wait_recv()
            block = out.at[place(source, parity), cols]
            copy = remote(block, block, passed.at[d - 1, p], relayed.at[d - 1, p], {"ctx": twin})
            copy.start()
            relays.append(copy)
    for copy in copies:
        copy.wait_send()
    for copy in locals_:
        copy.wait()
    for copy in relays:
        copy.wait()


def gathered(x, bc, dt):
    n = lax.axis_size("fsdp")
    pieces = (n - 1, 3)
    width = x.shape[1] + bc.shape[1] + dt.shape[1]
    return pl.pallas_call(
        functools.partial(gather_kernel, n),
        out_shape=jax.ShapeDtypeStruct((n * x.shape[0], width), bf16),
        in_specs=[pl.BlockSpec(memory_space=pltpu.VMEM)] * 3,
        out_specs=pl.BlockSpec(memory_space=pltpu.VMEM),
        scratch_shapes=[pltpu.SemaphoreType.DMA(pieces)] * 4 + [pltpu.SemaphoreType.DMA((3,))],
        compiler_params=pltpu.CompilerParams(collective_id=1, has_side_effects=True),
    )(x, bc, dt)


def total_kernel(n, part, out, slots, sent, came):
    me = lax.axis_index("tp")
    start_together([{"tp": turned(me, d, n)} for d in range(1, n)])
    copies = []
    for d in range(1, n):
        copy = remote(
            part, slots.at[d - 1], sent.at[d - 1], came.at[d - 1], {"tp": turned(me, d, n)}
        )
        copy.start()
        copies.append(copy)
    total = part[...]
    for d in range(1, n):
        copies[d - 1].wait_recv()
        total = total + slots[d - 1]
    out[...] = total
    for copy in copies:
        copy.wait_send()


def total_over_tp(part):
    n = lax.axis_size("tp")
    return pl.pallas_call(
        functools.partial(total_kernel, n),
        out_shape=jax.ShapeDtypeStruct(part.shape, f32),
        in_specs=[pl.BlockSpec(memory_space=pltpu.VMEM)],
        out_specs=pl.BlockSpec(memory_space=pltpu.VMEM),
        scratch_shapes=[
            pltpu.VMEM((n - 1,) + part.shape, f32),
            pltpu.SemaphoreType.DMA((n - 1,)),
            pltpu.SemaphoreType.DMA((n - 1,)),
        ],
        compiler_params=pltpu.CompilerParams(collective_id=2, has_side_effects=True),
    )(part)


def reduce_kernel(
    n, m, bc_cols, conv_bc,
    p_out, p_z, p_cat, m_scan, m_rim, m_gate, m_dt, m_gain,
    o_out, o_z, o_cat, o_small, o_wide,
    give, take, mid, slots, final, bc_slots, small, small_slots, wide_slots,
    s1, r1, s2, r2, s3, r3, s4, r4,
):
    f = lax.axis_index("fsdp")
    t = lax.axis_index("tp")
    parity, twin = twin_of(lax.axis_index("ctx"))
    start_together(
        [{"ctx": twin}]
        + [{"fsdp": turned(f, d, n)} for d in range(1, n)]
        + [{"tp": turned(t, d, m)} for d in range(1, m)]
    )
    inner = p_out.shape[1]
    rows = p_out.shape[0] // n
    half = rows // 2

    def piece(q, side):
        at = pl.ds(pl.multiple_of(q * rows + side * half, 16), half)
        return jnp.concatenate([p_out[at, :], p_z[at, :], p_cat[at, :]], axis=1)

    copies = []
    for q in range(n):
        give[q] = piece(q, 1 - parity).astype(bf16)
        copy = remote(give.at[q], take.at[q], s1.at[q], r1.at[q], {"ctx": twin})
        copy.start()
        copies.append(copy)
    w_scan = m_scan.shape[1]
    w_gate = m_gate.shape[1]
    w_dt = m_dt.shape[1]
    small[...] = jnp.zeros_like(small)
    small[:, 0:w_scan] = m_scan[...] + m_rim[...]
    at = w_scan
    small[:, at : at + w_gate] = m_gate[...]
    at += w_gate
    small[:, at : at + w_dt] = m_dt[0:8, :]
    small[:, at + w_dt : at + 2 * w_dt] = m_dt[8:16, :]
    at += 2 * w_dt
    small[0:1, at:] = m_gain[...]
    small_slots[0, pl.ds(parity, 1)] = small[...][None]
    copy = remote(
        small, small_slots.at[0, parity], s1.at[n], r1.at[n], {"ctx": twin}
    )
    copy.start()
    copies.append(copy)

    copies[n].wait()
    small_slots[1, pl.ds(f, 1)] = (small_slots[0, 0] + small_slots[0, 1])[None]
    seconds = []
    for d in range(1, n):
        copy = remote(
            small_slots.at[1, f], small_slots.at[1, f], s2.at[n - 1 + d - 1], r2.at[n - 1 + d - 1],
            {"fsdp": turned(f, d, n)},
        )
        copy.start()
        seconds.append(copy)
    for q in range(n):
        copies[q].wait()
        mid[q] = (piece(q, parity) + take[q].astype(f32)).astype(bf16)
    slots[pl.ds(f, 1)] = mid[pl.ds(f, 1)]
    for d in range(1, n):
        peer = turned(f, d, n)
        copy = remote(
            mid.at[peer], slots.at[f], s2.at[d - 1], r2.at[d - 1], {"fsdp": peer}
        )
        copy.start()
        seconds.append(copy)
    for copy in seconds:
        copy.wait()
    small_sum = small_slots[1, 0]
    whole = slots[0].astype(f32)
    for q in range(1, n):
        small_sum = small_sum + small_slots[1, q]
        whole = whole + slots[q].astype(f32)
    final[...] = whole
    bc_at = slice(3 * inner, 3 * inner + bc_cols)
    bc_slots[pl.ds(t, 1)] = whole[:, bc_at][None]
    wide = jnp.concatenate([small_sum[:, conv_bc:w_scan], small_sum[:, at:]], axis=1)
    wide_slots[pl.ds(t, 1)] = wide[None]
    o_small[...] = small_sum[:, :at]
    thirds_ = []
    for d in range(1, m):
        peer = {"tp": turned(t, d, m)}
        for p, buf in enumerate((bc_slots, wide_slots)):
            copy = remote(buf.at[t], buf.at[t], s3.at[2 * (d - 1) + p], r3.at[2 * (d - 1) + p], peer)
            copy.start()
            thirds_.append(copy)
    for copy in thirds_:
        copy.wait()
    bc_sum = bc_slots[0]
    wide_sum = wide_slots[0]
    for q in range(1, m):
        bc_sum = bc_sum + bc_slots[q]
        wide_sum = wide_sum + wide_slots[q]
    o_wide[...] = wide_sum
    final[:, bc_at] = bc_sum
    here = pl.ds(pl.multiple_of(parity * half, 8), half)
    o_out[here, :] = final[:, :inner]
    o_z[here, :] = final[:, inner : 2 * inner]
    o_cat[here, :] = final[:, 2 * inner :]
    lasts = []
    for p, (out, cols) in enumerate(
        ((o_out, slice(0, inner)), (o_z, slice(inner, 2 * inner)), (o_cat, slice(2 * inner, None)))
    ):
        copy = remote(
            final.at[:, cols] if cols.stop else final.at[:, 2 * inner : final.shape[1]],
            out.at[here, :], s4.at[p], r4.at[p], {"ctx": twin},
        )
        copy.start()
        lasts.append(copy)
    for copy in lasts:
        copy.wait()


def reduced(parts, miscs, bc_cols):
    n, m = lax.axis_size("fsdp"), lax.axis_size("tp")
    p_out, _p_z, p_cat = parts
    rows = p_out.shape[0] // n
    half = rows // 2
    inner = p_out.shape[1]
    wide = 2 * inner + p_cat.shape[1]
    m_scan, _m_rim, m_gate, m_dt, m_gain = miscs
    kept = m_scan.shape[1] + m_gate.shape[1] + 2 * m_dt.shape[1]
    small = kept + m_gain.shape[1]
    crossing = m_scan.shape[1] - inner + m_gain.shape[1]
    dma = pltpu.SemaphoreType.DMA

    def shape(*dims):
        return jax.ShapeDtypeStruct(dims, f32)

    return pl.pallas_call(
        functools.partial(reduce_kernel, n, m, bc_cols, inner),
        out_shape=[
            shape(rows, inner), shape(rows, inner), shape(rows, p_cat.shape[1]),
            shape(8, kept), shape(8, crossing),
        ],
        in_specs=[pl.BlockSpec(memory_space=pltpu.VMEM)] * 8,
        out_specs=[pl.BlockSpec(memory_space=pltpu.VMEM)] * 5,
        scratch_shapes=[
            pltpu.VMEM((n, half, wide), bf16),
            pltpu.VMEM((n, half, wide), bf16),
            pltpu.VMEM((n, half, wide), bf16),
            pltpu.VMEM((n, half, wide), bf16),
            pltpu.VMEM((half, wide), f32),
            pltpu.VMEM((m, half, bc_cols), f32),
            pltpu.VMEM((8, small), f32),
            pltpu.VMEM((2, max(n, 2), 8, small), f32),
            pltpu.VMEM((m, 8, crossing), f32),
            dma((n + 1,)), dma((n + 1,)), dma((2 * n - 2,)), dma((2 * n - 2,)),
            dma((2 * m - 2,)), dma((2 * m - 2,)), dma((3,)), dma((3,)),
        ],
        compiler_params=pltpu.CompilerParams(
            collective_id=3, has_side_effects=True, vmem_limit_bytes=48 * 1024 * 1024
        ),
    )(*parts, *miscs)


def constants(inner, heads):
    lane_head = np.arange(inner) // (inner // heads)
    e8 = (np.arange(HEAD_ROWS)[:, None] == lane_head[None, :]).astype(np.float32)

    def spread(kind):
        m = np.zeros((128, inner), np.float32)
        m[HEAD_ROWS * kind : HEAD_ROWS * (kind + 1)] = e8
        return jnp.asarray(np.concatenate([m, m], axis=0), bf16)

    def gather(kind):
        m = np.zeros((inner, 128), np.float32)
        m[:, HEAD_ROWS * kind : HEAD_ROWS * (kind + 1)] = e8.T
        return jnp.asarray(np.concatenate([m, m], axis=0), bf16)

    at = np.arange(STRETCH)
    upper = jnp.asarray((at[:, None] <= at[None, :]).astype(np.float32), bf16)
    lower = jnp.asarray((at[:, None] >= at[None, :]).astype(np.float32), bf16)
    return jnp.asarray(e8), spread, gather, upper, lower


def passed_along(block, axis, distance):
    devices = range(lax.axis_size(axis))
    route = [(i - distance, i) for i in devices if i - distance in devices]
    return lax.ppermute(block, axis, route)


def entering(decay, state, axis, reverse):
    size = lax.axis_size(axis)
    if size == 2:
        return passed_along(state, axis, -1 if reverse else 1)
    index = lax.axis_index(axis)
    decays = lax.all_gather(decay.astype(bf16), axis)
    states = lax.all_gather(state, axis)

    def lap(k, before):
        at = size - 1 - k if reverse else k
        reached = at > index if reverse else at < index
        new = decays[at].astype(f32) * before + states[at].astype(f32)
        return jnp.where(reached, new, before)

    return lax.fori_loop(0, size, lap, jnp.zeros(state.shape, f32)).astype(bf16)


def call(kernel, blocks, ins, outs, scratch, micros=0):
    def spec(shape, how):
        if how == "smem":
            return pl.BlockSpec(memory_space=pltpu.SMEM)
        return pl.BlockSpec(shape, how)

    return pl.pallas_call(
        kernel,
        grid=(blocks,),
        in_specs=[spec(shape, how) for _a, shape, how in ins],
        out_specs=[spec(shape, how) for _s, shape, how in outs],
        out_shape=[s for s, _sh, _h in outs],
        scratch_shapes=scratch,
        cost_estimate=pl.CostEstimate(
            flops=0, transcendentals=0, bytes_accessed=3_000_000 * micros
        )
        if micros
        else None,
        compiler_params=pltpu.CompilerParams(
            dimension_semantics=("arbitrary",), vmem_limit_bytes=56 * 1024 * 1024
        ),
    )(*[a for a, _s, _h in ins])


def local(
    tokens, grad_out, lengths, norm_gain, w_z, w_x, w_bc, w_dt, conv_x_w, conv_x_b,
    conv_bc_w, conv_bc_b, dt_bias, a_log, d_skip, gate_gain, w_out,
):
    rows, model = tokens.shape
    inner = w_z.shape[1]
    heads = dt_bias.shape[0]
    states = w_bc.shape[1] // 2
    taps = conv_x_w.shape[0]
    blocks = rows // STRETCH
    width = inner + 2 * states
    tp_size = lax.axis_size("tp")
    slice_width = model // tp_size
    tp_index = lax.axis_index("tp")
    ctx_index = lax.axis_index("ctx")
    e8, spread, gather, upper, lower = constants(inner, heads)

    w_joined = gathered(w_x, w_bc, jnp.pad(w_dt, ((0, 0), (0, 128 - heads))))
    wz_out = lax.all_gather(jnp.concatenate([w_z, w_out.T], axis=1), "fsdp", axis=0, tiled=True)

    starts = jnp.cumsum(lengths[0]) - lengths[0]
    info = jnp.concatenate([(ctx_index * rows).astype(jnp.int32)[None], starts.astype(jnp.int32)])
    halo = passed_along(tokens[rows - 16 :], "ctx", 1)
    gain = norm_gain[None, :]
    conv_w = jnp.concatenate([conv_x_w, conv_bc_w], axis=1)
    conv_b = jnp.concatenate([conv_x_b, conv_bc_b])[None, :]

    def head_rows(x):
        return jnp.broadcast_to(jnp.pad(x, (0, HEAD_ROWS - heads))[:, None], (HEAD_ROWS, STRETCH))

    bias = head_rows(dt_bias)
    rate = head_rows(jnp.exp(a_log))
    per_head = inner // heads
    dskip = jnp.repeat(d_skip, per_head)[None, :]
    ggain = gate_gain[None, :]

    def shape(dims, kind):
        return jax.ShapeDtypeStruct(dims, kind)

    def whole(x):
        return (x, x.shape, lambda i: (0,) * x.ndim)

    def by_rows(x, flip=False):
        if flip:
            return (x, (STRETCH, x.shape[1]), lambda i: (blocks - 1 - i, 0))
        return (x, (STRETCH, x.shape[1]), lambda i: (i, 0))

    def by_lanes(x, flip=False):
        if flip:
            return (x, (x.shape[0], STRETCH), lambda i: (0, blocks - 1 - i))
        return (x, (x.shape[0], STRETCH), lambda i: (0, i))

    def by_block(x, flip=False):
        if flip:
            return (x, (1,) + x.shape[1:], lambda i: (blocks - 1 - i, 0, 0))
        return (x, (1,) + x.shape[1:], lambda i: (i, 0, 0))

    def fixed(x):
        return (x, x.shape, lambda i: (0,) * len(x.shape))

    info_in = (info, None, "smem")
    state_dims = (blocks, states, inner)
    normed, joined_x, joined_bc, vbc, slope_x, slope_bc, pre, step, cum, s_part, end_state, decay = call(
        entry_kernel,
        blocks,
        [
            info_in, by_rows(tokens), whole(halo), whole(gain), whole(w_joined),
            whole(conv_w), whole(conv_b), whole(bias), whole(rate), whole(upper),
            whole(spread(0)), whole(e8),
        ],
        [
            by_rows(shape((rows, model), bf16)),
            by_rows(shape((rows, inner), bf16)),
            by_rows(shape((rows, 2 * states), bf16)),
            by_rows(shape((rows, width), bf16)),
            by_rows(shape((rows, inner), bf16)),
            by_rows(shape((rows, 2 * states), f32)),
            by_lanes(shape((HEAD_ROWS, rows), f32)),
            by_lanes(shape((HEAD_ROWS, rows), f32)),
            by_lanes(shape((HEAD_ROWS, rows), f32)),
            by_block(shape(state_dims, f32)),
            fixed(shape((states, inner), bf16)),
            fixed(shape((1, inner), f32)),
        ],
        [
            pltpu.VMEM((STRETCH + 8, width), f32),
            pltpu.VMEM((states, inner), f32),
            pltpu.VMEM((1, inner), f32),
        ],
    )
    incoming = entering(decay, end_state, "ctx", False)
    z_part, out, gn, branch, sums, state_in = call(
        mix_kernel,
        blocks,
        [
            info_in, by_rows(vbc), by_lanes(step), by_lanes(cum), by_block(s_part),
            whole(incoming), by_rows(normed), by_rows(grad_out), whole(wz_out), whole(dskip),
            whole(ggain), whole(spread(1)), whole(spread(2)), whole(e8),
        ],
        [
            by_rows(shape((rows, inner), f32)),
            by_rows(shape((rows, inner), f32)),
            by_rows(shape((rows, inner), f32)),
            by_lanes(shape((model, rows), bf16)),
            by_lanes(shape((2, rows), f32)),
            by_block(shape(state_dims, bf16)),
        ],
        [pltpu.VMEM((states, inner), f32), pltpu.VMEM((STRETCH, STRETCH), f32)],
    )
    sums = total_over_tp(sums)
    branch = lax.psum_scatter(branch, "tp", scatter_dimension=0, tiled=True)
    g_z, g_b, g_c, normed_two, a_sum, gs_part, start_state, misc_gate = call(
        gate_kernel,
        blocks,
        [
            info_in, by_lanes(sums, True), by_lanes(cum, True), by_rows(out, True),
            by_rows(z_part, True), by_rows(gn, True), by_rows(vbc, True), by_block(state_in, True),
            whole(dskip), whole(ggain), whole(spread(2)), whole(e8), whole(gather(0)),
        ],
        [
            by_rows(shape((rows, inner), bf16), True),
            by_rows(shape((rows, inner), bf16), True),
            by_rows(shape((rows, inner), bf16), True),
            by_rows(shape((rows, inner), bf16), True),
            by_lanes(shape((HEAD_ROWS, rows), f32), True),
            by_block(shape(state_dims, f32), True),
            fixed(shape((states, inner), bf16)),
            fixed(shape((8, inner), f32)),
        ],
        [pltpu.VMEM((states, inner), f32)],
    )
    outgoing = entering(decay, start_state, "ctx", True)
    g_cat, tail, head, misc_scan, misc_dt = call(
        scan_kernel,
        blocks,
        [
            info_in, by_rows(vbc, True), by_rows(g_b, True), by_rows(g_c, True),
            by_lanes(step, True), by_lanes(cum, True), by_lanes(pre, True), by_lanes(a_sum, True),
            by_block(state_in, True), by_block(gs_part, True), whole(outgoing),
            by_rows(slope_x, True), by_rows(slope_bc, True), by_rows(joined_x, True),
            by_rows(joined_bc, True), whole(conv_w), whole(dskip), whole(rate), whole(spread(1)),
            whole(spread(2)), whole(e8), whole(gather(0)), whole(gather(1)),
            whole(gather(2)), whole(lower),
        ],
        [
            by_rows(shape((rows, width + 128), bf16), True),
            fixed(shape((8, width), f32)),
            fixed(shape((8, width), f32)),
            fixed(shape((8, width), f32)),
            fixed(shape((2 * HEAD_ROWS, STRETCH), f32)),
        ],
        [
            pltpu.VMEM((states, inner), f32),
            pltpu.VMEM((STRETCH + 8, width), f32),
            pltpu.VMEM((STRETCH, STRETCH), f32),
            pltpu.VMEM((STRETCH, STRETCH), f32),
        ],
    )
    next_rows = passed_along(head, "ctx", -1)
    feature = jnp.arange(model, dtype=jnp.int32) // slice_width
    mine = (feature == tp_index).astype(f32)[None, :]
    last_joined = jnp.concatenate([joined_x[rows - 16 :], joined_bc[rows - 16 :]], axis=1)
    g_resid, rim, rim_w, gain_part = call(
        exit_kernel,
        blocks,
        [
            info_in, by_rows(tokens, True), by_rows(grad_out, True), whole(mine),
            by_rows(g_z, True), by_rows(g_cat, True), whole(tail), whole(next_rows), whole(last_joined), whole(conv_w), whole(gain),
            whole(wz_out), whole(w_joined),
        ],
        [
            by_lanes(shape((model, rows), bf16), True),
            fixed(shape((16, width), bf16)),
            fixed(shape((8, width), f32)),
            fixed(shape((1, model), f32)),
        ],
        [pltpu.VMEM((16, width), f32)],
    )
    g_resid = lax.psum_scatter(g_resid, "tp", scatter_dimension=0, tiled=True)

    part_out = tn(grad_out, normed_two)
    part_z = tn(normed, g_z)
    part_cat = tn(normed, g_cat)
    part_rim = tn(normed[rows - 16 :], rim)
    part_cat = part_cat + jnp.pad(part_rim, ((0, 0), (0, 128)))
    s_out, s_z, s_cat, s_small, s_wide = reduced(
        (part_out, part_z, part_cat),
        (misc_scan, rim_w, misc_gate, misc_dt, gain_part),
        2 * states,
    )
    if lax.axis_size("ctx") > 2:
        s_out, s_z, s_cat, s_small, s_wide = jax.tree.map(
            lambda part: lax.psum(0.5 * part, "ctx"), (s_out, s_z, s_cat, s_small, s_wide)
        )
    grad_w_out = s_out.T
    grad_w_z = s_z
    grad_w_x = s_cat[:, :inner]
    grad_w_bc = s_cat[:, inner : inner + 2 * states]
    grad_w_dt = s_cat[:, inner + 2 * states : inner + 2 * states + heads]
    grad_conv_x_w = s_small[:taps, :inner]
    grad_conv_x_b = s_small[taps, :inner]
    grad_gate_gain = s_small[0, width : width + inner]
    grad_d_skip = jnp.sum(s_small[1, width : width + inner].reshape(heads, per_head), axis=1)
    dt_at = width + inner
    grad_a_log = jnp.sum(s_small[:heads, dt_at : dt_at + STRETCH], axis=1)
    grad_dt_bias = jnp.sum(s_small[:heads, dt_at + STRETCH : dt_at + 2 * STRETCH], axis=1)
    grad_conv_bc_w = s_wide[:taps, : 2 * states]
    grad_conv_bc_b = s_wide[taps, : 2 * states]
    here = tp_index * slice_width
    grad_norm_gain = lax.dynamic_slice_in_dim(s_wide[0, 2 * states :], here, slice_width, 0)
    place = tp_index.astype(jnp.int32)[None]

    layer_out = call(
        functools.partial(finish_kernel, tp_size),
        blocks // 2,
        [
            (place, None, "smem"),
            (branch, (slice_width, 2 * STRETCH), lambda i: (0, i)),
            (tokens, (2 * STRETCH, model), lambda i: (i, 0)),
            (sums, (2, 2 * STRETCH), lambda i: (0, i)),
        ],
        [(shape((slice_width, rows), bf16), (slice_width, 2 * STRETCH), lambda i: (0, i))],
        [],
    )[0].T
    grad_tokens = g_resid.T
    return (
        layer_out, grad_tokens, grad_norm_gain, grad_w_z, grad_w_x, grad_w_bc, grad_w_dt,
        grad_conv_x_w, grad_conv_x_b, grad_conv_bc_w, grad_conv_bc_b, grad_dt_bias, grad_a_log,
        grad_d_skip, grad_gate_gain, grad_w_out,
    )


def solution(mesh):
    both = ("fsdp", "ctx")
    in_specs = (
        P(both, None), P(both, None), P("fsdp", None), P(), P("fsdp", "tp"), P("fsdp", "tp"),
        P("fsdp", None), P("fsdp", "tp"), P(None, "tp"), P("tp"), P(), P(), P("tp"), P("tp"),
        P("tp"), P("tp"), P("tp", "fsdp"),
    )
    out_specs = (
        P(both, "tp"), P(both, "tp"), P("tp"), P("fsdp", "tp"), P("fsdp", "tp"), P("fsdp", None),
        P("fsdp", "tp"), P(None, "tp"), P("tp"), P(), P(), P("tp"), P("tp"), P("tp"), P("tp"),
        P("tp", "fsdp"),
    )
    return jax.shard_map(local, mesh=mesh, in_specs=in_specs, out_specs=out_specs, check_vma=False)
```

```python
import functools

import jax
import jax.numpy as jnp
import numpy as np
from jax import lax
from jax.experimental import pallas as pl
from jax.experimental.pallas import tpu as pltpu
from jax.sharding import PartitionSpec as P

STRETCH = 256
TAPS = 4
INNER = 1536
HEAD_ROWS = 8
LOG2E = 1.4426950408889634

epsilon = 1e-05
f32 = jnp.float32
bf16 = jnp.bfloat16


def nn(left, right):
    return lax.dot_general(left, right, (((1,), (0,)), ((), ())), preferred_element_type=f32)


def nt(left, right):
    return lax.dot_general(left, right, (((1,), (1,)), ((), ())), preferred_element_type=f32)


def tn(left, right):
    return lax.dot_general(left, right, (((0,), (0,)), ((), ())), preferred_element_type=f32)


def halves(x):
    high = x.astype(bf16)
    return high, (x - high.astype(f32)).astype(bf16)


def thirds(x):
    high = x.astype(bf16)
    rest = x - high.astype(f32)
    mid = rest.astype(bf16)
    return high, mid, (rest - mid.astype(f32)).astype(bf16)


def exact_rows(x, ones_matrix):
    high, mid, low = thirds(x)
    r = HEAD_ROWS
    out = nn(jnp.concatenate([high, mid, low, jnp.zeros_like(low)], axis=0), ones_matrix)
    return out[:r] + out[r : 2 * r] + out[2 * r : 3 * r]


def columns_of(rows):
    have = sum(r.shape[0] for r in rows)
    pad = jnp.zeros((128 - have, rows[0].shape[1]), f32)
    cols = jnp.transpose(jnp.concatenate(list(rows) + [pad], axis=0))
    high, low = halves(cols)
    return cols, jnp.concatenate([high, low], axis=1)


def segment_start(pos, starts):
    found = jnp.zeros_like(pos)
    for s in starts:
        found = jnp.where(pos >= s, s, found)
    return found


def joined_ok(u, distance, starts):
    ok = jnp.ones(u.shape, jnp.bool_)
    for s in starts[1:]:
        ok = ok & jnp.logical_not((u < s) & (u + distance >= s))
    return ok


def iota(shape, axis):
    return lax.broadcasted_iota(jnp.int32, shape, axis)


def read_info(rows, lengths, block):
    first = lax.axis_index("ctx") * rows
    starts = [jnp.int32(0)]
    for k in range(lengths.shape[1] - 1):
        starts.append(starts[-1] + lengths[0, k])
    base = first + block * STRETCH
    end_start = segment_start(base + STRETCH - 1, starts)
    flag = jnp.where(end_start < base, 1.0, 0.0).astype(f32)
    return starts, base, end_start, flag


def norm_rows(tok):
    x = tok.astype(f32)
    inverse = lax.rsqrt(jnp.mean(x * x, axis=1, keepdims=True) + epsilon)
    return x * inverse, inverse


def lanes_of(column, e8):
    return jnp.sum(column * e8, axis=0, keepdims=True)


def entry_kernel(
    rows, info, tok, halo, par, wj, tri, ew, e8,
    nrm_o, jx_o, jb_o, vbc_o, sx_o, sb_o, pre_o, step_o, cum_o, s_o, end_o, dec_o,
    ext, run, dec,
):
    i = pl.program_id(0)
    starts, base, end_start, flag = read_info(rows, info, i)
    inner = jx_o.shape[1]
    width = inner + jb_o.shape[1]
    gain, cb, cw, taps = par[0:1, :], par[1:2, :], par[4:8, :], TAPS

    @pl.when(i == 0)
    def _():
        unit, _inv = norm_rows(halo[...])
        before = nn((unit * gain).astype(bf16), wj[:, :width])
        ext[0:8, :] = before.astype(bf16).astype(f32)[8:16]
        run[...] = jnp.zeros_like(run)
        dec[...] = jnp.ones_like(dec)

    unit, _inv = norm_rows(tok[...])
    normed = (unit * gain).astype(bf16)
    nrm_o[...] = normed
    product = nn(normed, wj[...])
    joined = product[:, :width].astype(bf16)
    jx_o[...] = joined[:, :inner]
    jb_o[...] = joined[:, inner:]
    ext[8 : 8 + STRETCH, :] = joined.astype(f32)
    pos = base + iota((STRETCH, 128), 0)
    first_of = segment_start(pos, starts)
    valid = [
        jnp.where(pos - (taps - 1 - k) >= first_of, 1.0, 0.0).astype(f32) for k in range(taps - 1)
    ]
    for g in range(width // 128):
        at = slice(128 * g, 128 * (g + 1))
        acc = cb[:, at] + cw[taps - 1 : taps, at] * ext[8 : 8 + STRETCH, at]
        for k in range(taps - 1):
            low = 8 - (taps - 1) + k
            acc = acc + cw[k : k + 1, at] * (ext[low : low + STRETCH, at] * valid[k])
        sig = jax.nn.sigmoid(acc)
        act = acc * sig
        vbc_o[:, at] = act.astype(bf16)
        slope = sig + act * (1.0 - sig)
        if 128 * g < inner:
            sx_o[:, at] = slope.astype(bf16)
        else:
            sb_o[:, 128 * g - inner : 128 * (g + 1) - inner] = slope
    ext[0:8, :] = ext[STRETCH : STRETCH + 8, :]
    pre = jnp.transpose(product[:, width:])[:HEAD_ROWS] + par[8:16, 0:1]
    step = jax.nn.softplus(pre)
    logd = -step * jnp.exp(par[8:16, 1:2])
    cum = exact_rows(logd, tri[...])
    pre_o[...] = pre
    step_o[...] = step
    cum_o[...] = cum
    cum_e = cum[:, STRETCH - 1 : STRETCH]
    where_s = base + iota((1, STRETCH), 1)
    keep = jnp.where(where_s >= end_start, 1.0, 0.0).astype(f32)
    weight = jnp.exp(cum_e - cum) * step * keep
    _cols, both = columns_of([weight])
    spread = nn(both, ew[...])
    v = vbc_o[:, :inner].astype(f32)
    b = vbc_o[:, inner : inner + 128]
    state = tn(b, (v * spread).astype(bf16))
    s_o[0] = state
    through = lanes_of(jnp.exp(cum_e) * flag, e8[...])
    run[...] = through * run[...] + state
    dec[...] = dec[...] * through
    end_o[...] = run[...].astype(bf16)
    dec_o[...] = dec[...]


def mix_kernel(
    rows, info, vbc, step, cum, s_in, inc, normed, gout, wz_out, par, e_step, e_scale, e8,
    z_o, out_o, gn_o, sum_o, st_o, br_o,
    run, gram,
):
    i = pl.program_id(0)
    starts, base, _end_start, flag = read_info(rows, info, i)
    inner = out_o.shape[1]
    gain = par[2:3, :inner]
    dskip = lanes_of(par[8:16, 2:3], e8[...])

    @pl.when(i == 0)
    def _():
        run[...] = inc[...].astype(f32)

    st = run[...].astype(bf16)
    st_o[0] = st
    cum_v = cum[...]
    cum_e = cum_v[:, STRETCH - 1 : STRETCH]
    through = lanes_of(jnp.exp(cum_e) * flag, e8[...])
    run[...] = through * run[...] + s_in[0]

    row_first = segment_start(base + iota((1, STRETCH), 1), starts)
    scale = jnp.exp(cum_v) * jnp.where(row_first < base, 1.0, 0.0).astype(f32)
    cum2 = cum_v * LOG2E
    cols, both = columns_of([cum2, step[...], scale])
    step_x = nn(both, e_step[...])
    scale_x = nn(both, e_scale[...])
    b = vbc[:, inner : inner + 128]
    c = vbc[:, inner + 128 : inner + 256]
    t_at = iota((STRETCH, STRETCH), 0)
    s_at = iota((STRETCH, STRETCH), 1)
    t_first = segment_start(t_at + base, starts)
    mask = (s_at <= t_at) & (s_at + base >= t_first)
    gram[...] = jnp.where(mask, nt(c, b), 0.0)
    carried = nn(c, st) * scale_x
    lane = iota((STRETCH, 128), 1)
    pieces = []
    for p in range(inner // 128):
        at = slice(128 * p, 128 * (p + 1))
        v = vbc[:, at].astype(f32)
        sv = v * step_x[:, at]
        acc = carried[:, at] + dskip[:, at] * v
        for j in range(2):
            h = 2 * p + j
            half = jnp.where((lane < 64) if j == 0 else (lane >= 64), sv, 0.0).astype(bf16)
            gap = cols[:, h : h + 1] - cum2[h : h + 1, :]
            m = (gram[...] * jnp.exp2(jnp.minimum(gap, 0.0))).astype(bf16)
            acc = acc + nn(m, half)
        pieces.append(acc)
    out = jnp.concatenate(pieces, axis=1)
    out_o[...] = out
    zf = nn(normed[...], wz_out[:, :inner])
    z_o[...] = zf
    gated = out * (zf * jax.nn.sigmoid(zf))
    gn = nn(gout[...], wz_out[:, inner:])
    gn_o[...] = gn
    gg = gated * gain
    br_o[...] = nt(wz_out[:, inner:], gg.astype(bf16)).astype(bf16)
    ss = jnp.sum(gated * gated, axis=1, keepdims=True)
    dq = jnp.sum(gn * gg, axis=1, keepdims=True)
    sum_o[...] = jnp.transpose(jnp.where(lane == 0, ss, dq))[0:2]


def gate_kernel(
    rows, info, sums, cum, out, z, gn, vc, st, par, e_scale, e8, f_sum,
    gz_o, gb_o, gc_o, n2_o, a_o, gs_o, start_o, misc_o,
    run,
):
    step_id = pl.program_id(0)
    blocks = pl.num_programs(0)
    i = blocks - 1 - step_id
    starts, base, _end_start, flag = read_info(rows, info, i)
    inner = z.shape[1]
    gain = par[2:3, :inner]
    dskip = lanes_of(par[8:16, 2:3], e8[...])

    @pl.when(step_id == 0)
    def _():
        run[...] = jnp.zeros_like(run)
        misc_o[...] = jnp.zeros_like(misc_o)

    alpha = lax.rsqrt(sums[0:1, :] / INNER + epsilon)
    beta = alpha * alpha * alpha * sums[1:2, :] / INNER
    cum_v = cum[...]
    row_first = segment_start(base + iota((1, STRETCH), 1), starts)
    scale = jnp.exp(cum_v) * jnp.where(row_first < base, 1.0, 0.0).astype(f32)
    cols, both = columns_of([alpha, beta, jnp.zeros((14, STRETCH), f32), scale])
    alpha_c = cols[:, 0:1]
    beta_c = cols[:, 1:2]
    scale_x = nn(both, e_scale[...])
    v = vc[:, :inner].astype(f32)
    c = vc[:, inner + 128 : inner + 256]
    zf = z[...]
    sig = jax.nn.sigmoid(zf)
    act = zf * sig
    o = out[...]
    gated = o * act
    g_n = gn[...]
    unit = gated * alpha_c
    g_gated = alpha_c * (g_n * gain) - beta_c * gated
    g_out = g_gated * act
    gz_o[...] = (g_gated * o * (sig + act * (1.0 - sig))).astype(bf16)
    gb = g_out.astype(bf16)
    gb_o[...] = gb
    n2_o[...] = (unit * gain).astype(bf16)
    misc_o[0:1, :] += jnp.sum(g_n * unit, axis=0, keepdims=True)
    misc_o[1:2, :] += jnp.sum(g_out * v, axis=0, keepdims=True)
    gf = gb.astype(f32)
    carried = nn(c, st[0]) * scale_x
    prod = gf * (o - dskip * v) + (g_out - gf) * carried
    high, low = halves(prod)
    sums_c = nn(jnp.concatenate([high, low], axis=1), f_sum[...])
    a_o[...] = jnp.transpose(sums_c)[0:HEAD_ROWS]
    gc = (g_out * scale_x).astype(bf16)
    gc_o[...] = gc
    gs = tn(c, gc)
    gs_o[0] = gs
    through = lanes_of(jnp.exp(cum_v[:, STRETCH - 1 : STRETCH]) * flag, e8[...])
    run[...] = through * run[...] + gs
    start_o[...] = run[...].astype(bf16)


def scan_kernel(
    rows, info, vbc, gb, gc, step, cum, pre, a_sum, st, gs_in, outg, sx, sb, jx, jb, par,
    e_step, e_w, e8, f_one, f_two, f_three, tril,
    gcat_o, tail_o, head_o, misc_o, dt_o,
    run, ext, gram, acc,
):
    step_id = pl.program_id(0)
    blocks = pl.num_programs(0)
    i = blocks - 1 - step_id
    starts, base, end_start, flag = read_info(rows, info, i)
    inner = gb.shape[1]
    width = inner + jb.shape[1]
    cw, taps = par[4:8, :], TAPS
    rate = jnp.exp(par[8:16, 1:2])
    dskip = lanes_of(par[8:16, 2:3], e8[...])

    @pl.when(step_id == 0)
    def _():
        run[...] = outg[...].astype(f32)
        ext[STRETCH : STRETCH + 8, :] = jnp.zeros((8, width), f32)
        misc_o[...] = jnp.zeros_like(misc_o)
        dt_o[...] = jnp.zeros_like(dt_o)

    cum_v = cum[...]
    step_v = step[...]
    cum_e = cum_v[:, STRETCH - 1 : STRETCH]
    after = run[...]
    low_after = after.astype(bf16)
    state = st[0]
    through = lanes_of(jnp.exp(cum_e) * flag, e8[...])
    g_through = jnp.sum(after * state.astype(f32), axis=0, keepdims=True) * through
    end_more = jnp.sum(e8[...] * g_through, axis=1, keepdims=True)
    run[...] = through * after + gs_in[0]

    where_s = base + iota((1, STRETCH), 1)
    row_first = segment_start(where_s, starts)
    end_decay = jnp.exp(cum_e - cum_v) * jnp.where(where_s >= end_start, 1.0, 0.0).astype(f32)
    weight = end_decay * step_v
    cum2 = cum_v * LOG2E
    cols, both = columns_of([cum2, step_v, weight])
    step_x = nn(both, e_step[...])
    w_x = nn(both, e_w[...])
    b = vbc[:, inner : inner + 128]
    c = vbc[:, inner + 128 : inner + 256]
    s_at = iota((STRETCH, STRETCH), 0)
    t_at = iota((STRETCH, STRETCH), 1)
    mask = (s_at <= t_at) & (s_at + base >= row_first)
    gram[...] = jnp.where(mask, nt(b, c), 0.0)
    acc[...] = jnp.zeros_like(acc)
    y = nn(b, low_after)
    lane = iota((STRETCH, 128), 1)
    us = []
    svs = []
    for p in range(inner // 128):
        at = slice(128 * p, 128 * (p + 1))
        sv = (vbc[:, at].astype(f32) * step_x[:, at]).astype(bf16).astype(f32)
        svs.append(sv)
        g_pair = gb[:, at]
        g_wide = g_pair.astype(f32)
        u = jnp.zeros((STRETCH, 128), f32)
        for j in range(2):
            h = 2 * p + j
            side = (lane < 64) if j == 0 else (lane >= 64)
            gap = cum2[h : h + 1, :] - cols[:, h : h + 1]
            decay = jnp.exp2(jnp.minimum(gap, 0.0))
            m = (gram[...] * decay).astype(bf16)
            u = u + nn(m, jnp.where(side, g_wide, 0.0).astype(bf16))
            g_m = nt(jnp.where(side, sv, 0.0).astype(bf16), g_pair)
            acc[...] += g_m * decay
        us.append(u)
    u = jnp.concatenate(us, axis=1)
    g_gram = jnp.where(mask, acc[...], 0.0).astype(bf16)
    v = vbc[:, :inner].astype(f32)
    gf = gb[...].astype(f32)
    wv = (v * w_x).astype(bf16)
    ext[0:STRETCH, inner : inner + 128] = (nn(g_gram, c) + nt(wv, low_after)) * sb[:, :128]
    ext[0:STRETCH, inner + 128 :] = (tn(g_gram, b) + nt(gc[...], state)) * sb[:, 128:]
    gv = dskip * gf + step_x * u + w_x * y
    h1, l1 = halves(v * u)
    h2, l2 = halves(v * y)
    h3, l3 = halves(jnp.concatenate(svs, axis=1) * u)
    sums_c = (
        nn(jnp.concatenate([h1, l1], axis=1), f_one[...])
        + nn(jnp.concatenate([h2, l2], axis=1), f_two[...])
        + nn(jnp.concatenate([h3, l3], axis=1), f_three[...])
    )
    sums_r = jnp.transpose(sums_c)
    g_step0 = sums_r[0:HEAD_ROWS]
    g_end = sums_r[HEAD_ROWS : 2 * HEAD_ROWS]
    ends = g_end * weight
    g_cum = a_sum[...] - sums_r[2 * HEAD_ROWS : 3 * HEAD_ROWS] - ends
    end_add = jnp.sum(ends, axis=1, keepdims=True) + end_more
    g_log = exact_rows(g_cum, tril[...]) + end_add
    g_step = g_step0 + g_end * end_decay - g_log * rate
    g_pre_dt = g_step * jax.nn.sigmoid(pre[...])
    dt_o[0:HEAD_ROWS, :] += g_log * (-step_v * rate)
    dt_o[HEAD_ROWS:, :] += g_pre_dt
    pad = jnp.zeros((128 - HEAD_ROWS, STRETCH), f32)
    gcat_o[:, width:] = jnp.transpose(jnp.concatenate([g_pre_dt, pad], axis=0)).astype(bf16)

    ext[0:STRETCH, :inner] = gv * sx[...].astype(f32)
    pos = base + iota((STRETCH, 128), 0)
    ok = [
        jnp.where(joined_ok(pos, d, starts), 1.0, 0.0).astype(f32) for d in range(taps - 1, 0, -1)
    ]
    for g in range(width // 128):
        at = slice(128 * g, 128 * (g + 1))
        if 128 * g < inner:
            j_f = jx[:, at].astype(f32)
        else:
            j_f = jb[:, 128 * g - inner : 128 * (g + 1) - inner].astype(f32)
        own = ext[0:STRETCH, at]
        misc_o[taps : taps + 1, at] += jnp.sum(own, axis=0, keepdims=True)
        misc_o[taps - 1 : taps, at] += jnp.sum(own * j_f, axis=0, keepdims=True)
        total = own * cw[taps - 1 : taps, at]
        for k in range(taps - 1):
            d = taps - 1 - k
            term = ext[d : d + STRETCH, at] * ok[k]
            misc_o[k : k + 1, at] += jnp.sum(term * j_f, axis=0, keepdims=True)
            total = total + term * cw[k : k + 1, at]
        gcat_o[:, at] = total.astype(bf16)

        @pl.when(step_id == 0)
        def _():
            tail_o[:, at] = total[STRETCH - 8 :]

    head_o[...] = ext[0:8, :]
    ext[STRETCH : STRETCH + 8, :] = ext[0:8, :]


def exit_kernel(
    rows, blocks, rim_side, info, tok, gout, mine, gz, gcat, par, wz_out, wj, *rest
):
    step_id = pl.program_id(0)
    i = blocks - 1 - step_id
    starts, base, _end_start, _flag = read_info(rows, info, i)
    inner = gz.shape[1]
    if rim_side:
        tail, nxt, last_j, gr_o, gain_o, rim_o, rim_w_o, fix = rest
        taps, width = TAPS, tail.shape[1]
        cw = par[4:8, :width]
    else:
        gr_o, gain_o = rest
    gain = par[0:1, :]

    g_normed = nt(gz[...], wz_out[:, :inner]) + nt(gcat[...], wj[...])

    def finish(g_normed):
        unit, inverse = norm_rows(tok[...])
        scaled = g_normed * gain
        mean = jnp.mean(scaled * unit, axis=1, keepdims=True)
        own = gout[...].astype(f32) * mine[...]
        gr_o[...] = jnp.transpose(own + inverse * (scaled - unit * mean)).astype(bf16)
        gain_o[...] += jnp.sum(g_normed * unit, axis=0, keepdims=True)

    @pl.when(step_id == 0)
    def _():
        gain_o[...] = jnp.zeros_like(gain_o)

    if not rim_side:
        finish(g_normed)
        return

    @pl.when(step_id == 0)
    def _():
        fix[0:8, :] = jnp.zeros((8, width), f32)
        fix[8:16, :] = nxt[...]
        places = base + STRETCH - 8 + iota((8, 128), 0)
        wide = last_j[8:16, :].astype(f32)
        total = tail[...]
        for k in range(taps - 1):
            d = taps - 1 - k
            ok = jnp.where(joined_ok(places, d, starts), 1.0, 0.0).astype(f32)
            inside = jnp.where(iota((8, width), 0) >= 8 - d, fix[d : d + 8, :], 0.0)
            term = inside * jnp.concatenate([ok] * (width // 128), axis=1)
            total = total + term * cw[k : k + 1, :]
            rim_w_o[k : k + 1, :] = jnp.sum(term * wide, axis=0, keepdims=True)
        rim_w_o[taps - 1 : 8, :] = jnp.zeros((9 - taps, width), f32)
        fix[0:8, :] = jnp.zeros((8, width), f32)
        fix[8:16, :] = total.astype(bf16).astype(f32) - tail[...].astype(bf16).astype(f32)
        rim_o[...] = fix[...].astype(bf16)

    @pl.when(step_id == 0)
    def _():
        more = nt(rim_o[...], wj[:, :width])
        finish(g_normed + jnp.concatenate([jnp.zeros((STRETCH - 16, more.shape[1]), f32), more]))

    @pl.when(step_id > 0)
    def _():
        finish(g_normed)


def finish_kernel(parts, place, part, base, sums, out):
    wide = part[...].astype(f32) * lax.rsqrt(sums[0:1, :] / INNER + epsilon)
    size = out.shape[0]
    for k in range(parts):

        @pl.when(place[0] == k)
        def _():
            add = jnp.transpose(base[:, size * k : size * (k + 1)].astype(f32))
            out[...] = (wide + add).astype(bf16)


MESH = pl.DeviceIdType.MESH


def start_together(peers):
    barrier = pltpu.get_barrier_semaphore()
    for peer in peers:
        pl.semaphore_signal(barrier, inc=1, device_id=peer, device_id_type=MESH)
    pl.semaphore_wait(barrier, len(peers))


def remote(src, dst, sent, came, peer):
    return pltpu.make_async_remote_copy(
        src_ref=src, dst_ref=dst, send_sem=sent, recv_sem=came, device_id=peer, device_id_type=MESH
    )


def turned(index, distance, size):
    return lax.rem(index + distance + size, size)


def twin_of(index):
    parity = lax.rem(index, 2)
    return parity, index + 1 - 2 * parity


def gather_kernel(n, chain, x, bc, dt, tok, out, halo, sent, came, passed, relayed, own, hop):
    f = lax.axis_index("fsdp")
    parity, twin = twin_of(lax.axis_index("ctx"))
    rows = x.shape[0]
    half = rows // 2
    here = lax.axis_index("ctx")
    following = turned(here, 1, chain)
    sides = [{"ctx": twin}] if chain == 2 else [{"ctx": following}, {"ctx": turned(here, -1, chain)}]
    start_together([{"fsdp": turned(f, d, n)} for d in range(1, n)] + sides)
    pieces = []
    at = 0
    for ref in (x, bc, dt):
        pieces.append((ref, slice(at, at + ref.shape[1])))
        at += ref.shape[1]

    def place(source, side):
        return pl.ds(pl.multiple_of(source * rows + side * half, 16), half)

    mine = pl.ds(pl.multiple_of(parity * half, 16), half)
    copies = []
    for d in range(1, n):
        for p, (ref, cols) in enumerate(pieces):
            copy = remote(
                ref.at[mine, :], out.at[place(f, parity), cols],
                sent.at[d - 1, p], came.at[d - 1, p], {"fsdp": turned(f, d, n)},
            )
            copy.start()
            copies.append(copy)
    edge = halo.shape[0]
    copy = remote(
        tok.at[pl.ds(tok.shape[0] - edge, edge), :], halo, hop.at[0], hop.at[1], {"ctx": following}
    )
    copy.start()
    locals_ = [copy]
    for p, (ref, cols) in enumerate(pieces):
        copy = pltpu.make_async_copy(
            ref, out.at[pl.ds(pl.multiple_of(f * rows, 16), rows), cols], own.at[p]
        )
        copy.start()
        locals_.append(copy)
    relays = []
    for d in range(1, n):
        source = turned(f, -d, n)
        for p, (ref, cols) in enumerate(pieces):
            copies[(d - 1) * len(pieces) + p].wait_recv()
            block = out.at[place(source, parity), cols]
            copy = remote(block, block, passed.at[d - 1, p], relayed.at[d - 1, p], {"ctx": twin})
            copy.start()
            relays.append(copy)
    for copy in copies:
        copy.wait_send()
    for copy in locals_:
        copy.wait()
    for copy in relays:
        copy.wait()


def gathered(x, bc, dt, tok):
    n = lax.axis_size("fsdp")
    pieces = (n - 1, 3)
    width = x.shape[1] + bc.shape[1] + dt.shape[1]
    return pl.pallas_call(
        functools.partial(gather_kernel, n, lax.axis_size("ctx")),
        out_shape=[
            jax.ShapeDtypeStruct((n * x.shape[0], width), bf16),
            jax.ShapeDtypeStruct((16, tok.shape[1]), bf16),
        ],
        in_specs=[pl.BlockSpec(memory_space=pltpu.VMEM)] * 3 + [pl.BlockSpec(memory_space=pl.ANY)],
        out_specs=[pl.BlockSpec(memory_space=pltpu.VMEM)] * 2,
        scratch_shapes=[pltpu.SemaphoreType.DMA(pieces)] * 4
        + [pltpu.SemaphoreType.DMA((3,)), pltpu.SemaphoreType.DMA((2,))],
        compiler_params=pltpu.CompilerParams(collective_id=1, has_side_effects=True),
    )(x, bc, dt, tok)


def total_kernel(n, part, out, slots, sent, came):
    me = lax.axis_index("tp")
    start_together([{"tp": turned(me, d, n)} for d in range(1, n)])
    copies = []
    for d in range(1, n):
        copy = remote(
            part, slots.at[d - 1], sent.at[d - 1], came.at[d - 1], {"tp": turned(me, d, n)}
        )
        copy.start()
        copies.append(copy)
    total = part[...]
    for d in range(1, n):
        copies[d - 1].wait_recv()
        total = total + slots[d - 1]
    out[...] = total
    for copy in copies:
        copy.wait_send()


def total_over_tp(part):
    n = lax.axis_size("tp")
    return pl.pallas_call(
        functools.partial(total_kernel, n),
        out_shape=jax.ShapeDtypeStruct(part.shape, f32),
        in_specs=[pl.BlockSpec(memory_space=pltpu.VMEM)],
        out_specs=pl.BlockSpec(memory_space=pltpu.VMEM),
        scratch_shapes=[
            pltpu.VMEM((n - 1,) + part.shape, f32),
            pltpu.SemaphoreType.DMA((n - 1,)),
            pltpu.SemaphoreType.DMA((n - 1,)),
        ],
        compiler_params=pltpu.CompilerParams(collective_id=2, has_side_effects=True),
    )(part)


def reduce_kernel(
    n, m, bc_cols, conv_bc,
    p_out, p_z, p_cat, m_scan, m_rim, m_gate, m_dt, m_gain,
    o_out, o_z, o_cat, o_small, o_wide,
    give, take, mid, slots, final, bc_slots, small, small_slots, wide_slots,
    s1, r1, s2, r2, s3, r3, s4, r4,
):
    f = lax.axis_index("fsdp")
    t = lax.axis_index("tp")
    parity, twin = twin_of(lax.axis_index("ctx"))
    start_together(
        [{"ctx": twin}]
        + [{"fsdp": turned(f, d, n)} for d in range(1, n)]
        + [{"tp": turned(t, d, m)} for d in range(1, m)]
    )
    inner = p_out.shape[1]
    rows = p_out.shape[0] // n
    half = rows // 2

    def piece(q, side):
        at = pl.ds(pl.multiple_of(q * rows + side * half, 16), half)
        return jnp.concatenate([p_out[at, :], p_z[at, :], p_cat[at, :]], axis=1)

    copies = []
    for q in range(n):
        give[q] = piece(q, 1 - parity).astype(bf16)
        copy = remote(give.at[q], take.at[q], s1.at[q], r1.at[q], {"ctx": twin})
        copy.start()
        copies.append(copy)
    w_scan = m_scan.shape[1]
    w_gate = m_gate.shape[1]
    w_dt = m_dt.shape[1]
    small[...] = jnp.zeros_like(small)
    small[:, 0:w_scan] = m_scan[...] + m_rim[...]
    at = w_scan
    small[:, at : at + w_gate] = m_gate[...]
    at += w_gate
    small[:, at : at + w_dt] = m_dt[0:8, :]
    small[:, at + w_dt : at + 2 * w_dt] = m_dt[8:16, :]
    at += 2 * w_dt
    small[0:1, at:] = m_gain[...]
    small_slots[0, pl.ds(parity, 1)] = small[...][None]
    copy = remote(
        small, small_slots.at[0, parity], s1.at[n], r1.at[n], {"ctx": twin}
    )
    copy.start()
    copies.append(copy)

    copies[n].wait()
    small_slots[1, pl.ds(f, 1)] = (small_slots[0, 0] + small_slots[0, 1])[None]
    seconds = []
    for d in range(1, n):
        copy = remote(
            small_slots.at[1, f], small_slots.at[1, f], s2.at[n - 1 + d - 1], r2.at[n - 1 + d - 1],
            {"fsdp": turned(f, d, n)},
        )
        copy.start()
        seconds.append(copy)
    for q in range(n):
        copies[q].wait()
        mid[q] = (piece(q, parity) + take[q].astype(f32)).astype(bf16)
    slots[pl.ds(f, 1)] = mid[pl.ds(f, 1)]
    for d in range(1, n):
        peer = turned(f, d, n)
        copy = remote(
            mid.at[peer], slots.at[f], s2.at[d - 1], r2.at[d - 1], {"fsdp": peer}
        )
        copy.start()
        seconds.append(copy)
    for copy in seconds:
        copy.wait()
    small_sum = small_slots[1, 0]
    whole = slots[0].astype(f32)
    for q in range(1, n):
        small_sum = small_sum + small_slots[1, q]
        whole = whole + slots[q].astype(f32)
    final[...] = whole
    bc_at = slice(3 * inner, 3 * inner + bc_cols)
    bc_slots[pl.ds(t, 1)] = whole[:, bc_at].astype(bf16)[None]
    wide = jnp.concatenate([small_sum[:, conv_bc:w_scan], small_sum[:, at:]], axis=1)
    wide_slots[pl.ds(t, 1)] = wide[None]
    o_small[...] = small_sum[:, :at]
    thirds_ = []
    for d in range(1, m):
        peer = {"tp": turned(t, d, m)}
        for p, buf in enumerate((bc_slots, wide_slots)):
            copy = remote(buf.at[t], buf.at[t], s3.at[2 * (d - 1) + p], r3.at[2 * (d - 1) + p], peer)
            copy.start()
            thirds_.append(copy)
    for copy in thirds_:
        copy.wait()
    bc_sum = bc_slots[0].astype(f32)
    wide_sum = wide_slots[0]
    for q in range(1, m):
        bc_sum = bc_sum + bc_slots[q].astype(f32)
        wide_sum = wide_sum + wide_slots[q]
    o_wide[...] = wide_sum
    final[:, bc_at] = bc_sum
    here = pl.ds(pl.multiple_of(parity * half, 8), half)
    o_out[here, :] = final[:, :inner]
    o_z[here, :] = final[:, inner : 2 * inner]
    o_cat[here, :] = final[:, 2 * inner :]
    lasts = []
    for p, (out, cols) in enumerate(
        ((o_out, slice(0, inner)), (o_z, slice(inner, 2 * inner)), (o_cat, slice(2 * inner, None)))
    ):
        copy = remote(
            final.at[:, cols] if cols.stop else final.at[:, 2 * inner : final.shape[1]],
            out.at[here, :], s4.at[p], r4.at[p], {"ctx": twin},
        )
        copy.start()
        lasts.append(copy)
    for copy in lasts:
        copy.wait()


def reduced(parts, miscs, bc_cols):
    n, m = lax.axis_size("fsdp"), lax.axis_size("tp")
    p_out, _p_z, p_cat = parts
    rows = p_out.shape[0] // n
    half = rows // 2
    inner = p_out.shape[1]
    wide = 2 * inner + p_cat.shape[1]
    m_scan, _m_rim, m_gate, m_dt, m_gain = miscs
    kept = m_scan.shape[1] + m_gate.shape[1] + 2 * m_dt.shape[1]
    small = kept + m_gain.shape[1]
    crossing = m_scan.shape[1] - inner + m_gain.shape[1]
    dma = pltpu.SemaphoreType.DMA

    def shape(*dims):
        return jax.ShapeDtypeStruct(dims, f32)

    return pl.pallas_call(
        functools.partial(reduce_kernel, n, m, bc_cols, inner),
        out_shape=[
            shape(rows, inner), shape(rows, inner), shape(rows, p_cat.shape[1]),
            shape(8, kept), shape(8, crossing),
        ],
        in_specs=[pl.BlockSpec(memory_space=pltpu.VMEM)] * 8,
        out_specs=[pl.BlockSpec(memory_space=pltpu.VMEM)] * 5,
        scratch_shapes=[
            pltpu.VMEM((n, half, wide), bf16),
            pltpu.VMEM((n, half, wide), bf16),
            pltpu.VMEM((n, half, wide), bf16),
            pltpu.VMEM((n, half, wide), bf16),
            pltpu.VMEM((half, wide), f32),
            pltpu.VMEM((m, half, bc_cols), bf16),
            pltpu.VMEM((8, small), f32),
            pltpu.VMEM((2, max(n, 2), 8, small), f32),
            pltpu.VMEM((m, 8, crossing), f32),
            dma((n + 1,)), dma((n + 1,)), dma((2 * n - 2,)), dma((2 * n - 2,)),
            dma((2 * m - 2,)), dma((2 * m - 2,)), dma((3,)), dma((3,)),
        ],
        compiler_params=pltpu.CompilerParams(
            collective_id=3, has_side_effects=True, vmem_limit_bytes=48 * 1024 * 1024
        ),
    )(*parts, *miscs)


def constants(inner, heads):
    lane_head = np.arange(inner) // (inner // heads)
    e8 = (np.arange(HEAD_ROWS)[:, None] == lane_head[None, :]).astype(np.float32)

    def spread(kind):
        m = np.zeros((128, inner), np.float32)
        m[HEAD_ROWS * kind : HEAD_ROWS * (kind + 1)] = e8
        return jnp.asarray(np.concatenate([m, m], axis=0), bf16)

    def gather(kind):
        m = np.zeros((inner, 128), np.float32)
        m[:, HEAD_ROWS * kind : HEAD_ROWS * (kind + 1)] = e8.T
        return jnp.asarray(np.concatenate([m, m], axis=0), bf16)

    at = np.arange(STRETCH)
    upper = jnp.asarray((at[:, None] <= at[None, :]).astype(np.float32), bf16)
    lower = jnp.asarray((at[:, None] >= at[None, :]).astype(np.float32), bf16)
    return jnp.asarray(e8), spread, gather, upper, lower


def passed_along(block, axis, distance):
    devices = range(lax.axis_size(axis))
    route = [(i - distance, i) for i in devices if i - distance in devices]
    return lax.ppermute(block, axis, route)


def entering(decay, state, axis, reverse):
    size = lax.axis_size(axis)
    if size == 2:
        return passed_along(state, axis, -1 if reverse else 1)
    index = lax.axis_index(axis)
    decays = lax.all_gather(decay.astype(bf16), axis)
    states = lax.all_gather(state, axis)

    def lap(k, before):
        at = size - 1 - k if reverse else k
        reached = at > index if reverse else at < index
        new = decays[at].astype(f32) * before + states[at].astype(f32)
        return jnp.where(reached, new, before)

    return lax.fori_loop(0, size, lap, jnp.zeros(state.shape, f32)).astype(bf16)


def call(kernel, blocks, ins, outs, scratch, kept=()):
    def spec(shape, how):
        if how == "smem":
            return pl.BlockSpec(memory_space=pltpu.SMEM)
        return pl.BlockSpec(shape, how)

    def body(*refs):
        kernel(*refs[: len(ins)], *refs[len(ins) + len(kept) :])

    return pl.pallas_call(
        body,
        grid=(blocks,),
        in_specs=[spec(shape, how) for _a, shape, how in ins]
        + [pl.BlockSpec(memory_space=pl.ANY)] * len(kept),
        out_specs=[spec(shape, how) for _s, shape, how in outs],
        out_shape=[s for s, _sh, _h in outs],
        scratch_shapes=scratch,
        input_output_aliases={len(ins) + k: k for k in range(len(kept))},
        compiler_params=pltpu.CompilerParams(
            dimension_semantics=("arbitrary",), vmem_limit_bytes=56 * 1024 * 1024
        ),
    )(*[a for a, _s, _h in ins], *kept)


def local(
    tokens, grad_out, lengths, norm_gain, w_z, w_x, w_bc, w_dt, conv_x_w, conv_x_b,
    conv_bc_w, conv_bc_b, dt_bias, a_log, d_skip, gate_gain, w_out,
):
    rows, model = tokens.shape
    inner = w_z.shape[1]
    heads = dt_bias.shape[0]
    states = w_bc.shape[1] // 2
    taps = conv_x_w.shape[0]
    blocks = rows // STRETCH
    width = inner + 2 * states
    tp_size = lax.axis_size("tp")
    slice_width = model // tp_size
    tp_index = lax.axis_index("tp")
    ctx_index = lax.axis_index("ctx")
    e8, spread, gather, upper, lower = constants(inner, heads)

    w_joined, halo = gathered(w_x, w_bc, jnp.pad(w_dt, ((0, 0), (0, 128 - heads))), tokens)
    second = jnp.concatenate([w_z, w_out.T], axis=1)
    second, w_joined = lax.optimization_barrier((second, w_joined))
    wz_out = lax.all_gather(second, "fsdp", axis=0, tiled=True)
    per_head = inner // heads

    def line(*vectors):
        joint = jnp.concatenate(vectors) if len(vectors) > 1 else vectors[0]
        return jnp.pad(joint, (0, model - joint.shape[0]))[None, :]

    per_heads = jnp.stack([dt_bias, a_log, d_skip], axis=1)
    params = jnp.concatenate(
        [
            line(norm_gain), line(conv_x_b, conv_bc_b), line(gate_gain), jnp.zeros((1, model), f32),
            jnp.pad(conv_x_w, ((0, 0), (0, model - inner)))
            + jnp.pad(conv_bc_w, ((0, 0), (inner, model - width))),
            jnp.pad(per_heads, ((0, HEAD_ROWS - heads), (0, model - 3))),
        ],
        axis=0,
    )

    def shape(dims, kind):
        return jax.ShapeDtypeStruct(dims, kind)

    def whole(x):
        return (x, x.shape, lambda i: (0,) * x.ndim)

    def by_rows(x, flip=False):
        if flip:
            return (x, (STRETCH, x.shape[1]), lambda i: (blocks - 1 - i, 0))
        return (x, (STRETCH, x.shape[1]), lambda i: (i, 0))

    def by_lanes(x, flip=False):
        if flip:
            return (x, (x.shape[0], STRETCH), lambda i: (0, blocks - 1 - i))
        return (x, (x.shape[0], STRETCH), lambda i: (0, i))

    def by_block(x, flip=False):
        if flip:
            return (x, (1,) + x.shape[1:], lambda i: (blocks - 1 - i, 0, 0))
        return (x, (1,) + x.shape[1:], lambda i: (i, 0, 0))

    def fixed(x):
        return (x, x.shape, lambda i: (0,) * len(x.shape))

    info_in = (lengths, None, "smem")
    state_dims = (blocks, states, inner)
    normed, joined_x, joined_bc, vbc, slope_x, slope_bc, pre, step, cum, s_part, end_state, decay = call(
        functools.partial(entry_kernel, rows),
        blocks,
        [
            info_in, by_rows(tokens), whole(halo), whole(params), whole(w_joined), whole(upper),
            whole(spread(0)), whole(e8),
        ],
        [
            by_rows(shape((rows, model), bf16)),
            by_rows(shape((rows, inner), bf16)),
            by_rows(shape((rows, 2 * states), bf16)),
            by_rows(shape((rows, width), bf16)),
            by_rows(shape((rows, inner), bf16)),
            by_rows(shape((rows, 2 * states), f32)),
            by_lanes(shape((HEAD_ROWS, rows), f32)),
            by_lanes(shape((HEAD_ROWS, rows), f32)),
            by_lanes(shape((HEAD_ROWS, rows), f32)),
            by_block(shape(state_dims, f32)),
            fixed(shape((states, inner), bf16)),
            fixed(shape((1, inner), f32)),
        ],
        [
            pltpu.VMEM((STRETCH + 8, width), f32),
            pltpu.VMEM((states, inner), f32),
            pltpu.VMEM((1, inner), f32),
        ],
    )
    incoming = entering(decay, end_state, "ctx", False)
    z_part, out, gn, sums, state_in, branch = call(
        functools.partial(mix_kernel, rows),
        blocks,
        [
            info_in, by_rows(vbc), by_lanes(step), by_lanes(cum), by_block(s_part),
            whole(incoming), by_rows(normed), by_rows(grad_out), whole(wz_out), whole(params),
            whole(spread(1)), whole(spread(2)), whole(e8),
        ],
        [
            by_rows(shape((rows, inner), f32)),
            by_rows(shape((rows, inner), f32)),
            by_rows(shape((rows, inner), f32)),
            by_lanes(shape((2, rows), f32)),
            by_block(shape(state_dims, bf16)),
            by_lanes(shape((model, rows), bf16)),
        ],
        [pltpu.VMEM((states, inner), f32), pltpu.VMEM((STRETCH, STRETCH), f32)],
    )
    branch = lax.psum_scatter(branch, "tp", scatter_dimension=0, tiled=True)
    sums = total_over_tp(sums)
    g_z, g_b, g_c, normed_two, a_sum, gs_part, start_state, misc_gate = call(
        functools.partial(gate_kernel, rows),
        blocks,
        [
            info_in, by_lanes(sums, True), by_lanes(cum, True), by_rows(out, True),
            by_rows(z_part, True), by_rows(gn, True), by_rows(vbc, True), by_block(state_in, True),
            whole(params), whole(spread(2)), whole(e8), whole(gather(0)),
        ],
        [
            by_rows(shape((rows, inner), bf16), True),
            by_rows(shape((rows, inner), bf16), True),
            by_rows(shape((rows, inner), bf16), True),
            by_rows(shape((rows, inner), bf16), True),
            by_lanes(shape((HEAD_ROWS, rows), f32), True),
            by_block(shape(state_dims, f32), True),
            fixed(shape((states, inner), bf16)),
            fixed(shape((8, inner), f32)),
        ],
        [pltpu.VMEM((states, inner), f32)],
    )
    outgoing = entering(decay, start_state, "ctx", True)
    g_cat, tail, head, misc_scan, misc_dt = call(
        functools.partial(scan_kernel, rows),
        blocks,
        [
            info_in, by_rows(vbc, True), by_rows(g_b, True), by_rows(g_c, True),
            by_lanes(step, True), by_lanes(cum, True), by_lanes(pre, True), by_lanes(a_sum, True),
            by_block(state_in, True), by_block(gs_part, True), whole(outgoing),
            by_rows(slope_x, True), by_rows(slope_bc, True), by_rows(joined_x, True),
            by_rows(joined_bc, True), whole(params), whole(spread(1)),
            whole(spread(2)), whole(e8), whole(gather(0)), whole(gather(1)),
            whole(gather(2)), whole(lower),
        ],
        [
            by_rows(shape((rows, width + 128), bf16), True),
            fixed(shape((8, width), f32)),
            fixed(shape((8, width), f32)),
            fixed(shape((8, width), f32)),
            fixed(shape((2 * HEAD_ROWS, STRETCH), f32)),
        ],
        [
            pltpu.VMEM((states, inner), f32),
            pltpu.VMEM((STRETCH + 8, width), f32),
            pltpu.VMEM((STRETCH, STRETCH), f32),
            pltpu.VMEM((STRETCH, STRETCH), f32),
        ],
    )
    next_rows = passed_along(head, "ctx", -1)
    feature = jnp.arange(model, dtype=jnp.int32) // slice_width
    mine = (feature == tp_index).astype(f32)[None, :]
    last_joined = jnp.concatenate([joined_x[rows - 16 :], joined_bc[rows - 16 :]], axis=1)
    def exit_call(first, extra_in, extra_out, scratch):
        top = count = blocks

        def flipped(x):
            return (x, (STRETCH, x.shape[1]), lambda i: (top - 1 - i, 0))

        return call(
            functools.partial(exit_kernel, rows, top, first),
            count,
            [
                info_in, flipped(tokens), flipped(grad_out), whole(mine), flipped(g_z),
                flipped(g_cat), whole(params), whole(wz_out), whole(w_joined),
            ]
            + extra_in,
            [
                (
                    shape((model, count * STRETCH), bf16),
                    (model, STRETCH),
                    lambda i: (0, count - 1 - i),
                ),
                fixed(shape((1, model), f32)),
            ]
            + extra_out,
            scratch,
        )

    g_resid, gain_part, rim, rim_w = exit_call(
        True,
        [whole(tail), whole(next_rows), whole(last_joined)],
        [fixed(shape((16, width), bf16)), fixed(shape((8, width), f32))],
        [pltpu.VMEM((16, width), f32)],
    )
    g_resid = lax.psum_scatter(g_resid, "tp", scatter_dimension=0, tiled=True)

    part_out = tn(grad_out, normed_two)
    part_z = tn(normed, g_z)
    part_cat = tn(normed, g_cat)
    part_rim = tn(normed[rows - 16 :], rim)
    part_cat = part_cat + jnp.pad(part_rim, ((0, 0), (0, 128)))
    s_out, s_z, s_cat, s_small, s_wide = reduced(
        (part_out, part_z, part_cat),
        (misc_scan, rim_w, misc_gate, misc_dt, gain_part),
        2 * states,
    )
    if lax.axis_size("ctx") > 2:
        s_out, s_z, s_cat, s_small, s_wide = jax.tree.map(
            lambda part: lax.psum(0.5 * part, "ctx"), (s_out, s_z, s_cat, s_small, s_wide)
        )
    grad_w_out = s_out.T
    grad_w_z = s_z
    grad_w_x = s_cat[:, :inner]
    grad_w_bc = s_cat[:, inner : inner + 2 * states]
    grad_w_dt = s_cat[:, inner + 2 * states : inner + 2 * states + heads]
    grad_conv_x_w = s_small[:taps, :inner]
    grad_conv_x_b = s_small[taps, :inner]
    grad_gate_gain = s_small[0, width : width + inner]
    grad_d_skip = jnp.sum(s_small[1, width : width + inner].reshape(heads, per_head), axis=1)
    dt_at = width + inner
    grad_a_log = jnp.sum(s_small[:heads, dt_at : dt_at + STRETCH], axis=1)
    grad_dt_bias = jnp.sum(s_small[:heads, dt_at + STRETCH : dt_at + 2 * STRETCH], axis=1)
    grad_conv_bc_w = s_wide[:taps, : 2 * states]
    grad_conv_bc_b = s_wide[taps, : 2 * states]
    here = tp_index * slice_width
    grad_norm_gain = lax.dynamic_slice_in_dim(s_wide[0, 2 * states :], here, slice_width, 0)
    place = tp_index.astype(jnp.int32)[None]

    wide = 2 * STRETCH
    layer_out = call(
        functools.partial(finish_kernel, tp_size),
        blocks // 2,
        [
            (place, None, "smem"),
            (branch, (slice_width, wide), lambda i: (0, i)),
            (tokens, (wide, model), lambda i: (i, 0)),
            (sums, (2, wide), lambda i: (0, i)),
        ],
        [(shape((slice_width, rows), bf16), (slice_width, wide), lambda i: (0, i))],
        [],
    )[0].T
    grad_tokens = g_resid.T
    return (
        layer_out, grad_tokens, grad_norm_gain, grad_w_z, grad_w_x, grad_w_bc, grad_w_dt,
        grad_conv_x_w, grad_conv_x_b, grad_conv_bc_w, grad_conv_bc_b, grad_dt_bias, grad_a_log,
        grad_d_skip, grad_gate_gain, grad_w_out,
    )


def solution(mesh):
    both = ("fsdp", "ctx")
    in_specs = (
        P(both, None), P(both, None), P("fsdp", None), P(), P("fsdp", "tp"), P("fsdp", "tp"),
        P("fsdp", None), P("fsdp", "tp"), P(None, "tp"), P("tp"), P(), P(), P("tp"), P("tp"),
        P("tp"), P("tp"), P("tp", "fsdp"),
    )
    out_specs = (
        P(both, "tp"), P(both, "tp"), P("tp"), P("fsdp", "tp"), P("fsdp", "tp"), P("fsdp", None),
        P("fsdp", "tp"), P(None, "tp"), P("tp"), P(), P(), P("tp"), P("tp"), P("tp"), P("tp"),
        P("tp", "fsdp"),
    )
    return jax.shard_map(local, mesh=mesh, in_specs=in_specs, out_specs=out_specs, check_vma=False)
```

```python
import functools

import jax
import jax.numpy as jnp
import numpy as np
from jax import lax
from jax.experimental import pallas as pl
from jax.experimental.pallas import tpu as pltpu
from jax.sharding import PartitionSpec as P

STRETCH = 256
TAPS = 4
INNER = 1536
HEAD_ROWS = 8
LOG2E = 1.4426950408889634

epsilon = 1e-05
f32 = jnp.float32
bf16 = jnp.bfloat16


def nn(left, right):
    return lax.dot_general(left, right, (((1,), (0,)), ((), ())), preferred_element_type=f32)


def nt(left, right):
    return lax.dot_general(left, right, (((1,), (1,)), ((), ())), preferred_element_type=f32)


def tn(left, right):
    return lax.dot_general(left, right, (((0,), (0,)), ((), ())), preferred_element_type=f32)


def halves(x):
    high = x.astype(bf16)
    return high, (x - high.astype(f32)).astype(bf16)


def thirds(x):
    high = x.astype(bf16)
    rest = x - high.astype(f32)
    mid = rest.astype(bf16)
    return high, mid, (rest - mid.astype(f32)).astype(bf16)


def exact_rows(x, ones_matrix):
    high, mid, low = thirds(x)
    r = HEAD_ROWS
    out = nn(jnp.concatenate([high, mid, low, jnp.zeros_like(low)], axis=0), ones_matrix)
    return out[:r] + out[r : 2 * r] + out[2 * r : 3 * r]


def columns_of(rows):
    have = sum(r.shape[0] for r in rows)
    pad = jnp.zeros((128 - have, rows[0].shape[1]), f32)
    cols = jnp.transpose(jnp.concatenate(list(rows) + [pad], axis=0))
    high, low = halves(cols)
    return cols, jnp.concatenate([high, low], axis=1)


def segment_start(pos, starts):
    found = jnp.zeros_like(pos)
    for s in starts:
        found = jnp.where(pos >= s, s, found)
    return found


def joined_ok(u, distance, starts):
    ok = jnp.ones(u.shape, jnp.bool_)
    for s in starts[1:]:
        ok = ok & jnp.logical_not((u < s) & (u + distance >= s))
    return ok


def iota(shape, axis):
    return lax.broadcasted_iota(jnp.int32, shape, axis)


def read_info(rows, lengths, block):
    first = lax.axis_index("ctx") * rows
    starts = [jnp.int32(0)]
    for k in range(lengths.shape[1] - 1):
        starts.append(starts[-1] + lengths[0, k])
    base = first + block * STRETCH
    end_start = segment_start(base + STRETCH - 1, starts)
    flag = jnp.where(end_start < base, 1.0, 0.0).astype(f32)
    return starts, base, end_start, flag


def norm_rows(tok):
    x = tok.astype(f32)
    inverse = lax.rsqrt(jnp.mean(x * x, axis=1, keepdims=True) + epsilon)
    return x * inverse, inverse


def lanes_of(column, e8):
    return jnp.sum(column * e8, axis=0, keepdims=True)


def entry_kernel(
    rows, info, tok, halo, par, wj, tri, ew, e8,
    nrm_o, jx_o, jb_o, vbc_o, sx_o, sb_o, pre_o, step_o, cum_o, s_o, end_o, dec_o,
    ext, run, dec,
):
    i = pl.program_id(0)
    starts, base, end_start, flag = read_info(rows, info, i)
    inner = jx_o.shape[1]
    width = inner + jb_o.shape[1]
    gain, cb, cw, taps = par[0:1, :], par[1:2, :], par[4:8, :], TAPS

    @pl.when(i == 0)
    def _():
        unit, _inv = norm_rows(halo[...])
        before = nn((unit * gain).astype(bf16), wj[:, :width])
        ext[0:8, :] = before.astype(bf16).astype(f32)[8:16]
        run[...] = jnp.zeros_like(run)
        dec[...] = jnp.ones_like(dec)

    unit, _inv = norm_rows(tok[...])
    normed = (unit * gain).astype(bf16)
    nrm_o[...] = normed
    product = nn(normed, wj[...])
    joined = product[:, :width].astype(bf16)
    jx_o[...] = joined[:, :inner]
    jb_o[...] = joined[:, inner:]
    ext[8 : 8 + STRETCH, :] = joined.astype(f32)
    pos = base + iota((STRETCH, 128), 0)
    first_of = segment_start(pos, starts)
    valid = [
        jnp.where(pos - (taps - 1 - k) >= first_of, 1.0, 0.0).astype(f32) for k in range(taps - 1)
    ]
    for g in range(width // 128):
        at = slice(128 * g, 128 * (g + 1))
        acc = cb[:, at] + cw[taps - 1 : taps, at] * ext[8 : 8 + STRETCH, at]
        for k in range(taps - 1):
            low = 8 - (taps - 1) + k
            acc = acc + cw[k : k + 1, at] * (ext[low : low + STRETCH, at] * valid[k])
        sig = jax.nn.sigmoid(acc)
        act = acc * sig
        vbc_o[:, at] = act.astype(bf16)
        slope = sig + act * (1.0 - sig)
        if 128 * g < inner:
            sx_o[:, at] = slope.astype(bf16)
        else:
            sb_o[:, 128 * g - inner : 128 * (g + 1) - inner] = slope
    ext[0:8, :] = ext[STRETCH : STRETCH + 8, :]
    pre = jnp.transpose(product[:, width:])[:HEAD_ROWS] + par[8:16, 0:1]
    step = jax.nn.softplus(pre)
    logd = -step * jnp.exp(par[8:16, 1:2])
    cum = exact_rows(logd, tri[...])
    pre_o[...] = pre
    step_o[...] = step
    cum_o[...] = cum
    cum_e = cum[:, STRETCH - 1 : STRETCH]
    where_s = base + iota((1, STRETCH), 1)
    keep = jnp.where(where_s >= end_start, 1.0, 0.0).astype(f32)
    weight = jnp.exp(cum_e - cum) * step * keep
    _cols, both = columns_of([weight])
    spread = nn(both, ew[...])
    v = vbc_o[:, :inner].astype(f32)
    b = vbc_o[:, inner : inner + 128]
    state = tn(b, (v * spread).astype(bf16))
    s_o[0] = state
    through = lanes_of(jnp.exp(cum_e) * flag, e8[...])
    run[...] = through * run[...] + state
    dec[...] = dec[...] * through
    end_o[...] = run[...].astype(bf16)
    dec_o[...] = dec[...]


def mix_kernel(
    rows, info, vbc, step, cum, s_in, inc, normed, gout, wz_out, par, e_step, e_scale, e8,
    z_o, out_o, gn_o, sum_o, st_o, br_o,
    run, gram,
):
    i = pl.program_id(0)
    starts, base, _end_start, flag = read_info(rows, info, i)
    inner = out_o.shape[1]
    gain = par[2:3, :inner]
    dskip = lanes_of(par[8:16, 2:3], e8[...])

    @pl.when(i == 0)
    def _():
        run[...] = inc[...].astype(f32)

    st = run[...].astype(bf16)
    st_o[0] = st
    cum_v = cum[...]
    cum_e = cum_v[:, STRETCH - 1 : STRETCH]
    through = lanes_of(jnp.exp(cum_e) * flag, e8[...])
    run[...] = through * run[...] + s_in[0]

    row_first = segment_start(base + iota((1, STRETCH), 1), starts)
    scale = jnp.exp(cum_v) * jnp.where(row_first < base, 1.0, 0.0).astype(f32)
    cum2 = cum_v * LOG2E
    cols, both = columns_of([cum2, step[...], scale])
    step_x = nn(both, e_step[...])
    scale_x = nn(both, e_scale[...])
    b = vbc[:, inner : inner + 128]
    c = vbc[:, inner + 128 : inner + 256]
    carried = nn(c, st) * scale_x
    half = STRETCH // 2
    low, high = slice(0, half), slice(half, STRETCH)
    t_at = iota((half, STRETCH), 0)
    s_at = iota((half, STRETCH), 1)
    causal = (s_at <= t_at)[:, low]
    first_low = segment_start(iota((half, half), 0) + base, starts)
    first_high = segment_start(t_at + (base + half), starts)
    mask_a = causal & ((s_at + base)[:, low] >= first_low)
    mask_b = (s_at <= t_at + half) & (s_at + base >= first_high)
    gram[low, low] = jnp.where(mask_a, nt(c[low], b[low]), 0.0)
    gram[high, :] = jnp.where(mask_b, nt(c[high], b), 0.0)
    lane = iota((STRETCH, 128), 1)
    pieces = []
    for p in range(inner // 128):
        at = slice(128 * p, 128 * (p + 1))
        v = vbc[:, at].astype(f32)
        sv = (v * step_x[:, at]).astype(bf16)
        rest = carried[:, at] + dskip[:, at] * v
        acc_low, acc_high = rest[low], rest[high]
        for j in range(2):
            h = 2 * p + j
            side = (lane < 64) if j == 0 else (lane >= 64)
            part = jnp.where(side, sv, jnp.zeros_like(sv))
            row = cum2[h : h + 1, :]
            first_gap = cols[low, h : h + 1] - row[:, low]
            cross_gap = cols[high, h : h + 1] - row[:, low]
            last_gap = cols[high, h : h + 1] - row[:, high]
            decay_b = jnp.concatenate(
                [jnp.exp2(cross_gap), jnp.exp2(jnp.minimum(last_gap, 0.0))], axis=1
            )
            decay_a = jnp.exp2(jnp.minimum(first_gap, 0.0))
            acc_low = acc_low + nn((gram[low, low] * decay_a).astype(bf16), part[low])
            acc_high = acc_high + nn((gram[high, :] * decay_b).astype(bf16), part)
        pieces.append(jnp.concatenate([acc_low, acc_high], axis=0))
    out = jnp.concatenate(pieces, axis=1)
    out_o[...] = out
    zf = nn(normed[...], wz_out[:, :inner])
    z_o[...] = zf
    gated = out * (zf * jax.nn.sigmoid(zf))
    gn = nn(gout[...], wz_out[:, inner:])
    gn_o[...] = gn
    gg = gated * gain
    br_o[...] = nt(wz_out[:, inner:], gg.astype(bf16)).astype(bf16)
    ss = jnp.sum(gated * gated, axis=1, keepdims=True)
    dq = jnp.sum(gn * gg, axis=1, keepdims=True)
    sum_o[...] = jnp.transpose(jnp.where(lane == 0, ss, dq))[0:2]


def gate_kernel(
    rows, info, sums, cum, out, z, gn, vc, st, par, e_scale, e8, f_sum,
    gz_o, gb_o, gc_o, n2_o, a_o, gs_o, start_o, misc_o,
    run,
):
    step_id = pl.program_id(0)
    blocks = pl.num_programs(0)
    i = blocks - 1 - step_id
    starts, base, _end_start, flag = read_info(rows, info, i)
    inner = z.shape[1]
    gain = par[2:3, :inner]
    dskip = lanes_of(par[8:16, 2:3], e8[...])

    @pl.when(step_id == 0)
    def _():
        run[...] = jnp.zeros_like(run)
        misc_o[...] = jnp.zeros_like(misc_o)

    alpha = lax.rsqrt(sums[0:1, :] / INNER + epsilon)
    beta = alpha * alpha * alpha * sums[1:2, :] / INNER
    cum_v = cum[...]
    row_first = segment_start(base + iota((1, STRETCH), 1), starts)
    scale = jnp.exp(cum_v) * jnp.where(row_first < base, 1.0, 0.0).astype(f32)
    cols, both = columns_of([alpha, beta, jnp.zeros((14, STRETCH), f32), scale])
    alpha_c = cols[:, 0:1]
    beta_c = cols[:, 1:2]
    scale_x = nn(both, e_scale[...])
    v = vc[:, :inner].astype(f32)
    c = vc[:, inner + 128 : inner + 256]
    zf = z[...]
    sig = jax.nn.sigmoid(zf)
    act = zf * sig
    o = out[...]
    gated = o * act
    g_n = gn[...]
    unit = gated * alpha_c
    g_gated = alpha_c * (g_n * gain) - beta_c * gated
    g_out = g_gated * act
    gz_o[...] = (g_gated * o * (sig + act * (1.0 - sig))).astype(bf16)
    gb = g_out.astype(bf16)
    gb_o[...] = gb
    n2_o[...] = (unit * gain).astype(bf16)
    misc_o[0:1, :] += jnp.sum(g_n * unit, axis=0, keepdims=True)
    misc_o[1:2, :] += jnp.sum(g_out * v, axis=0, keepdims=True)
    gf = gb.astype(f32)
    carried = nn(c, st[0]) * scale_x
    prod = gf * (o - dskip * v) + (g_out - gf) * carried
    high, low = halves(prod)
    sums_c = nn(jnp.concatenate([high, low], axis=1), f_sum[...])
    a_o[...] = jnp.transpose(sums_c)[0:HEAD_ROWS]
    gc = (g_out * scale_x).astype(bf16)
    gc_o[...] = gc
    gs = tn(c, gc)
    gs_o[0] = gs
    through = lanes_of(jnp.exp(cum_v[:, STRETCH - 1 : STRETCH]) * flag, e8[...])
    run[...] = through * run[...] + gs
    start_o[...] = run[...].astype(bf16)


def scan_kernel(
    rows, info, vbc, gb, gc, step, cum, pre, a_sum, st, gs_in, outg, sx, sb, jx, jb, par,
    e_step, e_w, e8, f_all, tril,
    gcat_o, tail_o, head_o, misc_o, dt_o,
    run, ext, gram, acc, prod,
):
    step_id = pl.program_id(0)
    blocks = pl.num_programs(0)
    i = blocks - 1 - step_id
    starts, base, end_start, flag = read_info(rows, info, i)
    inner = gb.shape[1]
    width = inner + jb.shape[1]
    cw, taps = par[4:8, :], TAPS
    rate = jnp.exp(par[8:16, 1:2])
    dskip = lanes_of(par[8:16, 2:3], e8[...])

    @pl.when(step_id == 0)
    def _():
        run[...] = outg[...].astype(f32)
        ext[...] = jnp.zeros((8, width), f32)
        misc_o[...] = jnp.zeros_like(misc_o)
        dt_o[...] = jnp.zeros_like(dt_o)

    cum_v = cum[...]
    step_v = step[...]
    cum_e = cum_v[:, STRETCH - 1 : STRETCH]
    after = run[...]
    low_after = after.astype(bf16)
    state = st[0]
    through = lanes_of(jnp.exp(cum_e) * flag, e8[...])
    g_through = jnp.sum(after * state.astype(f32), axis=0, keepdims=True) * through
    end_more = jnp.sum(e8[...] * g_through, axis=1, keepdims=True)
    run[...] = through * after + gs_in[0]

    where_s = base + iota((1, STRETCH), 1)
    row_first = segment_start(where_s, starts)
    end_decay = jnp.exp(cum_e - cum_v) * jnp.where(where_s >= end_start, 1.0, 0.0).astype(f32)
    weight = end_decay * step_v
    cum2 = cum_v * LOG2E
    ok_rows = [
        jnp.where(joined_ok(where_s, d, starts), 1.0, 0.0).astype(f32)
        for d in range(taps - 1, 0, -1)
    ]
    cols, both = columns_of([cum2, step_v, weight] + ok_rows)
    b = vbc[:, inner : inner + 128]
    c = vbc[:, inner + 128 : inner + 256]
    half = STRETCH // 2
    low, high = slice(0, half), slice(half, STRETCH)
    s_at = iota((half, STRETCH), 0)
    t_at = iota((half, STRETCH), 1)
    mask_a = (s_at <= t_at) & (s_at + base >= row_first)
    mask_b = (s_at <= t_at)[:, low] & ((s_at + (base + half)) >= row_first)[:, high]
    gram[low, :] = jnp.where(mask_a, nt(b[low], c), 0.0)
    gram[high, low] = jnp.where(mask_b, nt(b[high], c[high]), 0.0)
    acc[...] = jnp.zeros_like(acc)
    lane = iota((STRETCH, 128), 1)
    ok = [
        jnp.broadcast_to(cols[:, 3 * HEAD_ROWS + k : 3 * HEAD_ROWS + k + 1], (STRETCH, 128))
        for k in range(taps - 1)
    ]

    def convolve(at, own, j_f):
        following = ext[:, at]
        joint = jnp.concatenate([own, following], axis=0)
        ext[:, at] = own[0:8]
        misc_o[taps : taps + 1, at] += jnp.sum(own, axis=0, keepdims=True)
        misc_o[taps - 1 : taps, at] += jnp.sum(own * j_f, axis=0, keepdims=True)
        total = own * cw[taps - 1 : taps, at]
        for k in range(taps - 1):
            d = taps - 1 - k
            term = pltpu.roll(joint, STRETCH + 8 - d, axis=0)[:STRETCH] * ok[k]
            misc_o[k : k + 1, at] += jnp.sum(term * j_f, axis=0, keepdims=True)
            total = total + term * cw[k : k + 1, at]
        gcat_o[:, at] = total.astype(bf16)
        tail_o[:, at] = jnp.where(step_id == 0, total[STRETCH - 8 :], tail_o[:, at])

    g_b = jnp.zeros((STRETCH, 128), f32)
    g_c = jnp.zeros((STRETCH, 128), f32)
    for p in range(inner // 128):
        at = slice(128 * p, 128 * (p + 1))
        step_x = nn(both, e_step[:, at])
        v = vbc[:, at].astype(f32)
        sv = (v * step_x).astype(bf16)
        g_pair = gb[:, at]
        u_low = jnp.zeros((half, 128), f32)
        u_high = jnp.zeros((half, 128), f32)
        for j in range(2):
            h = 2 * p + j
            side = (lane < 64) if j == 0 else (lane >= 64)
            g_side = jnp.where(side, g_pair, jnp.zeros_like(g_pair))
            sv_side = jnp.where(side, sv, jnp.zeros_like(sv))
            row = cum2[h : h + 1, :]
            first_gap = row[:, low] - cols[low, h : h + 1]
            cross_gap = row[:, high] - cols[low, h : h + 1]
            last_gap = row[:, high] - cols[high, h : h + 1]
            decay_a = jnp.concatenate(
                [jnp.exp2(jnp.minimum(first_gap, 0.0)), jnp.exp2(cross_gap)], axis=1
            )
            decay_b = jnp.exp2(jnp.minimum(last_gap, 0.0))
            u_low = u_low + nn((gram[low, :] * decay_a).astype(bf16), g_side)
            u_high = u_high + nn((gram[high, low] * decay_b).astype(bf16), g_side[high])
            acc[low, :] += nt(sv_side[low], g_pair) * decay_a
            acc[high, low] += nt(sv_side[high], g_pair[high]) * decay_b
        u = jnp.concatenate([u_low, u_high], axis=0)
        w_x = nn(both, e_w[:, at])
        y = nn(b, low_after[:, at])
        h1, l1 = halves(sv.astype(f32) * u)
        prod[:, at] = h1
        prod[:, inner + 128 * p : inner + 128 * (p + 1)] = l1
        prod[:, 2 * inner + 128 * p : 2 * inner + 128 * (p + 1)] = (v * y).astype(bf16)
        g_b = g_b + nt((v * w_x).astype(bf16), low_after[:, at])
        g_c = g_c + nt(gc[:, at], state[:, at])
        gv = dskip[:, at] * g_pair.astype(f32) + step_x * u + w_x * y
        convolve(at, gv * sx[:, at].astype(f32), jx[:, at].astype(f32))

    gg_a = jnp.where(mask_a, acc[low, :], 0.0).astype(bf16)
    gg_b = jnp.where(mask_b, acc[high, low], 0.0).astype(bf16)
    g_b = g_b + jnp.concatenate([nn(gg_a, c), nn(gg_b, c[high])], axis=0)
    g_c = g_c + tn(gg_a, b[low])
    g_c = g_c + jnp.concatenate([jnp.zeros((half, 128), f32), tn(gg_b, b[high])], axis=0)
    for k, part in enumerate((g_b, g_c)):
        here = slice(128 * k, 128 * (k + 1))
        convolve(
            slice(inner + 128 * k, inner + 128 * (k + 1)),
            part * sb[:, here],
            jb[:, here].astype(f32),
        )

    sums_r = jnp.transpose(nn(prod[...], f_all[...]))
    g_mixed = sums_r[0:HEAD_ROWS]
    g_end = sums_r[HEAD_ROWS : 2 * HEAD_ROWS]
    ends = g_end * weight
    g_cum = a_sum[...] - g_mixed - ends
    end_add = jnp.sum(ends, axis=1, keepdims=True) + end_more
    g_log = exact_rows(g_cum, tril[...]) + end_add
    slope_dt = jax.nn.sigmoid(pre[...])
    ratio = jnp.where(step_v > 0.0, slope_dt / step_v, 1.0)
    g_pre_dt = (g_end * end_decay - g_log * rate) * slope_dt + g_mixed * ratio
    dt_o[0:HEAD_ROWS, :] += g_log * (-step_v * rate)
    dt_o[HEAD_ROWS:, :] += g_pre_dt
    pad = jnp.zeros((128 - HEAD_ROWS, STRETCH), f32)
    gcat_o[:, width:] = jnp.transpose(jnp.concatenate([g_pre_dt, pad], axis=0)).astype(bf16)

    head_o[...] = ext[...]


def exit_kernel(
    rows, blocks, rim_side, info, tok, gout, mine, gz, gcat, par, wz_out, wj, *rest
):
    step_id = pl.program_id(0)
    i = blocks - 1 - step_id
    starts, base, _end_start, _flag = read_info(rows, info, i)
    inner = gz.shape[1]
    if rim_side:
        tail, nxt, last_j, gr_o, gain_o, rim_o, rim_w_o, fix = rest
        taps, width = TAPS, tail.shape[1]
        cw = par[4:8, :width]
    else:
        gr_o, gain_o = rest
    gain = par[0:1, :]

    g_normed = nt(gz[...], wz_out[:, :inner]) + nt(gcat[...], wj[...])

    def finish(g_normed):
        unit, inverse = norm_rows(tok[...])
        scaled = g_normed * gain
        mean = jnp.mean(scaled * unit, axis=1, keepdims=True)
        own = gout[...].astype(f32) * mine[...]
        gr_o[...] = jnp.transpose(own + inverse * (scaled - unit * mean)).astype(bf16)
        gain_o[...] += jnp.sum(g_normed * unit, axis=0, keepdims=True)

    @pl.when(step_id == 0)
    def _():
        gain_o[...] = jnp.zeros_like(gain_o)

    if not rim_side:
        finish(g_normed)
        return

    @pl.when(step_id == 0)
    def _():
        fix[0:8, :] = jnp.zeros((8, width), f32)
        fix[8:16, :] = nxt[...]
        places = base + STRETCH - 8 + iota((8, 128), 0)
        wide = last_j[8:16, :].astype(f32)
        total = tail[...]
        for k in range(taps - 1):
            d = taps - 1 - k
            ok = jnp.where(joined_ok(places, d, starts), 1.0, 0.0).astype(f32)
            inside = jnp.where(iota((8, width), 0) >= 8 - d, fix[d : d + 8, :], 0.0)
            term = inside * jnp.concatenate([ok] * (width // 128), axis=1)
            total = total + term * cw[k : k + 1, :]
            rim_w_o[k : k + 1, :] = jnp.sum(term * wide, axis=0, keepdims=True)
        rim_w_o[taps - 1 : 8, :] = jnp.zeros((9 - taps, width), f32)
        fix[0:8, :] = jnp.zeros((8, width), f32)
        fix[8:16, :] = total.astype(bf16).astype(f32) - tail[...].astype(bf16).astype(f32)
        rim_o[...] = fix[...].astype(bf16)

    @pl.when(step_id == 0)
    def _():
        more = nt(rim_o[...], wj[:, :width])
        finish(g_normed + jnp.concatenate([jnp.zeros((STRETCH - 16, more.shape[1]), f32), more]))

    @pl.when(step_id > 0)
    def _():
        finish(g_normed)


def finish_kernel(parts, place, part, base, sums, out):
    wide = part[...].astype(f32) * lax.rsqrt(sums[0:1, :] / INNER + epsilon)
    size = out.shape[0]
    for k in range(parts):

        @pl.when(place[0] == k)
        def _():
            add = jnp.transpose(base[:, size * k : size * (k + 1)].astype(f32))
            out[...] = (wide + add).astype(bf16)


MESH = pl.DeviceIdType.MESH


def start_together(peers):
    barrier = pltpu.get_barrier_semaphore()
    for peer in peers:
        pl.semaphore_signal(barrier, inc=1, device_id=peer, device_id_type=MESH)
    pl.semaphore_wait(barrier, len(peers))


def remote(src, dst, sent, came, peer):
    return pltpu.make_async_remote_copy(
        src_ref=src, dst_ref=dst, send_sem=sent, recv_sem=came, device_id=peer, device_id_type=MESH
    )


def turned(index, distance, size):
    return lax.rem(index + distance + size, size)


def twin_of(index):
    parity = lax.rem(index, 2)
    return parity, index + 1 - 2 * parity


def gather_kernel(n, chain, x, bc, dt, tok, out, halo, sent, came, passed, relayed, own, hop):
    f = lax.axis_index("fsdp")
    parity, twin = twin_of(lax.axis_index("ctx"))
    rows = x.shape[0]
    half = rows // 2
    here = lax.axis_index("ctx")
    following = turned(here, 1, chain)
    sides = [{"ctx": twin}] if chain == 2 else [{"ctx": following}, {"ctx": turned(here, -1, chain)}]
    start_together([{"fsdp": turned(f, d, n)} for d in range(1, n)] + sides)
    pieces = []
    at = 0
    for ref in (x, bc, dt):
        pieces.append((ref, slice(at, at + ref.shape[1])))
        at += ref.shape[1]

    def place(source, side):
        return pl.ds(pl.multiple_of(source * rows + side * half, 16), half)

    mine = pl.ds(pl.multiple_of(parity * half, 16), half)
    copies = []
    for d in range(1, n):
        for p, (ref, cols) in enumerate(pieces):
            copy = remote(
                ref.at[mine, :], out.at[place(f, parity), cols],
                sent.at[d - 1, p], came.at[d - 1, p], {"fsdp": turned(f, d, n)},
            )
            copy.start()
            copies.append(copy)
    edge = halo.shape[0]
    copy = remote(
        tok.at[pl.ds(tok.shape[0] - edge, edge), :], halo, hop.at[0], hop.at[1], {"ctx": following}
    )
    copy.start()
    locals_ = [copy]
    for p, (ref, cols) in enumerate(pieces):
        copy = pltpu.make_async_copy(
            ref, out.at[pl.ds(pl.multiple_of(f * rows, 16), rows), cols], own.at[p]
        )
        copy.start()
        locals_.append(copy)
    relays = []
    for d in range(1, n):
        source = turned(f, -d, n)
        for p, (ref, cols) in enumerate(pieces):
            copies[(d - 1) * len(pieces) + p].wait_recv()
            block = out.at[place(source, parity), cols]
            copy = remote(block, block, passed.at[d - 1, p], relayed.at[d - 1, p], {"ctx": twin})
            copy.start()
            relays.append(copy)
    for copy in copies:
        copy.wait_send()
    for copy in locals_:
        copy.wait()
    for copy in relays:
        copy.wait()


def gathered(x, bc, dt, tok):
    n = lax.axis_size("fsdp")
    pieces = (n - 1, 3)
    width = x.shape[1] + bc.shape[1] + dt.shape[1]
    return pl.pallas_call(
        functools.partial(gather_kernel, n, lax.axis_size("ctx")),
        out_shape=[
            jax.ShapeDtypeStruct((n * x.shape[0], width), bf16),
            jax.ShapeDtypeStruct((16, tok.shape[1]), bf16),
        ],
        in_specs=[pl.BlockSpec(memory_space=pltpu.VMEM)] * 3 + [pl.BlockSpec(memory_space=pl.ANY)],
        out_specs=[pl.BlockSpec(memory_space=pltpu.VMEM)] * 2,
        scratch_shapes=[pltpu.SemaphoreType.DMA(pieces)] * 4
        + [pltpu.SemaphoreType.DMA((3,)), pltpu.SemaphoreType.DMA((2,))],
        compiler_params=pltpu.CompilerParams(collective_id=1, has_side_effects=True),
    )(x, bc, dt, tok)


def total_kernel(n, part, out, slots, sent, came):
    me = lax.axis_index("tp")
    start_together([{"tp": turned(me, d, n)} for d in range(1, n)])
    copies = []
    for d in range(1, n):
        copy = remote(
            part, slots.at[d - 1], sent.at[d - 1], came.at[d - 1], {"tp": turned(me, d, n)}
        )
        copy.start()
        copies.append(copy)
    total = part[...]
    for d in range(1, n):
        copies[d - 1].wait_recv()
        total = total + slots[d - 1]
    out[...] = total
    for copy in copies:
        copy.wait_send()


def total_over_tp(part):
    n = lax.axis_size("tp")
    return pl.pallas_call(
        functools.partial(total_kernel, n),
        out_shape=jax.ShapeDtypeStruct(part.shape, f32),
        in_specs=[pl.BlockSpec(memory_space=pltpu.VMEM)],
        out_specs=pl.BlockSpec(memory_space=pltpu.VMEM),
        scratch_shapes=[
            pltpu.VMEM((n - 1,) + part.shape, f32),
            pltpu.SemaphoreType.DMA((n - 1,)),
            pltpu.SemaphoreType.DMA((n - 1,)),
        ],
        compiler_params=pltpu.CompilerParams(collective_id=2, has_side_effects=True),
    )(part)


def reduce_kernel(
    n, m, bc_cols, conv_bc,
    p_out, p_z, p_cat, m_scan, m_rim, m_gate, m_dt, m_gain,
    o_out, o_z, o_cat, o_small, o_wide,
    give, take, mid, slots, final, bc_slots, small, small_slots, wide_slots,
    s1, r1, s2, r2, s3, r3, s4, r4,
):
    f = lax.axis_index("fsdp")
    t = lax.axis_index("tp")
    parity, twin = twin_of(lax.axis_index("ctx"))
    start_together(
        [{"ctx": twin}]
        + [{"fsdp": turned(f, d, n)} for d in range(1, n)]
        + [{"tp": turned(t, d, m)} for d in range(1, m)]
    )
    inner = p_out.shape[1]
    rows = p_out.shape[0] // n
    half = rows // 2

    def piece(q, side):
        at = pl.ds(pl.multiple_of(q * rows + side * half, 16), half)
        return jnp.concatenate([p_out[at, :], p_z[at, :], p_cat[at, :]], axis=1)

    copies = []
    for q in range(n):
        give[q] = piece(q, 1 - parity).astype(bf16)
        copy = remote(give.at[q], take.at[q], s1.at[q], r1.at[q], {"ctx": twin})
        copy.start()
        copies.append(copy)
    w_scan = m_scan.shape[1]
    w_gate = m_gate.shape[1]
    w_dt = m_dt.shape[1]
    small[...] = jnp.zeros_like(small)
    small[:, 0:w_scan] = m_scan[...] + m_rim[...]
    at = w_scan
    small[:, at : at + w_gate] = m_gate[...]
    at += w_gate
    small[:, at : at + w_dt] = m_dt[0:8, :]
    small[:, at + w_dt : at + 2 * w_dt] = m_dt[8:16, :]
    at += 2 * w_dt
    small[0:1, at:] = m_gain[...]
    small_slots[0, pl.ds(parity, 1)] = small[...][None]
    copy = remote(
        small, small_slots.at[0, parity], s1.at[n], r1.at[n], {"ctx": twin}
    )
    copy.start()
    copies.append(copy)

    copies[n].wait()
    small_slots[1, pl.ds(f, 1)] = (small_slots[0, 0] + small_slots[0, 1])[None]
    seconds = []
    for d in range(1, n):
        copy = remote(
            small_slots.at[1, f], small_slots.at[1, f], s2.at[n - 1 + d - 1], r2.at[n - 1 + d - 1],
            {"fsdp": turned(f, d, n)},
        )
        copy.start()
        seconds.append(copy)
    for q in range(n):
        copies[q].wait()
        mid[q] = (piece(q, parity) + take[q].astype(f32)).astype(bf16)
    slots[pl.ds(f, 1)] = mid[pl.ds(f, 1)]
    for d in range(1, n):
        peer = turned(f, d, n)
        copy = remote(
            mid.at[peer], slots.at[f], s2.at[d - 1], r2.at[d - 1], {"fsdp": peer}
        )
        copy.start()
        seconds.append(copy)
    for copy in seconds:
        copy.wait()
    small_sum = small_slots[1, 0]
    whole = slots[0].astype(f32)
    for q in range(1, n):
        small_sum = small_sum + small_slots[1, q]
        whole = whole + slots[q].astype(f32)
    final[...] = whole
    bc_at = slice(3 * inner, 3 * inner + bc_cols)
    bc_slots[pl.ds(t, 1)] = whole[:, bc_at].astype(bf16)[None]
    wide = jnp.concatenate([small_sum[:, conv_bc:w_scan], small_sum[:, at:]], axis=1)
    wide_slots[pl.ds(t, 1)] = wide[None]
    o_small[...] = small_sum[:, :at]
    thirds_ = []
    for d in range(1, m):
        peer = {"tp": turned(t, d, m)}
        for p, buf in enumerate((bc_slots, wide_slots)):
            copy = remote(buf.at[t], buf.at[t], s3.at[2 * (d - 1) + p], r3.at[2 * (d - 1) + p], peer)
            copy.start()
            thirds_.append(copy)
    for copy in thirds_:
        copy.wait()
    bc_sum = bc_slots[0].astype(f32)
    wide_sum = wide_slots[0]
    for q in range(1, m):
        bc_sum = bc_sum + bc_slots[q].astype(f32)
        wide_sum = wide_sum + wide_slots[q]
    o_wide[...] = wide_sum
    final[:, bc_at] = bc_sum
    here = pl.ds(pl.multiple_of(parity * half, 8), half)
    o_out[here, :] = final[:, :inner]
    o_z[here, :] = final[:, inner : 2 * inner]
    o_cat[here, :] = final[:, 2 * inner :]
    lasts = []
    for p, (out, cols) in enumerate(
        ((o_out, slice(0, inner)), (o_z, slice(inner, 2 * inner)), (o_cat, slice(2 * inner, None)))
    ):
        copy = remote(
            final.at[:, cols] if cols.stop else final.at[:, 2 * inner : final.shape[1]],
            out.at[here, :], s4.at[p], r4.at[p], {"ctx": twin},
        )
        copy.start()
        lasts.append(copy)
    for copy in lasts:
        copy.wait()


def reduced(parts, miscs, bc_cols):
    n, m = lax.axis_size("fsdp"), lax.axis_size("tp")
    p_out, _p_z, p_cat = parts
    rows = p_out.shape[0] // n
    half = rows // 2
    inner = p_out.shape[1]
    wide = 2 * inner + p_cat.shape[1]
    m_scan, _m_rim, m_gate, m_dt, m_gain = miscs
    kept = m_scan.shape[1] + m_gate.shape[1] + 2 * m_dt.shape[1]
    small = kept + m_gain.shape[1]
    crossing = m_scan.shape[1] - inner + m_gain.shape[1]
    dma = pltpu.SemaphoreType.DMA

    def shape(*dims):
        return jax.ShapeDtypeStruct(dims, f32)

    return pl.pallas_call(
        functools.partial(reduce_kernel, n, m, bc_cols, inner),
        out_shape=[
            shape(rows, inner), shape(rows, inner), shape(rows, p_cat.shape[1]),
            shape(8, kept), shape(8, crossing),
        ],
        in_specs=[pl.BlockSpec(memory_space=pltpu.VMEM)] * 8,
        out_specs=[pl.BlockSpec(memory_space=pltpu.VMEM)] * 5,
        scratch_shapes=[
            pltpu.VMEM((n, half, wide), bf16),
            pltpu.VMEM((n, half, wide), bf16),
            pltpu.VMEM((n, half, wide), bf16),
            pltpu.VMEM((n, half, wide), bf16),
            pltpu.VMEM((half, wide), f32),
            pltpu.VMEM((m, half, bc_cols), bf16),
            pltpu.VMEM((8, small), f32),
            pltpu.VMEM((2, max(n, 2), 8, small), f32),
            pltpu.VMEM((m, 8, crossing), f32),
            dma((n + 1,)), dma((n + 1,)), dma((2 * n - 2,)), dma((2 * n - 2,)),
            dma((2 * m - 2,)), dma((2 * m - 2,)), dma((3,)), dma((3,)),
        ],
        compiler_params=pltpu.CompilerParams(
            collective_id=3, has_side_effects=True, vmem_limit_bytes=48 * 1024 * 1024
        ),
    )(*parts, *miscs)


def constants(inner, heads):
    lane_head = np.arange(inner) // (inner // heads)
    e8 = (np.arange(HEAD_ROWS)[:, None] == lane_head[None, :]).astype(np.float32)

    def spread(kind):
        m = np.zeros((128, inner), np.float32)
        m[HEAD_ROWS * kind : HEAD_ROWS * (kind + 1)] = e8
        return jnp.asarray(np.concatenate([m, m], axis=0), bf16)

    def gather(kind):
        m = np.zeros((inner, 128), np.float32)
        m[:, HEAD_ROWS * kind : HEAD_ROWS * (kind + 1)] = e8.T
        return jnp.asarray(np.concatenate([m, m], axis=0), bf16)

    at = np.arange(STRETCH)
    upper = jnp.asarray((at[:, None] <= at[None, :]).astype(np.float32), bf16)
    lower = jnp.asarray((at[:, None] >= at[None, :]).astype(np.float32), bf16)
    return jnp.asarray(e8), spread, gather, upper, lower


def passed_along(block, axis, distance):
    devices = range(lax.axis_size(axis))
    route = [(i - distance, i) for i in devices if i - distance in devices]
    return lax.ppermute(block, axis, route)


def entering(decay, state, axis, reverse):
    size = lax.axis_size(axis)
    if size == 2:
        return passed_along(state, axis, -1 if reverse else 1)
    index = lax.axis_index(axis)
    decays = lax.all_gather(decay.astype(bf16), axis)
    states = lax.all_gather(state, axis)

    def lap(k, before):
        at = size - 1 - k if reverse else k
        reached = at > index if reverse else at < index
        new = decays[at].astype(f32) * before + states[at].astype(f32)
        return jnp.where(reached, new, before)

    return lax.fori_loop(0, size, lap, jnp.zeros(state.shape, f32)).astype(bf16)


def call(kernel, blocks, ins, outs, scratch, kept=()):
    def spec(shape, how):
        if how == "smem":
            return pl.BlockSpec(memory_space=pltpu.SMEM)
        return pl.BlockSpec(shape, how)

    def body(*refs):
        kernel(*refs[: len(ins)], *refs[len(ins) + len(kept) :])

    return pl.pallas_call(
        body,
        grid=(blocks,),
        in_specs=[spec(shape, how) for _a, shape, how in ins]
        + [pl.BlockSpec(memory_space=pl.ANY)] * len(kept),
        out_specs=[spec(shape, how) for _s, shape, how in outs],
        out_shape=[s for s, _sh, _h in outs],
        scratch_shapes=scratch,
        input_output_aliases={len(ins) + k: k for k in range(len(kept))},
        compiler_params=pltpu.CompilerParams(
            dimension_semantics=("arbitrary",), vmem_limit_bytes=56 * 1024 * 1024
        ),
    )(*[a for a, _s, _h in ins], *kept)


def local(
    tokens, grad_out, lengths, norm_gain, w_z, w_x, w_bc, w_dt, conv_x_w, conv_x_b,
    conv_bc_w, conv_bc_b, dt_bias, a_log, d_skip, gate_gain, w_out,
):
    rows, model = tokens.shape
    inner = w_z.shape[1]
    heads = dt_bias.shape[0]
    states = w_bc.shape[1] // 2
    taps = conv_x_w.shape[0]
    blocks = rows // STRETCH
    width = inner + 2 * states
    tp_size = lax.axis_size("tp")
    slice_width = model // tp_size
    tp_index = lax.axis_index("tp")
    ctx_index = lax.axis_index("ctx")
    e8, spread, gather, upper, lower = constants(inner, heads)

    w_joined, halo = gathered(w_x, w_bc, jnp.pad(w_dt, ((0, 0), (0, 128 - heads))), tokens)
    second = jnp.concatenate([w_z, w_out.T], axis=1)
    second, w_joined = lax.optimization_barrier((second, w_joined))
    wz_out = lax.all_gather(second, "fsdp", axis=0, tiled=True)
    per_head = inner // heads

    def line(*vectors):
        joint = jnp.concatenate(vectors) if len(vectors) > 1 else vectors[0]
        return jnp.pad(joint, (0, model - joint.shape[0]))[None, :]

    per_heads = jnp.stack([dt_bias, a_log, d_skip], axis=1)
    params = jnp.concatenate(
        [
            line(norm_gain), line(conv_x_b, conv_bc_b), line(gate_gain), jnp.zeros((1, model), f32),
            jnp.pad(conv_x_w, ((0, 0), (0, model - inner)))
            + jnp.pad(conv_bc_w, ((0, 0), (inner, model - width))),
            jnp.pad(per_heads, ((0, HEAD_ROWS - heads), (0, model - 3))),
        ],
        axis=0,
    )

    def shape(dims, kind):
        return jax.ShapeDtypeStruct(dims, kind)

    def whole(x):
        return (x, x.shape, lambda i: (0,) * x.ndim)

    def by_rows(x, flip=False):
        if flip:
            return (x, (STRETCH, x.shape[1]), lambda i: (blocks - 1 - i, 0))
        return (x, (STRETCH, x.shape[1]), lambda i: (i, 0))

    def by_lanes(x, flip=False):
        if flip:
            return (x, (x.shape[0], STRETCH), lambda i: (0, blocks - 1 - i))
        return (x, (x.shape[0], STRETCH), lambda i: (0, i))

    def by_block(x, flip=False):
        if flip:
            return (x, (1,) + x.shape[1:], lambda i: (blocks - 1 - i, 0, 0))
        return (x, (1,) + x.shape[1:], lambda i: (i, 0, 0))

    def fixed(x):
        return (x, x.shape, lambda i: (0,) * len(x.shape))

    info_in = (lengths, None, "smem")
    state_dims = (blocks, states, inner)
    normed, joined_x, joined_bc, vbc, slope_x, slope_bc, pre, step, cum, s_part, end_state, decay = call(
        functools.partial(entry_kernel, rows),
        blocks,
        [
            info_in, by_rows(tokens), whole(halo), whole(params), whole(w_joined), whole(upper),
            whole(spread(0)), whole(e8),
        ],
        [
            by_rows(shape((rows, model), bf16)),
            by_rows(shape((rows, inner), bf16)),
            by_rows(shape((rows, 2 * states), bf16)),
            by_rows(shape((rows, width), bf16)),
            by_rows(shape((rows, inner), bf16)),
            by_rows(shape((rows, 2 * states), f32)),
            by_lanes(shape((HEAD_ROWS, rows), f32)),
            by_lanes(shape((HEAD_ROWS, rows), f32)),
            by_lanes(shape((HEAD_ROWS, rows), f32)),
            by_block(shape(state_dims, f32)),
            fixed(shape((states, inner), bf16)),
            fixed(shape((1, inner), f32)),
        ],
        [
            pltpu.VMEM((STRETCH + 8, width), f32),
            pltpu.VMEM((states, inner), f32),
            pltpu.VMEM((1, inner), f32),
        ],
    )
    incoming = entering(decay, end_state, "ctx", False)
    z_part, out, gn, sums, state_in, branch = call(
        functools.partial(mix_kernel, rows),
        blocks,
        [
            info_in, by_rows(vbc), by_lanes(step), by_lanes(cum), by_block(s_part),
            whole(incoming), by_rows(normed), by_rows(grad_out), whole(wz_out), whole(params),
            whole(spread(1)), whole(spread(2)), whole(e8),
        ],
        [
            by_rows(shape((rows, inner), f32)),
            by_rows(shape((rows, inner), f32)),
            by_rows(shape((rows, inner), f32)),
            by_lanes(shape((2, rows), f32)),
            by_block(shape(state_dims, bf16)),
            by_lanes(shape((model, rows), bf16)),
        ],
        [pltpu.VMEM((states, inner), f32), pltpu.VMEM((STRETCH, STRETCH), f32)],
    )
    branch = lax.psum_scatter(branch, "tp", scatter_dimension=0, tiled=True)
    sums = total_over_tp(sums)
    g_z, g_b, g_c, normed_two, a_sum, gs_part, start_state, misc_gate = call(
        functools.partial(gate_kernel, rows),
        blocks,
        [
            info_in, by_lanes(sums, True), by_lanes(cum, True), by_rows(out, True),
            by_rows(z_part, True), by_rows(gn, True), by_rows(vbc, True), by_block(state_in, True),
            whole(params), whole(spread(2)), whole(e8), whole(gather(0)),
        ],
        [
            by_rows(shape((rows, inner), bf16), True),
            by_rows(shape((rows, inner), bf16), True),
            by_rows(shape((rows, inner), bf16), True),
            by_rows(shape((rows, inner), bf16), True),
            by_lanes(shape((HEAD_ROWS, rows), f32), True),
            by_block(shape(state_dims, f32), True),
            fixed(shape((states, inner), bf16)),
            fixed(shape((8, inner), f32)),
        ],
        [pltpu.VMEM((states, inner), f32)],
    )
    sum_all = jnp.concatenate([gather(0), gather(1)[:inner]], axis=0)
    outgoing = entering(decay, start_state, "ctx", True)
    g_cat, tail, head, misc_scan, misc_dt = call(
        functools.partial(scan_kernel, rows),
        blocks,
        [
            info_in, by_rows(vbc, True), by_rows(g_b, True), by_rows(g_c, True),
            by_lanes(step, True), by_lanes(cum, True), by_lanes(pre, True), by_lanes(a_sum, True),
            by_block(state_in, True), by_block(gs_part, True), whole(outgoing),
            by_rows(slope_x, True), by_rows(slope_bc, True), by_rows(joined_x, True),
            by_rows(joined_bc, True), whole(params), whole(spread(1)),
            whole(spread(2)), whole(e8), whole(sum_all), whole(lower),
        ],
        [
            by_rows(shape((rows, width + 128), bf16), True),
            fixed(shape((8, width), f32)),
            fixed(shape((8, width), f32)),
            fixed(shape((8, width), f32)),
            fixed(shape((2 * HEAD_ROWS, STRETCH), f32)),
        ],
        [
            pltpu.VMEM((states, inner), f32),
            pltpu.VMEM((8, width), f32),
            pltpu.VMEM((STRETCH, STRETCH), f32),
            pltpu.VMEM((STRETCH, STRETCH), f32),
            pltpu.VMEM((STRETCH, 3 * inner), bf16),
        ],
    )
    next_rows = passed_along(head, "ctx", -1)
    feature = jnp.arange(model, dtype=jnp.int32) // slice_width
    mine = (feature == tp_index).astype(f32)[None, :]
    last_joined = jnp.concatenate([joined_x[rows - 16 :], joined_bc[rows - 16 :]], axis=1)
    def exit_call(first, extra_in, extra_out, scratch):
        top = count = blocks

        def flipped(x):
            return (x, (STRETCH, x.shape[1]), lambda i: (top - 1 - i, 0))

        return call(
            functools.partial(exit_kernel, rows, top, first),
            count,
            [
                info_in, flipped(tokens), flipped(grad_out), whole(mine), flipped(g_z),
                flipped(g_cat), whole(params), whole(wz_out), whole(w_joined),
            ]
            + extra_in,
            [
                (
                    shape((model, count * STRETCH), bf16),
                    (model, STRETCH),
                    lambda i: (0, count - 1 - i),
                ),
                fixed(shape((1, model), f32)),
            ]
            + extra_out,
            scratch,
        )

    g_resid, gain_part, rim, rim_w = exit_call(
        True,
        [whole(tail), whole(next_rows), whole(last_joined)],
        [fixed(shape((16, width), bf16)), fixed(shape((8, width), f32))],
        [pltpu.VMEM((16, width), f32)],
    )
    g_resid = lax.psum_scatter(g_resid, "tp", scatter_dimension=0, tiled=True)

    part_out = tn(grad_out, normed_two)
    part_z = tn(normed, g_z)
    part_cat = tn(normed, g_cat)
    part_rim = tn(normed[rows - 16 :], rim)
    part_cat = part_cat + jnp.pad(part_rim, ((0, 0), (0, 128)))
    s_out, s_z, s_cat, s_small, s_wide = reduced(
        (part_out, part_z, part_cat),
        (misc_scan, rim_w, misc_gate, misc_dt, gain_part),
        2 * states,
    )
    if lax.axis_size("ctx") > 2:
        s_out, s_z, s_cat, s_small, s_wide = jax.tree.map(
            lambda part: lax.psum(0.5 * part, "ctx"), (s_out, s_z, s_cat, s_small, s_wide)
        )
    grad_w_out = s_out.T
    grad_w_z = s_z
    grad_w_x = s_cat[:, :inner]
    grad_w_bc = s_cat[:, inner : inner + 2 * states]
    grad_w_dt = s_cat[:, inner + 2 * states : inner + 2 * states + heads]
    grad_conv_x_w = s_small[:taps, :inner]
    grad_conv_x_b = s_small[taps, :inner]
    grad_gate_gain = s_small[0, width : width + inner]
    grad_d_skip = jnp.sum(s_small[1, width : width + inner].reshape(heads, per_head), axis=1)
    dt_at = width + inner
    grad_a_log = jnp.sum(s_small[:heads, dt_at : dt_at + STRETCH], axis=1)
    grad_dt_bias = jnp.sum(s_small[:heads, dt_at + STRETCH : dt_at + 2 * STRETCH], axis=1)
    grad_conv_bc_w = s_wide[:taps, : 2 * states]
    grad_conv_bc_b = s_wide[taps, : 2 * states]
    here = tp_index * slice_width
    grad_norm_gain = lax.dynamic_slice_in_dim(s_wide[0, 2 * states :], here, slice_width, 0)
    place = tp_index.astype(jnp.int32)[None]

    wide = 2 * STRETCH
    layer_out = call(
        functools.partial(finish_kernel, tp_size),
        blocks // 2,
        [
            (place, None, "smem"),
            (branch, (slice_width, wide), lambda i: (0, i)),
            (tokens, (wide, model), lambda i: (i, 0)),
            (sums, (2, wide), lambda i: (0, i)),
        ],
        [(shape((slice_width, rows), bf16), (slice_width, wide), lambda i: (0, i))],
        [],
    )[0].T
    grad_tokens = g_resid.T
    return (
        layer_out, grad_tokens, grad_norm_gain, grad_w_z, grad_w_x, grad_w_bc, grad_w_dt,
        grad_conv_x_w, grad_conv_x_b, grad_conv_bc_w, grad_conv_bc_b, grad_dt_bias, grad_a_log,
        grad_d_skip, grad_gate_gain, grad_w_out,
    )


def solution(mesh):
    both = ("fsdp", "ctx")
    in_specs = (
        P(both, None), P(both, None), P("fsdp", None), P(), P("fsdp", "tp"), P("fsdp", "tp"),
        P("fsdp", None), P("fsdp", "tp"), P(None, "tp"), P("tp"), P(), P(), P("tp"), P("tp"),
        P("tp"), P("tp"), P("tp", "fsdp"),
    )
    out_specs = (
        P(both, "tp"), P(both, "tp"), P("tp"), P("fsdp", "tp"), P("fsdp", "tp"), P("fsdp", None),
        P("fsdp", "tp"), P(None, "tp"), P("tp"), P(), P(), P("tp"), P("tp"), P("tp"), P("tp"),
        P("tp", "fsdp"),
    )
    return jax.shard_map(local, mesh=mesh, in_specs=in_specs, out_specs=out_specs, check_vma=False)
```

```python
import functools

import jax
import jax.numpy as jnp
import numpy as np
from jax import lax
from jax.experimental import pallas as pl
from jax.experimental.pallas import tpu as pltpu
from jax.sharding import PartitionSpec as P

STRETCH = 256
TAPS = 4
INNER = 1536
HEAD_ROWS = 8
LOG2E = 1.4426950408889634

epsilon = 1e-05
f32 = jnp.float32
bf16 = jnp.bfloat16


def nn(left, right):
    return lax.dot_general(left, right, (((1,), (0,)), ((), ())), preferred_element_type=f32)


def nt(left, right):
    return lax.dot_general(left, right, (((1,), (1,)), ((), ())), preferred_element_type=f32)


def tn(left, right):
    return lax.dot_general(left, right, (((0,), (0,)), ((), ())), preferred_element_type=f32)


def halves(x):
    high = x.astype(bf16)
    return high, (x - high.astype(f32)).astype(bf16)


def thirds(x):
    high = x.astype(bf16)
    rest = x - high.astype(f32)
    mid = rest.astype(bf16)
    return high, mid, (rest - mid.astype(f32)).astype(bf16)


def exact_rows(x, ones_matrix):
    high, mid, low = thirds(x)
    r = HEAD_ROWS
    out = nn(jnp.concatenate([high, mid, low, jnp.zeros_like(low)], axis=0), ones_matrix)
    return out[:r] + out[r : 2 * r] + out[2 * r : 3 * r]


def columns_of(rows):
    have = sum(r.shape[0] for r in rows)
    pad = jnp.zeros((128 - have, rows[0].shape[1]), f32)
    cols = jnp.transpose(jnp.concatenate(list(rows) + [pad], axis=0))
    high, low = halves(cols)
    return cols, jnp.concatenate([high, low], axis=1)


def segment_start(pos, starts):
    found = jnp.zeros_like(pos)
    for s in starts:
        found = jnp.where(pos >= s, s, found)
    return found


def joined_ok(u, distance, starts):
    ok = jnp.ones(u.shape, jnp.bool_)
    for s in starts[1:]:
        ok = ok & jnp.logical_not((u < s) & (u + distance >= s))
    return ok


def iota(shape, axis):
    return lax.broadcasted_iota(jnp.int32, shape, axis)


def read_info(rows, lengths, block):
    first = lax.axis_index("ctx") * rows
    starts = [jnp.int32(0)]
    for k in range(lengths.shape[1] - 1):
        starts.append(starts[-1] + lengths[0, k])
    base = first + block * STRETCH
    end_start = segment_start(base + STRETCH - 1, starts)
    flag = jnp.where(end_start < base, 1.0, 0.0).astype(f32)
    return starts, base, end_start, flag


def norm_rows(tok):
    x = tok.astype(f32)
    inverse = lax.rsqrt(jnp.mean(x * x, axis=1, keepdims=True) + epsilon)
    return x * inverse, inverse


def lanes_of(column, e8):
    return jnp.sum(column * e8, axis=0, keepdims=True)


MESH = pl.DeviceIdType.MESH


def start_together(peers):
    barrier = pltpu.get_barrier_semaphore()
    for peer in peers:
        pl.semaphore_signal(barrier, inc=1, device_id=peer, device_id_type=MESH)
    pl.semaphore_wait(barrier, len(peers))


def remote(src, dst, sent, came, peer):
    return pltpu.make_async_remote_copy(
        src_ref=src, dst_ref=dst, send_sem=sent, recv_sem=came, device_id=peer, device_id_type=MESH
    )


def turned(index, distance, size):
    return lax.rem(index + distance + size, size)


def twin_of(index):
    parity = lax.rem(index, 2)
    return parity, index + 1 - 2 * parity


def entry_kernel(
    rows, n, chain, info, nrm, halo, par, wj, tri, ew, e8, w_z, w_out_t,
    jx_o, jb_o, vbc_o, sx_o, sb_o, pre_o, step_o, cum_o, s_o, end_o, dec_o, inc_o, wz_o,
    ext, run, dec, got, sent, came, own, hop,
):
    i = pl.program_id(0)
    f = lax.axis_index("fsdp")
    here = lax.axis_index("ctx")
    _parity, twin = twin_of(here)
    peers = [{"fsdp": turned(f, d, n)} for d in range(1, n)] + [{"ctx": twin}]
    barrier = pltpu.get_barrier_semaphore()
    slab = w_z.shape[0]

    @pl.when(i == 0)
    def _():
        for peer in peers:
            pl.semaphore_signal(barrier, inc=1, device_id=peer, device_id_type=MESH)

    def weight_copies():
        at = pl.ds(pl.multiple_of(f * slab, 16), slab)
        for p, ref in enumerate((w_z, w_out_t)):
            cols = slice(p * ref.shape[1], (p + 1) * ref.shape[1])
            target = wz_o.at[at, cols]
            yield pltpu.make_async_copy(ref, target, own.at[p])
            for d in range(1, n):
                yield remote(
                    ref, target, sent.at[d - 1, p], came.at[d - 1, p], {"fsdp": turned(f, d, n)}
                )

    starts, base, end_start, flag = read_info(rows, info, i)
    inner = jx_o.shape[1]
    width = inner + jb_o.shape[1]
    gain, cb, cw, taps = par[0:1, :], par[1:2, :], par[4:8, :], TAPS

    @pl.when(i == 0)
    def _():
        unit, _inv = norm_rows(halo[...])
        before = nn((unit * gain).astype(bf16), wj[:, :width])
        ext[0:8, :] = before.astype(bf16).astype(f32)[8:16]
        run[...] = jnp.zeros_like(run)
        dec[...] = jnp.ones_like(dec)

    normed = nrm[...]
    product = nn(normed, wj[...])
    joined = product[:, :width].astype(bf16)
    jx_o[...] = joined[:, :inner]
    jb_o[...] = joined[:, inner:]
    ext[8 : 8 + STRETCH, :] = joined.astype(f32)
    pos = base + iota((STRETCH, 128), 0)
    first_of = segment_start(pos, starts)
    valid = [
        jnp.where(pos - (taps - 1 - k) >= first_of, 1.0, 0.0).astype(f32) for k in range(taps - 1)
    ]
    for g in range(width // 128):
        at = slice(128 * g, 128 * (g + 1))
        acc = cb[:, at] + cw[taps - 1 : taps, at] * ext[8 : 8 + STRETCH, at]
        for k in range(taps - 1):
            low = 8 - (taps - 1) + k
            acc = acc + cw[k : k + 1, at] * (ext[low : low + STRETCH, at] * valid[k])
        sig = jax.nn.sigmoid(acc)
        act = acc * sig
        vbc_o[:, at] = act.astype(bf16)
        slope = sig + act * (1.0 - sig)
        if 128 * g < inner:
            sx_o[:, at] = slope.astype(bf16)
        else:
            sb_o[:, 128 * g - inner : 128 * (g + 1) - inner] = slope
    ext[0:8, :] = ext[STRETCH : STRETCH + 8, :]
    pre = jnp.transpose(product[:, width:])[:HEAD_ROWS] + par[8:16, 0:1]
    step = jax.nn.softplus(pre)
    logd = -step * jnp.exp(par[8:16, 1:2])
    cum = exact_rows(logd, tri[...])
    pre_o[...] = pre
    step_o[...] = step
    cum_o[...] = cum
    cum_e = cum[:, STRETCH - 1 : STRETCH]
    where_s = base + iota((1, STRETCH), 1)
    keep = jnp.where(where_s >= end_start, 1.0, 0.0).astype(f32)
    weight = jnp.exp(cum_e - cum) * step * keep
    _cols, both = columns_of([weight])
    spread = nn(both, ew[...])
    v = vbc_o[:, :inner].astype(f32)
    b = vbc_o[:, inner : inner + 128]
    state = tn(b, (v * spread).astype(bf16))
    s_o[0] = state
    through = lanes_of(jnp.exp(cum_e) * flag, e8[...])
    run[...] = through * run[...] + state
    dec[...] = dec[...] * through
    end_o[...] = run[...].astype(bf16)
    dec_o[...] = dec[...]

    @pl.when(i == 0)
    def _():
        pl.semaphore_wait(barrier, len(peers))
        for copy in weight_copies():
            copy.start()

    @pl.when(i == pl.num_programs(0) - 1)
    def _():
        if chain == 2:
            copy = remote(end_o, got, hop.at[0], hop.at[1], {"ctx": twin})
            copy.start()
            copy.wait()
            inc_o[...] = jnp.where(here > 0, got[...], jnp.zeros_like(got))
        else:
            inc_o[...] = jnp.zeros_like(inc_o)
        for copy in weight_copies():
            copy.wait()


def mix_kernel(
    rows, info, vbc, step, cum, s_in, inc, normed, gout, wz_out, par, e_step, e_scale, e8,
    z_o, out_o, gn_o, sum_o, st_o, br_o,
    run, gram,
):
    i = pl.program_id(0)
    starts, base, _end_start, flag = read_info(rows, info, i)
    inner = out_o.shape[1]
    gain = par[2:3, :inner]
    dskip = lanes_of(par[8:16, 2:3], e8[...])

    @pl.when(i == 0)
    def _():
        run[...] = inc[...].astype(f32)

    st = run[...].astype(bf16)
    st_o[0] = st
    cum_v = cum[...]
    cum_e = cum_v[:, STRETCH - 1 : STRETCH]
    through = lanes_of(jnp.exp(cum_e) * flag, e8[...])
    run[...] = through * run[...] + s_in[0]

    row_first = segment_start(base + iota((1, STRETCH), 1), starts)
    scale = jnp.exp(cum_v) * jnp.where(row_first < base, 1.0, 0.0).astype(f32)
    cum2 = cum_v * LOG2E
    cols, both = columns_of([cum2, step[...], scale])
    step_x = nn(both, e_step[...])
    scale_x = nn(both, e_scale[...])
    b = vbc[:, inner : inner + 128]
    c = vbc[:, inner + 128 : inner + 256]
    carried = nn(c, st) * scale_x
    half = STRETCH // 2
    low, high = slice(0, half), slice(half, STRETCH)
    t_at = iota((half, STRETCH), 0)
    s_at = iota((half, STRETCH), 1)
    causal = (s_at <= t_at)[:, low]
    first_low = segment_start(iota((half, half), 0) + base, starts)
    first_high = segment_start(t_at + (base + half), starts)
    mask_a = causal & ((s_at + base)[:, low] >= first_low)
    mask_b = (s_at <= t_at + half) & (s_at + base >= first_high)
    gram[low, low] = jnp.where(mask_a, nt(c[low], b[low]), 0.0)
    gram[high, :] = jnp.where(mask_b, nt(c[high], b), 0.0)
    lane = iota((STRETCH, 128), 1)
    pieces = []
    for p in range(inner // 128):
        at = slice(128 * p, 128 * (p + 1))
        v = vbc[:, at].astype(f32)
        sv = (v * step_x[:, at]).astype(bf16)
        rest = carried[:, at] + dskip[:, at] * v
        acc_low, acc_high = rest[low], rest[high]
        for j in range(2):
            h = 2 * p + j
            side = (lane < 64) if j == 0 else (lane >= 64)
            part = jnp.where(side, sv, jnp.zeros_like(sv))
            row = cum2[h : h + 1, :]
            first_gap = cols[low, h : h + 1] - row[:, low]
            cross_gap = cols[high, h : h + 1] - row[:, low]
            last_gap = cols[high, h : h + 1] - row[:, high]
            decay_b = jnp.concatenate(
                [jnp.exp2(cross_gap), jnp.exp2(jnp.minimum(last_gap, 0.0))], axis=1
            )
            decay_a = jnp.exp2(jnp.minimum(first_gap, 0.0))
            acc_low = acc_low + nn((gram[low, low] * decay_a).astype(bf16), part[low])
            acc_high = acc_high + nn((gram[high, :] * decay_b).astype(bf16), part)
        pieces.append(jnp.concatenate([acc_low, acc_high], axis=0))
    out = jnp.concatenate(pieces, axis=1)
    out_o[...] = out
    zf = nn(normed[...], wz_out[:, :inner])
    z_o[...] = zf
    gated = out * (zf * jax.nn.sigmoid(zf))
    gn = nn(gout[...], wz_out[:, inner:])
    gn_o[...] = gn
    gg = gated * gain
    br_o[...] = nt(wz_out[:, inner:], gg.astype(bf16)).astype(bf16)
    ss = jnp.sum(gated * gated, axis=1, keepdims=True)
    dq = jnp.sum(gn * gg, axis=1, keepdims=True)
    sum_o[...] = jnp.transpose(jnp.where(lane == 0, ss, dq))[0:2]


def gate_kernel(
    rows, info, sums, cum, out, z, gn, vc, st, par, e_scale, e8, f_sum,
    gz_o, gb_o, gc_o, n2_o, a_o, gs_o, start_o, misc_o,
    run,
):
    step_id = pl.program_id(0)
    blocks = pl.num_programs(0)
    i = blocks - 1 - step_id
    starts, base, _end_start, flag = read_info(rows, info, i)
    inner = z.shape[1]
    gain = par[2:3, :inner]
    dskip = lanes_of(par[8:16, 2:3], e8[...])

    @pl.when(step_id == 0)
    def _():
        run[...] = jnp.zeros_like(run)
        misc_o[...] = jnp.zeros_like(misc_o)

    alpha = lax.rsqrt(sums[0:1, :] / INNER + epsilon)
    beta = alpha * alpha * alpha * sums[1:2, :] / INNER
    cum_v = cum[...]
    row_first = segment_start(base + iota((1, STRETCH), 1), starts)
    scale = jnp.exp(cum_v) * jnp.where(row_first < base, 1.0, 0.0).astype(f32)
    cols, both = columns_of([alpha, beta, jnp.zeros((14, STRETCH), f32), scale])
    alpha_c = cols[:, 0:1]
    beta_c = cols[:, 1:2]
    scale_x = nn(both, e_scale[...])
    v = vc[:, :inner].astype(f32)
    c = vc[:, inner + 128 : inner + 256]
    zf = z[...]
    sig = jax.nn.sigmoid(zf)
    act = zf * sig
    o = out[...]
    gated = o * act
    g_n = gn[...]
    unit = gated * alpha_c
    g_gated = alpha_c * (g_n * gain) - beta_c * gated
    g_out = g_gated * act
    gz_o[...] = (g_gated * o * (sig + act * (1.0 - sig))).astype(bf16)
    gb = g_out.astype(bf16)
    gb_o[...] = gb
    n2_o[...] = (unit * gain).astype(bf16)
    misc_o[0:1, :] += jnp.sum(g_n * unit, axis=0, keepdims=True)
    misc_o[1:2, :] += jnp.sum(g_out * v, axis=0, keepdims=True)
    gf = gb.astype(f32)
    carried = nn(c, st[0]) * scale_x
    prod = gf * (o - dskip * v) + (g_out - gf) * carried
    high, low = halves(prod)
    sums_c = nn(jnp.concatenate([high, low], axis=1), f_sum[...])
    a_o[...] = jnp.transpose(sums_c)[0:HEAD_ROWS]
    gc = (g_out * scale_x).astype(bf16)
    gc_o[...] = gc
    gs = tn(c, gc)
    gs_o[0] = gs
    through = lanes_of(jnp.exp(cum_v[:, STRETCH - 1 : STRETCH]) * flag, e8[...])
    run[...] = through * run[...] + gs
    start_o[...] = run[...].astype(bf16)


def scan_kernel(
    rows, info, vbc, gb, gc, step, cum, pre, a_sum, st, gs_in, outg, sx, sb, jx, jb, par,
    e_step, e_w, e8, f_all, tril,
    gcat_o, tail_o, head_o, misc_o, dt_o,
    run, ext, gram, acc, prod,
):
    step_id = pl.program_id(0)
    blocks = pl.num_programs(0)
    i = blocks - 1 - step_id
    starts, base, end_start, flag = read_info(rows, info, i)
    inner = gb.shape[1]
    width = inner + jb.shape[1]
    cw, taps = par[4:8, :], TAPS
    rate = jnp.exp(par[8:16, 1:2])
    dskip = lanes_of(par[8:16, 2:3], e8[...])

    @pl.when(step_id == 0)
    def _():
        run[...] = outg[...].astype(f32)
        ext[...] = jnp.zeros((8, width), f32)
        misc_o[...] = jnp.zeros_like(misc_o)
        dt_o[...] = jnp.zeros_like(dt_o)

    cum_v = cum[...]
    step_v = step[...]
    cum_e = cum_v[:, STRETCH - 1 : STRETCH]
    after = run[...]
    low_after = after.astype(bf16)
    state = st[0]
    through = lanes_of(jnp.exp(cum_e) * flag, e8[...])
    g_through = jnp.sum(after * state.astype(f32), axis=0, keepdims=True) * through
    end_more = jnp.sum(e8[...] * g_through, axis=1, keepdims=True)
    run[...] = through * after + gs_in[0]

    where_s = base + iota((1, STRETCH), 1)
    row_first = segment_start(where_s, starts)
    end_decay = jnp.exp(cum_e - cum_v) * jnp.where(where_s >= end_start, 1.0, 0.0).astype(f32)
    weight = end_decay * step_v
    cum2 = cum_v * LOG2E
    ok_rows = [
        jnp.where(joined_ok(where_s, d, starts), 1.0, 0.0).astype(f32)
        for d in range(taps - 1, 0, -1)
    ]
    cols, both = columns_of([cum2, step_v, weight] + ok_rows)
    b = vbc[:, inner : inner + 128]
    c = vbc[:, inner + 128 : inner + 256]
    half = STRETCH // 2
    low, high = slice(0, half), slice(half, STRETCH)
    s_at = iota((half, STRETCH), 0)
    t_at = iota((half, STRETCH), 1)
    mask_a = (s_at <= t_at) & (s_at + base >= row_first)
    mask_b = (s_at <= t_at)[:, low] & ((s_at + (base + half)) >= row_first)[:, high]
    gram[low, :] = jnp.where(mask_a, nt(b[low], c), 0.0)
    gram[high, low] = jnp.where(mask_b, nt(b[high], c[high]), 0.0)
    acc[...] = jnp.zeros_like(acc)
    lane = iota((STRETCH, 128), 1)
    ok = [
        jnp.broadcast_to(cols[:, 3 * HEAD_ROWS + k : 3 * HEAD_ROWS + k + 1], (STRETCH, 128))
        for k in range(taps - 1)
    ]

    def convolve(at, own, j_f):
        following = ext[:, at]
        joint = jnp.concatenate([own, following], axis=0)
        ext[:, at] = own[0:8]
        misc_o[taps : taps + 1, at] += jnp.sum(own, axis=0, keepdims=True)
        misc_o[taps - 1 : taps, at] += jnp.sum(own * j_f, axis=0, keepdims=True)
        total = own * cw[taps - 1 : taps, at]
        for k in range(taps - 1):
            d = taps - 1 - k
            term = pltpu.roll(joint, STRETCH + 8 - d, axis=0)[:STRETCH] * ok[k]
            misc_o[k : k + 1, at] += jnp.sum(term * j_f, axis=0, keepdims=True)
            total = total + term * cw[k : k + 1, at]
        gcat_o[:, at] = total.astype(bf16)
        tail_o[:, at] = jnp.where(step_id == 0, total[STRETCH - 8 :], tail_o[:, at])

    g_b = jnp.zeros((STRETCH, 128), f32)
    g_c = jnp.zeros((STRETCH, 128), f32)
    for p in range(inner // 128):
        at = slice(128 * p, 128 * (p + 1))
        step_x = nn(both, e_step[:, at])
        v = vbc[:, at].astype(f32)
        sv = (v * step_x).astype(bf16)
        g_pair = gb[:, at]
        u_low = jnp.zeros((half, 128), f32)
        u_high = jnp.zeros((half, 128), f32)
        for j in range(2):
            h = 2 * p + j
            side = (lane < 64) if j == 0 else (lane >= 64)
            g_side = jnp.where(side, g_pair, jnp.zeros_like(g_pair))
            sv_side = jnp.where(side, sv, jnp.zeros_like(sv))
            row = cum2[h : h + 1, :]
            first_gap = row[:, low] - cols[low, h : h + 1]
            cross_gap = row[:, high] - cols[low, h : h + 1]
            last_gap = row[:, high] - cols[high, h : h + 1]
            decay_a = jnp.concatenate(
                [jnp.exp2(jnp.minimum(first_gap, 0.0)), jnp.exp2(cross_gap)], axis=1
            )
            decay_b = jnp.exp2(jnp.minimum(last_gap, 0.0))
            u_low = u_low + nn((gram[low, :] * decay_a).astype(bf16), g_side)
            u_high = u_high + nn((gram[high, low] * decay_b).astype(bf16), g_side[high])
            acc[low, :] += nt(sv_side[low], g_pair) * decay_a
            acc[high, low] += nt(sv_side[high], g_pair[high]) * decay_b
        u = jnp.concatenate([u_low, u_high], axis=0)
        w_x = nn(both, e_w[:, at])
        y = nn(b, low_after[:, at])
        h1, l1 = halves(sv.astype(f32) * u)
        prod[:, at] = h1
        prod[:, inner + 128 * p : inner + 128 * (p + 1)] = l1
        prod[:, 2 * inner + 128 * p : 2 * inner + 128 * (p + 1)] = (v * y).astype(bf16)
        g_b = g_b + nt((v * w_x).astype(bf16), low_after[:, at])
        g_c = g_c + nt(gc[:, at], state[:, at])
        gv = dskip[:, at] * g_pair.astype(f32) + step_x * u + w_x * y
        convolve(at, gv * sx[:, at].astype(f32), jx[:, at].astype(f32))

    gg_a = jnp.where(mask_a, acc[low, :], 0.0).astype(bf16)
    gg_b = jnp.where(mask_b, acc[high, low], 0.0).astype(bf16)
    g_b = g_b + jnp.concatenate([nn(gg_a, c), nn(gg_b, c[high])], axis=0)
    g_c = g_c + tn(gg_a, b[low])
    g_c = g_c + jnp.concatenate([jnp.zeros((half, 128), f32), tn(gg_b, b[high])], axis=0)
    for k, part in enumerate((g_b, g_c)):
        here = slice(128 * k, 128 * (k + 1))
        convolve(
            slice(inner + 128 * k, inner + 128 * (k + 1)),
            part * sb[:, here],
            jb[:, here].astype(f32),
        )

    sums_r = jnp.transpose(nn(prod[...], f_all[...]))
    g_mixed = sums_r[0:HEAD_ROWS]
    g_end = sums_r[HEAD_ROWS : 2 * HEAD_ROWS]
    ends = g_end * weight
    g_cum = a_sum[...] - g_mixed - ends
    end_add = jnp.sum(ends, axis=1, keepdims=True) + end_more
    g_log = exact_rows(g_cum, tril[...]) + end_add
    slope_dt = jax.nn.sigmoid(pre[...])
    ratio = jnp.where(step_v > 0.0, slope_dt / step_v, 1.0)
    g_pre_dt = (g_end * end_decay - g_log * rate) * slope_dt + g_mixed * ratio
    dt_o[0:HEAD_ROWS, :] += g_log * (-step_v * rate)
    dt_o[HEAD_ROWS:, :] += g_pre_dt
    pad = jnp.zeros((128 - HEAD_ROWS, STRETCH), f32)
    gcat_o[:, width:] = jnp.transpose(jnp.concatenate([g_pre_dt, pad], axis=0)).astype(bf16)

    head_o[...] = ext[...]


def exit_kernel(
    rows, blocks, rim_side, info, tok, gout, mine, gz, gcat, par, wz_out, wj, *rest
):
    step_id = pl.program_id(0)
    i = blocks - 1 - step_id
    starts, base, _end_start, _flag = read_info(rows, info, i)
    inner = gz.shape[1]
    if rim_side:
        tail, nxt, last_j, gr_o, gain_o, rim_o, rim_w_o, fix = rest
        taps, width = TAPS, tail.shape[1]
        cw = par[4:8, :width]
    else:
        gr_o, gain_o = rest
    gain = par[0:1, :]

    g_normed = nt(gz[...], wz_out[:, :inner]) + nt(gcat[...], wj[...])

    def finish(g_normed):
        unit, inverse = norm_rows(tok[...])
        scaled = g_normed * gain
        mean = jnp.mean(scaled * unit, axis=1, keepdims=True)
        own = gout[...].astype(f32) * mine[...]
        gr_o[...] = jnp.transpose(own + inverse * (scaled - unit * mean)).astype(bf16)
        gain_o[...] += jnp.sum(g_normed * unit, axis=0, keepdims=True)

    @pl.when(step_id == 0)
    def _():
        gain_o[...] = jnp.zeros_like(gain_o)

    if not rim_side:
        finish(g_normed)
        return

    @pl.when(step_id == 0)
    def _():
        fix[0:8, :] = jnp.zeros((8, width), f32)
        fix[8:16, :] = nxt[...]
        places = base + STRETCH - 8 + iota((8, 128), 0)
        wide = last_j[8:16, :].astype(f32)
        total = tail[...]
        for k in range(taps - 1):
            d = taps - 1 - k
            ok = jnp.where(joined_ok(places, d, starts), 1.0, 0.0).astype(f32)
            inside = jnp.where(iota((8, width), 0) >= 8 - d, fix[d : d + 8, :], 0.0)
            term = inside * jnp.concatenate([ok] * (width // 128), axis=1)
            total = total + term * cw[k : k + 1, :]
            rim_w_o[k : k + 1, :] = jnp.sum(term * wide, axis=0, keepdims=True)
        rim_w_o[taps - 1 : 8, :] = jnp.zeros((9 - taps, width), f32)
        fix[0:8, :] = jnp.zeros((8, width), f32)
        fix[8:16, :] = total.astype(bf16).astype(f32) - tail[...].astype(bf16).astype(f32)
        rim_o[...] = fix[...].astype(bf16)

    @pl.when(step_id == 0)
    def _():
        more = nt(rim_o[...], wj[:, :width])
        finish(g_normed + jnp.concatenate([jnp.zeros((STRETCH - 16, more.shape[1]), f32), more]))

    @pl.when(step_id > 0)
    def _():
        finish(g_normed)


def finish_kernel(parts, place, part, base, sums, out):
    wide = part[...].astype(f32) * lax.rsqrt(sums[0:1, :] / INNER + epsilon)
    size = out.shape[0]
    for k in range(parts):

        @pl.when(place[0] == k)
        def _():
            add = jnp.transpose(base[:, size * k : size * (k + 1)].astype(f32))
            out[...] = (wide + add).astype(bf16)


def gather_kernel(
    n, chain, x, bc, dt, par, tok, out, halo, nrm, sent, came, passed, relayed, own, hop
):
    f = lax.axis_index("fsdp")
    parity, twin = twin_of(lax.axis_index("ctx"))
    rows = x.shape[0]
    half = rows // 2
    here = lax.axis_index("ctx")
    following = turned(here, 1, chain)
    sides = [{"ctx": twin}] if chain == 2 else [{"ctx": following}, {"ctx": turned(here, -1, chain)}]
    start_together([{"fsdp": turned(f, d, n)} for d in range(1, n)] + sides)
    pieces = []
    at = 0
    for ref in (x, bc, dt):
        pieces.append((ref, slice(at, at + ref.shape[1])))
        at += ref.shape[1]

    def place(source, side):
        return pl.ds(pl.multiple_of(source * rows + side * half, 16), half)

    mine = pl.ds(pl.multiple_of(parity * half, 16), half)
    copies = []
    for d in range(1, n):
        for p, (ref, cols) in enumerate(pieces):
            copy = remote(
                ref.at[mine, :], out.at[place(f, parity), cols],
                sent.at[d - 1, p], came.at[d - 1, p], {"fsdp": turned(f, d, n)},
            )
            copy.start()
            copies.append(copy)
    edge = halo.shape[0]
    copy = remote(
        tok.at[pl.ds(tok.shape[0] - edge, edge), :], halo, hop.at[0], hop.at[1], {"ctx": following}
    )
    copy.start()
    locals_ = [copy]
    for p, (ref, cols) in enumerate(pieces):
        copy = pltpu.make_async_copy(
            ref, out.at[pl.ds(pl.multiple_of(f * rows, 16), rows), cols], own.at[p]
        )
        copy.start()
        locals_.append(copy)
    gain = par[...][None, :]

    def norm_block(tok_block, nrm_block):
        unit, _inverse = norm_rows(tok_block[...])
        nrm_block[...] = (unit * gain).astype(bf16)

    block = pl.BlockSpec((2 * STRETCH, tok.shape[1]), lambda i: (i, 0))
    pltpu.emit_pipeline(
        norm_block, grid=(tok.shape[0] // (2 * STRETCH),), in_specs=[block], out_specs=[block]
    )(tok, nrm)

    relays = []
    for d in range(1, n):
        source = turned(f, -d, n)
        for p, (ref, cols) in enumerate(pieces):
            copies[(d - 1) * len(pieces) + p].wait_recv()
            piece = out.at[place(source, parity), cols]
            copy = remote(piece, piece, passed.at[d - 1, p], relayed.at[d - 1, p], {"ctx": twin})
            copy.start()
            relays.append(copy)
    for copy in copies:
        copy.wait_send()
    for copy in locals_:
        copy.wait()
    for copy in relays:
        copy.wait()


def gathered(x, bc, dt, par, tok):
    n = lax.axis_size("fsdp")
    pieces = (n - 1, 3)
    width = x.shape[1] + bc.shape[1] + dt.shape[1]
    return pl.pallas_call(
        functools.partial(gather_kernel, n, lax.axis_size("ctx")),
        out_shape=[
            jax.ShapeDtypeStruct((n * x.shape[0], width), bf16),
            jax.ShapeDtypeStruct((16, tok.shape[1]), bf16),
            jax.ShapeDtypeStruct(tok.shape, bf16),
        ],
        in_specs=[pl.BlockSpec(memory_space=pltpu.VMEM)] * 4 + [pl.BlockSpec(memory_space=pl.ANY)],
        out_specs=[pl.BlockSpec(memory_space=pltpu.VMEM)] * 2
        + [pl.BlockSpec(memory_space=pl.ANY)],
        scratch_shapes=[pltpu.SemaphoreType.DMA(pieces)] * 4
        + [pltpu.SemaphoreType.DMA((3,)), pltpu.SemaphoreType.DMA((2,))],
        compiler_params=pltpu.CompilerParams(collective_id=1, has_side_effects=True),
    )(x, bc, dt, par, tok)


def total_kernel(n, part, out, slots, sent, came):
    me = lax.axis_index("tp")
    start_together([{"tp": turned(me, d, n)} for d in range(1, n)])
    copies = []
    for d in range(1, n):
        copy = remote(
            part, slots.at[d - 1], sent.at[d - 1], came.at[d - 1], {"tp": turned(me, d, n)}
        )
        copy.start()
        copies.append(copy)
    total = part[...]
    for d in range(1, n):
        copies[d - 1].wait_recv()
        total = total + slots[d - 1]
    out[...] = total
    for copy in copies:
        copy.wait_send()


def total_over_tp(part):
    n = lax.axis_size("tp")
    return pl.pallas_call(
        functools.partial(total_kernel, n),
        out_shape=jax.ShapeDtypeStruct(part.shape, f32),
        in_specs=[pl.BlockSpec(memory_space=pltpu.VMEM)],
        out_specs=pl.BlockSpec(memory_space=pltpu.VMEM),
        scratch_shapes=[
            pltpu.VMEM((n - 1,) + part.shape, f32),
            pltpu.SemaphoreType.DMA((n - 1,)),
            pltpu.SemaphoreType.DMA((n - 1,)),
        ],
        compiler_params=pltpu.CompilerParams(collective_id=2, has_side_effects=True),
    )(part)


def reduce_kernel(
    n, m, bc_cols, conv_bc,
    p_out, p_z, p_cat, m_scan, m_rim, m_gate, m_dt, m_gain,
    o_out, o_z, o_cat, o_small, o_wide,
    give, take, mid, slots, final, bc_slots, small, small_slots, wide_slots,
    s1, r1, s2, r2, s3, r3, s4, r4,
):
    f = lax.axis_index("fsdp")
    t = lax.axis_index("tp")
    parity, twin = twin_of(lax.axis_index("ctx"))
    start_together(
        [{"ctx": twin}]
        + [{"fsdp": turned(f, d, n)} for d in range(1, n)]
        + [{"tp": turned(t, d, m)} for d in range(1, m)]
    )
    inner = p_out.shape[1]
    rows = p_out.shape[0] // n
    half = rows // 2

    def piece(q, side):
        at = pl.ds(pl.multiple_of(q * rows + side * half, 16), half)
        return jnp.concatenate([p_out[at, :], p_z[at, :], p_cat[at, :]], axis=1)

    copies = []
    for q in range(n):
        give[q] = piece(q, 1 - parity).astype(bf16)
        copy = remote(give.at[q], take.at[q], s1.at[q], r1.at[q], {"ctx": twin})
        copy.start()
        copies.append(copy)
    w_scan = m_scan.shape[1]
    w_gate = m_gate.shape[1]
    w_dt = m_dt.shape[1]
    small[...] = jnp.zeros_like(small)
    small[:, 0:w_scan] = m_scan[...] + m_rim[...]
    at = w_scan
    small[:, at : at + w_gate] = m_gate[...]
    at += w_gate
    small[:, at : at + w_dt] = m_dt[0:8, :]
    small[:, at + w_dt : at + 2 * w_dt] = m_dt[8:16, :]
    at += 2 * w_dt
    small[0:1, at:] = m_gain[...]
    small_slots[0, pl.ds(parity, 1)] = small[...][None]
    copy = remote(
        small, small_slots.at[0, parity], s1.at[n], r1.at[n], {"ctx": twin}
    )
    copy.start()
    copies.append(copy)

    copies[n].wait()
    small_slots[1, pl.ds(f, 1)] = (small_slots[0, 0] + small_slots[0, 1])[None]
    seconds = []
    for d in range(1, n):
        copy = remote(
            small_slots.at[1, f], small_slots.at[1, f], s2.at[n - 1 + d - 1], r2.at[n - 1 + d - 1],
            {"fsdp": turned(f, d, n)},
        )
        copy.start()
        seconds.append(copy)
    for q in range(n):
        copies[q].wait()
        mid[q] = (piece(q, parity) + take[q].astype(f32)).astype(bf16)
    slots[pl.ds(f, 1)] = mid[pl.ds(f, 1)]
    for d in range(1, n):
        peer = turned(f, d, n)
        copy = remote(
            mid.at[peer], slots.at[f], s2.at[d - 1], r2.at[d - 1], {"fsdp": peer}
        )
        copy.start()
        seconds.append(copy)
    for copy in seconds:
        copy.wait()
    small_sum = small_slots[1, 0]
    whole = slots[0].astype(f32)
    for q in range(1, n):
        small_sum = small_sum + small_slots[1, q]
        whole = whole + slots[q].astype(f32)
    final[...] = whole
    bc_at = slice(3 * inner, 3 * inner + bc_cols)
    bc_slots[pl.ds(t, 1)] = whole[:, bc_at].astype(bf16)[None]
    wide = jnp.concatenate([small_sum[:, conv_bc:w_scan], small_sum[:, at:]], axis=1)
    wide_slots[pl.ds(t, 1)] = wide[None]
    o_small[...] = small_sum[:, :at]
    thirds_ = []
    for d in range(1, m):
        peer = {"tp": turned(t, d, m)}
        for p, buf in enumerate((bc_slots, wide_slots)):
            copy = remote(buf.at[t], buf.at[t], s3.at[2 * (d - 1) + p], r3.at[2 * (d - 1) + p], peer)
            copy.start()
            thirds_.append(copy)
    for copy in thirds_:
        copy.wait()
    bc_sum = bc_slots[0].astype(f32)
    wide_sum = wide_slots[0]
    for q in range(1, m):
        bc_sum = bc_sum + bc_slots[q].astype(f32)
        wide_sum = wide_sum + wide_slots[q]
    o_wide[...] = wide_sum
    final[:, bc_at] = bc_sum
    here = pl.ds(pl.multiple_of(parity * half, 8), half)
    o_out[here, :] = final[:, :inner]
    o_z[here, :] = final[:, inner : 2 * inner]
    o_cat[here, :] = final[:, 2 * inner :]
    lasts = []
    for p, (out, cols) in enumerate(
        ((o_out, slice(0, inner)), (o_z, slice(inner, 2 * inner)), (o_cat, slice(2 * inner, None)))
    ):
        copy = remote(
            final.at[:, cols] if cols.stop else final.at[:, 2 * inner : final.shape[1]],
            out.at[here, :], s4.at[p], r4.at[p], {"ctx": twin},
        )
        copy.start()
        lasts.append(copy)
    for copy in lasts:
        copy.wait()


def reduced(parts, miscs, bc_cols):
    n, m = lax.axis_size("fsdp"), lax.axis_size("tp")
    p_out, _p_z, p_cat = parts
    rows = p_out.shape[0] // n
    half = rows // 2
    inner = p_out.shape[1]
    wide = 2 * inner + p_cat.shape[1]
    m_scan, _m_rim, m_gate, m_dt, m_gain = miscs
    kept = m_scan.shape[1] + m_gate.shape[1] + 2 * m_dt.shape[1]
    small = kept + m_gain.shape[1]
    crossing = m_scan.shape[1] - inner + m_gain.shape[1]
    dma = pltpu.SemaphoreType.DMA

    def shape(*dims):
        return jax.ShapeDtypeStruct(dims, f32)

    return pl.pallas_call(
        functools.partial(reduce_kernel, n, m, bc_cols, inner),
        out_shape=[
            shape(rows, inner), shape(rows, inner), shape(rows, p_cat.shape[1]),
            shape(8, kept), shape(8, crossing),
        ],
        in_specs=[pl.BlockSpec(memory_space=pltpu.VMEM)] * 8,
        out_specs=[pl.BlockSpec(memory_space=pltpu.VMEM)] * 5,
        scratch_shapes=[
            pltpu.VMEM((n, half, wide), bf16),
            pltpu.VMEM((n, half, wide), bf16),
            pltpu.VMEM((n, half, wide), bf16),
            pltpu.VMEM((n, half, wide), bf16),
            pltpu.VMEM((half, wide), f32),
            pltpu.VMEM((m, half, bc_cols), bf16),
            pltpu.VMEM((8, small), f32),
            pltpu.VMEM((2, max(n, 2), 8, small), f32),
            pltpu.VMEM((m, 8, crossing), f32),
            dma((n + 1,)), dma((n + 1,)), dma((2 * n - 2,)), dma((2 * n - 2,)),
            dma((2 * m - 2,)), dma((2 * m - 2,)), dma((3,)), dma((3,)),
        ],
        compiler_params=pltpu.CompilerParams(
            collective_id=3, has_side_effects=True, vmem_limit_bytes=48 * 1024 * 1024
        ),
    )(*parts, *miscs)


def constants(inner, heads):
    lane_head = np.arange(inner) // (inner // heads)
    e8 = (np.arange(HEAD_ROWS)[:, None] == lane_head[None, :]).astype(np.float32)

    def spread(kind):
        m = np.zeros((128, inner), np.float32)
        m[HEAD_ROWS * kind : HEAD_ROWS * (kind + 1)] = e8
        return jnp.asarray(np.concatenate([m, m], axis=0), bf16)

    def gather(kind):
        m = np.zeros((inner, 128), np.float32)
        m[:, HEAD_ROWS * kind : HEAD_ROWS * (kind + 1)] = e8.T
        return jnp.asarray(np.concatenate([m, m], axis=0), bf16)

    at = np.arange(STRETCH)
    upper = jnp.asarray((at[:, None] <= at[None, :]).astype(np.float32), bf16)
    lower = jnp.asarray((at[:, None] >= at[None, :]).astype(np.float32), bf16)
    return jnp.asarray(e8), spread, gather, upper, lower


def passed_along(block, axis, distance):
    devices = range(lax.axis_size(axis))
    route = [(i - distance, i) for i in devices if i - distance in devices]
    return lax.ppermute(block, axis, route)


def entering(decay, state, axis, reverse):
    size = lax.axis_size(axis)
    if size == 2:
        return passed_along(state, axis, -1 if reverse else 1)
    index = lax.axis_index(axis)
    decays = lax.all_gather(decay.astype(bf16), axis)
    states = lax.all_gather(state, axis)

    def lap(k, before):
        at = size - 1 - k if reverse else k
        reached = at > index if reverse else at < index
        new = decays[at].astype(f32) * before + states[at].astype(f32)
        return jnp.where(reached, new, before)

    return lax.fori_loop(0, size, lap, jnp.zeros(state.shape, f32)).astype(bf16)


def fill_params(raw, par):
    gain, gate, x_w, bc_w, x_b, bc_b, bias, rate, skip = raw
    inner = x_w.shape[1]
    width = inner + bc_w.shape[1]
    heads = bias.shape[0]

    @pl.when(pl.program_id(0) == 0)
    def _():
        par[0:1, :] = gain[...][None, :]
        par[1:2, :inner] = x_b[...][None, :]
        par[1:2, inner:width] = bc_b[...][None, :]
        par[2:3, :inner] = gate[...][None, :]
        par[4:8, :inner] = x_w[...]
        par[4:8, inner:width] = bc_w[...]
        row, lane = iota((HEAD_ROWS, 128), 0), iota((HEAD_ROWS, 128), 1)
        table = jnp.zeros((HEAD_ROWS, 128), f32)
        for h in range(heads):
            for k, ref in enumerate((bias, rate, skip)):
                table = jnp.where((row == h) & (lane == k), ref[h], table)
        par[8:16, 0:128] = table


def call(kernel, blocks, ins, outs, scratch, remote_id=None, raw=None):
    def spec(shape, how):
        if how == "smem":
            return pl.BlockSpec(memory_space=pltpu.SMEM)
        if how == "any":
            return pl.BlockSpec(memory_space=pl.ANY)
        return pl.BlockSpec(shape, how)

    places = [k for k, (_a, _s, how) in enumerate(ins) if how == "par"]
    ins = [entry for entry in ins if entry[2] != "par"]
    body = kernel
    if places:
        count = len(raw)
        model = raw[0].shape[0]
        scratch = list(scratch) + [pltpu.VMEM((16, model), f32)]

        def body(*refs):
            par = refs[-1]
            fill_params(refs[:count], par)
            rest = list(refs[count:-1])
            rest.insert(places[0], par)
            kernel(*rest)

        def fixed_at(x):
            if x.ndim == 1 and x.shape[0] < 128:
                return (x, None, "smem")
            return (x, x.shape, lambda i: (0,) * x.ndim)

        ins = [fixed_at(x) for x in raw] + ins

    return pl.pallas_call(
        body,
        grid=(blocks,),
        in_specs=[spec(shape, how) for _a, shape, how in ins],
        out_specs=[spec(shape, how) for _s, shape, how in outs],
        out_shape=[s for s, _sh, _h in outs],
        scratch_shapes=scratch,
        compiler_params=pltpu.CompilerParams(
            dimension_semantics=("arbitrary",),
            vmem_limit_bytes=56 * 1024 * 1024,
            collective_id=remote_id,
            has_side_effects=remote_id is not None,
        ),
    )(*[a for a, _s, _h in ins])


def local(
    tokens, grad_out, lengths, norm_gain, w_z, w_x, w_bc, w_dt, conv_x_w, conv_x_b,
    conv_bc_w, conv_bc_b, dt_bias, a_log, d_skip, gate_gain, w_out,
):
    rows, model = tokens.shape
    inner = w_z.shape[1]
    heads = dt_bias.shape[0]
    states = w_bc.shape[1] // 2
    taps = conv_x_w.shape[0]
    blocks = rows // STRETCH
    width = inner + 2 * states
    tp_size = lax.axis_size("tp")
    slice_width = model // tp_size
    tp_index = lax.axis_index("tp")
    ctx_index = lax.axis_index("ctx")
    e8, spread, gather, upper, lower = constants(inner, heads)

    per_head = inner // heads

    w_joined, halo, normed = gathered(
        w_x, w_bc, jnp.pad(w_dt, ((0, 0), (0, 128 - heads))), norm_gain, tokens
    )
    n = lax.axis_size("fsdp")
    chain = lax.axis_size("ctx")

    def shape(dims, kind):
        return jax.ShapeDtypeStruct(dims, kind)

    def whole(x):
        return (x, x.shape, lambda i: (0,) * x.ndim)

    def by_rows(x, flip=False):
        if flip:
            return (x, (STRETCH, x.shape[1]), lambda i: (blocks - 1 - i, 0))
        return (x, (STRETCH, x.shape[1]), lambda i: (i, 0))

    def by_lanes(x, flip=False):
        if flip:
            return (x, (x.shape[0], STRETCH), lambda i: (0, blocks - 1 - i))
        return (x, (x.shape[0], STRETCH), lambda i: (0, i))

    def by_block(x, flip=False):
        if flip:
            return (x, (1,) + x.shape[1:], lambda i: (blocks - 1 - i, 0, 0))
        return (x, (1,) + x.shape[1:], lambda i: (i, 0, 0))

    def fixed(x):
        return (x, x.shape, lambda i: (0,) * len(x.shape))

    info_in = (lengths, None, "smem")
    params_in = (None, None, "par")
    raw = (
        norm_gain, gate_gain, conv_x_w, conv_bc_w, conv_x_b, conv_bc_b, dt_bias, a_log, d_skip
    )
    run = functools.partial(call, raw=raw)
    state_dims = (blocks, states, inner)
    dma = pltpu.SemaphoreType.DMA
    (
        joined_x, joined_bc, vbc, slope_x, slope_bc, pre, step, cum, s_part, end_state, decay,
        incoming, wz_out,
    ) = run(
        functools.partial(entry_kernel, rows, n, chain),
        blocks,
        [
            info_in, by_rows(normed), whole(halo), params_in, whole(w_joined), whole(upper),
            whole(spread(0)), whole(e8), (w_z, None, "any"), (w_out.T, None, "any"),
        ],
        [
            by_rows(shape((rows, inner), bf16)),
            by_rows(shape((rows, 2 * states), bf16)),
            by_rows(shape((rows, width), bf16)),
            by_rows(shape((rows, inner), bf16)),
            by_rows(shape((rows, 2 * states), f32)),
            by_lanes(shape((HEAD_ROWS, rows), f32)),
            by_lanes(shape((HEAD_ROWS, rows), f32)),
            by_lanes(shape((HEAD_ROWS, rows), f32)),
            by_block(shape(state_dims, f32)),
            fixed(shape((states, inner), bf16)),
            fixed(shape((1, inner), f32)),
            fixed(shape((states, inner), bf16)),
            (shape((model, 2 * inner), bf16), None, "any"),
        ],
        [
            pltpu.VMEM((STRETCH + 8, width), f32),
            pltpu.VMEM((states, inner), f32),
            pltpu.VMEM((1, inner), f32),
            pltpu.VMEM((states, inner), bf16),
            dma((n - 1, 2)),
            dma((n - 1, 2)),
            dma((2,)),
            dma((2,)),
        ],
        remote_id=4,
    )
    if chain > 2:
        incoming = entering(decay, end_state, "ctx", False)
    z_part, out, gn, sums, state_in, branch = run(
        functools.partial(mix_kernel, rows),
        blocks,
        [
            info_in, by_rows(vbc), by_lanes(step), by_lanes(cum), by_block(s_part),
            whole(incoming), by_rows(normed), by_rows(grad_out), whole(wz_out), params_in,
            whole(spread(1)), whole(spread(2)), whole(e8),
        ],
        [
            by_rows(shape((rows, inner), f32)),
            by_rows(shape((rows, inner), f32)),
            by_rows(shape((rows, inner), f32)),
            by_lanes(shape((2, rows), f32)),
            by_block(shape(state_dims, bf16)),
            by_lanes(shape((model, rows), bf16)),
        ],
        [pltpu.VMEM((states, inner), f32), pltpu.VMEM((STRETCH, STRETCH), f32)],
    )
    branch = lax.psum_scatter(branch, "tp", scatter_dimension=0, tiled=True)
    sums = total_over_tp(sums)
    g_z, g_b, g_c, normed_two, a_sum, gs_part, start_state, misc_gate = run(
        functools.partial(gate_kernel, rows),
        blocks,
        [
            info_in, by_lanes(sums, True), by_lanes(cum, True), by_rows(out, True),
            by_rows(z_part, True), by_rows(gn, True), by_rows(vbc, True), by_block(state_in, True),
            params_in, whole(spread(2)), whole(e8), whole(gather(0)),
        ],
        [
            by_rows(shape((rows, inner), bf16), True),
            by_rows(shape((rows, inner), bf16), True),
            by_rows(shape((rows, inner), bf16), True),
            by_rows(shape((rows, inner), bf16), True),
            by_lanes(shape((HEAD_ROWS, rows), f32), True),
            by_block(shape(state_dims, f32), True),
            fixed(shape((states, inner), bf16)),
            fixed(shape((8, inner), f32)),
        ],
        [pltpu.VMEM((states, inner), f32)],
    )
    sum_all = jnp.concatenate([gather(0), gather(1)[:inner]], axis=0)
    outgoing = entering(decay, start_state, "ctx", True)
    g_cat, tail, head, misc_scan, misc_dt = run(
        functools.partial(scan_kernel, rows),
        blocks,
        [
            info_in, by_rows(vbc, True), by_rows(g_b, True), by_rows(g_c, True),
            by_lanes(step, True), by_lanes(cum, True), by_lanes(pre, True), by_lanes(a_sum, True),
            by_block(state_in, True), by_block(gs_part, True), whole(outgoing),
            by_rows(slope_x, True), by_rows(slope_bc, True), by_rows(joined_x, True),
            by_rows(joined_bc, True), params_in, whole(spread(1)),
            whole(spread(2)), whole(e8), whole(sum_all), whole(lower),
        ],
        [
            by_rows(shape((rows, width + 128), bf16), True),
            fixed(shape((8, width), f32)),
            fixed(shape((8, width), f32)),
            fixed(shape((8, width), f32)),
            fixed(shape((2 * HEAD_ROWS, STRETCH), f32)),
        ],
        [
            pltpu.VMEM((states, inner), f32),
            pltpu.VMEM((8, width), f32),
            pltpu.VMEM((STRETCH, STRETCH), f32),
            pltpu.VMEM((STRETCH, STRETCH), f32),
            pltpu.VMEM((STRETCH, 3 * inner), bf16),
        ],
    )
    next_rows = passed_along(head, "ctx", -1)
    feature = jnp.arange(model, dtype=jnp.int32) // slice_width
    mine = (feature == tp_index).astype(f32)[None, :]
    last_joined = jnp.concatenate([joined_x[rows - 16 :], joined_bc[rows - 16 :]], axis=1)
    def exit_call(first, extra_in, extra_out, scratch):
        top = count = blocks

        def flipped(x):
            return (x, (STRETCH, x.shape[1]), lambda i: (top - 1 - i, 0))

        return run(
            functools.partial(exit_kernel, rows, top, first),
            count,
            [
                info_in, flipped(tokens), flipped(grad_out), whole(mine), flipped(g_z),
                flipped(g_cat), params_in, whole(wz_out), whole(w_joined),
            ]
            + extra_in,
            [
                (
                    shape((model, count * STRETCH), bf16),
                    (model, STRETCH),
                    lambda i: (0, count - 1 - i),
                ),
                fixed(shape((1, model), f32)),
            ]
            + extra_out,
            scratch,
        )

    g_resid, gain_part, rim, rim_w = exit_call(
        True,
        [whole(tail), whole(next_rows), whole(last_joined)],
        [fixed(shape((16, width), bf16)), fixed(shape((8, width), f32))],
        [pltpu.VMEM((16, width), f32)],
    )
    g_resid = lax.psum_scatter(g_resid, "tp", scatter_dimension=0, tiled=True)

    part_out = tn(grad_out, normed_two)
    part_z = tn(normed, g_z)
    part_cat = tn(normed, g_cat)
    part_rim = tn(normed[rows - 16 :], rim)
    part_cat = part_cat + jnp.pad(part_rim, ((0, 0), (0, 128)))
    s_out, s_z, s_cat, s_small, s_wide = reduced(
        (part_out, part_z, part_cat),
        (misc_scan, rim_w, misc_gate, misc_dt, gain_part),
        2 * states,
    )
    if lax.axis_size("ctx") > 2:
        s_out, s_z, s_cat, s_small, s_wide = jax.tree.map(
            lambda part: lax.psum(0.5 * part, "ctx"), (s_out, s_z, s_cat, s_small, s_wide)
        )
    grad_w_out = s_out.T
    grad_w_z = s_z
    grad_w_x = s_cat[:, :inner]
    grad_w_bc = s_cat[:, inner : inner + 2 * states]
    grad_w_dt = s_cat[:, inner + 2 * states : inner + 2 * states + heads]
    grad_conv_x_w = s_small[:taps, :inner]
    grad_conv_x_b = s_small[taps, :inner]
    grad_gate_gain = s_small[0, width : width + inner]
    grad_d_skip = jnp.sum(s_small[1, width : width + inner].reshape(heads, per_head), axis=1)
    dt_at = width + inner
    grad_a_log = jnp.sum(s_small[:heads, dt_at : dt_at + STRETCH], axis=1)
    grad_dt_bias = jnp.sum(s_small[:heads, dt_at + STRETCH : dt_at + 2 * STRETCH], axis=1)
    grad_conv_bc_w = s_wide[:taps, : 2 * states]
    grad_conv_bc_b = s_wide[taps, : 2 * states]
    here = tp_index * slice_width
    grad_norm_gain = lax.dynamic_slice_in_dim(s_wide[0, 2 * states :], here, slice_width, 0)
    place = tp_index.astype(jnp.int32)[None]

    wide = 2 * STRETCH
    layer_out = run(
        functools.partial(finish_kernel, tp_size),
        blocks // 2,
        [
            (place, None, "smem"),
            (branch, (slice_width, wide), lambda i: (0, i)),
            (tokens, (wide, model), lambda i: (i, 0)),
            (sums, (2, wide), lambda i: (0, i)),
        ],
        [(shape((slice_width, rows), bf16), (slice_width, wide), lambda i: (0, i))],
        [],
    )[0].T
    grad_tokens = g_resid.T
    return (
        layer_out, grad_tokens, grad_norm_gain, grad_w_z, grad_w_x, grad_w_bc, grad_w_dt,
        grad_conv_x_w, grad_conv_x_b, grad_conv_bc_w, grad_conv_bc_b, grad_dt_bias, grad_a_log,
        grad_d_skip, grad_gate_gain, grad_w_out,
    )


def solution(mesh):
    both = ("fsdp", "ctx")
    in_specs = (
        P(both, None), P(both, None), P("fsdp", None), P(), P("fsdp", "tp"), P("fsdp", "tp"),
        P("fsdp", None), P("fsdp", "tp"), P(None, "tp"), P("tp"), P(), P(), P("tp"), P("tp"),
        P("tp"), P("tp"), P("tp", "fsdp"),
    )
    out_specs = (
        P(both, "tp"), P(both, "tp"), P("tp"), P("fsdp", "tp"), P("fsdp", "tp"), P("fsdp", None),
        P("fsdp", "tp"), P(None, "tp"), P("tp"), P(), P(), P("tp"), P("tp"), P("tp"), P("tp"),
        P("tp", "fsdp"),
    )
    return jax.shard_map(local, mesh=mesh, in_specs=in_specs, out_specs=out_specs, check_vma=False)
```

```python
import functools

import jax
import jax.numpy as jnp
import numpy as np
from jax import lax
from jax.experimental import pallas as pl
from jax.experimental.pallas import tpu as pltpu
from jax.sharding import PartitionSpec as P

STRETCH = 256
TAPS = 4
INNER = 1536
HEAD_ROWS = 8
LOG2E = 1.4426950408889634

epsilon = 1e-05
f32 = jnp.float32
bf16 = jnp.bfloat16


def nn(left, right):
    return lax.dot_general(left, right, (((1,), (0,)), ((), ())), preferred_element_type=f32)


def nt(left, right):
    return lax.dot_general(left, right, (((1,), (1,)), ((), ())), preferred_element_type=f32)


def tn(left, right):
    return lax.dot_general(left, right, (((0,), (0,)), ((), ())), preferred_element_type=f32)


def halves(x):
    high = x.astype(bf16)
    return high, (x - high.astype(f32)).astype(bf16)


def thirds(x):
    high = x.astype(bf16)
    rest = x - high.astype(f32)
    mid = rest.astype(bf16)
    return high, mid, (rest - mid.astype(f32)).astype(bf16)


def exact_rows(x, ones_matrix):
    high, mid, low = thirds(x)
    r = HEAD_ROWS
    out = nn(jnp.concatenate([high, mid, low, jnp.zeros_like(low)], axis=0), ones_matrix)
    return out[:r] + out[r : 2 * r] + out[2 * r : 3 * r]


def columns_of(rows):
    have = sum(r.shape[0] for r in rows)
    pad = jnp.zeros((128 - have, rows[0].shape[1]), f32)
    cols = jnp.transpose(jnp.concatenate(list(rows) + [pad], axis=0))
    high, low = halves(cols)
    return cols, jnp.concatenate([high, low], axis=1)


def segment_start(pos, starts):
    found = jnp.zeros_like(pos)
    for s in starts:
        found = jnp.where(pos >= s, s, found)
    return found


def joined_ok(u, distance, starts):
    ok = jnp.ones(u.shape, jnp.bool_)
    for s in starts[1:]:
        ok = ok & jnp.logical_not((u < s) & (u + distance >= s))
    return ok


def iota(shape, axis):
    return lax.broadcasted_iota(jnp.int32, shape, axis)


def read_info(rows, lengths, block):
    first = lax.axis_index("ctx") * rows
    starts = [jnp.int32(0)]
    for k in range(lengths.shape[1] - 1):
        starts.append(starts[-1] + lengths[0, k])
    base = first + block * STRETCH
    end_start = segment_start(base + STRETCH - 1, starts)
    flag = jnp.where(end_start < base, 1.0, 0.0).astype(f32)
    return starts, base, end_start, flag


def norm_rows(tok):
    x = tok.astype(f32)
    inverse = lax.rsqrt(jnp.mean(x * x, axis=1, keepdims=True) + epsilon)
    return x * inverse, inverse


def lanes_of(column, e8):
    return jnp.sum(column * e8, axis=0, keepdims=True)


MESH = pl.DeviceIdType.MESH


def start_together(peers):
    barrier = pltpu.get_barrier_semaphore()
    for peer in peers:
        pl.semaphore_signal(barrier, inc=1, device_id=peer, device_id_type=MESH)
    pl.semaphore_wait(barrier, len(peers))


def remote(src, dst, sent, came, peer):
    return pltpu.make_async_remote_copy(
        src_ref=src, dst_ref=dst, send_sem=sent, recv_sem=came, device_id=peer, device_id_type=MESH
    )


def turned(index, distance, size):
    return lax.rem(index + distance + size, size)


def twin_of(index):
    parity = lax.rem(index, 2)
    return parity, index + 1 - 2 * parity


def entry_kernel(
    rows, n, chain, sub, subs, info, nrm, halo, par, wj, tri, ew, e8, w_z, w_out_t,
    jx_o, jb_o, vbc_o, sx_o, sb_o, pre_o, step_o, cum_o, s_o, end_o, dec_o, inc_o, wz_o,
    ext, run, dec, got, sent, came, own, hop,
):
    i = pl.program_id(0) * subs + sub
    skip = STRETCH * sub
    f = lax.axis_index("fsdp")
    here = lax.axis_index("ctx")
    _parity, twin = twin_of(here)
    peers = [{"fsdp": turned(f, d, n)} for d in range(1, n)] + [{"ctx": twin}]
    barrier = pltpu.get_barrier_semaphore()
    slab = w_z.shape[0]

    def at_first(body):
        if sub == 0:
            pl.when(pl.program_id(0) == 0)(body)

    def at_last(body):
        if sub == subs - 1:
            pl.when(pl.program_id(0) == pl.num_programs(0) - 1)(body)

    @at_first
    def _():
        for peer in peers:
            pl.semaphore_signal(barrier, inc=1, device_id=peer, device_id_type=MESH)

    def weight_copies():
        at = pl.ds(pl.multiple_of(f * slab, 16), slab)
        for p, ref in enumerate((w_z, w_out_t)):
            cols = slice(p * ref.shape[1], (p + 1) * ref.shape[1])
            target = wz_o.at[at, cols]
            yield pltpu.make_async_copy(ref, target, own.at[p])
            for d in range(1, n):
                yield remote(
                    ref, target, sent.at[d - 1, p], came.at[d - 1, p], {"fsdp": turned(f, d, n)}
                )

    starts, base, end_start, flag = read_info(rows, info, i)
    inner = jx_o.shape[1]
    width = inner + jb_o.shape[1]
    gain, cb, cw, taps = par[0:1, :], par[1:2, :], par[4:8, :], TAPS

    @at_first
    def _():
        unit, _inv = norm_rows(halo[...])
        before = nn((unit * gain).astype(bf16), wj[:, :width])
        ext[0:8, :] = before.astype(bf16).astype(f32)[8:16]
        run[...] = jnp.zeros_like(run)
        dec[...] = jnp.ones_like(dec)

    normed = nrm[...]
    product = nn(normed, wj[...])
    joined = product[:, :width].astype(bf16)
    jx_o[...] = joined[:, :inner]
    jb_o[...] = joined[:, inner:]
    ext[8 + skip : 8 + skip + STRETCH, :] = joined.astype(f32)
    pos = base + iota((STRETCH, 128), 0)
    first_of = segment_start(pos, starts)
    valid = [
        jnp.where(pos - (taps - 1 - k) >= first_of, 1.0, 0.0).astype(f32) for k in range(taps - 1)
    ]
    for g in range(width // 128):
        at = slice(128 * g, 128 * (g + 1))
        acc = cb[:, at] + cw[taps - 1 : taps, at] * ext[8 + skip : 8 + skip + STRETCH, at]
        for k in range(taps - 1):
            low = skip + 8 - (taps - 1) + k
            acc = acc + cw[k : k + 1, at] * (ext[low : low + STRETCH, at] * valid[k])
        sig = jax.nn.sigmoid(acc)
        act = acc * sig
        vbc_o[:, at] = act.astype(bf16)
        slope = sig + act * (1.0 - sig)
        if 128 * g < inner:
            sx_o[:, at] = slope.astype(bf16)
        else:
            sb_o[:, 128 * g - inner : 128 * (g + 1) - inner] = slope
    if sub == subs - 1:
        ext[0:8, :] = ext[skip + STRETCH : skip + STRETCH + 8, :]
    pre = jnp.transpose(product[:, width:])[:HEAD_ROWS] + par[8:16, 0:1]
    step = jax.nn.softplus(pre)
    logd = -step * jnp.exp(par[8:16, 1:2])
    cum = exact_rows(logd, tri[...])
    pre_o[...] = pre
    step_o[...] = step
    cum_o[...] = cum
    cum_e = cum[:, STRETCH - 1 : STRETCH]
    where_s = base + iota((1, STRETCH), 1)
    keep = jnp.where(where_s >= end_start, 1.0, 0.0).astype(f32)
    weight = jnp.exp(cum_e - cum) * step * keep
    _cols, both = columns_of([weight])
    spread = nn(both, ew[...])
    v = vbc_o[:, :inner].astype(f32)
    b = vbc_o[:, inner : inner + 128]
    state = tn(b, (v * spread).astype(bf16))
    s_o[0] = state
    through = lanes_of(jnp.exp(cum_e) * flag, e8[...])
    run[...] = through * run[...] + state
    dec[...] = dec[...] * through
    end_o[...] = run[...].astype(bf16)
    dec_o[...] = dec[...]

    @at_first
    def _():
        pl.semaphore_wait(barrier, len(peers))
        for copy in weight_copies():
            copy.start()

    @at_last
    def _():
        if chain == 2:
            copy = remote(end_o, got, hop.at[0], hop.at[1], {"ctx": twin})
            copy.start()
            copy.wait()
            inc_o[...] = jnp.where(here > 0, got[...], jnp.zeros_like(got))
        else:
            inc_o[...] = jnp.zeros_like(inc_o)
        for copy in weight_copies():
            copy.wait()


def view(ref, kind, sub):
    if kind == "r":
        return ref.at[pl.ds(STRETCH * sub, STRETCH), :]
    if kind == "l":
        return ref.at[:, pl.ds(STRETCH * sub, STRETCH)]
    if kind == "b":
        return ref.at[pl.ds(sub, 1)]
    return ref


def in_turn(kernel, subs, kinds):
    def body(*refs):
        for sub in range(subs):
            kernel(sub, subs, *[view(ref, kind, sub) for ref, kind in zip(refs, kinds)])

    return body


def mix_kernel(
    rows, sub, subs, info, vbc, step, cum, s_in, inc, normed, gout, wz_out, par, e_step, e_scale, e8,
    z_o, out_o, sum_o, st_o, br_o,
    run, gram,
):
    i = pl.program_id(0) * subs + sub
    starts, base, _end_start, flag = read_info(rows, info, i)
    inner = out_o.shape[1]
    gain = par[2:3, :inner]
    dskip = lanes_of(par[8:16, 2:3], e8[...])

    if sub == 0:

        @pl.when(i == 0)
        def _():
            run[...] = inc[...].astype(f32)

    st = run[...].astype(bf16)
    st_o[0] = st
    cum_v = cum[...]
    cum_e = cum_v[:, STRETCH - 1 : STRETCH]
    through = lanes_of(jnp.exp(cum_e) * flag, e8[...])
    run[...] = through * run[...] + s_in[0]

    row_first = segment_start(base + iota((1, STRETCH), 1), starts)
    scale = jnp.exp(cum_v) * jnp.where(row_first < base, 1.0, 0.0).astype(f32)
    cum2 = cum_v * LOG2E
    cols, both = columns_of([cum2, step[...], scale])
    step_x = nn(both, e_step[...])
    scale_x = nn(both, e_scale[...])
    b = vbc[:, inner : inner + 128]
    c = vbc[:, inner + 128 : inner + 256]
    carried = nn(c, st) * scale_x
    half = STRETCH // 2
    low, high = slice(0, half), slice(half, STRETCH)
    t_at = iota((half, STRETCH), 0)
    s_at = iota((half, STRETCH), 1)
    causal = (s_at <= t_at)[:, low]
    first_low = segment_start(iota((half, half), 0) + base, starts)
    first_high = segment_start(t_at + (base + half), starts)
    mask_a = causal & ((s_at + base)[:, low] >= first_low)
    mask_b = (s_at <= t_at + half) & (s_at + base >= first_high)
    gram[low, low] = jnp.where(mask_a, nt(c[low], b[low]), 0.0)
    gram[high, :] = jnp.where(mask_b, nt(c[high], b), 0.0)
    lane = iota((STRETCH, 128), 1)
    pieces = []
    for p in range(inner // 128):
        at = slice(128 * p, 128 * (p + 1))
        v = vbc[:, at].astype(f32)
        sv = (v * step_x[:, at]).astype(bf16)
        rest = carried[:, at] + dskip[:, at] * v
        acc_low, acc_high = rest[low], rest[high]
        for j in range(2):
            h = 2 * p + j
            side = (lane < 64) if j == 0 else (lane >= 64)
            part = jnp.where(side, sv, jnp.zeros_like(sv))
            row = cum2[h : h + 1, :]
            first_gap = cols[low, h : h + 1] - row[:, low]
            cross_gap = cols[high, h : h + 1] - row[:, low]
            last_gap = cols[high, h : h + 1] - row[:, high]
            decay_b = jnp.concatenate(
                [jnp.exp2(cross_gap), jnp.exp2(jnp.minimum(last_gap, 0.0))], axis=1
            )
            decay_a = jnp.exp2(jnp.minimum(first_gap, 0.0))
            acc_low = acc_low + nn((gram[low, low] * decay_a).astype(bf16), part[low])
            acc_high = acc_high + nn((gram[high, :] * decay_b).astype(bf16), part)
        pieces.append(jnp.concatenate([acc_low, acc_high], axis=0))
    out = jnp.concatenate(pieces, axis=1)
    out_o[...] = out
    zf = nn(normed[...], wz_out[:, :inner])
    z_o[...] = zf
    gated = out * (zf * jax.nn.sigmoid(zf))
    gg = gated * gain
    branch = nt(wz_out[:, inner:], gg.astype(bf16))
    br_o[...] = branch.astype(bf16)
    ss = jnp.sum(gated * gated, axis=1, keepdims=True)
    sum_o[0:1, :] = jnp.transpose(jnp.broadcast_to(ss, (STRETCH, 128)))[0:1]
    sum_o[1:2, :] = jnp.sum(jnp.transpose(gout[...]).astype(f32) * branch, axis=0, keepdims=True)


def gate_kernel(
    rows, info, sums, cum, out, z, gout, wz_out, vc, st, par, e_scale, e8, f_sum,
    gz_o, gb_o, gc_o, n2_o, a_o, gs_o, start_o, misc_o,
    run,
):
    step_id = pl.program_id(0)
    blocks = pl.num_programs(0)
    i = blocks - 1 - step_id
    starts, base, _end_start, flag = read_info(rows, info, i)
    inner = z.shape[1]
    gain = par[2:3, :inner]
    dskip = lanes_of(par[8:16, 2:3], e8[...])

    @pl.when(step_id == 0)
    def _():
        run[...] = jnp.zeros_like(run)
        misc_o[...] = jnp.zeros_like(misc_o)

    alpha = lax.rsqrt(sums[0:1, :] / INNER + epsilon)
    beta = alpha * alpha * alpha * sums[1:2, :] / INNER
    cum_v = cum[...]
    row_first = segment_start(base + iota((1, STRETCH), 1), starts)
    scale = jnp.exp(cum_v) * jnp.where(row_first < base, 1.0, 0.0).astype(f32)
    cols, both = columns_of([alpha, beta, jnp.zeros((14, STRETCH), f32), scale])
    alpha_c = cols[:, 0:1]
    beta_c = cols[:, 1:2]
    scale_x = nn(both, e_scale[...])
    v = vc[:, :inner].astype(f32)
    c = vc[:, inner + 128 : inner + 256]
    zf = z[...]
    sig = jax.nn.sigmoid(zf)
    act = zf * sig
    o = out[...]
    gated = o * act
    g_n = nn(gout[...], wz_out[:, inner:])
    unit = gated * alpha_c
    g_gated = alpha_c * (g_n * gain) - beta_c * gated
    g_out = g_gated * act
    gz_o[...] = (g_gated * o * (sig + act * (1.0 - sig))).astype(bf16)
    gb = g_out.astype(bf16)
    gb_o[...] = gb
    n2_o[...] = (unit * gain).astype(bf16)
    misc_o[0:1, :] += jnp.sum(g_n * unit, axis=0, keepdims=True)
    misc_o[1:2, :] += jnp.sum(g_out * v, axis=0, keepdims=True)
    gf = gb.astype(f32)
    carried = nn(c, st[0]) * scale_x
    prod = gf * (o - dskip * v) + (g_out - gf) * carried
    high, low = halves(prod)
    sums_c = nn(jnp.concatenate([high, low], axis=1), f_sum[...])
    a_o[...] = jnp.transpose(sums_c)[0:HEAD_ROWS]
    gc = (g_out * scale_x).astype(bf16)
    gc_o[...] = gc
    gs = tn(c, gc)
    gs_o[0] = gs
    through = lanes_of(jnp.exp(cum_v[:, STRETCH - 1 : STRETCH]) * flag, e8[...])
    run[...] = through * run[...] + gs
    start_o[...] = run[...].astype(bf16)


def scan_kernel(
    rows, info, vbc, gb, gc, step, cum, pre, a_sum, st, gs_in, outg, sx, sb, jx, jb, par,
    e_step, e_w, e8, f_all, tril,
    gcat_o, tail_o, head_o, misc_o, dt_o,
    run, ext, gram, acc, prod,
):
    step_id = pl.program_id(0)
    blocks = pl.num_programs(0)
    i = blocks - 1 - step_id
    starts, base, end_start, flag = read_info(rows, info, i)
    inner = gb.shape[1]
    width = inner + jb.shape[1]
    cw, taps = par[4:8, :], TAPS
    rate = jnp.exp(par[8:16, 1:2])
    dskip = lanes_of(par[8:16, 2:3], e8[...])

    @pl.when(step_id == 0)
    def _():
        run[...] = outg[...].astype(f32)
        ext[...] = jnp.zeros((8, width), f32)
        misc_o[...] = jnp.zeros_like(misc_o)
        dt_o[...] = jnp.zeros_like(dt_o)

    cum_v = cum[...]
    step_v = step[...]
    cum_e = cum_v[:, STRETCH - 1 : STRETCH]
    after = run[...]
    low_after = after.astype(bf16)
    state = st[0]
    through = lanes_of(jnp.exp(cum_e) * flag, e8[...])
    g_through = jnp.sum(after * state.astype(f32), axis=0, keepdims=True) * through
    end_more = jnp.sum(e8[...] * g_through, axis=1, keepdims=True)
    run[...] = through * after + gs_in[0]

    where_s = base + iota((1, STRETCH), 1)
    row_first = segment_start(where_s, starts)
    end_decay = jnp.exp(cum_e - cum_v) * jnp.where(where_s >= end_start, 1.0, 0.0).astype(f32)
    weight = end_decay * step_v
    cum2 = cum_v * LOG2E
    ok_rows = [
        jnp.where(joined_ok(where_s, d, starts), 1.0, 0.0).astype(f32)
        for d in range(taps - 1, 0, -1)
    ]
    cols, both = columns_of([cum2, step_v, weight] + ok_rows)
    b = vbc[:, inner : inner + 128]
    c = vbc[:, inner + 128 : inner + 256]
    half = STRETCH // 2
    low, high = slice(0, half), slice(half, STRETCH)
    s_at = iota((half, STRETCH), 0)
    t_at = iota((half, STRETCH), 1)
    mask_a = (s_at <= t_at) & (s_at + base >= row_first)
    mask_b = (s_at <= t_at)[:, low] & ((s_at + (base + half)) >= row_first)[:, high]
    gram[low, :] = jnp.where(mask_a, nt(b[low], c), 0.0)
    gram[high, low] = jnp.where(mask_b, nt(b[high], c[high]), 0.0)
    acc[...] = jnp.zeros_like(acc)
    lane = iota((STRETCH, 128), 1)
    ok = [
        jnp.broadcast_to(cols[:, 3 * HEAD_ROWS + k : 3 * HEAD_ROWS + k + 1], (STRETCH, 128))
        for k in range(taps - 1)
    ]

    def convolve(at, own, j_f):
        following = ext[:, at]
        joint = jnp.concatenate([own, following], axis=0)
        ext[:, at] = own[0:8]
        misc_o[taps : taps + 1, at] += jnp.sum(own, axis=0, keepdims=True)
        misc_o[taps - 1 : taps, at] += jnp.sum(own * j_f, axis=0, keepdims=True)
        total = own * cw[taps - 1 : taps, at]
        for k in range(taps - 1):
            d = taps - 1 - k
            term = pltpu.roll(joint, STRETCH + 8 - d, axis=0)[:STRETCH] * ok[k]
            misc_o[k : k + 1, at] += jnp.sum(term * j_f, axis=0, keepdims=True)
            total = total + term * cw[k : k + 1, at]
        gcat_o[:, at] = total.astype(bf16)
        tail_o[:, at] = jnp.where(step_id == 0, total[STRETCH - 8 :], tail_o[:, at])

    g_b = jnp.zeros((STRETCH, 128), f32)
    g_c = jnp.zeros((STRETCH, 128), f32)
    for p in range(inner // 128):
        at = slice(128 * p, 128 * (p + 1))
        step_x = nn(both, e_step[:, at])
        v = vbc[:, at].astype(f32)
        sv = (v * step_x).astype(bf16)
        g_pair = gb[:, at]
        u_low = jnp.zeros((half, 128), f32)
        u_high = jnp.zeros((half, 128), f32)
        for j in range(2):
            h = 2 * p + j
            side = (lane < 64) if j == 0 else (lane >= 64)
            g_side = jnp.where(side, g_pair, jnp.zeros_like(g_pair))
            sv_side = jnp.where(side, sv, jnp.zeros_like(sv))
            row = cum2[h : h + 1, :]
            first_gap = row[:, low] - cols[low, h : h + 1]
            cross_gap = row[:, high] - cols[low, h : h + 1]
            last_gap = row[:, high] - cols[high, h : h + 1]
            decay_a = jnp.concatenate(
                [jnp.exp2(jnp.minimum(first_gap, 0.0)), jnp.exp2(cross_gap)], axis=1
            )
            decay_b = jnp.exp2(jnp.minimum(last_gap, 0.0))
            u_low = u_low + nn((gram[low, :] * decay_a).astype(bf16), g_side)
            u_high = u_high + nn((gram[high, low] * decay_b).astype(bf16), g_side[high])
            acc[low, :] += nt(sv_side[low], g_pair) * decay_a
            acc[high, low] += nt(sv_side[high], g_pair[high]) * decay_b
        u = jnp.concatenate([u_low, u_high], axis=0)
        w_x = nn(both, e_w[:, at])
        y = nn(b, low_after[:, at])
        h1, l1 = halves(sv.astype(f32) * u)
        prod[:, at] = h1
        prod[:, inner + 128 * p : inner + 128 * (p + 1)] = l1
        prod[:, 2 * inner + 128 * p : 2 * inner + 128 * (p + 1)] = (v * y).astype(bf16)
        g_b = g_b + nt((v * w_x).astype(bf16), low_after[:, at])
        g_c = g_c + nt(gc[:, at], state[:, at])
        gv = dskip[:, at] * g_pair.astype(f32) + step_x * u + w_x * y
        convolve(at, gv * sx[:, at].astype(f32), jx[:, at].astype(f32))

    gg_a = jnp.where(mask_a, acc[low, :], 0.0).astype(bf16)
    gg_b = jnp.where(mask_b, acc[high, low], 0.0).astype(bf16)
    g_b = g_b + jnp.concatenate([nn(gg_a, c), nn(gg_b, c[high])], axis=0)
    g_c = g_c + tn(gg_a, b[low])
    g_c = g_c + jnp.concatenate([jnp.zeros((half, 128), f32), tn(gg_b, b[high])], axis=0)
    for k, part in enumerate((g_b, g_c)):
        here = slice(128 * k, 128 * (k + 1))
        convolve(
            slice(inner + 128 * k, inner + 128 * (k + 1)),
            part * sb[:, here],
            jb[:, here].astype(f32),
        )

    sums_r = jnp.transpose(nn(prod[...], f_all[...]))
    g_mixed = sums_r[0:HEAD_ROWS]
    g_end = sums_r[HEAD_ROWS : 2 * HEAD_ROWS]
    ends = g_end * weight
    g_cum = a_sum[...] - g_mixed - ends
    end_add = jnp.sum(ends, axis=1, keepdims=True) + end_more
    g_log = exact_rows(g_cum, tril[...]) + end_add
    slope_dt = jax.nn.sigmoid(pre[...])
    ratio = jnp.where(step_v > 0.0, slope_dt / step_v, 1.0)
    g_pre_dt = (g_end * end_decay - g_log * rate) * slope_dt + g_mixed * ratio
    dt_o[0:HEAD_ROWS, :] += g_log * (-step_v * rate)
    dt_o[HEAD_ROWS:, :] += g_pre_dt
    pad = jnp.zeros((128 - HEAD_ROWS, STRETCH), f32)
    gcat_o[:, width:] = jnp.transpose(jnp.concatenate([g_pre_dt, pad], axis=0)).astype(bf16)

    head_o[...] = ext[...]


def exit_kernel(
    rows, blocks, rim_side, info, tok, gout, mine, gz, gcat, par, wz_out, wj, *rest
):
    step_id = pl.program_id(0)
    i = blocks - 1 - step_id
    starts, base, _end_start, _flag = read_info(rows, info, i)
    inner = gz.shape[1]
    if rim_side:
        tail, nxt, last_j, gr_o, gain_o, rim_o, rim_w_o, fix = rest
        taps, width = TAPS, tail.shape[1]
        cw = par[4:8, :width]
    else:
        gr_o, gain_o = rest
    gain = par[0:1, :]

    g_normed = nt(gz[...], wz_out[:, :inner]) + nt(gcat[...], wj[...])

    def finish(g_normed):
        unit, inverse = norm_rows(tok[...])
        scaled = g_normed * gain
        mean = jnp.mean(scaled * unit, axis=1, keepdims=True)
        own = gout[...].astype(f32) * mine[...]
        gr_o[...] = jnp.transpose(own + inverse * (scaled - unit * mean)).astype(bf16)
        gain_o[...] += jnp.sum(g_normed * unit, axis=0, keepdims=True)

    @pl.when(step_id == 0)
    def _():
        gain_o[...] = jnp.zeros_like(gain_o)

    if not rim_side:
        finish(g_normed)
        return

    @pl.when(step_id == 0)
    def _():
        fix[0:8, :] = jnp.zeros((8, width), f32)
        fix[8:16, :] = nxt[...]
        places = base + STRETCH - 8 + iota((8, 128), 0)
        wide = last_j[8:16, :].astype(f32)
        total = tail[...]
        for k in range(taps - 1):
            d = taps - 1 - k
            ok = jnp.where(joined_ok(places, d, starts), 1.0, 0.0).astype(f32)
            inside = jnp.where(iota((8, width), 0) >= 8 - d, fix[d : d + 8, :], 0.0)
            term = inside * jnp.concatenate([ok] * (width // 128), axis=1)
            total = total + term * cw[k : k + 1, :]
            rim_w_o[k : k + 1, :] = jnp.sum(term * wide, axis=0, keepdims=True)
        rim_w_o[taps - 1 : 8, :] = jnp.zeros((9 - taps, width), f32)
        fix[0:8, :] = jnp.zeros((8, width), f32)
        fix[8:16, :] = total.astype(bf16).astype(f32) - tail[...].astype(bf16).astype(f32)
        rim_o[...] = fix[...].astype(bf16)

    @pl.when(step_id == 0)
    def _():
        more = nt(rim_o[...], wj[:, :width])
        finish(g_normed + jnp.concatenate([jnp.zeros((STRETCH - 16, more.shape[1]), f32), more]))

    @pl.when(step_id > 0)
    def _():
        finish(g_normed)


def finish_kernel(parts, place, part, base, sums, out):
    wide = part[...].astype(f32) * lax.rsqrt(sums[0:1, :] / INNER + epsilon)
    size = out.shape[0]
    for k in range(parts):

        @pl.when(place[0] == k)
        def _():
            add = jnp.transpose(base[:, size * k : size * (k + 1)].astype(f32))
            out[...] = (wide + add).astype(bf16)


def gather_kernel(
    n, chain, x, bc, dt, par, tok, out, halo, nrm, sent, came, passed, relayed, own, hop
):
    f = lax.axis_index("fsdp")
    parity, twin = twin_of(lax.axis_index("ctx"))
    rows = x.shape[0]
    half = rows // 2
    here = lax.axis_index("ctx")
    following = turned(here, 1, chain)
    sides = [{"ctx": twin}] if chain == 2 else [{"ctx": following}, {"ctx": turned(here, -1, chain)}]
    start_together([{"fsdp": turned(f, d, n)} for d in range(1, n)] + sides)
    pieces = []
    at = 0
    for ref in (x, bc, dt):
        pieces.append((ref, slice(at, at + ref.shape[1])))
        at += ref.shape[1]

    def place(source, side):
        return pl.ds(pl.multiple_of(source * rows + side * half, 16), half)

    mine = pl.ds(pl.multiple_of(parity * half, 16), half)
    copies = []
    for d in range(1, n):
        for p, (ref, cols) in enumerate(pieces):
            copy = remote(
                ref.at[mine, :], out.at[place(f, parity), cols],
                sent.at[d - 1, p], came.at[d - 1, p], {"fsdp": turned(f, d, n)},
            )
            copy.start()
            copies.append(copy)
    edge = halo.shape[0]
    copy = remote(
        tok.at[pl.ds(tok.shape[0] - edge, edge), :], halo, hop.at[0], hop.at[1], {"ctx": following}
    )
    copy.start()
    locals_ = [copy]
    for p, (ref, cols) in enumerate(pieces):
        copy = pltpu.make_async_copy(
            ref, out.at[pl.ds(pl.multiple_of(f * rows, 16), rows), cols], own.at[p]
        )
        copy.start()
        locals_.append(copy)
    gain = par[...][None, :]

    def norm_block(tok_block, nrm_block):
        unit, _inverse = norm_rows(tok_block[...])
        nrm_block[...] = (unit * gain).astype(bf16)

    block = pl.BlockSpec((2 * STRETCH, tok.shape[1]), lambda i: (i, 0))
    pltpu.emit_pipeline(
        norm_block, grid=(tok.shape[0] // (2 * STRETCH),), in_specs=[block], out_specs=[block]
    )(tok, nrm)

    relays = []
    for d in range(1, n):
        source = turned(f, -d, n)
        for p, (ref, cols) in enumerate(pieces):
            copies[(d - 1) * len(pieces) + p].wait_recv()
            piece = out.at[place(source, parity), cols]
            copy = remote(piece, piece, passed.at[d - 1, p], relayed.at[d - 1, p], {"ctx": twin})
            copy.start()
            relays.append(copy)
    for copy in copies:
        copy.wait_send()
    for copy in locals_:
        copy.wait()
    for copy in relays:
        copy.wait()


def gathered(x, bc, dt, par, tok):
    n = lax.axis_size("fsdp")
    pieces = (n - 1, 3)
    width = x.shape[1] + bc.shape[1] + dt.shape[1]
    return pl.pallas_call(
        functools.partial(gather_kernel, n, lax.axis_size("ctx")),
        out_shape=[
            jax.ShapeDtypeStruct((n * x.shape[0], width), bf16),
            jax.ShapeDtypeStruct((16, tok.shape[1]), bf16),
            jax.ShapeDtypeStruct(tok.shape, bf16),
        ],
        in_specs=[pl.BlockSpec(memory_space=pltpu.VMEM)] * 4 + [pl.BlockSpec(memory_space=pl.ANY)],
        out_specs=[pl.BlockSpec(memory_space=pltpu.VMEM)] * 2
        + [pl.BlockSpec(memory_space=pl.ANY)],
        scratch_shapes=[pltpu.SemaphoreType.DMA(pieces)] * 4
        + [pltpu.SemaphoreType.DMA((3,)), pltpu.SemaphoreType.DMA((2,))],
        compiler_params=pltpu.CompilerParams(collective_id=1, has_side_effects=True),
    )(x, bc, dt, par, tok)


def total_kernel(n, part, out, slots, sent, came):
    me = lax.axis_index("tp")
    start_together([{"tp": turned(me, d, n)} for d in range(1, n)])
    copies = []
    for d in range(1, n):
        copy = remote(
            part, slots.at[d - 1], sent.at[d - 1], came.at[d - 1], {"tp": turned(me, d, n)}
        )
        copy.start()
        copies.append(copy)
    total = part[...]
    for d in range(1, n):
        copies[d - 1].wait_recv()
        total = total + slots[d - 1]
    out[...] = total
    for copy in copies:
        copy.wait_send()


def total_over_tp(part):
    n = lax.axis_size("tp")
    return pl.pallas_call(
        functools.partial(total_kernel, n),
        out_shape=jax.ShapeDtypeStruct(part.shape, f32),
        in_specs=[pl.BlockSpec(memory_space=pltpu.VMEM)],
        out_specs=pl.BlockSpec(memory_space=pltpu.VMEM),
        scratch_shapes=[
            pltpu.VMEM((n - 1,) + part.shape, f32),
            pltpu.SemaphoreType.DMA((n - 1,)),
            pltpu.SemaphoreType.DMA((n - 1,)),
        ],
        compiler_params=pltpu.CompilerParams(collective_id=2, has_side_effects=True),
    )(part)


def reduce_kernel(
    n, m, bc_cols, conv_bc,
    p_out, p_z, p_cat, m_scan, m_rim, m_gate, m_dt, m_gain,
    o_out, o_z, o_cat, o_small, o_wide,
    give, take, mid, slots, final, bc_slots, small, small_slots, wide_slots, gain_slots,
    s1, r1, s2, r2, s3, r3, s4, r4,
):
    f = lax.axis_index("fsdp")
    t = lax.axis_index("tp")
    parity, twin = twin_of(lax.axis_index("ctx"))
    start_together(
        [{"ctx": twin}]
        + [{"fsdp": turned(f, d, n)} for d in range(1, n)]
        + [{"tp": turned(t, d, m)} for d in range(1, m)]
    )
    inner = p_out.shape[1]
    rows = p_out.shape[0] // n
    half = rows // 2

    def piece(q, side):
        at = pl.ds(pl.multiple_of(q * rows + side * half, 16), half)
        return jnp.concatenate([p_out[at, :], p_z[at, :], p_cat[at, :]], axis=1)

    copies = []
    for q in range(n):
        give[q] = piece(q, 1 - parity).astype(bf16)
        copy = remote(give.at[q], take.at[q], s1.at[q], r1.at[q], {"ctx": twin})
        copy.start()
        copies.append(copy)
    w_scan = m_scan.shape[1]
    w_gate = m_gate.shape[1]
    w_dt = m_dt.shape[1]
    small[...] = jnp.zeros_like(small)
    small[:, 0:w_scan] = m_scan[...] + m_rim[...]
    at = w_scan
    small[:, at : at + w_gate] = m_gate[...]
    at += w_gate
    small[:, at : at + w_dt] = m_dt[0:8, :]
    small[:, at + w_dt : at + 2 * w_dt] = m_dt[8:16, :]
    at += 2 * w_dt
    small[0:1, at:] = m_gain[...]
    small_slots[0, pl.ds(parity, 1)] = small[...][None]
    copy = remote(
        small, small_slots.at[0, parity], s1.at[n], r1.at[n], {"ctx": twin}
    )
    copy.start()
    copies.append(copy)

    copies[n].wait()
    small_slots[1, pl.ds(f, 1)] = (small_slots[0, 0] + small_slots[0, 1])[None]
    seconds = []
    for d in range(1, n):
        copy = remote(
            small_slots.at[1, f], small_slots.at[1, f], s2.at[n - 1 + d - 1], r2.at[n - 1 + d - 1],
            {"fsdp": turned(f, d, n)},
        )
        copy.start()
        seconds.append(copy)
    for q in range(n):
        copies[q].wait()
        mid[q] = (piece(q, parity) + take[q].astype(f32)).astype(bf16)
    slots[pl.ds(f, 1)] = mid[pl.ds(f, 1)]
    for d in range(1, n):
        peer = turned(f, d, n)
        copy = remote(
            mid.at[peer], slots.at[f], s2.at[d - 1], r2.at[d - 1], {"fsdp": peer}
        )
        copy.start()
        seconds.append(copy)
    for copy in seconds:
        copy.wait()
    small_sum = small_slots[1, 0]
    whole = slots[0].astype(f32)
    for q in range(1, n):
        small_sum = small_sum + small_slots[1, q]
        whole = whole + slots[q].astype(f32)
    final[...] = whole
    bc_at = slice(3 * inner, 3 * inner + bc_cols)
    bc_slots[pl.ds(t, 1)] = whole[:, bc_at].astype(bf16)[None]
    wide_slots[pl.ds(t, 1)] = small_sum[:, conv_bc:w_scan][None]
    gain_slots[pl.ds(t, 1)] = small_sum[0:1, at:][None]
    o_small[...] = small_sum[:, :at]
    thirds_ = []
    for d in range(1, m):
        peer = {"tp": turned(t, d, m)}
        for p, buf in enumerate((bc_slots, wide_slots, gain_slots)):
            copy = remote(buf.at[t], buf.at[t], s3.at[3 * (d - 1) + p], r3.at[3 * (d - 1) + p], peer)
            copy.start()
            thirds_.append(copy)
    for copy in thirds_:
        copy.wait()
    bc_sum = bc_slots[0].astype(f32)
    wide_sum = wide_slots[0]
    gain_sum = gain_slots[0]
    for q in range(1, m):
        bc_sum = bc_sum + bc_slots[q].astype(f32)
        wide_sum = wide_sum + wide_slots[q]
        gain_sum = gain_sum + gain_slots[q]
    o_wide[:, :bc_cols] = wide_sum
    o_wide[:, bc_cols:] = jnp.broadcast_to(gain_sum, (8, gain_sum.shape[1]))
    final[:, bc_at] = bc_sum
    here = pl.ds(pl.multiple_of(parity * half, 8), half)
    o_out[here, :] = final[:, :inner]
    o_z[here, :] = final[:, inner : 2 * inner]
    o_cat[here, :] = final[:, 2 * inner :]
    lasts = []
    for p, (out, cols) in enumerate(
        ((o_out, slice(0, inner)), (o_z, slice(inner, 2 * inner)), (o_cat, slice(2 * inner, None)))
    ):
        copy = remote(
            final.at[:, cols] if cols.stop else final.at[:, 2 * inner : final.shape[1]],
            out.at[here, :], s4.at[p], r4.at[p], {"ctx": twin},
        )
        copy.start()
        lasts.append(copy)
    for copy in lasts:
        copy.wait()


def reduced(parts, miscs, bc_cols):
    n, m = lax.axis_size("fsdp"), lax.axis_size("tp")
    p_out, _p_z, p_cat = parts
    rows = p_out.shape[0] // n
    half = rows // 2
    inner = p_out.shape[1]
    wide = 2 * inner + p_cat.shape[1]
    m_scan, _m_rim, m_gate, m_dt, m_gain = miscs
    kept = m_scan.shape[1] + m_gate.shape[1] + 2 * m_dt.shape[1]
    small = kept + m_gain.shape[1]
    crossing = m_scan.shape[1] - inner + m_gain.shape[1]
    dma = pltpu.SemaphoreType.DMA

    def shape(*dims):
        return jax.ShapeDtypeStruct(dims, f32)

    return pl.pallas_call(
        functools.partial(reduce_kernel, n, m, bc_cols, inner),
        out_shape=[
            shape(rows, inner), shape(rows, inner), shape(rows, p_cat.shape[1]),
            shape(8, kept), shape(8, crossing),
        ],
        in_specs=[pl.BlockSpec(memory_space=pltpu.VMEM)] * 8,
        out_specs=[pl.BlockSpec(memory_space=pltpu.VMEM)] * 5,
        scratch_shapes=[
            pltpu.VMEM((n, half, wide), bf16),
            pltpu.VMEM((n, half, wide), bf16),
            pltpu.VMEM((n, half, wide), bf16),
            pltpu.VMEM((n, half, wide), bf16),
            pltpu.VMEM((half, wide), f32),
            pltpu.VMEM((m, half, bc_cols), bf16),
            pltpu.VMEM((8, small), f32),
            pltpu.VMEM((2, max(n, 2), 8, small), f32),
            pltpu.VMEM((m, 8, bc_cols), f32),
            pltpu.VMEM((m, 1, m_gain.shape[1]), f32),
            dma((n + 1,)), dma((n + 1,)), dma((2 * n - 2,)), dma((2 * n - 2,)),
            dma((3 * m - 3,)), dma((3 * m - 3,)), dma((3,)), dma((3,)),
        ],
        compiler_params=pltpu.CompilerParams(
            collective_id=3, has_side_effects=True, vmem_limit_bytes=48 * 1024 * 1024
        ),
    )(*parts, *miscs)


def constants(inner, heads):
    lane_head = np.arange(inner) // (inner // heads)
    e8 = (np.arange(HEAD_ROWS)[:, None] == lane_head[None, :]).astype(np.float32)

    def spread(kind):
        m = np.zeros((128, inner), np.float32)
        m[HEAD_ROWS * kind : HEAD_ROWS * (kind + 1)] = e8
        return jnp.asarray(np.concatenate([m, m], axis=0), bf16)

    def gather(kind):
        m = np.zeros((inner, 128), np.float32)
        m[:, HEAD_ROWS * kind : HEAD_ROWS * (kind + 1)] = e8.T
        return jnp.asarray(np.concatenate([m, m], axis=0), bf16)

    at = np.arange(STRETCH)
    upper = jnp.asarray((at[:, None] <= at[None, :]).astype(np.float32), bf16)
    lower = jnp.asarray((at[:, None] >= at[None, :]).astype(np.float32), bf16)
    return jnp.asarray(e8), spread, gather, upper, lower


def passed_along(block, axis, distance):
    devices = range(lax.axis_size(axis))
    route = [(i - distance, i) for i in devices if i - distance in devices]
    return lax.ppermute(block, axis, route)


def entering(decay, state, axis, reverse):
    size = lax.axis_size(axis)
    if size == 2:
        return passed_along(state, axis, -1 if reverse else 1)
    index = lax.axis_index(axis)
    decays = lax.all_gather(decay.astype(bf16), axis)
    states = lax.all_gather(state, axis)

    def lap(k, before):
        at = size - 1 - k if reverse else k
        reached = at > index if reverse else at < index
        new = decays[at].astype(f32) * before + states[at].astype(f32)
        return jnp.where(reached, new, before)

    return lax.fori_loop(0, size, lap, jnp.zeros(state.shape, f32)).astype(bf16)


def fill_params(raw, par):
    gain, gate, x_w, bc_w, x_b, bc_b, bias, rate, skip = raw
    inner = x_w.shape[1]
    width = inner + bc_w.shape[1]
    heads = bias.shape[0]

    @pl.when(pl.program_id(0) == 0)
    def _():
        par[0:1, :] = gain[...][None, :]
        par[1:2, :inner] = x_b[...][None, :]
        par[1:2, inner:width] = bc_b[...][None, :]
        par[2:3, :inner] = gate[...][None, :]
        par[4:8, :inner] = x_w[...]
        par[4:8, inner:width] = bc_w[...]
        row, lane = iota((HEAD_ROWS, 128), 0), iota((HEAD_ROWS, 128), 1)
        table = jnp.zeros((HEAD_ROWS, 128), f32)
        for h in range(heads):
            for k, ref in enumerate((bias, rate, skip)):
                table = jnp.where((row == h) & (lane == k), ref[h], table)
        par[8:16, 0:128] = table


def call(kernel, blocks, ins, outs, scratch, remote_id=None, raw=None):
    def spec(shape, how):
        if how == "smem":
            return pl.BlockSpec(memory_space=pltpu.SMEM)
        if how == "any":
            return pl.BlockSpec(memory_space=pl.ANY)
        return pl.BlockSpec(shape, how)

    places = [k for k, (_a, _s, how) in enumerate(ins) if how == "par"]
    ins = [entry for entry in ins if entry[2] != "par"]
    body = kernel
    if places:
        count = len(raw)
        model = raw[0].shape[0]
        scratch = list(scratch) + [pltpu.VMEM((16, model), f32)]

        def body(*refs):
            par = refs[-1]
            fill_params(refs[:count], par)
            rest = list(refs[count:-1])
            rest.insert(places[0], par)
            kernel(*rest)

        def fixed_at(x):
            if x.ndim == 1 and x.shape[0] < 128:
                return (x, None, "smem")
            return (x, x.shape, lambda i: (0,) * x.ndim)

        ins = [fixed_at(x) for x in raw] + ins

    return pl.pallas_call(
        body,
        grid=(blocks,),
        in_specs=[spec(shape, how) for _a, shape, how in ins],
        out_specs=[spec(shape, how) for _s, shape, how in outs],
        out_shape=[s for s, _sh, _h in outs],
        scratch_shapes=scratch,
        compiler_params=pltpu.CompilerParams(
            dimension_semantics=("arbitrary",),
            vmem_limit_bytes=56 * 1024 * 1024,
            collective_id=remote_id,
            has_side_effects=remote_id is not None,
        ),
    )(*[a for a, _s, _h in ins])


def local(
    tokens, grad_out, lengths, norm_gain, w_z, w_x, w_bc, w_dt, conv_x_w, conv_x_b,
    conv_bc_w, conv_bc_b, dt_bias, a_log, d_skip, gate_gain, w_out,
):
    rows, model = tokens.shape
    inner = w_z.shape[1]
    heads = dt_bias.shape[0]
    states = w_bc.shape[1] // 2
    taps = conv_x_w.shape[0]
    blocks = rows // STRETCH
    width = inner + 2 * states
    tp_size = lax.axis_size("tp")
    slice_width = model // tp_size
    tp_index = lax.axis_index("tp")
    ctx_index = lax.axis_index("ctx")
    e8, spread, gather, upper, lower = constants(inner, heads)

    per_head = inner // heads

    w_joined, halo, normed = gathered(
        w_x, w_bc, jnp.pad(w_dt, ((0, 0), (0, 128 - heads))), norm_gain, tokens
    )
    n = lax.axis_size("fsdp")
    chain = lax.axis_size("ctx")

    def shape(dims, kind):
        return jax.ShapeDtypeStruct(dims, kind)

    def whole(x):
        return (x, x.shape, lambda i: (0,) * x.ndim)

    def by_rows(x, flip=False):
        if flip:
            return (x, (STRETCH, x.shape[1]), lambda i: (blocks - 1 - i, 0))
        return (x, (STRETCH, x.shape[1]), lambda i: (i, 0))

    def by_lanes(x, flip=False):
        if flip:
            return (x, (x.shape[0], STRETCH), lambda i: (0, blocks - 1 - i))
        return (x, (x.shape[0], STRETCH), lambda i: (0, i))

    def by_block(x, flip=False):
        if flip:
            return (x, (1,) + x.shape[1:], lambda i: (blocks - 1 - i, 0, 0))
        return (x, (1,) + x.shape[1:], lambda i: (i, 0, 0))

    def fixed(x):
        return (x, x.shape, lambda i: (0,) * len(x.shape))

    info_in = (lengths, None, "smem")
    params_in = (None, None, "par")
    raw = (
        norm_gain, gate_gain, conv_x_w, conv_bc_w, conv_x_b, conv_bc_b, dt_bias, a_log, d_skip
    )
    run = functools.partial(call, raw=raw)
    state_dims = (blocks, states, inner)
    subs = 2 if blocks % 2 == 0 else 1

    def several(entries, kinds):
        scales = {"r": (subs, 1), "l": (1, subs), "b": (subs, 1, 1)}
        grown = []
        for entry, kind in zip(entries, kinds):
            if kind == "w":
                grown.append(entry)
                continue
            dims = tuple(d * k for d, k in zip(entry[1], scales[kind]))
            grown.append((entry[0], dims, entry[2]))
        return grown

    dma = pltpu.SemaphoreType.DMA
    entry_in, entry_out = "wrwwwwwwww", "rrrrrlllbwwww"
    (
        joined_x, joined_bc, vbc, slope_x, slope_bc, pre, step, cum, s_part, end_state, decay,
        incoming, wz_out,
    ) = run(
        in_turn(
            functools.partial(entry_kernel, rows, n, chain), 1, entry_in + entry_out + "w" * 8
        ),
        blocks,
        list([
            info_in, by_rows(normed), whole(halo), params_in, whole(w_joined), whole(upper),
            whole(spread(0)), whole(e8), (w_z, None, "any"), (w_out.T, None, "any"),
        ]),
        list([
            by_rows(shape((rows, inner), bf16)),
            by_rows(shape((rows, 2 * states), bf16)),
            by_rows(shape((rows, width), bf16)),
            by_rows(shape((rows, inner), bf16)),
            by_rows(shape((rows, 2 * states), f32)),
            by_lanes(shape((HEAD_ROWS, rows), f32)),
            by_lanes(shape((HEAD_ROWS, rows), f32)),
            by_lanes(shape((HEAD_ROWS, rows), f32)),
            by_block(shape(state_dims, f32)),
            fixed(shape((states, inner), bf16)),
            fixed(shape((1, inner), f32)),
            fixed(shape((states, inner), bf16)),
            (shape((model, 2 * inner), bf16), None, "any"),
        ]),
        [
            pltpu.VMEM((STRETCH + 8, width), f32),
            pltpu.VMEM((states, inner), f32),
            pltpu.VMEM((1, inner), f32),
            pltpu.VMEM((states, inner), bf16),
            dma((n - 1, 2)),
            dma((n - 1, 2)),
            dma((2,)),
            dma((2,)),
        ],
        remote_id=4,
    )
    if chain > 2:
        incoming = entering(decay, end_state, "ctx", False)
    mix_in, mix_out = "wrllbwrrwwwww", "rrlbl"
    z_part, out, sums, state_in, branch = run(
        in_turn(functools.partial(mix_kernel, rows), subs, mix_in + mix_out + "wr"),
        blocks // subs,
        several(
            [
                info_in, by_rows(vbc), by_lanes(step), by_lanes(cum), by_block(s_part),
                whole(incoming), by_rows(normed), by_rows(grad_out), whole(wz_out), params_in,
                whole(spread(1)), whole(spread(2)), whole(e8),
            ],
            mix_in,
        ),
        several(
            [
                by_rows(shape((rows, inner), f32)),
                by_rows(shape((rows, inner), f32)),
                by_lanes(shape((2, rows), f32)),
                by_block(shape(state_dims, bf16)),
                by_lanes(shape((model, rows), bf16)),
            ],
            mix_out,
        ),
        [pltpu.VMEM((states, inner), f32), pltpu.VMEM((subs * STRETCH, STRETCH), f32)],
    )
    branch = lax.psum_scatter(branch, "tp", scatter_dimension=0, tiled=True)
    sums = total_over_tp(sums)
    g_z, g_b, g_c, normed_two, a_sum, gs_part, start_state, misc_gate = run(
        functools.partial(gate_kernel, rows),
        blocks,
        [
            info_in, by_lanes(sums, True), by_lanes(cum, True), by_rows(out, True),
            by_rows(z_part, True), by_rows(grad_out, True), whole(wz_out), by_rows(vbc, True),
            by_block(state_in, True),
            params_in, whole(spread(2)), whole(e8), whole(gather(0)),
        ],
        [
            by_rows(shape((rows, inner), bf16), True),
            by_rows(shape((rows, inner), bf16), True),
            by_rows(shape((rows, inner), bf16), True),
            by_rows(shape((rows, inner), bf16), True),
            by_lanes(shape((HEAD_ROWS, rows), f32), True),
            by_block(shape(state_dims, f32), True),
            fixed(shape((states, inner), bf16)),
            fixed(shape((8, inner), f32)),
        ],
        [pltpu.VMEM((states, inner), f32)],
    )
    sum_all = jnp.concatenate([gather(0), gather(1)[:inner]], axis=0)
    outgoing = entering(decay, start_state, "ctx", True)
    g_cat, tail, head, misc_scan, misc_dt = run(
        functools.partial(scan_kernel, rows),
        blocks,
        [
            info_in, by_rows(vbc, True), by_rows(g_b, True), by_rows(g_c, True),
            by_lanes(step, True), by_lanes(cum, True), by_lanes(pre, True), by_lanes(a_sum, True),
            by_block(state_in, True), by_block(gs_part, True), whole(outgoing),
            by_rows(slope_x, True), by_rows(slope_bc, True), by_rows(joined_x, True),
            by_rows(joined_bc, True), params_in, whole(spread(1)),
            whole(spread(2)), whole(e8), whole(sum_all), whole(lower),
        ],
        [
            by_rows(shape((rows, width + 128), bf16), True),
            fixed(shape((8, width), f32)),
            fixed(shape((8, width), f32)),
            fixed(shape((8, width), f32)),
            fixed(shape((2 * HEAD_ROWS, STRETCH), f32)),
        ],
        [
            pltpu.VMEM((states, inner), f32),
            pltpu.VMEM((8, width), f32),
            pltpu.VMEM((STRETCH, STRETCH), f32),
            pltpu.VMEM((STRETCH, STRETCH), f32),
            pltpu.VMEM((STRETCH, 3 * inner), bf16),
        ],
    )
    next_rows = passed_along(head, "ctx", -1)
    feature = jnp.arange(model, dtype=jnp.int32) // slice_width
    mine = (feature == tp_index).astype(f32)[None, :]
    last_joined = jnp.concatenate([joined_x[rows - 16 :], joined_bc[rows - 16 :]], axis=1)
    def exit_call(first, extra_in, extra_out, scratch):
        top = count = blocks

        def flipped(x):
            return (x, (STRETCH, x.shape[1]), lambda i: (top - 1 - i, 0))

        return run(
            functools.partial(exit_kernel, rows, top, first),
            count,
            [
                info_in, flipped(tokens), flipped(grad_out), whole(mine), flipped(g_z),
                flipped(g_cat), params_in, whole(wz_out), whole(w_joined),
            ]
            + extra_in,
            [
                (
                    shape((model, count * STRETCH), bf16),
                    (model, STRETCH),
                    lambda i: (0, count - 1 - i),
                ),
                fixed(shape((1, model), f32)),
            ]
            + extra_out,
            scratch,
        )

    g_resid, gain_part, rim, rim_w = exit_call(
        True,
        [whole(tail), whole(next_rows), whole(last_joined)],
        [fixed(shape((16, width), bf16)), fixed(shape((8, width), f32))],
        [pltpu.VMEM((16, width), f32)],
    )
    g_resid = lax.psum_scatter(g_resid, "tp", scatter_dimension=0, tiled=True)

    part_out = tn(grad_out, normed_two)
    part_z = tn(normed, g_z)
    part_cat = tn(normed, g_cat)
    part_rim = tn(normed[rows - 16 :], rim)
    part_cat = part_cat + jnp.pad(part_rim, ((0, 0), (0, 128)))
    s_out, s_z, s_cat, s_small, s_wide = reduced(
        (part_out, part_z, part_cat),
        (misc_scan, rim_w, misc_gate, misc_dt, gain_part),
        2 * states,
    )
    if lax.axis_size("ctx") > 2:
        s_out, s_z, s_cat, s_small, s_wide = jax.tree.map(
            lambda part: lax.psum(0.5 * part, "ctx"), (s_out, s_z, s_cat, s_small, s_wide)
        )
    grad_w_out = s_out.T
    grad_w_z = s_z
    grad_w_x = s_cat[:, :inner]
    grad_w_bc = s_cat[:, inner : inner + 2 * states]
    grad_w_dt = s_cat[:, inner + 2 * states : inner + 2 * states + heads]
    grad_conv_x_w = s_small[:taps, :inner]
    grad_conv_x_b = s_small[taps, :inner]
    grad_gate_gain = s_small[0, width : width + inner]
    grad_d_skip = jnp.sum(s_small[1, width : width + inner].reshape(heads, per_head), axis=1)
    dt_at = width + inner
    grad_a_log = jnp.sum(s_small[:heads, dt_at : dt_at + STRETCH], axis=1)
    grad_dt_bias = jnp.sum(s_small[:heads, dt_at + STRETCH : dt_at + 2 * STRETCH], axis=1)
    grad_conv_bc_w = s_wide[:taps, : 2 * states]
    grad_conv_bc_b = s_wide[taps, : 2 * states]
    here = tp_index * slice_width
    grad_norm_gain = lax.dynamic_slice_in_dim(s_wide[0, 2 * states :], here, slice_width, 0)
    place = tp_index.astype(jnp.int32)[None]

    wide = 2 * STRETCH
    layer_out = run(
        functools.partial(finish_kernel, tp_size),
        blocks // 2,
        [
            (place, None, "smem"),
            (branch, (slice_width, wide), lambda i: (0, i)),
            (tokens, (wide, model), lambda i: (i, 0)),
            (sums, (2, wide), lambda i: (0, i)),
        ],
        [(shape((slice_width, rows), bf16), (slice_width, wide), lambda i: (0, i))],
        [],
    )[0].T
    grad_tokens = g_resid.T
    return (
        layer_out, grad_tokens, grad_norm_gain, grad_w_z, grad_w_x, grad_w_bc, grad_w_dt,
        grad_conv_x_w, grad_conv_x_b, grad_conv_bc_w, grad_conv_bc_b, grad_dt_bias, grad_a_log,
        grad_d_skip, grad_gate_gain, grad_w_out,
    )


def solution(mesh):
    both = ("fsdp", "ctx")
    in_specs = (
        P(both, None), P(both, None), P("fsdp", None), P(), P("fsdp", "tp"), P("fsdp", "tp"),
        P("fsdp", None), P("fsdp", "tp"), P(None, "tp"), P("tp"), P(), P(), P("tp"), P("tp"),
        P("tp"), P("tp"), P("tp", "fsdp"),
    )
    out_specs = (
        P(both, "tp"), P(both, "tp"), P("tp"), P("fsdp", "tp"), P("fsdp", "tp"), P("fsdp", None),
        P("fsdp", "tp"), P(None, "tp"), P("tp"), P(), P(), P("tp"), P("tp"), P("tp"), P("tp"),
        P("tp", "fsdp"),
    )
    return jax.shard_map(local, mesh=mesh, in_specs=in_specs, out_specs=out_specs, check_vma=False)
```

```python
import functools

import jax
import jax.numpy as jnp
import numpy as np
from jax import lax
from jax.experimental import pallas as pl
from jax.experimental.pallas import tpu as pltpu
from jax.sharding import PartitionSpec as P

STRETCH = 256
TAPS = 4
INNER = 1536
HEAD_ROWS = 8
LOG2E = 1.4426950408889634

epsilon = 1e-05
f32 = jnp.float32
bf16 = jnp.bfloat16


def nn(left, right):
    return lax.dot_general(left, right, (((1,), (0,)), ((), ())), preferred_element_type=f32)


def nt(left, right):
    return lax.dot_general(left, right, (((1,), (1,)), ((), ())), preferred_element_type=f32)


def tn(left, right):
    return lax.dot_general(left, right, (((0,), (0,)), ((), ())), preferred_element_type=f32)


def halves(x):
    high = x.astype(bf16)
    return high, (x - high.astype(f32)).astype(bf16)


def thirds(x):
    high = x.astype(bf16)
    rest = x - high.astype(f32)
    mid = rest.astype(bf16)
    return high, mid, (rest - mid.astype(f32)).astype(bf16)


def exact_rows(x, ones_matrix):
    high, mid, low = thirds(x)
    r = HEAD_ROWS
    out = nn(jnp.concatenate([high, mid, low, jnp.zeros_like(low)], axis=0), ones_matrix)
    return out[:r] + out[r : 2 * r] + out[2 * r : 3 * r]


def columns_of(rows):
    have = sum(r.shape[0] for r in rows)
    pad = jnp.zeros((128 - have, rows[0].shape[1]), f32)
    cols = jnp.transpose(jnp.concatenate(list(rows) + [pad], axis=0))
    high, low = halves(cols)
    return cols, jnp.concatenate([high, low], axis=1)


def segment_start(pos, starts):
    found = jnp.zeros_like(pos)
    for s in starts:
        found = jnp.where(pos >= s, s, found)
    return found


def joined_ok(u, distance, starts):
    ok = jnp.ones(u.shape, jnp.bool_)
    for s in starts[1:]:
        ok = ok & jnp.logical_not((u < s) & (u + distance >= s))
    return ok


def iota(shape, axis):
    return lax.broadcasted_iota(jnp.int32, shape, axis)


def read_info(rows, lengths, block):
    first = lax.axis_index("ctx") * rows
    starts = [jnp.int32(0)]
    for k in range(lengths.shape[1] - 1):
        starts.append(starts[-1] + lengths[0, k])
    base = first + block * STRETCH
    end_start = segment_start(base + STRETCH - 1, starts)
    flag = jnp.where(end_start < base, 1.0, 0.0).astype(f32)
    return starts, base, end_start, flag


def norm_rows(tok):
    x = tok.astype(f32)
    inverse = lax.rsqrt(jnp.mean(x * x, axis=1, keepdims=True) + epsilon)
    return x * inverse, inverse


def lanes_of(column, e8):
    return jnp.sum(column * e8, axis=0, keepdims=True)


MESH = pl.DeviceIdType.MESH


def start_together(peers):
    barrier = pltpu.get_barrier_semaphore()
    for peer in peers:
        pl.semaphore_signal(barrier, inc=1, device_id=peer, device_id_type=MESH)
    pl.semaphore_wait(barrier, len(peers))


def remote(src, dst, sent, came, peer):
    return pltpu.make_async_remote_copy(
        src_ref=src, dst_ref=dst, send_sem=sent, recv_sem=came, device_id=peer, device_id_type=MESH
    )


def turned(index, distance, size):
    return lax.rem(index + distance + size, size)


def twin_of(index):
    parity = lax.rem(index, 2)
    return parity, index + 1 - 2 * parity


def entry_kernel(
    rows, n, chain, sub, subs, info, nrm, halo, par, wj, tri, ew, e8, w_z, w_out_t,
    jx_o, jb_o, vbc_o, sx_o, sb_o, pre_o, step_o, cum_o, s_o, end_o, dec_o, inc_o, wz_o,
    ext, run, dec, got, sent, came, own, hop,
):
    i = pl.program_id(0) * subs + sub
    skip = STRETCH * sub
    f = lax.axis_index("fsdp")
    here = lax.axis_index("ctx")
    _parity, twin = twin_of(here)
    peers = [{"fsdp": turned(f, d, n)} for d in range(1, n)] + [{"ctx": twin}]
    barrier = pltpu.get_barrier_semaphore()
    slab = w_z.shape[0]

    def at_first(body):
        if sub == 0:
            pl.when(pl.program_id(0) == 0)(body)

    def at_last(body):
        if sub == subs - 1:
            pl.when(pl.program_id(0) == pl.num_programs(0) - 1)(body)

    @at_first
    def _():
        for peer in peers:
            pl.semaphore_signal(barrier, inc=1, device_id=peer, device_id_type=MESH)

    def weight_copies():
        at = pl.ds(pl.multiple_of(f * slab, 16), slab)
        for p, ref in enumerate((w_z, w_out_t)):
            cols = slice(p * ref.shape[1], (p + 1) * ref.shape[1])
            target = wz_o.at[at, cols]
            yield pltpu.make_async_copy(ref, target, own.at[p])
            for d in range(1, n):
                yield remote(
                    ref, target, sent.at[d - 1, p], came.at[d - 1, p], {"fsdp": turned(f, d, n)}
                )

    starts, base, end_start, flag = read_info(rows, info, i)
    inner = jx_o.shape[1]
    width = inner + jb_o.shape[1]
    gain, cb, cw, taps = par[0:1, :], par[1:2, :], par[4:8, :], TAPS

    @at_first
    def _():
        unit, _inv = norm_rows(halo[...])
        before = nn((unit * gain).astype(bf16), wj[:, :width])
        ext[0:8, :] = before.astype(bf16).astype(f32)[8:16]
        run[...] = jnp.zeros_like(run)
        dec[...] = jnp.ones_like(dec)

    normed = nrm[...]
    product = nn(normed, wj[...])
    joined = product[:, :width].astype(bf16)
    jx_o[...] = joined[:, :inner]
    jb_o[...] = joined[:, inner:]
    ext[8 + skip : 8 + skip + STRETCH, :] = joined.astype(f32)
    pos = base + iota((STRETCH, 128), 0)
    first_of = segment_start(pos, starts)
    valid = [
        jnp.where(pos - (taps - 1 - k) >= first_of, 1.0, 0.0).astype(f32) for k in range(taps - 1)
    ]
    for g in range(width // 128):
        at = slice(128 * g, 128 * (g + 1))
        acc = cb[:, at] + cw[taps - 1 : taps, at] * ext[8 + skip : 8 + skip + STRETCH, at]
        for k in range(taps - 1):
            low = skip + 8 - (taps - 1) + k
            acc = acc + cw[k : k + 1, at] * (ext[low : low + STRETCH, at] * valid[k])
        sig = jax.nn.sigmoid(acc)
        act = acc * sig
        vbc_o[:, at] = act.astype(bf16)
        slope = sig + act * (1.0 - sig)
        if 128 * g < inner:
            sx_o[:, at] = slope.astype(bf16)
        else:
            sb_o[:, 128 * g - inner : 128 * (g + 1) - inner] = slope
    if sub == subs - 1:
        ext[0:8, :] = ext[skip + STRETCH : skip + STRETCH + 8, :]
    pre = jnp.transpose(product[:, width:])[:HEAD_ROWS] + par[8:16, 0:1]
    step = jax.nn.softplus(pre)
    logd = -step * jnp.exp(par[8:16, 1:2])
    cum = exact_rows(logd, tri[...])
    pre_o[...] = pre
    step_o[...] = step
    cum_o[...] = cum
    cum_e = cum[:, STRETCH - 1 : STRETCH]
    where_s = base + iota((1, STRETCH), 1)
    keep = jnp.where(where_s >= end_start, 1.0, 0.0).astype(f32)
    weight = jnp.exp(cum_e - cum) * step * keep
    _cols, both = columns_of([weight])
    spread = nn(both, ew[...])
    v = vbc_o[:, :inner].astype(f32)
    b = vbc_o[:, inner : inner + 128]
    state = tn(b, (v * spread).astype(bf16))
    s_o[0] = state
    through = lanes_of(jnp.exp(cum_e) * flag, e8[...])
    run[...] = through * run[...] + state
    dec[...] = dec[...] * through
    end_o[...] = run[...].astype(bf16)
    dec_o[...] = dec[...]

    @at_first
    def _():
        pl.semaphore_wait(barrier, len(peers))
        for copy in weight_copies():
            copy.start()

    @at_last
    def _():
        if chain == 2:
            copy = remote(end_o, got, hop.at[0], hop.at[1], {"ctx": twin})
            copy.start()
            copy.wait()
            inc_o[...] = jnp.where(here > 0, got[...], jnp.zeros_like(got))
        else:
            inc_o[...] = jnp.zeros_like(inc_o)
        for copy in weight_copies():
            copy.wait()


def view(ref, kind, sub):
    if kind == "r":
        return ref.at[pl.ds(STRETCH * sub, STRETCH), :]
    if kind == "l":
        return ref.at[:, pl.ds(STRETCH * sub, STRETCH)]
    if kind == "b":
        return ref.at[pl.ds(sub, 1)]
    return ref


def in_turn(kernel, subs, kinds):
    def body(*refs):
        for sub in range(subs):
            kernel(sub, subs, *[view(ref, kind, sub) for ref, kind in zip(refs, kinds)])

    return body


def mix_kernel(
    rows, sub, subs, info, vbc, step, cum, s_in, inc, normed, gout, wz_out, par, e_step, e_scale, e8,
    z_o, out_o, gn_o, sum_o, st_o, br_o,
    run, gram,
):
    i = pl.program_id(0) * subs + sub
    starts, base, _end_start, flag = read_info(rows, info, i)
    inner = out_o.shape[1]
    gain = par[2:3, :inner]
    dskip = lanes_of(par[8:16, 2:3], e8[...])

    if sub == 0:

        @pl.when(i == 0)
        def _():
            run[...] = inc[...].astype(f32)

    st = run[...].astype(bf16)
    st_o[0] = st
    cum_v = cum[...]
    cum_e = cum_v[:, STRETCH - 1 : STRETCH]
    through = lanes_of(jnp.exp(cum_e) * flag, e8[...])
    run[...] = through * run[...] + s_in[0]

    row_first = segment_start(base + iota((1, STRETCH), 1), starts)
    scale = jnp.exp(cum_v) * jnp.where(row_first < base, 1.0, 0.0).astype(f32)
    cum2 = cum_v * LOG2E
    cols, both = columns_of([cum2, step[...], scale])
    step_x = nn(both, e_step[...])
    scale_x = nn(both, e_scale[...])
    b = vbc[:, inner : inner + 128]
    c = vbc[:, inner + 128 : inner + 256]
    carried = nn(c, st) * scale_x
    half = STRETCH // 2
    low, high = slice(0, half), slice(half, STRETCH)
    t_at = iota((half, STRETCH), 0)
    s_at = iota((half, STRETCH), 1)
    causal = (s_at <= t_at)[:, low]
    first_low = segment_start(iota((half, half), 0) + base, starts)
    first_high = segment_start(t_at + (base + half), starts)
    mask_a = causal & ((s_at + base)[:, low] >= first_low)
    mask_b = (s_at <= t_at + half) & (s_at + base >= first_high)
    gram[low, low] = jnp.where(mask_a, nt(c[low], b[low]), 0.0)
    gram[high, :] = jnp.where(mask_b, nt(c[high], b), 0.0)
    lane = iota((STRETCH, 128), 1)
    pieces = []
    for p in range(inner // 128):
        at = slice(128 * p, 128 * (p + 1))
        v = vbc[:, at].astype(f32)
        sv = (v * step_x[:, at]).astype(bf16)
        rest = carried[:, at] + dskip[:, at] * v
        acc_low, acc_high = rest[low], rest[high]
        for j in range(2):
            h = 2 * p + j
            side = (lane < 64) if j == 0 else (lane >= 64)
            part = jnp.where(side, sv, jnp.zeros_like(sv))
            row = cum2[h : h + 1, :]
            first_gap = cols[low, h : h + 1] - row[:, low]
            cross_gap = cols[high, h : h + 1] - row[:, low]
            last_gap = cols[high, h : h + 1] - row[:, high]
            decay_b = jnp.concatenate(
                [jnp.exp2(cross_gap), jnp.exp2(jnp.minimum(last_gap, 0.0))], axis=1
            )
            decay_a = jnp.exp2(jnp.minimum(first_gap, 0.0))
            acc_low = acc_low + nn((gram[low, low] * decay_a).astype(bf16), part[low])
            acc_high = acc_high + nn((gram[high, :] * decay_b).astype(bf16), part)
        pieces.append(jnp.concatenate([acc_low, acc_high], axis=0))
    out = jnp.concatenate(pieces, axis=1)
    out_o[...] = out
    zf = nn(normed[...], wz_out[:, :inner])
    z_o[...] = zf
    gated = out * (zf * jax.nn.sigmoid(zf))
    gn = nn(gout[...], wz_out[:, inner:])
    gn_o[...] = gn
    gg = gated * gain
    br_o[...] = nt(wz_out[:, inner:], gg.astype(bf16)).astype(bf16)
    ss = jnp.sum(gated * gated, axis=1, keepdims=True)
    dq = jnp.sum(gn * gg, axis=1, keepdims=True)
    sum_o[...] = jnp.transpose(jnp.where(lane == 0, ss, dq))[0:2]


def gate_kernel(
    rows, info, sums, cum, out, z, gn, vc, st, par, e_scale, e8, f_sum,
    gz_o, gb_o, gc_o, n2_o, a_o, gs_o, start_o, misc_o,
    run,
):
    step_id = pl.program_id(0)
    blocks = pl.num_programs(0)
    i = blocks - 1 - step_id
    starts, base, _end_start, flag = read_info(rows, info, i)
    inner = z.shape[1]
    gain = par[2:3, :inner]
    dskip = lanes_of(par[8:16, 2:3], e8[...])

    @pl.when(step_id == 0)
    def _():
        run[...] = jnp.zeros_like(run)
        misc_o[...] = jnp.zeros_like(misc_o)

    alpha = lax.rsqrt(sums[0:1, :] / INNER + epsilon)
    beta = alpha * alpha * alpha * sums[1:2, :] / INNER
    cum_v = cum[...]
    row_first = segment_start(base + iota((1, STRETCH), 1), starts)
    scale = jnp.exp(cum_v) * jnp.where(row_first < base, 1.0, 0.0).astype(f32)
    cols, both = columns_of([alpha, beta, jnp.zeros((14, STRETCH), f32), scale])
    alpha_c = cols[:, 0:1]
    beta_c = cols[:, 1:2]
    scale_x = nn(both, e_scale[...])
    v = vc[:, :inner].astype(f32)
    c = vc[:, inner + 128 : inner + 256]
    zf = z[...]
    sig = jax.nn.sigmoid(zf)
    act = zf * sig
    o = out[...]
    gated = o * act
    g_n = gn[...]
    unit = gated * alpha_c
    g_gated = alpha_c * (g_n * gain) - beta_c * gated
    g_out = g_gated * act
    gz_o[...] = (g_gated * o * (sig + act * (1.0 - sig))).astype(bf16)
    gb = g_out.astype(bf16)
    gb_o[...] = gb
    n2_o[...] = (unit * gain).astype(bf16)
    misc_o[0:1, :] += jnp.sum(g_n * unit, axis=0, keepdims=True)
    misc_o[1:2, :] += jnp.sum(g_out * v, axis=0, keepdims=True)
    gf = gb.astype(f32)
    carried = nn(c, st[0]) * scale_x
    prod = gf * (o - dskip * v) + (g_out - gf) * carried
    high, low = halves(prod)
    sums_c = nn(jnp.concatenate([high, low], axis=1), f_sum[...])
    a_o[...] = jnp.transpose(sums_c)[0:HEAD_ROWS]
    gc = (g_out * scale_x).astype(bf16)
    gc_o[...] = gc
    gs = tn(c, gc)
    gs_o[0] = gs
    through = lanes_of(jnp.exp(cum_v[:, STRETCH - 1 : STRETCH]) * flag, e8[...])
    run[...] = through * run[...] + gs
    start_o[...] = run[...].astype(bf16)


def scan_kernel(
    rows, info, vbc, gb, gc, step, cum, pre, a_sum, st, gs_in, outg, sx, sb, jx, jb, par,
    e_step, e_w, e8, f_all, tril,
    gcat_o, tail_o, head_o, misc_o, dt_o,
    run, ext, gram, acc, prod,
):
    step_id = pl.program_id(0)
    blocks = pl.num_programs(0)
    i = blocks - 1 - step_id
    starts, base, end_start, flag = read_info(rows, info, i)
    inner = gb.shape[1]
    width = inner + jb.shape[1]
    cw, taps = par[4:8, :], TAPS
    rate = jnp.exp(par[8:16, 1:2])
    dskip = lanes_of(par[8:16, 2:3], e8[...])

    @pl.when(step_id == 0)
    def _():
        run[...] = outg[...].astype(f32)
        ext[...] = jnp.zeros((8, width), f32)
        misc_o[...] = jnp.zeros_like(misc_o)
        dt_o[...] = jnp.zeros_like(dt_o)

    cum_v = cum[...]
    step_v = step[...]
    cum_e = cum_v[:, STRETCH - 1 : STRETCH]
    after = run[...]
    low_after = after.astype(bf16)
    state = st[0]
    through = lanes_of(jnp.exp(cum_e) * flag, e8[...])
    g_through = jnp.sum(after * state.astype(f32), axis=0, keepdims=True) * through
    end_more = jnp.sum(e8[...] * g_through, axis=1, keepdims=True)
    run[...] = through * after + gs_in[0]

    where_s = base + iota((1, STRETCH), 1)
    row_first = segment_start(where_s, starts)
    end_decay = jnp.exp(cum_e - cum_v) * jnp.where(where_s >= end_start, 1.0, 0.0).astype(f32)
    weight = end_decay * step_v
    cum2 = cum_v * LOG2E
    ok_rows = [
        jnp.where(joined_ok(where_s, d, starts), 1.0, 0.0).astype(f32)
        for d in range(taps - 1, 0, -1)
    ]
    cols, both = columns_of([cum2, step_v, weight] + ok_rows)
    b = vbc[:, inner : inner + 128]
    c = vbc[:, inner + 128 : inner + 256]
    half = STRETCH // 2
    low, high = slice(0, half), slice(half, STRETCH)
    s_at = iota((half, STRETCH), 0)
    t_at = iota((half, STRETCH), 1)
    mask_a = (s_at <= t_at) & (s_at + base >= row_first)
    mask_b = (s_at <= t_at)[:, low] & ((s_at + (base + half)) >= row_first)[:, high]
    gram[low, :] = jnp.where(mask_a, nt(b[low], c), 0.0)
    gram[high, low] = jnp.where(mask_b, nt(b[high], c[high]), 0.0)
    acc[...] = jnp.zeros_like(acc)
    lane = iota((STRETCH, 128), 1)
    ok = [
        jnp.broadcast_to(cols[:, 3 * HEAD_ROWS + k : 3 * HEAD_ROWS + k + 1], (STRETCH, 128))
        for k in range(taps - 1)
    ]

    def convolve(at, own, j_f):
        following = ext[:, at]
        joint = jnp.concatenate([own, following], axis=0)
        ext[:, at] = own[0:8]
        misc_o[taps : taps + 1, at] += jnp.sum(own, axis=0, keepdims=True)
        misc_o[taps - 1 : taps, at] += jnp.sum(own * j_f, axis=0, keepdims=True)
        total = own * cw[taps - 1 : taps, at]
        for k in range(taps - 1):
            d = taps - 1 - k
            term = pltpu.roll(joint, STRETCH + 8 - d, axis=0)[:STRETCH] * ok[k]
            misc_o[k : k + 1, at] += jnp.sum(term * j_f, axis=0, keepdims=True)
            total = total + term * cw[k : k + 1, at]
        gcat_o[:, at] = total.astype(bf16)
        tail_o[:, at] = jnp.where(step_id == 0, total[STRETCH - 8 :], tail_o[:, at])

    g_b = jnp.zeros((STRETCH, 128), f32)
    g_c = jnp.zeros((STRETCH, 128), f32)
    for p in range(inner // 128):
        at = slice(128 * p, 128 * (p + 1))
        step_x = nn(both, e_step[:, at])
        v = vbc[:, at].astype(f32)
        sv = (v * step_x).astype(bf16)
        g_pair = gb[:, at]
        u_low = jnp.zeros((half, 128), f32)
        u_high = jnp.zeros((half, 128), f32)
        for j in range(2):
            h = 2 * p + j
            side = (lane < 64) if j == 0 else (lane >= 64)
            g_side = jnp.where(side, g_pair, jnp.zeros_like(g_pair))
            sv_side = jnp.where(side, sv, jnp.zeros_like(sv))
            row = cum2[h : h + 1, :]
            first_gap = row[:, low] - cols[low, h : h + 1]
            cross_gap = row[:, high] - cols[low, h : h + 1]
            last_gap = row[:, high] - cols[high, h : h + 1]
            decay_a = jnp.concatenate(
                [jnp.exp2(jnp.minimum(first_gap, 0.0)), jnp.exp2(cross_gap)], axis=1
            )
            decay_b = jnp.exp2(jnp.minimum(last_gap, 0.0))
            u_low = u_low + nn((gram[low, :] * decay_a).astype(bf16), g_side)
            u_high = u_high + nn((gram[high, low] * decay_b).astype(bf16), g_side[high])
            acc[low, :] += nt(sv_side[low], g_pair) * decay_a
            acc[high, low] += nt(sv_side[high], g_pair[high]) * decay_b
        u = jnp.concatenate([u_low, u_high], axis=0)
        w_x = nn(both, e_w[:, at])
        y = nn(b, low_after[:, at])
        h1, l1 = halves(sv.astype(f32) * u)
        prod[:, at] = h1
        prod[:, inner + 128 * p : inner + 128 * (p + 1)] = l1
        prod[:, 2 * inner + 128 * p : 2 * inner + 128 * (p + 1)] = (v * y).astype(bf16)
        g_b = g_b + nt((v * w_x).astype(bf16), low_after[:, at])
        g_c = g_c + nt(gc[:, at], state[:, at])
        gv = dskip[:, at] * g_pair.astype(f32) + step_x * u + w_x * y
        convolve(at, gv * sx[:, at].astype(f32), jx[:, at].astype(f32))

    gg_a = jnp.where(mask_a, acc[low, :], 0.0).astype(bf16)
    gg_b = jnp.where(mask_b, acc[high, low], 0.0).astype(bf16)
    g_b = g_b + jnp.concatenate([nn(gg_a, c), nn(gg_b, c[high])], axis=0)
    g_c = g_c + tn(gg_a, b[low])
    g_c = g_c + jnp.concatenate([jnp.zeros((half, 128), f32), tn(gg_b, b[high])], axis=0)
    for k, part in enumerate((g_b, g_c)):
        here = slice(128 * k, 128 * (k + 1))
        convolve(
            slice(inner + 128 * k, inner + 128 * (k + 1)),
            part * sb[:, here],
            jb[:, here].astype(f32),
        )

    sums_r = jnp.transpose(nn(prod[...], f_all[...]))
    g_mixed = sums_r[0:HEAD_ROWS]
    g_end = sums_r[HEAD_ROWS : 2 * HEAD_ROWS]
    ends = g_end * weight
    g_cum = a_sum[...] - g_mixed - ends
    end_add = jnp.sum(ends, axis=1, keepdims=True) + end_more
    g_log = exact_rows(g_cum, tril[...]) + end_add
    slope_dt = jax.nn.sigmoid(pre[...])
    ratio = jnp.where(step_v > 0.0, slope_dt / step_v, 1.0)
    g_pre_dt = (g_end * end_decay - g_log * rate) * slope_dt + g_mixed * ratio
    dt_o[0:HEAD_ROWS, :] += g_log * (-step_v * rate)
    dt_o[HEAD_ROWS:, :] += g_pre_dt
    pad = jnp.zeros((128 - HEAD_ROWS, STRETCH), f32)
    gcat_o[:, width:] = jnp.transpose(jnp.concatenate([g_pre_dt, pad], axis=0)).astype(bf16)

    head_o[...] = ext[...]


def exit_kernel(
    rows, blocks, rim_side, info, tok, gout, mine, gz, gcat, par, wz_out, wj, *rest
):
    step_id = pl.program_id(0)
    i = blocks - 1 - step_id
    starts, base, _end_start, _flag = read_info(rows, info, i)
    inner = gz.shape[1]
    if rim_side:
        tail, nxt, last_j, gr_o, gain_o, rim_o, rim_w_o, fix = rest
        taps, width = TAPS, tail.shape[1]
        cw = par[4:8, :width]
    else:
        gr_o, gain_o = rest
    gain = par[0:1, :]

    g_normed = nt(gz[...], wz_out[:, :inner]) + nt(gcat[...], wj[...])

    def finish(g_normed):
        unit, inverse = norm_rows(tok[...])
        scaled = g_normed * gain
        mean = jnp.mean(scaled * unit, axis=1, keepdims=True)
        own = gout[...].astype(f32) * mine[...]
        gr_o[...] = jnp.transpose(own + inverse * (scaled - unit * mean)).astype(bf16)
        gain_o[...] += jnp.sum(g_normed * unit, axis=0, keepdims=True)

    @pl.when(step_id == 0)
    def _():
        gain_o[...] = jnp.zeros_like(gain_o)

    if not rim_side:
        finish(g_normed)
        return

    @pl.when(step_id == 0)
    def _():
        fix[0:8, :] = jnp.zeros((8, width), f32)
        fix[8:16, :] = nxt[...]
        places = base + STRETCH - 8 + iota((8, 128), 0)
        wide = last_j[8:16, :].astype(f32)
        total = tail[...]
        for k in range(taps - 1):
            d = taps - 1 - k
            ok = jnp.where(joined_ok(places, d, starts), 1.0, 0.0).astype(f32)
            inside = jnp.where(iota((8, width), 0) >= 8 - d, fix[d : d + 8, :], 0.0)
            term = inside * jnp.concatenate([ok] * (width // 128), axis=1)
            total = total + term * cw[k : k + 1, :]
            rim_w_o[k : k + 1, :] = jnp.sum(term * wide, axis=0, keepdims=True)
        rim_w_o[taps - 1 : 8, :] = jnp.zeros((9 - taps, width), f32)
        fix[0:8, :] = jnp.zeros((8, width), f32)
        fix[8:16, :] = total.astype(bf16).astype(f32) - tail[...].astype(bf16).astype(f32)
        rim_o[...] = fix[...].astype(bf16)

    @pl.when(step_id == 0)
    def _():
        more = nt(rim_o[...], wj[:, :width])
        finish(g_normed + jnp.concatenate([jnp.zeros((STRETCH - 16, more.shape[1]), f32), more]))

    @pl.when(step_id > 0)
    def _():
        finish(g_normed)


def finish_kernel(parts, place, part, base, sums, out):
    wide = part[...].astype(f32) * lax.rsqrt(sums[0:1, :] / INNER + epsilon)
    size = out.shape[0]
    for k in range(parts):

        @pl.when(place[0] == k)
        def _():
            add = jnp.transpose(base[:, size * k : size * (k + 1)].astype(f32))
            out[...] = (wide + add).astype(bf16)


def gather_kernel(
    n, chain, x, bc, dt, par, tok, out, halo, nrm, sent, came, passed, relayed, own, hop
):
    f = lax.axis_index("fsdp")
    parity, twin = twin_of(lax.axis_index("ctx"))
    rows = x.shape[0]
    half = rows // 2
    here = lax.axis_index("ctx")
    following = turned(here, 1, chain)
    sides = [{"ctx": twin}] if chain == 2 else [{"ctx": following}, {"ctx": turned(here, -1, chain)}]
    start_together([{"fsdp": turned(f, d, n)} for d in range(1, n)] + sides)
    pieces = []
    at = 0
    for ref in (x, bc, dt):
        pieces.append((ref, slice(at, at + ref.shape[1])))
        at += ref.shape[1]

    def place(source, side):
        return pl.ds(pl.multiple_of(source * rows + side * half, 16), half)

    mine = pl.ds(pl.multiple_of(parity * half, 16), half)
    copies = []
    for d in range(1, n):
        for p, (ref, cols) in enumerate(pieces):
            copy = remote(
                ref.at[mine, :], out.at[place(f, parity), cols],
                sent.at[d - 1, p], came.at[d - 1, p], {"fsdp": turned(f, d, n)},
            )
            copy.start()
            copies.append(copy)
    edge = halo.shape[0]
    copy = remote(
        tok.at[pl.ds(tok.shape[0] - edge, edge), :], halo, hop.at[0], hop.at[1], {"ctx": following}
    )
    copy.start()
    locals_ = [copy]
    for p, (ref, cols) in enumerate(pieces):
        copy = pltpu.make_async_copy(
            ref, out.at[pl.ds(pl.multiple_of(f * rows, 16), rows), cols], own.at[p]
        )
        copy.start()
        locals_.append(copy)
    gain = par[...][None, :]

    def norm_block(tok_block, nrm_block):
        unit, _inverse = norm_rows(tok_block[...])
        nrm_block[...] = (unit * gain).astype(bf16)

    block = pl.BlockSpec((2 * STRETCH, tok.shape[1]), lambda i: (i, 0))
    pltpu.emit_pipeline(
        norm_block, grid=(tok.shape[0] // (2 * STRETCH),), in_specs=[block], out_specs=[block]
    )(tok, nrm)

    relays = []
    for d in range(1, n):
        source = turned(f, -d, n)
        for p, (ref, cols) in enumerate(pieces):
            copies[(d - 1) * len(pieces) + p].wait_recv()
            piece = out.at[place(source, parity), cols]
            copy = remote(piece, piece, passed.at[d - 1, p], relayed.at[d - 1, p], {"ctx": twin})
            copy.start()
            relays.append(copy)
    for copy in copies:
        copy.wait_send()
    for copy in locals_:
        copy.wait()
    for copy in relays:
        copy.wait()


def gathered(x, bc, dt, par, tok):
    n = lax.axis_size("fsdp")
    pieces = (n - 1, 3)
    width = x.shape[1] + bc.shape[1] + dt.shape[1]
    return pl.pallas_call(
        functools.partial(gather_kernel, n, lax.axis_size("ctx")),
        out_shape=[
            jax.ShapeDtypeStruct((n * x.shape[0], width), bf16),
            jax.ShapeDtypeStruct((16, tok.shape[1]), bf16),
            jax.ShapeDtypeStruct(tok.shape, bf16),
        ],
        in_specs=[pl.BlockSpec(memory_space=pltpu.VMEM)] * 4 + [pl.BlockSpec(memory_space=pl.ANY)],
        out_specs=[pl.BlockSpec(memory_space=pltpu.VMEM)] * 2
        + [pl.BlockSpec(memory_space=pl.ANY)],
        scratch_shapes=[pltpu.SemaphoreType.DMA(pieces)] * 4
        + [pltpu.SemaphoreType.DMA((3,)), pltpu.SemaphoreType.DMA((2,))],
        compiler_params=pltpu.CompilerParams(collective_id=1, has_side_effects=True),
    )(x, bc, dt, par, tok)


def total_kernel(n, part, out, slots, sent, came):
    me = lax.axis_index("tp")
    start_together([{"tp": turned(me, d, n)} for d in range(1, n)])
    copies = []
    for d in range(1, n):
        copy = remote(
            part, slots.at[d - 1], sent.at[d - 1], came.at[d - 1], {"tp": turned(me, d, n)}
        )
        copy.start()
        copies.append(copy)
    total = part[...]
    for d in range(1, n):
        copies[d - 1].wait_recv()
        total = total + slots[d - 1]
    out[...] = total
    for copy in copies:
        copy.wait_send()


def total_over_tp(part):
    n = lax.axis_size("tp")
    return pl.pallas_call(
        functools.partial(total_kernel, n),
        out_shape=jax.ShapeDtypeStruct(part.shape, f32),
        in_specs=[pl.BlockSpec(memory_space=pltpu.VMEM)],
        out_specs=pl.BlockSpec(memory_space=pltpu.VMEM),
        scratch_shapes=[
            pltpu.VMEM((n - 1,) + part.shape, f32),
            pltpu.SemaphoreType.DMA((n - 1,)),
            pltpu.SemaphoreType.DMA((n - 1,)),
        ],
        compiler_params=pltpu.CompilerParams(collective_id=2, has_side_effects=True),
    )(part)


def share_over_tp(m, t, shares, sent, came):
    copies = []
    for p, (buf, own) in enumerate(shares):
        buf[pl.ds(t, 1)] = own[None]
    for d in range(1, m):
        for p, (buf, _own) in enumerate(shares):
            k = 3 * (d - 1) + p
            copy = remote(buf.at[t], buf.at[t], sent.at[k], came.at[k], {"tp": turned(t, d, m)})
            copy.start()
            copies.append(copy)
    for copy in copies:
        copy.wait()
    totals = []
    for buf, _own in shares:
        total = buf[0].astype(f32)
        for q in range(1, m):
            total = total + buf[q].astype(f32)
        totals.append(total)
    return totals


def fold_over_tp(m, t, shares, sent, came):
    at_edge = (t == 0) | (t == 3)
    in_middle = jnp.logical_not(at_edge)
    inward = jnp.where(t == 0, 1, 2)
    outward = jnp.where(t == 1, 0, 3)
    across = 3 - t

    def copy_of(phase, p, src, dst, peer):
        buf = shares[p][0]
        k = 3 * phase + p
        return remote(buf.at[src], buf.at[dst], sent.at[k], came.at[k], {"tp": peer})

    every = range(len(shares))
    for buf, own in shares:
        buf[0] = own

    @pl.when(at_edge)
    def _():
        for p in every:
            copy_of(0, p, 0, 1, inward).start()
        for p in every:
            copy_of(0, p, 0, 1, inward).wait_send()
        for p in every:
            copy_of(2, p, 4, 4, inward).wait_recv()

    @pl.when(in_middle)
    def _():
        for p in every:
            buf = shares[p][0]
            copy_of(0, p, 0, 1, outward).wait_recv()
            buf[2] = (buf[0].astype(f32) + buf[1].astype(f32)).astype(buf.dtype)
            copy_of(1, p, 2, 3, across).start()
        for p in every:
            buf = shares[p][0]
            copy_of(1, p, 2, 3, across).wait()
            buf[4] = (buf[2].astype(f32) + buf[3].astype(f32)).astype(buf.dtype)
            copy_of(2, p, 4, 4, outward).start()
        for p in every:
            copy_of(2, p, 4, 4, outward).wait_send()

    return [buf[4].astype(f32) for buf, _own in shares]


def reduce_kernel(
    n, m, bc_cols, conv_bc,
    p_out, p_z, p_cat, m_scan, m_rim, m_gate, m_dt, m_gain,
    o_all, o_small, o_wide,
    give, take, mid, slots, final, bc_slots, small, small_slots, wide_slots, gain_slots,
    s1, r1, s2, r2, s3, r3, s4, r4,
):
    f = lax.axis_index("fsdp")
    t = lax.axis_index("tp")
    parity, twin = twin_of(lax.axis_index("ctx"))
    start_together(
        [{"ctx": twin}]
        + [{"fsdp": turned(f, d, n)} for d in range(1, n)]
        + [{"tp": turned(t, d, m)} for d in range(1, m)]
    )
    inner = p_out.shape[1]
    rows = p_out.shape[0] // n
    half = rows // 2

    def piece(q, side):
        at = pl.ds(pl.multiple_of(q * rows + side * half, 16), half)
        return jnp.concatenate([p_out[at, :], p_z[at, :], p_cat[at, :]], axis=1)

    copies = []
    for q in range(n):
        give[q] = piece(q, 1 - parity).astype(bf16)
        copy = remote(give.at[q], take.at[q], s1.at[q], r1.at[q], {"ctx": twin})
        copy.start()
        copies.append(copy)
    w_scan = m_scan.shape[1]
    w_gate = m_gate.shape[1]
    w_dt = m_dt.shape[1]
    small[...] = jnp.zeros_like(small)
    small[:, 0:w_scan] = m_scan[...] + m_rim[...]
    at = w_scan
    small[:, at : at + w_gate] = m_gate[...]
    at += w_gate
    small[:, at : at + w_dt] = m_dt[0:8, :]
    small[:, at + w_dt : at + 2 * w_dt] = m_dt[8:16, :]
    at += 2 * w_dt
    small[0:1, at:] = m_gain[...]
    small_slots[0, pl.ds(parity, 1)] = small[...][None]
    copy = remote(
        small, small_slots.at[0, parity], s1.at[n], r1.at[n], {"ctx": twin}
    )
    copy.start()
    copies.append(copy)

    copies[n].wait()
    small_slots[1, pl.ds(f, 1)] = (small_slots[0, 0] + small_slots[0, 1])[None]
    seconds = []
    for d in range(1, n):
        copy = remote(
            small_slots.at[1, f], small_slots.at[1, f], s2.at[n - 1 + d - 1], r2.at[n - 1 + d - 1],
            {"fsdp": turned(f, d, n)},
        )
        copy.start()
        seconds.append(copy)
    for q in range(n):
        copies[q].wait()
        mid[q] = (piece(q, parity) + take[q].astype(f32)).astype(bf16)
    slots[pl.ds(f, 1)] = mid[pl.ds(f, 1)]
    for d in range(1, n):
        peer = turned(f, d, n)
        copy = remote(
            mid.at[peer], slots.at[f], s2.at[d - 1], r2.at[d - 1], {"fsdp": peer}
        )
        copy.start()
        seconds.append(copy)
    for copy in seconds:
        copy.wait()
    small_sum = small_slots[1, 0]
    whole = slots[0].astype(f32)
    for q in range(1, n):
        small_sum = small_sum + small_slots[1, q]
        whole = whole + slots[q].astype(f32)
    final[...] = whole
    bc_at = slice(3 * inner, 3 * inner + bc_cols)
    o_small[...] = small_sum[:, :at]
    shares = (
        (bc_slots, whole[:, bc_at].astype(bf16)),
        (wide_slots, small_sum[:, conv_bc:w_scan]),
        (gain_slots, small_sum[0:1, at:]),
    )
    bc_sum, wide_sum, gain_sum = (fold_over_tp if m == 4 else share_over_tp)(m, t, shares, s3, r3)
    o_wide[:, :bc_cols] = wide_sum
    o_wide[:, bc_cols:] = jnp.broadcast_to(gain_sum, (8, gain_sum.shape[1]))
    final[:, bc_at] = bc_sum
    here = pl.ds(pl.multiple_of(parity * half, 8), half)
    o_all[here, :] = final[...]
    copy = remote(final, o_all.at[here, :], s4.at[0], r4.at[0], {"ctx": twin})
    copy.start()
    copy.wait()


def reduced(parts, miscs, bc_cols):
    n, m = lax.axis_size("fsdp"), lax.axis_size("tp")
    p_out, _p_z, p_cat = parts
    rows = p_out.shape[0] // n
    half = rows // 2
    inner = p_out.shape[1]
    wide = 2 * inner + p_cat.shape[1]
    m_scan, _m_rim, m_gate, m_dt, m_gain = miscs
    kept = m_scan.shape[1] + m_gate.shape[1] + 2 * m_dt.shape[1]
    small = kept + m_gain.shape[1]
    crossing = m_scan.shape[1] - inner + m_gain.shape[1]
    dma = pltpu.SemaphoreType.DMA

    def shape(*dims):
        return jax.ShapeDtypeStruct(dims, f32)

    return pl.pallas_call(
        functools.partial(reduce_kernel, n, m, bc_cols, inner),
        out_shape=[
            shape(rows, wide), shape(8, kept), shape(8, crossing),
        ],
        in_specs=[pl.BlockSpec(memory_space=pltpu.VMEM)] * 8,
        out_specs=[pl.BlockSpec(memory_space=pltpu.VMEM)] * 3,
        scratch_shapes=[
            pltpu.VMEM((n, half, wide), bf16),
            pltpu.VMEM((n, half, wide), bf16),
            pltpu.VMEM((n, half, wide), bf16),
            pltpu.VMEM((n, half, wide), bf16),
            pltpu.VMEM((half, wide), f32),
            pltpu.VMEM((max(m, 5), half, bc_cols), bf16),
            pltpu.VMEM((8, small), f32),
            pltpu.VMEM((2, max(n, 2), 8, small), f32),
            pltpu.VMEM((max(m, 5), 8, bc_cols), f32),
            pltpu.VMEM((max(m, 5), 1, m_gain.shape[1]), f32),
            dma((n + 1,)), dma((n + 1,)), dma((2 * n - 2,)), dma((2 * n - 2,)),
            dma((3 * m,)), dma((3 * m,)), dma((1,)), dma((1,)),
        ],
        compiler_params=pltpu.CompilerParams(
            collective_id=3, has_side_effects=True, vmem_limit_bytes=48 * 1024 * 1024
        ),
    )(*parts, *miscs)


def constants(inner, heads):
    lane_head = np.arange(inner) // (inner // heads)
    e8 = (np.arange(HEAD_ROWS)[:, None] == lane_head[None, :]).astype(np.float32)

    def spread(kind):
        m = np.zeros((128, inner), np.float32)
        m[HEAD_ROWS * kind : HEAD_ROWS * (kind + 1)] = e8
        return jnp.asarray(np.concatenate([m, m], axis=0), bf16)

    def gather(kind):
        m = np.zeros((inner, 128), np.float32)
        m[:, HEAD_ROWS * kind : HEAD_ROWS * (kind + 1)] = e8.T
        return jnp.asarray(np.concatenate([m, m], axis=0), bf16)

    at = np.arange(STRETCH)
    upper = jnp.asarray((at[:, None] <= at[None, :]).astype(np.float32), bf16)
    lower = jnp.asarray((at[:, None] >= at[None, :]).astype(np.float32), bf16)
    return jnp.asarray(e8), spread, gather, upper, lower


def passed_along(block, axis, distance):
    devices = range(lax.axis_size(axis))
    route = [(i - distance, i) for i in devices if i - distance in devices]
    return lax.ppermute(block, axis, route)


def entering(decay, state, axis, reverse):
    size = lax.axis_size(axis)
    if size == 2:
        return passed_along(state, axis, -1 if reverse else 1)
    index = lax.axis_index(axis)
    decays = lax.all_gather(decay.astype(bf16), axis)
    states = lax.all_gather(state, axis)

    def lap(k, before):
        at = size - 1 - k if reverse else k
        reached = at > index if reverse else at < index
        new = decays[at].astype(f32) * before + states[at].astype(f32)
        return jnp.where(reached, new, before)

    return lax.fori_loop(0, size, lap, jnp.zeros(state.shape, f32)).astype(bf16)


def fill_params(raw, par):
    gain, gate, x_w, bc_w, x_b, bc_b, bias, rate, skip = raw
    inner = x_w.shape[1]
    width = inner + bc_w.shape[1]
    heads = bias.shape[0]

    @pl.when(pl.program_id(0) == 0)
    def _():
        par[0:1, :] = gain[...][None, :]
        par[1:2, :inner] = x_b[...][None, :]
        par[1:2, inner:width] = bc_b[...][None, :]
        par[2:3, :inner] = gate[...][None, :]
        par[4:8, :inner] = x_w[...]
        par[4:8, inner:width] = bc_w[...]
        row, lane = iota((HEAD_ROWS, 128), 0), iota((HEAD_ROWS, 128), 1)
        table = jnp.zeros((HEAD_ROWS, 128), f32)
        for h in range(heads):
            for k, ref in enumerate((bias, rate, skip)):
                table = jnp.where((row == h) & (lane == k), ref[h], table)
        par[8:16, 0:128] = table


def call(kernel, blocks, ins, outs, scratch, remote_id=None, raw=None):
    def spec(shape, how):
        if how == "smem":
            return pl.BlockSpec(memory_space=pltpu.SMEM)
        if how == "any":
            return pl.BlockSpec(memory_space=pl.ANY)
        return pl.BlockSpec(shape, how)

    places = [k for k, (_a, _s, how) in enumerate(ins) if how == "par"]
    ins = [entry for entry in ins if entry[2] != "par"]
    body = kernel
    if places:
        count = len(raw)
        model = raw[0].shape[0]
        scratch = list(scratch) + [pltpu.VMEM((16, model), f32)]

        def body(*refs):
            par = refs[-1]
            fill_params(refs[:count], par)
            rest = list(refs[count:-1])
            rest.insert(places[0], par)
            kernel(*rest)

        def fixed_at(x):
            if x.ndim == 1 and x.shape[0] < 128:
                return (x, None, "smem")
            return (x, x.shape, lambda i: (0,) * x.ndim)

        ins = [fixed_at(x) for x in raw] + ins

    return pl.pallas_call(
        body,
        grid=(blocks,),
        in_specs=[spec(shape, how) for _a, shape, how in ins],
        out_specs=[spec(shape, how) for _s, shape, how in outs],
        out_shape=[s for s, _sh, _h in outs],
        scratch_shapes=scratch,
        compiler_params=pltpu.CompilerParams(
            dimension_semantics=("arbitrary",),
            vmem_limit_bytes=56 * 1024 * 1024,
            collective_id=remote_id,
            has_side_effects=remote_id is not None,
        ),
    )(*[a for a, _s, _h in ins])


def local(
    tokens, grad_out, lengths, norm_gain, w_z, w_x, w_bc, w_dt, conv_x_w, conv_x_b,
    conv_bc_w, conv_bc_b, dt_bias, a_log, d_skip, gate_gain, w_out,
):
    rows, model = tokens.shape
    inner = w_z.shape[1]
    heads = dt_bias.shape[0]
    states = w_bc.shape[1] // 2
    taps = conv_x_w.shape[0]
    blocks = rows // STRETCH
    width = inner + 2 * states
    tp_size = lax.axis_size("tp")
    slice_width = model // tp_size
    tp_index = lax.axis_index("tp")
    ctx_index = lax.axis_index("ctx")
    e8, spread, gather, upper, lower = constants(inner, heads)

    per_head = inner // heads

    w_joined, halo, normed = gathered(
        w_x, w_bc, jnp.pad(w_dt, ((0, 0), (0, 128 - heads))), norm_gain, tokens
    )
    n = lax.axis_size("fsdp")
    chain = lax.axis_size("ctx")

    def shape(dims, kind):
        return jax.ShapeDtypeStruct(dims, kind)

    def whole(x):
        return (x, x.shape, lambda i: (0,) * x.ndim)

    def by_rows(x, flip=False):
        if flip:
            return (x, (STRETCH, x.shape[1]), lambda i: (blocks - 1 - i, 0))
        return (x, (STRETCH, x.shape[1]), lambda i: (i, 0))

    def by_lanes(x, flip=False):
        if flip:
            return (x, (x.shape[0], STRETCH), lambda i: (0, blocks - 1 - i))
        return (x, (x.shape[0], STRETCH), lambda i: (0, i))

    def by_block(x, flip=False):
        if flip:
            return (x, (1,) + x.shape[1:], lambda i: (blocks - 1 - i, 0, 0))
        return (x, (1,) + x.shape[1:], lambda i: (i, 0, 0))

    def fixed(x):
        return (x, x.shape, lambda i: (0,) * len(x.shape))

    info_in = (lengths, None, "smem")
    params_in = (None, None, "par")
    raw = (
        norm_gain, gate_gain, conv_x_w, conv_bc_w, conv_x_b, conv_bc_b, dt_bias, a_log, d_skip
    )
    run = functools.partial(call, raw=raw)
    state_dims = (blocks, states, inner)
    subs = 2 if blocks % 2 == 0 else 1

    def several(entries, kinds):
        scales = {"r": (subs, 1), "l": (1, subs), "b": (subs, 1, 1)}
        grown = []
        for entry, kind in zip(entries, kinds):
            if kind == "w":
                grown.append(entry)
                continue
            dims = tuple(d * k for d, k in zip(entry[1], scales[kind]))
            grown.append((entry[0], dims, entry[2]))
        return grown

    dma = pltpu.SemaphoreType.DMA
    entry_in, entry_out = "wrwwwwwwww", "rrrrrlllbwwww"
    (
        joined_x, joined_bc, vbc, slope_x, slope_bc, pre, step, cum, s_part, end_state, decay,
        incoming, wz_out,
    ) = run(
        in_turn(
            functools.partial(entry_kernel, rows, n, chain), 1, entry_in + entry_out + "w" * 8
        ),
        blocks,
        list([
            info_in, by_rows(normed), whole(halo), params_in, whole(w_joined), whole(upper),
            whole(spread(0)), whole(e8), (w_z, None, "any"), (w_out.T, None, "any"),
        ]),
        list([
            by_rows(shape((rows, inner), bf16)),
            by_rows(shape((rows, 2 * states), bf16)),
            by_rows(shape((rows, width), bf16)),
            by_rows(shape((rows, inner), bf16)),
            by_rows(shape((rows, 2 * states), f32)),
            by_lanes(shape((HEAD_ROWS, rows), f32)),
            by_lanes(shape((HEAD_ROWS, rows), f32)),
            by_lanes(shape((HEAD_ROWS, rows), f32)),
            by_block(shape(state_dims, f32)),
            fixed(shape((states, inner), bf16)),
            fixed(shape((1, inner), f32)),
            fixed(shape((states, inner), bf16)),
            (shape((model, 2 * inner), bf16), None, "any"),
        ]),
        [
            pltpu.VMEM((STRETCH + 8, width), f32),
            pltpu.VMEM((states, inner), f32),
            pltpu.VMEM((1, inner), f32),
            pltpu.VMEM((states, inner), bf16),
            dma((n - 1, 2)),
            dma((n - 1, 2)),
            dma((2,)),
            dma((2,)),
        ],
        remote_id=4,
    )
    if chain > 2:
        incoming = entering(decay, end_state, "ctx", False)
    mix_in, mix_out = "wrllbwrrwwwww", "rrrlbl"
    z_part, out, gn, sums, state_in, branch = run(
        in_turn(functools.partial(mix_kernel, rows), subs, mix_in + mix_out + "wr"),
        blocks // subs,
        several(
            [
                info_in, by_rows(vbc), by_lanes(step), by_lanes(cum), by_block(s_part),
                whole(incoming), by_rows(normed), by_rows(grad_out), whole(wz_out), params_in,
                whole(spread(1)), whole(spread(2)), whole(e8),
            ],
            mix_in,
        ),
        several(
            [
                by_rows(shape((rows, inner), f32)),
                by_rows(shape((rows, inner), f32)),
                by_rows(shape((rows, inner), f32)),
                by_lanes(shape((2, rows), f32)),
                by_block(shape(state_dims, bf16)),
                by_lanes(shape((model, rows), bf16)),
            ],
            mix_out,
        ),
        [pltpu.VMEM((states, inner), f32), pltpu.VMEM((subs * STRETCH, STRETCH), f32)],
    )
    branch = lax.psum_scatter(branch, "tp", scatter_dimension=0, tiled=True)
    sums = total_over_tp(sums)
    g_z, g_b, g_c, normed_two, a_sum, gs_part, start_state, misc_gate = run(
        functools.partial(gate_kernel, rows),
        blocks,
        [
            info_in, by_lanes(sums, True), by_lanes(cum, True), by_rows(out, True),
            by_rows(z_part, True), by_rows(gn, True), by_rows(vbc, True), by_block(state_in, True),
            params_in, whole(spread(2)), whole(e8), whole(gather(0)),
        ],
        [
            by_rows(shape((rows, inner), bf16), True),
            by_rows(shape((rows, inner), bf16), True),
            by_rows(shape((rows, inner), bf16), True),
            by_rows(shape((rows, inner), bf16), True),
            by_lanes(shape((HEAD_ROWS, rows), f32), True),
            by_block(shape(state_dims, f32), True),
            fixed(shape((states, inner), bf16)),
            fixed(shape((8, inner), f32)),
        ],
        [pltpu.VMEM((states, inner), f32)],
    )
    sum_all = jnp.concatenate([gather(0), gather(1)[:inner]], axis=0)
    outgoing = entering(decay, start_state, "ctx", True)
    g_cat, tail, head, misc_scan, misc_dt = run(
        functools.partial(scan_kernel, rows),
        blocks,
        [
            info_in, by_rows(vbc, True), by_rows(g_b, True), by_rows(g_c, True),
            by_lanes(step, True), by_lanes(cum, True), by_lanes(pre, True), by_lanes(a_sum, True),
            by_block(state_in, True), by_block(gs_part, True), whole(outgoing),
            by_rows(slope_x, True), by_rows(slope_bc, True), by_rows(joined_x, True),
            by_rows(joined_bc, True), params_in, whole(spread(1)),
            whole(spread(2)), whole(e8), whole(sum_all), whole(lower),
        ],
        [
            by_rows(shape((rows, width + 128), bf16), True),
            fixed(shape((8, width), f32)),
            fixed(shape((8, width), f32)),
            fixed(shape((8, width), f32)),
            fixed(shape((2 * HEAD_ROWS, STRETCH), f32)),
        ],
        [
            pltpu.VMEM((states, inner), f32),
            pltpu.VMEM((8, width), f32),
            pltpu.VMEM((STRETCH, STRETCH), f32),
            pltpu.VMEM((STRETCH, STRETCH), f32),
            pltpu.VMEM((STRETCH, 3 * inner), bf16),
        ],
    )
    next_rows = passed_along(head, "ctx", -1)
    feature = jnp.arange(model, dtype=jnp.int32) // slice_width
    mine = (feature == tp_index).astype(f32)[None, :]
    last_joined = jnp.concatenate([joined_x[rows - 16 :], joined_bc[rows - 16 :]], axis=1)
    def exit_call(first, extra_in, extra_out, scratch):
        top = count = blocks

        def flipped(x):
            return (x, (STRETCH, x.shape[1]), lambda i: (top - 1 - i, 0))

        return run(
            functools.partial(exit_kernel, rows, top, first),
            count,
            [
                info_in, flipped(tokens), flipped(grad_out), whole(mine), flipped(g_z),
                flipped(g_cat), params_in, whole(wz_out), whole(w_joined),
            ]
            + extra_in,
            [
                (
                    shape((model, count * STRETCH), bf16),
                    (model, STRETCH),
                    lambda i: (0, count - 1 - i),
                ),
                fixed(shape((1, model), f32)),
            ]
            + extra_out,
            scratch,
        )

    g_resid, gain_part, rim, rim_w = exit_call(
        True,
        [whole(tail), whole(next_rows), whole(last_joined)],
        [fixed(shape((16, width), bf16)), fixed(shape((8, width), f32))],
        [pltpu.VMEM((16, width), f32)],
    )
    g_resid = lax.psum_scatter(g_resid, "tp", scatter_dimension=0, tiled=True)

    part_out = tn(grad_out, normed_two)
    part_z = tn(normed, g_z)
    part_cat = tn(normed, g_cat)
    part_rim = tn(normed[rows - 16 :], rim)
    part_cat = part_cat + jnp.pad(part_rim, ((0, 0), (0, 128)))
    s_all, s_small, s_wide = reduced(
        (part_out, part_z, part_cat),
        (misc_scan, rim_w, misc_gate, misc_dt, gain_part),
        2 * states,
    )
    if lax.axis_size("ctx") > 2:
        s_all, s_small, s_wide = jax.tree.map(
            lambda part: lax.psum(0.5 * part, "ctx"), (s_all, s_small, s_wide)
        )
    grad_w_out = s_all[:, :inner].T
    grad_w_z = s_all[:, inner : 2 * inner]
    s_cat = s_all[:, 2 * inner :]
    grad_w_x = s_cat[:, :inner]
    grad_w_bc = s_cat[:, inner : inner + 2 * states]
    grad_w_dt = s_cat[:, inner + 2 * states : inner + 2 * states + heads]
    grad_conv_x_w = s_small[:taps, :inner]
    grad_conv_x_b = s_small[taps, :inner]
    grad_gate_gain = s_small[0, width : width + inner]
    grad_d_skip = jnp.sum(s_small[1, width : width + inner].reshape(heads, per_head), axis=1)
    dt_at = width + inner
    grad_a_log = jnp.sum(s_small[:heads, dt_at : dt_at + STRETCH], axis=1)
    grad_dt_bias = jnp.sum(s_small[:heads, dt_at + STRETCH : dt_at + 2 * STRETCH], axis=1)
    grad_conv_bc_w = s_wide[:taps, : 2 * states]
    grad_conv_bc_b = s_wide[taps, : 2 * states]
    here = tp_index * slice_width
    grad_norm_gain = lax.dynamic_slice_in_dim(s_wide[0, 2 * states :], here, slice_width, 0)
    place = tp_index.astype(jnp.int32)[None]

    wide = 2 * STRETCH
    layer_out = run(
        functools.partial(finish_kernel, tp_size),
        blocks // 2,
        [
            (place, None, "smem"),
            (branch, (slice_width, wide), lambda i: (0, i)),
            (tokens, (wide, model), lambda i: (i, 0)),
            (sums, (2, wide), lambda i: (0, i)),
        ],
        [(shape((slice_width, rows), bf16), (slice_width, wide), lambda i: (0, i))],
        [],
    )[0].T
    grad_tokens = g_resid.T
    return (
        layer_out, grad_tokens, grad_norm_gain, grad_w_z, grad_w_x, grad_w_bc, grad_w_dt,
        grad_conv_x_w, grad_conv_x_b, grad_conv_bc_w, grad_conv_bc_b, grad_dt_bias, grad_a_log,
        grad_d_skip, grad_gate_gain, grad_w_out,
    )


def solution(mesh):
    both = ("fsdp", "ctx")
    in_specs = (
        P(both, None), P(both, None), P("fsdp", None), P(), P("fsdp", "tp"), P("fsdp", "tp"),
        P("fsdp", None), P("fsdp", "tp"), P(None, "tp"), P("tp"), P(), P(), P("tp"), P("tp"),
        P("tp"), P("tp"), P("tp", "fsdp"),
    )
    out_specs = (
        P(both, "tp"), P(both, "tp"), P("tp"), P("fsdp", "tp"), P("fsdp", "tp"), P("fsdp", None),
        P("fsdp", "tp"), P(None, "tp"), P("tp"), P(), P(), P("tp"), P("tp"), P("tp"), P("tp"),
        P("tp", "fsdp"),
    )
    return jax.shard_map(local, mesh=mesh, in_specs=in_specs, out_specs=out_specs, check_vma=False)
```

```python
import functools

import jax
import jax.numpy as jnp
import numpy as np
from jax import lax
from jax.experimental import pallas as pl
from jax.experimental.pallas import tpu as pltpu
from jax.sharding import PartitionSpec as P

STRETCH = 256
TAPS = 4
INNER = 1536
HEAD_ROWS = 8
LOG2E = 1.4426950408889634

epsilon = 1e-05
f32 = jnp.float32
bf16 = jnp.bfloat16


def nn(left, right):
    return lax.dot_general(left, right, (((1,), (0,)), ((), ())), preferred_element_type=f32)


def nt(left, right):
    return lax.dot_general(left, right, (((1,), (1,)), ((), ())), preferred_element_type=f32)


def tn(left, right):
    return lax.dot_general(left, right, (((0,), (0,)), ((), ())), preferred_element_type=f32)


def halves(x):
    high = x.astype(bf16)
    return high, (x - high.astype(f32)).astype(bf16)


def thirds(x):
    high = x.astype(bf16)
    rest = x - high.astype(f32)
    mid = rest.astype(bf16)
    return high, mid, (rest - mid.astype(f32)).astype(bf16)


def exact_rows(x, ones_matrix):
    high, mid, low = thirds(x)
    r = HEAD_ROWS
    out = nn(jnp.concatenate([high, mid, low, jnp.zeros_like(low)], axis=0), ones_matrix)
    return out[:r] + out[r : 2 * r] + out[2 * r : 3 * r]


def columns_of(rows):
    have = sum(r.shape[0] for r in rows)
    pad = jnp.zeros((128 - have, rows[0].shape[1]), f32)
    cols = jnp.transpose(jnp.concatenate(list(rows) + [pad], axis=0))
    high, low = halves(cols)
    return cols, jnp.concatenate([high, low], axis=1)


def segment_start(pos, starts):
    found = jnp.zeros_like(pos)
    for s in starts:
        found = jnp.where(pos >= s, s, found)
    return found


def joined_ok(u, distance, starts):
    ok = jnp.ones(u.shape, jnp.bool_)
    for s in starts[1:]:
        ok = ok & jnp.logical_not((u < s) & (u + distance >= s))
    return ok


def iota(shape, axis):
    return lax.broadcasted_iota(jnp.int32, shape, axis)


def read_info(rows, lengths, block):
    first = lax.axis_index("ctx") * rows
    starts = [jnp.int32(0)]
    for k in range(lengths.shape[1] - 1):
        starts.append(starts[-1] + lengths[0, k])
    base = first + block * STRETCH
    end_start = segment_start(base + STRETCH - 1, starts)
    flag = jnp.where(end_start < base, 1.0, 0.0).astype(f32)
    return starts, base, end_start, flag


def norm_rows(tok):
    x = tok.astype(f32)
    inverse = lax.rsqrt(jnp.mean(x * x, axis=1, keepdims=True) + epsilon)
    return x * inverse, inverse


def lanes_of(column, e8):
    return jnp.sum(column * e8, axis=0, keepdims=True)


MESH = pl.DeviceIdType.MESH


def start_together(peers):
    barrier = pltpu.get_barrier_semaphore()
    for peer in peers:
        pl.semaphore_signal(barrier, inc=1, device_id=peer, device_id_type=MESH)
    pl.semaphore_wait(barrier, len(peers))


def remote(src, dst, sent, came, peer):
    return pltpu.make_async_remote_copy(
        src_ref=src, dst_ref=dst, send_sem=sent, recv_sem=came, device_id=peer, device_id_type=MESH
    )


def turned(index, distance, size):
    return lax.rem(index + distance + size, size)


def twin_of(index):
    parity = lax.rem(index, 2)
    return parity, index + 1 - 2 * parity


def entry_kernel(
    rows, n, chain, sub, subs, info, nrm, halo, par, wj, tri, ew, e8, w_z, w_out_t,
    jx_o, jb_o, vbc_o, sx_o, sb_o, pre_o, step_o, cum_o, s_o, end_o, dec_o, inc_o, wz_o,
    ext, run, dec, shifts, got, sent, came, own, hop,
):
    i = pl.program_id(0) * subs + sub
    f = lax.axis_index("fsdp")
    here = lax.axis_index("ctx")
    _parity, twin = twin_of(here)
    peers = [{"fsdp": turned(f, d, n)} for d in range(1, n)] + [{"ctx": twin}]
    barrier = pltpu.get_barrier_semaphore()
    slab = w_z.shape[0]

    def at_first(body):
        if sub == 0:
            pl.when(pl.program_id(0) == 0)(body)

    def at_last(body):
        if sub == subs - 1:
            pl.when(pl.program_id(0) == pl.num_programs(0) - 1)(body)

    @at_first
    def _():
        for peer in peers:
            pl.semaphore_signal(barrier, inc=1, device_id=peer, device_id_type=MESH)

    def weight_copies():
        at = pl.ds(pl.multiple_of(f * slab, 16), slab)
        for p, ref in enumerate((w_z, w_out_t)):
            cols = slice(p * ref.shape[1], (p + 1) * ref.shape[1])
            target = wz_o.at[at, cols]
            yield pltpu.make_async_copy(ref, target, own.at[p])
            for d in range(1, n):
                yield remote(
                    ref, target, sent.at[d - 1, p], came.at[d - 1, p], {"fsdp": turned(f, d, n)}
                )

    starts, base, end_start, flag = read_info(rows, info, i)
    inner = jx_o.shape[1]
    width = inner + jb_o.shape[1]
    gain, cb, cw, taps = par[0:1, :], par[1:2, :], par[4:8, :], TAPS

    @at_first
    def _():
        unit, _inv = norm_rows(halo[...])
        before = nn((unit * gain).astype(bf16), wj[:, :width])
        ext[0:8, :] = before.astype(bf16).astype(f32)[8:16]
        run[...] = jnp.zeros_like(run)
        dec[...] = jnp.ones_like(dec)
        gap = iota((STRETCH, STRETCH), 0) - iota((STRETCH, STRETCH), 1)
        for k in range(taps - 1):
            moves = jnp.where(gap == taps - 1 - k, 1.0, 0.0).astype(bf16)
            shifts[STRETCH * k : STRETCH * (k + 1), :] = moves

    normed = nrm[...]
    product = nn(normed, wj[...])
    joined = product[:, :width].astype(bf16)
    jx_o[...] = joined[:, :inner]
    jb_o[...] = joined[:, inner:]
    pos = base + iota((STRETCH, 128), 0)
    first_of = segment_start(pos, starts)
    valid = [
        jnp.where(pos - (taps - 1 - k) >= first_of, 1.0, 0.0).astype(f32) for k in range(taps - 1)
    ]
    row_at = iota((8, 128), 0)
    masked = jnp.concatenate(
        [
            shifts[STRETCH * k : STRETCH * (k + 1), :]
            * jnp.concatenate([ok.astype(bf16)] * (STRETCH // 128), axis=1)
            for k, ok in enumerate(valid)
        ],
        axis=0,
    )
    for g in range(width // 128):
        at = slice(128 * g, 128 * (g + 1))
        if g % 2 == 0:
            tile = nn(masked, joined[:, 128 * g : min(128 * (g + 2), width)])
        fresh = joined[:, at].astype(f32)
        before = ext[:, at]
        ext[:, at] = fresh[STRETCH - 8 :]
        acc = cb[:, at] + cw[taps - 1 : taps, at] * fresh
        part = slice(128 * (g % 2), 128 * (g % 2 + 1))
        for k in range(taps - 1):
            d = taps - 1 - k
            moved = tile[STRETCH * k : STRETCH * (k + 1), part]
            edge = jnp.where(row_at < d, pltpu.roll(before, d, axis=0), 0.0) * valid[k][0:8]
            moved = jnp.concatenate([moved[0:8] + edge, moved[8:]], axis=0)
            acc = acc + cw[k : k + 1, at] * moved
        sig = jax.nn.sigmoid(acc)
        act = acc * sig
        vbc_o[:, at] = act.astype(bf16)
        slope = sig + act * (1.0 - sig)
        if 128 * g < inner:
            sx_o[:, at] = slope.astype(bf16)
        else:
            sb_o[:, 128 * g - inner : 128 * (g + 1) - inner] = slope
    pre = jnp.transpose(product[:, width:])[:HEAD_ROWS] + par[8:16, 0:1]
    step = jax.nn.softplus(pre)
    logd = -step * jnp.exp(par[8:16, 1:2])
    cum = exact_rows(logd, tri[...])
    pre_o[...] = pre
    step_o[...] = step
    cum_o[...] = cum
    cum_e = cum[:, STRETCH - 1 : STRETCH]
    where_s = base + iota((1, STRETCH), 1)
    keep = jnp.where(where_s >= end_start, 1.0, 0.0).astype(f32)
    weight = jnp.exp(cum_e - cum) * step * keep
    _cols, both = columns_of([weight])
    spread = nn(both, ew[...])
    v = vbc_o[:, :inner].astype(f32)
    b = vbc_o[:, inner : inner + 128]
    state = tn(b, (v * spread).astype(bf16))
    s_o[0] = state
    through = lanes_of(jnp.exp(cum_e) * flag, e8[...])
    run[...] = through * run[...] + state
    dec[...] = dec[...] * through
    end_o[...] = run[...].astype(bf16)
    dec_o[...] = dec[...]

    @at_first
    def _():
        pl.semaphore_wait(barrier, len(peers))
        for copy in weight_copies():
            copy.start()

    @at_last
    def _():
        if chain == 2:
            copy = remote(end_o, got, hop.at[0], hop.at[1], {"ctx": twin})
            copy.start()
            copy.wait()
            inc_o[...] = jnp.where(here > 0, got[...], jnp.zeros_like(got))
        else:
            inc_o[...] = jnp.zeros_like(inc_o)
        for copy in weight_copies():
            copy.wait()


def view(ref, kind, sub):
    if kind == "r":
        return ref.at[pl.ds(STRETCH * sub, STRETCH), :]
    if kind == "l":
        return ref.at[:, pl.ds(STRETCH * sub, STRETCH)]
    if kind == "b":
        return ref.at[pl.ds(sub, 1)]
    return ref


def in_turn(kernel, subs, kinds):
    def body(*refs):
        for sub in range(subs):
            kernel(sub, subs, *[view(ref, kind, sub) for ref, kind in zip(refs, kinds)])

    return body


def mix_kernel(
    rows, sub, subs, info, vbc, step, cum, s_in, inc, normed, gout, wz_out, par, e_step, e_scale, e8,
    z_o, out_o, gn_o, sum_o, st_o, br_o,
    run, gram,
):
    i = pl.program_id(0) * subs + sub
    starts, base, _end_start, flag = read_info(rows, info, i)
    inner = out_o.shape[1]
    gain = par[2:3, :inner]
    dskip = lanes_of(par[8:16, 2:3], e8[...])

    if sub == 0:

        @pl.when(i == 0)
        def _():
            run[...] = inc[...].astype(f32)

    st = run[...].astype(bf16)
    st_o[0] = st
    cum_v = cum[...]
    cum_e = cum_v[:, STRETCH - 1 : STRETCH]
    through = lanes_of(jnp.exp(cum_e) * flag, e8[...])
    run[...] = through * run[...] + s_in[0]

    row_first = segment_start(base + iota((1, STRETCH), 1), starts)
    scale = jnp.exp(cum_v) * jnp.where(row_first < base, 1.0, 0.0).astype(f32)
    cum2 = cum_v * LOG2E
    cols, both = columns_of([cum2, step[...], scale])
    step_x = nn(both, e_step[...])
    scale_x = nn(both, e_scale[...])
    b = vbc[:, inner : inner + 128]
    c = vbc[:, inner + 128 : inner + 256]
    carried = nn(c, st) * scale_x
    half = STRETCH // 2
    low, high = slice(0, half), slice(half, STRETCH)
    t_at = iota((half, STRETCH), 0)
    s_at = iota((half, STRETCH), 1)
    causal = (s_at <= t_at)[:, low]
    first_low = segment_start(iota((half, half), 0) + base, starts)
    first_high = segment_start(t_at + (base + half), starts)
    mask_a = causal & ((s_at + base)[:, low] >= first_low)
    mask_b = (s_at <= t_at + half) & (s_at + base >= first_high)
    gram[low, low] = jnp.where(mask_a, nt(c[low], b[low]), 0.0)
    gram[high, :] = jnp.where(mask_b, nt(c[high], b), 0.0)
    lane = iota((STRETCH, 128), 1)
    pieces = []
    for p in range(inner // 128):
        at = slice(128 * p, 128 * (p + 1))
        v = vbc[:, at].astype(f32)
        sv = (v * step_x[:, at]).astype(bf16)
        rest = carried[:, at] + dskip[:, at] * v
        acc_low, acc_high = rest[low], rest[high]
        for j in range(2):
            h = 2 * p + j
            side = (lane < 64) if j == 0 else (lane >= 64)
            part = jnp.where(side, sv, jnp.zeros_like(sv))
            row = cum2[h : h + 1, :]
            first_gap = cols[low, h : h + 1] - row[:, low]
            cross_gap = cols[high, h : h + 1] - row[:, low]
            last_gap = cols[high, h : h + 1] - row[:, high]
            decay_b = jnp.concatenate(
                [jnp.exp2(cross_gap), jnp.exp2(jnp.minimum(last_gap, 0.0))], axis=1
            )
            decay_a = jnp.exp2(jnp.minimum(first_gap, 0.0))
            acc_low = acc_low + nn((gram[low, low] * decay_a).astype(bf16), part[low])
            acc_high = acc_high + nn((gram[high, :] * decay_b).astype(bf16), part)
        pieces.append(jnp.concatenate([acc_low, acc_high], axis=0))
    out = jnp.concatenate(pieces, axis=1)
    out_o[...] = out
    zf = nn(normed[...], wz_out[:, :inner])
    z_o[...] = zf
    gated = out * (zf * jax.nn.sigmoid(zf))
    gn = nn(gout[...], wz_out[:, inner:])
    gn_o[...] = gn
    gg = gated * gain
    br_o[...] = nt(wz_out[:, inner:], gg.astype(bf16)).astype(bf16)
    ss = jnp.sum(gated * gated, axis=1, keepdims=True)
    dq = jnp.sum(gn * gg, axis=1, keepdims=True)
    sum_o[...] = jnp.transpose(jnp.where(lane == 0, ss, dq))[0:2]


def gate_kernel(
    rows, info, sums, cum, out, z, gn, vc, st, par, e_scale, e8, f_sum,
    gz_o, gb_o, gc_o, n2_o, a_o, gs_o, start_o, misc_o,
    run,
):
    step_id = pl.program_id(0)
    blocks = pl.num_programs(0)
    i = blocks - 1 - step_id
    starts, base, _end_start, flag = read_info(rows, info, i)
    inner = z.shape[1]
    gain = par[2:3, :inner]
    dskip = lanes_of(par[8:16, 2:3], e8[...])

    @pl.when(step_id == 0)
    def _():
        run[...] = jnp.zeros_like(run)
        misc_o[...] = jnp.zeros_like(misc_o)

    alpha = lax.rsqrt(sums[0:1, :] / INNER + epsilon)
    beta = alpha * alpha * alpha * sums[1:2, :] / INNER
    cum_v = cum[...]
    row_first = segment_start(base + iota((1, STRETCH), 1), starts)
    scale = jnp.exp(cum_v) * jnp.where(row_first < base, 1.0, 0.0).astype(f32)
    cols, both = columns_of([alpha, beta, jnp.zeros((14, STRETCH), f32), scale])
    alpha_c = cols[:, 0:1]
    beta_c = cols[:, 1:2]
    scale_x = nn(both, e_scale[...])
    v = vc[:, :inner].astype(f32)
    c = vc[:, inner + 128 : inner + 256]
    zf = z[...]
    sig = jax.nn.sigmoid(zf)
    act = zf * sig
    o = out[...]
    gated = o * act
    g_n = gn[...]
    unit = gated * alpha_c
    g_gated = alpha_c * (g_n * gain) - beta_c * gated
    g_out = g_gated * act
    gz_o[...] = (g_gated * o * (sig + act * (1.0 - sig))).astype(bf16)
    gb = g_out.astype(bf16)
    gb_o[...] = gb
    n2_o[...] = (unit * gain).astype(bf16)
    misc_o[0:1, :] += jnp.sum(g_n * unit, axis=0, keepdims=True)
    misc_o[1:2, :] += jnp.sum(g_out * v, axis=0, keepdims=True)
    gf = gb.astype(f32)
    carried = nn(c, st[0]) * scale_x
    prod = gf * (o - dskip * v) + (g_out - gf) * carried
    high, low = halves(prod)
    sums_c = nn(jnp.concatenate([high, low], axis=1), f_sum[...])
    a_o[...] = jnp.transpose(sums_c)[0:HEAD_ROWS]
    gc = (g_out * scale_x).astype(bf16)
    gc_o[...] = gc
    gs = tn(c, gc)
    gs_o[0] = gs
    through = lanes_of(jnp.exp(cum_v[:, STRETCH - 1 : STRETCH]) * flag, e8[...])
    run[...] = through * run[...] + gs
    start_o[...] = run[...].astype(bf16)


def scan_kernel(
    rows, info, vbc, gb, gc, step, cum, pre, a_sum, st, gs_in, outg, sx, sb, jx, jb, par,
    e_step, e_w, e8, f_all, tril,
    gcat_o, tail_o, head_o, misc_o, dt_o,
    run, ext, gram, acc, prod,
):
    step_id = pl.program_id(0)
    blocks = pl.num_programs(0)
    i = blocks - 1 - step_id
    starts, base, end_start, flag = read_info(rows, info, i)
    inner = gb.shape[1]
    width = inner + jb.shape[1]
    cw, taps = par[4:8, :], TAPS
    rate = jnp.exp(par[8:16, 1:2])
    dskip = lanes_of(par[8:16, 2:3], e8[...])

    @pl.when(step_id == 0)
    def _():
        run[...] = outg[...].astype(f32)
        ext[...] = jnp.zeros((8, width), f32)
        misc_o[...] = jnp.zeros_like(misc_o)
        dt_o[...] = jnp.zeros_like(dt_o)

    cum_v = cum[...]
    step_v = step[...]
    cum_e = cum_v[:, STRETCH - 1 : STRETCH]
    after = run[...]
    low_after = after.astype(bf16)
    state = st[0]
    through = lanes_of(jnp.exp(cum_e) * flag, e8[...])
    g_through = jnp.sum(after * state.astype(f32), axis=0, keepdims=True) * through
    end_more = jnp.sum(e8[...] * g_through, axis=1, keepdims=True)
    run[...] = through * after + gs_in[0]

    where_s = base + iota((1, STRETCH), 1)
    row_first = segment_start(where_s, starts)
    end_decay = jnp.exp(cum_e - cum_v) * jnp.where(where_s >= end_start, 1.0, 0.0).astype(f32)
    weight = end_decay * step_v
    cum2 = cum_v * LOG2E
    ok_rows = [
        jnp.where(joined_ok(where_s, d, starts), 1.0, 0.0).astype(f32)
        for d in range(taps - 1, 0, -1)
    ]
    cols, both = columns_of([cum2, step_v, weight] + ok_rows)
    b = vbc[:, inner : inner + 128]
    c = vbc[:, inner + 128 : inner + 256]
    half = STRETCH // 2
    low, high = slice(0, half), slice(half, STRETCH)
    s_at = iota((half, STRETCH), 0)
    t_at = iota((half, STRETCH), 1)
    mask_a = (s_at <= t_at) & (s_at + base >= row_first)
    mask_b = (s_at <= t_at)[:, low] & ((s_at + (base + half)) >= row_first)[:, high]
    gram[low, :] = jnp.where(mask_a, nt(b[low], c), 0.0)
    gram[high, low] = jnp.where(mask_b, nt(b[high], c[high]), 0.0)
    acc[...] = jnp.zeros_like(acc)
    lane = iota((STRETCH, 128), 1)
    ok = [
        jnp.broadcast_to(cols[:, 3 * HEAD_ROWS + k : 3 * HEAD_ROWS + k + 1], (STRETCH, 128))
        for k in range(taps - 1)
    ]

    def convolve(at, own, j_f):
        following = ext[:, at]
        joint = jnp.concatenate([own, following], axis=0)
        ext[:, at] = own[0:8]
        misc_o[taps : taps + 1, at] += jnp.sum(own, axis=0, keepdims=True)
        misc_o[taps - 1 : taps, at] += jnp.sum(own * j_f, axis=0, keepdims=True)
        total = own * cw[taps - 1 : taps, at]
        for k in range(taps - 1):
            d = taps - 1 - k
            term = pltpu.roll(joint, STRETCH + 8 - d, axis=0)[:STRETCH] * ok[k]
            misc_o[k : k + 1, at] += jnp.sum(term * j_f, axis=0, keepdims=True)
            total = total + term * cw[k : k + 1, at]
        gcat_o[:, at] = total.astype(bf16)
        tail_o[:, at] = jnp.where(step_id == 0, total[STRETCH - 8 :], tail_o[:, at])

    g_b = jnp.zeros((STRETCH, 128), f32)
    g_c = jnp.zeros((STRETCH, 128), f32)
    for p in range(inner // 128):
        at = slice(128 * p, 128 * (p + 1))
        step_x = nn(both, e_step[:, at])
        v = vbc[:, at].astype(f32)
        sv = (v * step_x).astype(bf16)
        g_pair = gb[:, at]
        u_low = jnp.zeros((half, 128), f32)
        u_high = jnp.zeros((half, 128), f32)
        for j in range(2):
            h = 2 * p + j
            side = (lane < 64) if j == 0 else (lane >= 64)
            g_side = jnp.where(side, g_pair, jnp.zeros_like(g_pair))
            sv_side = jnp.where(side, sv, jnp.zeros_like(sv))
            row = cum2[h : h + 1, :]
            first_gap = row[:, low] - cols[low, h : h + 1]
            cross_gap = row[:, high] - cols[low, h : h + 1]
            last_gap = row[:, high] - cols[high, h : h + 1]
            decay_a = jnp.concatenate(
                [jnp.exp2(jnp.minimum(first_gap, 0.0)), jnp.exp2(cross_gap)], axis=1
            )
            decay_b = jnp.exp2(jnp.minimum(last_gap, 0.0))
            u_low = u_low + nn((gram[low, :] * decay_a).astype(bf16), g_side)
            u_high = u_high + nn((gram[high, low] * decay_b).astype(bf16), g_side[high])
            acc[low, :] += nt(sv_side[low], g_pair) * decay_a
            acc[high, low] += nt(sv_side[high], g_pair[high]) * decay_b
        u = jnp.concatenate([u_low, u_high], axis=0)
        w_x = nn(both, e_w[:, at])
        y = nn(b, low_after[:, at])
        h1, l1 = halves(sv.astype(f32) * u)
        prod[:, at] = h1
        prod[:, inner + 128 * p : inner + 128 * (p + 1)] = l1
        prod[:, 2 * inner + 128 * p : 2 * inner + 128 * (p + 1)] = (v * y).astype(bf16)
        g_b = g_b + nt((v * w_x).astype(bf16), low_after[:, at])
        g_c = g_c + nt(gc[:, at], state[:, at])
        gv = dskip[:, at] * g_pair.astype(f32) + step_x * u + w_x * y
        convolve(at, gv * sx[:, at].astype(f32), jx[:, at].astype(f32))

    gg_a = jnp.where(mask_a, acc[low, :], 0.0).astype(bf16)
    gg_b = jnp.where(mask_b, acc[high, low], 0.0).astype(bf16)
    g_b = g_b + jnp.concatenate([nn(gg_a, c), nn(gg_b, c[high])], axis=0)
    g_c = g_c + tn(gg_a, b[low])
    g_c = g_c + jnp.concatenate([jnp.zeros((half, 128), f32), tn(gg_b, b[high])], axis=0)
    for k, part in enumerate((g_b, g_c)):
        here = slice(128 * k, 128 * (k + 1))
        convolve(
            slice(inner + 128 * k, inner + 128 * (k + 1)),
            part * sb[:, here],
            jb[:, here].astype(f32),
        )

    sums_r = jnp.transpose(nn(prod[...], f_all[...]))
    g_mixed = sums_r[0:HEAD_ROWS]
    g_end = sums_r[HEAD_ROWS : 2 * HEAD_ROWS]
    ends = g_end * weight
    g_cum = a_sum[...] - g_mixed - ends
    end_add = jnp.sum(ends, axis=1, keepdims=True) + end_more
    g_log = exact_rows(g_cum, tril[...]) + end_add
    slope_dt = jax.nn.sigmoid(pre[...])
    ratio = jnp.where(step_v > 0.0, slope_dt / step_v, 1.0)
    g_pre_dt = (g_end * end_decay - g_log * rate) * slope_dt + g_mixed * ratio
    dt_o[0:HEAD_ROWS, :] += g_log * (-step_v * rate)
    dt_o[HEAD_ROWS:, :] += g_pre_dt
    pad = jnp.zeros((128 - HEAD_ROWS, STRETCH), f32)
    gcat_o[:, width:] = jnp.transpose(jnp.concatenate([g_pre_dt, pad], axis=0)).astype(bf16)

    head_o[...] = ext[...]


def exit_kernel(
    rows, blocks, rim_side, info, tok, gout, mine, gz, gcat, par, wz_out, wj, *rest
):
    step_id = pl.program_id(0)
    i = blocks - 1 - step_id
    starts, base, _end_start, _flag = read_info(rows, info, i)
    inner = gz.shape[1]
    if rim_side:
        tail, nxt, last_j, gr_o, gain_o, rim_o, rim_w_o, fix = rest
        taps, width = TAPS, tail.shape[1]
        cw = par[4:8, :width]
    else:
        gr_o, gain_o = rest
    gain = par[0:1, :]

    g_normed = nt(gz[...], wz_out[:, :inner]) + nt(gcat[...], wj[...])

    def finish(g_normed):
        unit, inverse = norm_rows(tok[...])
        scaled = g_normed * gain
        mean = jnp.mean(scaled * unit, axis=1, keepdims=True)
        own = gout[...].astype(f32) * mine[...]
        gr_o[...] = jnp.transpose(own + inverse * (scaled - unit * mean)).astype(bf16)
        gain_o[...] += jnp.sum(g_normed * unit, axis=0, keepdims=True)

    @pl.when(step_id == 0)
    def _():
        gain_o[...] = jnp.zeros_like(gain_o)

    if not rim_side:
        finish(g_normed)
        return

    @pl.when(step_id == 0)
    def _():
        fix[0:8, :] = jnp.zeros((8, width), f32)
        fix[8:16, :] = nxt[...]
        places = base + STRETCH - 8 + iota((8, 128), 0)
        wide = last_j[8:16, :].astype(f32)
        total = tail[...]
        for k in range(taps - 1):
            d = taps - 1 - k
            ok = jnp.where(joined_ok(places, d, starts), 1.0, 0.0).astype(f32)
            inside = jnp.where(iota((8, width), 0) >= 8 - d, fix[d : d + 8, :], 0.0)
            term = inside * jnp.concatenate([ok] * (width // 128), axis=1)
            total = total + term * cw[k : k + 1, :]
            rim_w_o[k : k + 1, :] = jnp.sum(term * wide, axis=0, keepdims=True)
        rim_w_o[taps - 1 : 8, :] = jnp.zeros((9 - taps, width), f32)
        fix[0:8, :] = jnp.zeros((8, width), f32)
        fix[8:16, :] = total.astype(bf16).astype(f32) - tail[...].astype(bf16).astype(f32)
        rim_o[...] = fix[...].astype(bf16)

    @pl.when(step_id == 0)
    def _():
        more = nt(rim_o[...], wj[:, :width])
        finish(g_normed + jnp.concatenate([jnp.zeros((STRETCH - 16, more.shape[1]), f32), more]))

    @pl.when(step_id > 0)
    def _():
        finish(g_normed)


def finish_kernel(parts, place, part, base, sums, out):
    wide = part[...].astype(f32) * lax.rsqrt(sums[0:1, :] / INNER + epsilon)
    size = out.shape[0]
    for k in range(parts):

        @pl.when(place[0] == k)
        def _():
            add = jnp.transpose(base[:, size * k : size * (k + 1)].astype(f32))
            out[...] = (wide + add).astype(bf16)


def gather_kernel(
    n, chain, x, bc, dt_t, par, tok, out, halo, nrm, dt, sent, came, passed, relayed, own, hop
):
    f = lax.axis_index("fsdp")
    parity, twin = twin_of(lax.axis_index("ctx"))
    half = x.shape[0] // 2
    here = lax.axis_index("ctx")
    following = turned(here, 1, chain)
    sides = [{"ctx": twin}] if chain == 2 else [{"ctx": following}, {"ctx": turned(here, -1, chain)}]
    start_together([{"fsdp": turned(f, d, n)} for d in range(1, n)] + sides)
    heads, rows = dt_t.shape
    wide = -(-rows // 128) * 128
    flat = jnp.concatenate(
        [dt_t[...].astype(f32), jnp.zeros((heads, wide - rows), f32)], axis=1
    )
    flat = jnp.concatenate([flat, jnp.zeros((128 - heads, wide), f32)], axis=0)
    dt[...] = jnp.transpose(flat)[:rows].astype(bf16)
    pieces = []
    at = 0
    for ref in (x, bc, dt):
        pieces.append((ref, slice(at, at + ref.shape[1])))
        at += ref.shape[1]

    def place(source, side):
        return pl.ds(pl.multiple_of(source * rows + side * half, 16), half)

    mine = pl.ds(pl.multiple_of(parity * half, 16), half)
    copies = []
    for d in range(1, n):
        for p, (ref, cols) in enumerate(pieces):
            copy = remote(
                ref.at[mine, :], out.at[place(f, parity), cols],
                sent.at[d - 1, p], came.at[d - 1, p], {"fsdp": turned(f, d, n)},
            )
            copy.start()
            copies.append(copy)
    edge = halo.shape[0]
    copy = remote(
        tok.at[pl.ds(tok.shape[0] - edge, edge), :], halo, hop.at[0], hop.at[1], {"ctx": following}
    )
    copy.start()
    locals_ = [copy]
    for p, (ref, cols) in enumerate(pieces):
        copy = pltpu.make_async_copy(
            ref, out.at[pl.ds(pl.multiple_of(f * rows, 16), rows), cols], own.at[p]
        )
        copy.start()
        locals_.append(copy)
    gain = par[...][None, :]

    def norm_block(tok_block, nrm_block):
        unit, _inverse = norm_rows(tok_block[...])
        nrm_block[...] = (unit * gain).astype(bf16)

    steps = tok.shape[0] // (2 * STRETCH)

    def normalise(first, count):
        block = pl.BlockSpec((2 * STRETCH, tok.shape[1]), lambda i: (i + first, 0))
        pltpu.emit_pipeline(norm_block, grid=(count,), in_specs=[block], out_specs=[block])(
            tok, nrm
        )

    relays = []

    def relay(d):
        source = turned(f, -d, n)
        for p, (ref, cols) in enumerate(pieces):
            copies[(d - 1) * len(pieces) + p].wait_recv()
            piece = out.at[place(source, parity), cols]
            copy = remote(piece, piece, passed.at[d - 1, p], relayed.at[d - 1, p], {"ctx": twin})
            copy.start()
            relays.append(copy)

    normalise(0, steps)
    for d in range(1, n):
        relay(d)
    for copy in copies:
        copy.wait_send()
    for copy in locals_:
        copy.wait()
    for copy in relays:
        copy.wait()


def gathered(x, bc, dt_t, par, tok):
    n = lax.axis_size("fsdp")
    pieces = (n - 1, 3)
    width = x.shape[1] + bc.shape[1] + 128
    return pl.pallas_call(
        functools.partial(gather_kernel, n, lax.axis_size("ctx")),
        out_shape=[
            jax.ShapeDtypeStruct((n * x.shape[0], width), bf16),
            jax.ShapeDtypeStruct((16, tok.shape[1]), bf16),
            jax.ShapeDtypeStruct(tok.shape, bf16),
        ],
        in_specs=[pl.BlockSpec(memory_space=pltpu.VMEM)] * 4 + [pl.BlockSpec(memory_space=pl.ANY)],
        out_specs=[pl.BlockSpec(memory_space=pltpu.VMEM)] * 2
        + [pl.BlockSpec(memory_space=pl.ANY)],
        scratch_shapes=[pltpu.VMEM((x.shape[0], 128), bf16)]
        + [pltpu.SemaphoreType.DMA(pieces)] * 4
        + [pltpu.SemaphoreType.DMA((3,)), pltpu.SemaphoreType.DMA((2,))],
        compiler_params=pltpu.CompilerParams(collective_id=1, has_side_effects=True),
    )(x, bc, dt_t, par, tok)


def total_kernel(n, part, out, slots, sent, came):
    me = lax.axis_index("tp")
    start_together([{"tp": turned(me, d, n)} for d in range(1, n)])
    copies = []
    for d in range(1, n):
        copy = remote(
            part, slots.at[d - 1], sent.at[d - 1], came.at[d - 1], {"tp": turned(me, d, n)}
        )
        copy.start()
        copies.append(copy)
    total = part[...]
    for d in range(1, n):
        copies[d - 1].wait_recv()
        total = total + slots[d - 1]
    out[...] = total
    for copy in copies:
        copy.wait_send()


def total_over_tp(part):
    n = lax.axis_size("tp")
    return pl.pallas_call(
        functools.partial(total_kernel, n),
        out_shape=jax.ShapeDtypeStruct(part.shape, f32),
        in_specs=[pl.BlockSpec(memory_space=pltpu.VMEM)],
        out_specs=pl.BlockSpec(memory_space=pltpu.VMEM),
        scratch_shapes=[
            pltpu.VMEM((n - 1,) + part.shape, f32),
            pltpu.SemaphoreType.DMA((n - 1,)),
            pltpu.SemaphoreType.DMA((n - 1,)),
        ],
        compiler_params=pltpu.CompilerParams(collective_id=2, has_side_effects=True),
    )(part)


def share_over_tp(m, t, shares, sent, came):
    copies = []
    for p, (buf, own) in enumerate(shares):
        buf[pl.ds(t, 1)] = own[None]
    for d in range(1, m):
        for p, (buf, _own) in enumerate(shares):
            k = 3 * (d - 1) + p
            copy = remote(buf.at[t], buf.at[t], sent.at[k], came.at[k], {"tp": turned(t, d, m)})
            copy.start()
            copies.append(copy)
    for copy in copies:
        copy.wait()
    totals = []
    for buf, _own in shares:
        total = buf[0].astype(f32)
        for q in range(1, m):
            total = total + buf[q].astype(f32)
        totals.append(total)
    return totals


def fold_over_tp(m, t, shares, sent, came):
    at_edge = (t == 0) | (t == 3)
    in_middle = jnp.logical_not(at_edge)
    inward = jnp.where(t == 0, 1, 2)
    outward = jnp.where(t == 1, 0, 3)
    across = 3 - t

    def copy_of(phase, p, src, dst, peer):
        buf = shares[p][0]
        k = 3 * phase + p
        return remote(buf.at[src], buf.at[dst], sent.at[k], came.at[k], {"tp": peer})

    every = range(len(shares))
    for buf, own in shares:
        buf[0] = own

    @pl.when(at_edge)
    def _():
        for p in every:
            copy_of(0, p, 0, 1, inward).start()
        for p in every:
            copy_of(0, p, 0, 1, inward).wait_send()
        for p in every:
            copy_of(2, p, 4, 4, inward).wait_recv()

    @pl.when(in_middle)
    def _():
        for p in every:
            buf = shares[p][0]
            copy_of(0, p, 0, 1, outward).wait_recv()
            buf[2] = (buf[0].astype(f32) + buf[1].astype(f32)).astype(buf.dtype)
            copy_of(1, p, 2, 3, across).start()
        for p in every:
            buf = shares[p][0]
            copy_of(1, p, 2, 3, across).wait()
            buf[4] = (buf[2].astype(f32) + buf[3].astype(f32)).astype(buf.dtype)
            copy_of(2, p, 4, 4, outward).start()
        for p in every:
            copy_of(2, p, 4, 4, outward).wait_send()

    return [buf[4].astype(f32) for buf, _own in shares]


def reduce_kernel(
    n, m, bc_cols, conv_bc,
    p_out, p_z, p_cat, m_scan, m_rim, m_gate, m_dt, m_gain,
    o_all, o_small, o_wide,
    give, take, mid, slots, final, bc_slots, small, small_slots, wide_slots, gain_slots,
    s1, r1, s2, r2, s3, r3, s4, r4,
):
    f = lax.axis_index("fsdp")
    t = lax.axis_index("tp")
    parity, twin = twin_of(lax.axis_index("ctx"))
    start_together(
        [{"ctx": twin}]
        + [{"fsdp": turned(f, d, n)} for d in range(1, n)]
        + [{"tp": turned(t, d, m)} for d in range(1, m)]
    )
    inner = p_out.shape[1]
    rows = p_out.shape[0] // n
    half = rows // 2

    def piece(q, side):
        at = pl.ds(pl.multiple_of(q * rows + side * half, 16), half)
        return jnp.concatenate([p_out[at, :], p_z[at, :], p_cat[at, :]], axis=1)

    copies = []
    for q in range(n):
        give[q] = piece(q, 1 - parity).astype(bf16)
        copy = remote(give.at[q], take.at[q], s1.at[q], r1.at[q], {"ctx": twin})
        copy.start()
        copies.append(copy)
    w_scan = m_scan.shape[1]
    w_gate = m_gate.shape[1]
    w_dt = m_dt.shape[1]
    small[...] = jnp.zeros_like(small)
    small[:, 0:w_scan] = m_scan[...] + m_rim[...]
    at = w_scan
    small[:, at : at + w_gate] = m_gate[...]
    at += w_gate
    small[:, at : at + w_dt] = m_dt[0:8, :]
    small[:, at + w_dt : at + 2 * w_dt] = m_dt[8:16, :]
    at += 2 * w_dt
    small[0:1, at:] = m_gain[...]
    small_slots[0, pl.ds(parity, 1)] = small[...][None]
    copy = remote(
        small, small_slots.at[0, parity], s1.at[n], r1.at[n], {"ctx": twin}
    )
    copy.start()
    copies.append(copy)

    copies[n].wait()
    small_slots[1, pl.ds(f, 1)] = (small_slots[0, 0] + small_slots[0, 1])[None]
    seconds = []
    for d in range(1, n):
        copy = remote(
            small_slots.at[1, f], small_slots.at[1, f], s2.at[n - 1 + d - 1], r2.at[n - 1 + d - 1],
            {"fsdp": turned(f, d, n)},
        )
        copy.start()
        seconds.append(copy)
    for q in range(n):
        copies[q].wait()
        mid[q] = (piece(q, parity) + take[q].astype(f32)).astype(bf16)
    slots[pl.ds(f, 1)] = mid[pl.ds(f, 1)]
    for d in range(1, n):
        peer = turned(f, d, n)
        copy = remote(
            mid.at[peer], slots.at[f], s2.at[d - 1], r2.at[d - 1], {"fsdp": peer}
        )
        copy.start()
        seconds.append(copy)
    for copy in seconds:
        copy.wait()
    small_sum = small_slots[1, 0]
    whole = slots[0].astype(f32)
    for q in range(1, n):
        small_sum = small_sum + small_slots[1, q]
        whole = whole + slots[q].astype(f32)
    final[...] = whole
    bc_at = slice(3 * inner, 3 * inner + bc_cols)
    o_small[...] = small_sum[:, :at]
    shares = (
        (bc_slots, whole[:, bc_at].astype(bf16)),
        (wide_slots, small_sum[:, conv_bc:w_scan]),
        (gain_slots, small_sum[0:1, at:]),
    )
    bc_sum, wide_sum, gain_sum = (fold_over_tp if m == 4 else share_over_tp)(m, t, shares, s3, r3)
    o_wide[:, :bc_cols] = wide_sum
    o_wide[:, bc_cols:] = jnp.broadcast_to(gain_sum, (8, gain_sum.shape[1]))
    final[:, bc_at] = bc_sum
    here = pl.ds(pl.multiple_of(parity * half, 8), half)
    o_all[here, :] = final[...]
    copy = remote(final, o_all.at[here, :], s4.at[0], r4.at[0], {"ctx": twin})
    copy.start()
    copy.wait()


def reduced(parts, miscs, bc_cols):
    n, m = lax.axis_size("fsdp"), lax.axis_size("tp")
    p_out, _p_z, p_cat = parts
    rows = p_out.shape[0] // n
    half = rows // 2
    inner = p_out.shape[1]
    wide = 2 * inner + p_cat.shape[1]
    m_scan, _m_rim, m_gate, m_dt, m_gain = miscs
    kept = m_scan.shape[1] + m_gate.shape[1] + 2 * m_dt.shape[1]
    small = kept + m_gain.shape[1]
    crossing = m_scan.shape[1] - inner + m_gain.shape[1]
    dma = pltpu.SemaphoreType.DMA

    def shape(*dims):
        return jax.ShapeDtypeStruct(dims, f32)

    return pl.pallas_call(
        functools.partial(reduce_kernel, n, m, bc_cols, inner),
        out_shape=[
            shape(rows, wide), shape(8, kept), shape(8, crossing),
        ],
        in_specs=[pl.BlockSpec(memory_space=pltpu.VMEM)] * 8,
        out_specs=[pl.BlockSpec(memory_space=pltpu.VMEM)] * 3,
        scratch_shapes=[
            pltpu.VMEM((n, half, wide), bf16),
            pltpu.VMEM((n, half, wide), bf16),
            pltpu.VMEM((n, half, wide), bf16),
            pltpu.VMEM((n, half, wide), bf16),
            pltpu.VMEM((half, wide), f32),
            pltpu.VMEM((max(m, 5), half, bc_cols), bf16),
            pltpu.VMEM((8, small), f32),
            pltpu.VMEM((2, max(n, 2), 8, small), f32),
            pltpu.VMEM((max(m, 5), 8, bc_cols), f32),
            pltpu.VMEM((max(m, 5), 1, m_gain.shape[1]), f32),
            dma((n + 1,)), dma((n + 1,)), dma((2 * n - 2,)), dma((2 * n - 2,)),
            dma((3 * m,)), dma((3 * m,)), dma((1,)), dma((1,)),
        ],
        compiler_params=pltpu.CompilerParams(
            collective_id=3, has_side_effects=True, vmem_limit_bytes=48 * 1024 * 1024
        ),
    )(*parts, *miscs)


def constants(inner, heads):
    lane_head = np.arange(inner) // (inner // heads)
    e8 = (np.arange(HEAD_ROWS)[:, None] == lane_head[None, :]).astype(np.float32)

    def spread(kind):
        m = np.zeros((128, inner), np.float32)
        m[HEAD_ROWS * kind : HEAD_ROWS * (kind + 1)] = e8
        return jnp.asarray(np.concatenate([m, m], axis=0), bf16)

    def gather(kind):
        m = np.zeros((inner, 128), np.float32)
        m[:, HEAD_ROWS * kind : HEAD_ROWS * (kind + 1)] = e8.T
        return jnp.asarray(np.concatenate([m, m], axis=0), bf16)

    at = np.arange(STRETCH)
    upper = jnp.asarray((at[:, None] <= at[None, :]).astype(np.float32), bf16)
    lower = jnp.asarray((at[:, None] >= at[None, :]).astype(np.float32), bf16)
    return jnp.asarray(e8), spread, gather, upper, lower


def passed_along(block, axis, distance):
    devices = range(lax.axis_size(axis))
    route = [(i - distance, i) for i in devices if i - distance in devices]
    return lax.ppermute(block, axis, route)


def entering(decay, state, axis, reverse):
    size = lax.axis_size(axis)
    if size == 2:
        return passed_along(state, axis, -1 if reverse else 1)
    index = lax.axis_index(axis)
    decays = lax.all_gather(decay.astype(bf16), axis)
    states = lax.all_gather(state, axis)

    def lap(k, before):
        at = size - 1 - k if reverse else k
        reached = at > index if reverse else at < index
        new = decays[at].astype(f32) * before + states[at].astype(f32)
        return jnp.where(reached, new, before)

    return lax.fori_loop(0, size, lap, jnp.zeros(state.shape, f32)).astype(bf16)


def fill_params(raw, par):
    gain, gate, x_w, bc_w, x_b, bc_b, bias, rate, skip = raw
    inner = x_w.shape[1]
    width = inner + bc_w.shape[1]
    heads = bias.shape[0]

    @pl.when(pl.program_id(0) == 0)
    def _():
        par[0:1, :] = gain[...][None, :]
        par[1:2, :inner] = x_b[...][None, :]
        par[1:2, inner:width] = bc_b[...][None, :]
        par[2:3, :inner] = gate[...][None, :]
        par[4:8, :inner] = x_w[...]
        par[4:8, inner:width] = bc_w[...]
        row, lane = iota((HEAD_ROWS, 128), 0), iota((HEAD_ROWS, 128), 1)
        table = jnp.zeros((HEAD_ROWS, 128), f32)
        for h in range(heads):
            for k, ref in enumerate((bias, rate, skip)):
                table = jnp.where((row == h) & (lane == k), ref[h], table)
        par[8:16, 0:128] = table


def call(kernel, blocks, ins, outs, scratch, remote_id=None, raw=None):
    def spec(shape, how):
        if how == "smem":
            return pl.BlockSpec(memory_space=pltpu.SMEM)
        if how == "any":
            return pl.BlockSpec(memory_space=pl.ANY)
        return pl.BlockSpec(shape, how)

    places = [k for k, (_a, _s, how) in enumerate(ins) if how == "par"]
    ins = [entry for entry in ins if entry[2] != "par"]
    body = kernel
    if places:
        count = len(raw)
        model = raw[0].shape[0]
        scratch = list(scratch) + [pltpu.VMEM((16, model), f32)]

        def body(*refs):
            par = refs[-1]
            fill_params(refs[:count], par)
            rest = list(refs[count:-1])
            rest.insert(places[0], par)
            kernel(*rest)

        def fixed_at(x):
            if x.ndim == 1 and x.shape[0] < 128:
                return (x, None, "smem")
            return (x, x.shape, lambda i: (0,) * x.ndim)

        ins = [fixed_at(x) for x in raw] + ins

    return pl.pallas_call(
        body,
        grid=(blocks,),
        in_specs=[spec(shape, how) for _a, shape, how in ins],
        out_specs=[spec(shape, how) for _s, shape, how in outs],
        out_shape=[s for s, _sh, _h in outs],
        scratch_shapes=scratch,
        compiler_params=pltpu.CompilerParams(
            dimension_semantics=("arbitrary",),
            vmem_limit_bytes=56 * 1024 * 1024,
            collective_id=remote_id,
            has_side_effects=remote_id is not None,
        ),
    )(*[a for a, _s, _h in ins])


def local(
    tokens, grad_out, lengths, norm_gain, w_z, w_x, w_bc, w_dt, conv_x_w, conv_x_b,
    conv_bc_w, conv_bc_b, dt_bias, a_log, d_skip, gate_gain, w_out,
):
    rows, model = tokens.shape
    inner = w_z.shape[1]
    heads = dt_bias.shape[0]
    states = w_bc.shape[1] // 2
    taps = conv_x_w.shape[0]
    blocks = rows // STRETCH
    width = inner + 2 * states
    tp_size = lax.axis_size("tp")
    slice_width = model // tp_size
    tp_index = lax.axis_index("tp")
    ctx_index = lax.axis_index("ctx")
    e8, spread, gather, upper, lower = constants(inner, heads)

    per_head = inner // heads

    w_joined, halo, normed = gathered(
        w_x, w_bc, w_dt.T, norm_gain, tokens
    )
    n = lax.axis_size("fsdp")
    chain = lax.axis_size("ctx")

    def shape(dims, kind):
        return jax.ShapeDtypeStruct(dims, kind)

    def whole(x):
        return (x, x.shape, lambda i: (0,) * x.ndim)

    def by_rows(x, flip=False):
        if flip:
            return (x, (STRETCH, x.shape[1]), lambda i: (blocks - 1 - i, 0))
        return (x, (STRETCH, x.shape[1]), lambda i: (i, 0))

    def by_lanes(x, flip=False):
        if flip:
            return (x, (x.shape[0], STRETCH), lambda i: (0, blocks - 1 - i))
        return (x, (x.shape[0], STRETCH), lambda i: (0, i))

    def by_block(x, flip=False):
        if flip:
            return (x, (1,) + x.shape[1:], lambda i: (blocks - 1 - i, 0, 0))
        return (x, (1,) + x.shape[1:], lambda i: (i, 0, 0))

    def fixed(x):
        return (x, x.shape, lambda i: (0,) * len(x.shape))

    info_in = (lengths, None, "smem")
    params_in = (None, None, "par")
    raw = (
        norm_gain, gate_gain, conv_x_w, conv_bc_w, conv_x_b, conv_bc_b, dt_bias, a_log, d_skip
    )
    run = functools.partial(call, raw=raw)
    state_dims = (blocks, states, inner)
    subs = 2 if blocks % 2 == 0 else 1

    def several(entries, kinds):
        scales = {"r": (subs, 1), "l": (1, subs), "b": (subs, 1, 1)}
        grown = []
        for entry, kind in zip(entries, kinds):
            if kind == "w":
                grown.append(entry)
                continue
            dims = tuple(d * k for d, k in zip(entry[1], scales[kind]))
            grown.append((entry[0], dims, entry[2]))
        return grown

    dma = pltpu.SemaphoreType.DMA
    entry_in, entry_out = "wrwwwwwwww", "rrrrrlllbwwww"
    (
        joined_x, joined_bc, vbc, slope_x, slope_bc, pre, step, cum, s_part, end_state, decay,
        incoming, wz_out,
    ) = run(
        in_turn(
            functools.partial(entry_kernel, rows, n, chain), 1, entry_in + entry_out + "w" * 9
        ),
        blocks,
        list([
            info_in, by_rows(normed), whole(halo), params_in, whole(w_joined), whole(upper),
            whole(spread(0)), whole(e8), (w_z, None, "any"), (w_out.T, None, "any"),
        ]),
        list([
            by_rows(shape((rows, inner), bf16)),
            by_rows(shape((rows, 2 * states), bf16)),
            by_rows(shape((rows, width), bf16)),
            by_rows(shape((rows, inner), bf16)),
            by_rows(shape((rows, 2 * states), f32)),
            by_lanes(shape((HEAD_ROWS, rows), f32)),
            by_lanes(shape((HEAD_ROWS, rows), f32)),
            by_lanes(shape((HEAD_ROWS, rows), f32)),
            by_block(shape(state_dims, f32)),
            fixed(shape((states, inner), bf16)),
            fixed(shape((1, inner), f32)),
            fixed(shape((states, inner), bf16)),
            (shape((model, 2 * inner), bf16), None, "any"),
        ]),
        [
            pltpu.VMEM((8, width), f32),
            pltpu.VMEM((states, inner), f32),
            pltpu.VMEM((1, inner), f32),
            pltpu.VMEM(((taps - 1) * STRETCH, STRETCH), bf16),
            pltpu.VMEM((states, inner), bf16),
            dma((n - 1, 2)),
            dma((n - 1, 2)),
            dma((2,)),
            dma((2,)),
        ],
        remote_id=4,
    )
    if chain > 2:
        incoming = entering(decay, end_state, "ctx", False)
    mix_in, mix_out = "wrllbwrrwwwww", "rrrlbl"
    z_part, out, gn, sums, state_in, branch = run(
        in_turn(functools.partial(mix_kernel, rows), subs, mix_in + mix_out + "wr"),
        blocks // subs,
        several(
            [
                info_in, by_rows(vbc), by_lanes(step), by_lanes(cum), by_block(s_part),
                whole(incoming), by_rows(normed), by_rows(grad_out), whole(wz_out), params_in,
                whole(spread(1)), whole(spread(2)), whole(e8),
            ],
            mix_in,
        ),
        several(
            [
                by_rows(shape((rows, inner), f32)),
                by_rows(shape((rows, inner), f32)),
                by_rows(shape((rows, inner), f32)),
                by_lanes(shape((2, rows), f32)),
                by_block(shape(state_dims, bf16)),
                by_lanes(shape((model, rows), bf16)),
            ],
            mix_out,
        ),
        [pltpu.VMEM((states, inner), f32), pltpu.VMEM((subs * STRETCH, STRETCH), f32)],
    )
    branch = lax.psum_scatter(branch, "tp", scatter_dimension=0, tiled=True)
    sums = total_over_tp(sums)
    g_z, g_b, g_c, normed_two, a_sum, gs_part, start_state, misc_gate = run(
        functools.partial(gate_kernel, rows),
        blocks,
        [
            info_in, by_lanes(sums, True), by_lanes(cum, True), by_rows(out, True),
            by_rows(z_part, True), by_rows(gn, True), by_rows(vbc, True), by_block(state_in, True),
            params_in, whole(spread(2)), whole(e8), whole(gather(0)),
        ],
        [
            by_rows(shape((rows, inner), bf16), True),
            by_rows(shape((rows, inner), bf16), True),
            by_rows(shape((rows, inner), bf16), True),
            by_rows(shape((rows, inner), bf16), True),
            by_lanes(shape((HEAD_ROWS, rows), f32), True),
            by_block(shape(state_dims, f32), True),
            fixed(shape((states, inner), bf16)),
            fixed(shape((8, inner), f32)),
        ],
        [pltpu.VMEM((states, inner), f32)],
    )
    sum_all = jnp.concatenate([gather(0), gather(1)[:inner]], axis=0)
    outgoing = entering(decay, start_state, "ctx", True)
    g_cat, tail, head, misc_scan, misc_dt = run(
        functools.partial(scan_kernel, rows),
        blocks,
        [
            info_in, by_rows(vbc, True), by_rows(g_b, True), by_rows(g_c, True),
            by_lanes(step, True), by_lanes(cum, True), by_lanes(pre, True), by_lanes(a_sum, True),
            by_block(state_in, True), by_block(gs_part, True), whole(outgoing),
            by_rows(slope_x, True), by_rows(slope_bc, True), by_rows(joined_x, True),
            by_rows(joined_bc, True), params_in, whole(spread(1)),
            whole(spread(2)), whole(e8), whole(sum_all), whole(lower),
        ],
        [
            by_rows(shape((rows, width + 128), bf16), True),
            fixed(shape((8, width), f32)),
            fixed(shape((8, width), f32)),
            fixed(shape((8, width), f32)),
            fixed(shape((2 * HEAD_ROWS, STRETCH), f32)),
        ],
        [
            pltpu.VMEM((states, inner), f32),
            pltpu.VMEM((8, width), f32),
            pltpu.VMEM((STRETCH, STRETCH), f32),
            pltpu.VMEM((STRETCH, STRETCH), f32),
            pltpu.VMEM((STRETCH, 3 * inner), bf16),
        ],
    )
    next_rows = passed_along(head, "ctx", -1)
    feature = jnp.arange(model, dtype=jnp.int32) // slice_width
    mine = (feature == tp_index).astype(f32)[None, :]
    last_joined = jnp.concatenate([joined_x[rows - 16 :], joined_bc[rows - 16 :]], axis=1)
    def exit_call(first, extra_in, extra_out, scratch):
        top = count = blocks

        def flipped(x):
            return (x, (STRETCH, x.shape[1]), lambda i: (top - 1 - i, 0))

        return run(
            functools.partial(exit_kernel, rows, top, first),
            count,
            [
                info_in, flipped(tokens), flipped(grad_out), whole(mine), flipped(g_z),
                flipped(g_cat), params_in, whole(wz_out), whole(w_joined),
            ]
            + extra_in,
            [
                (
                    shape((model, count * STRETCH), bf16),
                    (model, STRETCH),
                    lambda i: (0, count - 1 - i),
                ),
                fixed(shape((1, model), f32)),
            ]
            + extra_out,
            scratch,
        )

    g_resid, gain_part, rim, rim_w = exit_call(
        True,
        [whole(tail), whole(next_rows), whole(last_joined)],
        [fixed(shape((16, width), bf16)), fixed(shape((8, width), f32))],
        [pltpu.VMEM((16, width), f32)],
    )
    g_resid = lax.psum_scatter(g_resid, "tp", scatter_dimension=0, tiled=True)

    part_out = tn(grad_out, normed_two)
    part_z = tn(normed, g_z)
    part_cat = tn(normed, g_cat)
    part_rim = tn(normed[rows - 16 :], rim)
    part_cat = part_cat + jnp.pad(part_rim, ((0, 0), (0, 128)))
    s_all, s_small, s_wide = reduced(
        (part_out, part_z, part_cat),
        (misc_scan, rim_w, misc_gate, misc_dt, gain_part),
        2 * states,
    )
    if lax.axis_size("ctx") > 2:
        s_all, s_small, s_wide = jax.tree.map(
            lambda part: lax.psum(0.5 * part, "ctx"), (s_all, s_small, s_wide)
        )
    grad_w_out = s_all[:, :inner].T
    grad_w_z = s_all[:, inner : 2 * inner]
    s_cat = s_all[:, 2 * inner :]
    grad_w_x = s_cat[:, :inner]
    grad_w_bc = s_cat[:, inner : inner + 2 * states]
    grad_w_dt = s_cat[:, inner + 2 * states : inner + 2 * states + heads]
    grad_conv_x_w = s_small[:taps, :inner]
    grad_conv_x_b = s_small[taps, :inner]
    grad_gate_gain = s_small[0, width : width + inner]
    grad_d_skip = jnp.sum(s_small[1, width : width + inner].reshape(heads, per_head), axis=1)
    dt_at = width + inner
    grad_a_log = jnp.sum(s_small[:heads, dt_at : dt_at + STRETCH], axis=1)
    grad_dt_bias = jnp.sum(s_small[:heads, dt_at + STRETCH : dt_at + 2 * STRETCH], axis=1)
    grad_conv_bc_w = s_wide[:taps, : 2 * states]
    grad_conv_bc_b = s_wide[taps, : 2 * states]
    here = tp_index * slice_width
    grad_norm_gain = lax.dynamic_slice_in_dim(s_wide[0, 2 * states :], here, slice_width, 0)
    place = tp_index.astype(jnp.int32)[None]

    wide = 2 * STRETCH
    layer_out = run(
        functools.partial(finish_kernel, tp_size),
        blocks // 2,
        [
            (place, None, "smem"),
            (branch, (slice_width, wide), lambda i: (0, i)),
            (tokens, (wide, model), lambda i: (i, 0)),
            (sums, (2, wide), lambda i: (0, i)),
        ],
        [(shape((slice_width, rows), bf16), (slice_width, wide), lambda i: (0, i))],
        [],
    )[0].T
    grad_tokens = g_resid.T
    return (
        layer_out, grad_tokens, grad_norm_gain, grad_w_z, grad_w_x, grad_w_bc, grad_w_dt,
        grad_conv_x_w, grad_conv_x_b, grad_conv_bc_w, grad_conv_bc_b, grad_dt_bias, grad_a_log,
        grad_d_skip, grad_gate_gain, grad_w_out,
    )


def solution(mesh):
    both = ("fsdp", "ctx")
    in_specs = (
        P(both, None), P(both, None), P("fsdp", None), P(), P("fsdp", "tp"), P("fsdp", "tp"),
        P("fsdp", None), P("fsdp", "tp"), P(None, "tp"), P("tp"), P(), P(), P("tp"), P("tp"),
        P("tp"), P("tp"), P("tp", "fsdp"),
    )
    out_specs = (
        P(both, "tp"), P(both, "tp"), P("tp"), P("fsdp", "tp"), P("fsdp", "tp"), P("fsdp", None),
        P("fsdp", "tp"), P(None, "tp"), P("tp"), P(), P(), P("tp"), P("tp"), P("tp"), P("tp"),
        P("tp", "fsdp"),
    )
    return jax.shard_map(local, mesh=mesh, in_specs=in_specs, out_specs=out_specs, check_vma=False)
```

```python
import functools

import jax
import jax.numpy as jnp
import numpy as np
from jax import lax
from jax.experimental import pallas as pl
from jax.experimental.pallas import tpu as pltpu
from jax.sharding import PartitionSpec as P

STRETCH = 256
TAPS = 4
INNER = 1536
HEAD_ROWS = 8
LOG2E = 1.4426950408889634

epsilon = 1e-05
f32 = jnp.float32
bf16 = jnp.bfloat16


def nn(left, right):
    return lax.dot_general(left, right, (((1,), (0,)), ((), ())), preferred_element_type=f32)


def nt(left, right):
    return lax.dot_general(left, right, (((1,), (1,)), ((), ())), preferred_element_type=f32)


def tn(left, right):
    return lax.dot_general(left, right, (((0,), (0,)), ((), ())), preferred_element_type=f32)


def halves(x):
    high = x.astype(bf16)
    return high, (x - high.astype(f32)).astype(bf16)


def thirds(x):
    high = x.astype(bf16)
    rest = x - high.astype(f32)
    mid = rest.astype(bf16)
    return high, mid, (rest - mid.astype(f32)).astype(bf16)


def exact_rows(x, ones_matrix):
    high, mid, low = thirds(x)
    r = HEAD_ROWS
    out = nn(jnp.concatenate([high, mid, low, jnp.zeros_like(low)], axis=0), ones_matrix)
    return out[:r] + out[r : 2 * r] + out[2 * r : 3 * r]


def columns_of(rows):
    have = sum(r.shape[0] for r in rows)
    pad = jnp.zeros((128 - have, rows[0].shape[1]), f32)
    cols = jnp.transpose(jnp.concatenate(list(rows) + [pad], axis=0))
    high, low = halves(cols)
    return cols, jnp.concatenate([high, low], axis=1)


def segment_start(pos, starts):
    found = jnp.zeros_like(pos)
    for s in starts:
        found = jnp.where(pos >= s, s, found)
    return found


def joined_ok(u, distance, starts):
    ok = jnp.ones(u.shape, jnp.bool_)
    for s in starts[1:]:
        ok = ok & jnp.logical_not((u < s) & (u + distance >= s))
    return ok


def iota(shape, axis):
    return lax.broadcasted_iota(jnp.int32, shape, axis)


def read_info(rows, lengths, block):
    first = lax.axis_index("ctx") * rows
    starts = [jnp.int32(0)]
    for k in range(lengths.shape[1] - 1):
        starts.append(starts[-1] + lengths[0, k])
    base = first + block * STRETCH
    end_start = segment_start(base + STRETCH - 1, starts)
    flag = jnp.where(end_start < base, 1.0, 0.0).astype(f32)
    return starts, base, end_start, flag


def norm_rows(tok):
    x = tok.astype(f32)
    inverse = lax.rsqrt(jnp.mean(x * x, axis=1, keepdims=True) + epsilon)
    return x * inverse, inverse


def lanes_of(column, e8):
    return jnp.sum(column * e8, axis=0, keepdims=True)


MESH = pl.DeviceIdType.MESH


def start_together(peers):
    barrier = pltpu.get_barrier_semaphore()
    for peer in peers:
        pl.semaphore_signal(barrier, inc=1, device_id=peer, device_id_type=MESH)
    pl.semaphore_wait(barrier, len(peers))


def remote(src, dst, sent, came, peer):
    return pltpu.make_async_remote_copy(
        src_ref=src, dst_ref=dst, send_sem=sent, recv_sem=came, device_id=peer, device_id_type=MESH
    )


def turned(index, distance, size):
    return lax.rem(index + distance + size, size)


def twin_of(index):
    parity = lax.rem(index, 2)
    return parity, index + 1 - 2 * parity


def entry_kernel(
    rows, n, chain, sub, subs, info, nrm, halo, par, wj, tri, ew, e8, w_z, w_out_t,
    jx_o, jb_o, vbc_o, sx_o, sb_o, pre_o, step_o, cum_o, s_o, end_o, dec_o, inc_o, wz_o,
    ext, run, dec, shifts, got, sent, came, own, hop,
):
    i = pl.program_id(0) * subs + sub
    f = lax.axis_index("fsdp")
    here = lax.axis_index("ctx")
    _parity, twin = twin_of(here)
    peers = [{"fsdp": turned(f, d, n)} for d in range(1, n)] + [{"ctx": twin}]
    barrier = pltpu.get_barrier_semaphore()
    slab = w_z.shape[0]

    def at_first(body):
        if sub == 0:
            pl.when(pl.program_id(0) == 0)(body)

    def at_last(body):
        if sub == subs - 1:
            pl.when(pl.program_id(0) == pl.num_programs(0) - 1)(body)

    @at_first
    def _():
        for peer in peers:
            pl.semaphore_signal(barrier, inc=1, device_id=peer, device_id_type=MESH)

    def weight_copies():
        at = pl.ds(pl.multiple_of(f * slab, 16), slab)
        for p, ref in enumerate((w_z, w_out_t)):
            cols = slice(p * ref.shape[1], (p + 1) * ref.shape[1])
            target = wz_o.at[at, cols]
            yield pltpu.make_async_copy(ref, target, own.at[p])
            for d in range(1, n):
                yield remote(
                    ref, target, sent.at[d - 1, p], came.at[d - 1, p], {"fsdp": turned(f, d, n)}
                )

    starts, base, end_start, flag = read_info(rows, info, i)
    inner = jx_o.shape[1]
    width = inner + jb_o.shape[1]
    gain, cb, cw, taps = par[0:1, :], par[1:2, :], par[4:8, :], TAPS

    @at_first
    def _():
        unit, _inv = norm_rows(halo[...])
        before = nn((unit * gain).astype(bf16), wj[:, :width])
        ext[0:8, :] = before.astype(bf16).astype(f32)[8:16]
        run[...] = jnp.zeros_like(run)
        dec[...] = jnp.ones_like(dec)
        gap = iota((STRETCH, STRETCH), 0) - iota((STRETCH, STRETCH), 1)
        for k in range(taps - 1):
            moves = jnp.where(gap == taps - 1 - k, 1.0, 0.0).astype(bf16)
            shifts[STRETCH * k : STRETCH * (k + 1), :] = moves

    normed = nrm[...]
    product = nn(normed, wj[...])
    joined = product[:, :width].astype(bf16)
    jx_o[...] = joined[:, :inner]
    jb_o[...] = joined[:, inner:]
    pos = base + iota((STRETCH, 128), 0)
    first_of = segment_start(pos, starts)
    valid = [
        jnp.where(pos - (taps - 1 - k) >= first_of, 1.0, 0.0).astype(f32) for k in range(taps - 1)
    ]
    row_at = iota((8, 128), 0)
    masked = jnp.concatenate(
        [
            shifts[STRETCH * k : STRETCH * (k + 1), :]
            * jnp.concatenate([ok.astype(bf16)] * (STRETCH // 128), axis=1)
            for k, ok in enumerate(valid)
        ],
        axis=0,
    )
    for g in range(width // 128):
        at = slice(128 * g, 128 * (g + 1))
        if g % 2 == 0:
            tile = nn(masked, joined[:, 128 * g : min(128 * (g + 2), width)])
        fresh = joined[:, at].astype(f32)
        before = ext[:, at]
        ext[:, at] = fresh[STRETCH - 8 :]
        acc = cb[:, at] + cw[taps - 1 : taps, at] * fresh
        part = slice(128 * (g % 2), 128 * (g % 2 + 1))
        for k in range(taps - 1):
            d = taps - 1 - k
            moved = tile[STRETCH * k : STRETCH * (k + 1), part]
            edge = jnp.where(row_at < d, pltpu.roll(before, d, axis=0), 0.0) * valid[k][0:8]
            moved = jnp.concatenate([moved[0:8] + edge, moved[8:]], axis=0)
            acc = acc + cw[k : k + 1, at] * moved
        sig = jax.nn.sigmoid(acc)
        act = acc * sig
        vbc_o[:, at] = act.astype(bf16)
        slope = sig + act * (1.0 - sig)
        if 128 * g < inner:
            sx_o[:, at] = slope.astype(bf16)
        else:
            sb_o[:, 128 * g - inner : 128 * (g + 1) - inner] = slope
    pre = jnp.transpose(product[:, width:])[:HEAD_ROWS] + par[8:16, 0:1]
    step = jax.nn.softplus(pre)
    logd = -step * jnp.exp(par[8:16, 1:2])
    cum = exact_rows(logd, tri[...])
    pre_o[...] = pre
    step_o[...] = step
    cum_o[...] = cum
    cum_e = cum[:, STRETCH - 1 : STRETCH]
    where_s = base + iota((1, STRETCH), 1)
    keep = jnp.where(where_s >= end_start, 1.0, 0.0).astype(f32)
    weight = jnp.exp(cum_e - cum) * step * keep
    _cols, both = columns_of([weight])
    spread = nn(both, ew[...])
    v = vbc_o[:, :inner].astype(f32)
    b = vbc_o[:, inner : inner + 128]
    state = tn(b, (v * spread).astype(bf16))
    s_o[0] = state
    through = lanes_of(jnp.exp(cum_e) * flag, e8[...])
    run[...] = through * run[...] + state
    dec[...] = dec[...] * through
    end_o[...] = run[...].astype(bf16)
    dec_o[...] = dec[...]

    @at_first
    def _():
        pl.semaphore_wait(barrier, len(peers))
        for copy in weight_copies():
            copy.start()

    @at_last
    def _():
        if chain == 2:
            copy = remote(end_o, got, hop.at[0], hop.at[1], {"ctx": twin})
            copy.start()
            copy.wait()
            inc_o[...] = jnp.where(here > 0, got[...], jnp.zeros_like(got))
        else:
            inc_o[...] = jnp.zeros_like(inc_o)
        for copy in weight_copies():
            copy.wait()


def view(ref, kind, sub):
    if kind == "r":
        return ref.at[pl.ds(STRETCH * sub, STRETCH), :]
    if kind == "l":
        return ref.at[:, pl.ds(STRETCH * sub, STRETCH)]
    if kind == "b":
        return ref.at[pl.ds(sub, 1)]
    return ref


def in_turn(kernel, subs, kinds):
    def body(*refs):
        for sub in range(subs):
            kernel(sub, subs, *[view(ref, kind, sub) for ref, kind in zip(refs, kinds)])

    return body


def mix_kernel(
    rows, sub, subs, info, vbc, step, cum, s_in, inc, normed, gout, wz_out, par, e_step, e_scale, e8,
    z_o, out_o, gn_o, sum_o, st_o, br_o,
    run, gram,
):
    i = pl.program_id(0) * subs + sub
    starts, base, _end_start, flag = read_info(rows, info, i)
    inner = out_o.shape[1]
    gain = par[2:3, :inner]
    dskip = lanes_of(par[8:16, 2:3], e8[...])

    if sub == 0:

        @pl.when(i == 0)
        def _():
            run[...] = inc[...].astype(f32)

    st = run[...].astype(bf16)
    st_o[0] = st
    cum_v = cum[...]
    cum_e = cum_v[:, STRETCH - 1 : STRETCH]
    through = lanes_of(jnp.exp(cum_e) * flag, e8[...])
    run[...] = through * run[...] + s_in[0]

    row_first = segment_start(base + iota((1, STRETCH), 1), starts)
    scale = jnp.exp(cum_v) * jnp.where(row_first < base, 1.0, 0.0).astype(f32)
    cum2 = cum_v * LOG2E
    cols, both = columns_of([cum2, step[...], scale])
    step_x = nn(both, e_step[...])
    scale_x = nn(both, e_scale[...])
    b = vbc[:, inner : inner + 128]
    c = vbc[:, inner + 128 : inner + 256]
    carried = nn(c, st) * scale_x
    half = STRETCH // 2
    low, high = slice(0, half), slice(half, STRETCH)
    t_at = iota((half, STRETCH), 0)
    s_at = iota((half, STRETCH), 1)
    causal = (s_at <= t_at)[:, low]
    first_low = segment_start(iota((half, half), 0) + base, starts)
    first_high = segment_start(t_at + (base + half), starts)
    mask_a = causal & ((s_at + base)[:, low] >= first_low)
    mask_b = (s_at <= t_at + half) & (s_at + base >= first_high)
    gram[low, low] = jnp.where(mask_a, nt(c[low], b[low]), 0.0)
    gram[high, :] = jnp.where(mask_b, nt(c[high], b), 0.0)
    lane = iota((STRETCH, 128), 1)
    pieces = []
    for p in range(inner // 128):
        at = slice(128 * p, 128 * (p + 1))
        v = vbc[:, at].astype(f32)
        sv = (v * step_x[:, at]).astype(bf16)
        rest = carried[:, at] + dskip[:, at] * v
        acc_low, acc_high = rest[low], rest[high]
        for j in range(2):
            h = 2 * p + j
            side = (lane < 64) if j == 0 else (lane >= 64)
            part = jnp.where(side, sv, jnp.zeros_like(sv))
            row = cum2[h : h + 1, :]
            first_gap = cols[low, h : h + 1] - row[:, low]
            cross_gap = cols[high, h : h + 1] - row[:, low]
            last_gap = cols[high, h : h + 1] - row[:, high]
            decay_b = jnp.concatenate(
                [jnp.exp2(cross_gap), jnp.exp2(jnp.minimum(last_gap, 0.0))], axis=1
            )
            decay_a = jnp.exp2(jnp.minimum(first_gap, 0.0))
            acc_low = acc_low + nn((gram[low, low] * decay_a).astype(bf16), part[low])
            acc_high = acc_high + nn((gram[high, :] * decay_b).astype(bf16), part)
        pieces.append(jnp.concatenate([acc_low, acc_high], axis=0))
    out = jnp.concatenate(pieces, axis=1)
    out_o[...] = out
    zf = nn(normed[...], wz_out[:, :inner])
    z_o[...] = zf
    gated = out * (zf * jax.nn.sigmoid(zf))
    gn = nn(gout[...], wz_out[:, inner:])
    gn_o[...] = gn
    gg = gated * gain
    br_o[...] = nt(wz_out[:, inner:], gg.astype(bf16)).astype(bf16)
    ss = jnp.sum(gated * gated, axis=1, keepdims=True)
    dq = jnp.sum(gn * gg, axis=1, keepdims=True)
    sum_o[...] = jnp.transpose(jnp.where(lane == 0, ss, dq))[0:2]


def gate_kernel(
    rows, info, sums, cum, out, z, gn, vc, st, par, e_scale, e8, f_sum,
    gz_o, gb_o, gc_o, n2_o, a_o, gs_o, start_o, misc_o,
    run,
):
    step_id = pl.program_id(0)
    blocks = pl.num_programs(0)
    i = blocks - 1 - step_id
    starts, base, _end_start, flag = read_info(rows, info, i)
    inner = z.shape[1]
    gain = par[2:3, :inner]
    dskip = lanes_of(par[8:16, 2:3], e8[...])

    @pl.when(step_id == 0)
    def _():
        run[...] = jnp.zeros_like(run)
        misc_o[...] = jnp.zeros_like(misc_o)

    alpha = lax.rsqrt(sums[0:1, :] / INNER + epsilon)
    beta = alpha * alpha * alpha * sums[1:2, :] / INNER
    cum_v = cum[...]
    row_first = segment_start(base + iota((1, STRETCH), 1), starts)
    scale = jnp.exp(cum_v) * jnp.where(row_first < base, 1.0, 0.0).astype(f32)
    cols, both = columns_of([alpha, beta, jnp.zeros((14, STRETCH), f32), scale])
    alpha_c = cols[:, 0:1]
    beta_c = cols[:, 1:2]
    scale_x = nn(both, e_scale[...])
    v = vc[:, :inner].astype(f32)
    c = vc[:, inner + 128 : inner + 256]
    zf = z[...]
    sig = jax.nn.sigmoid(zf)
    act = zf * sig
    o = out[...]
    gated = o * act
    g_n = gn[...]
    unit = gated * alpha_c
    g_gated = alpha_c * (g_n * gain) - beta_c * gated
    g_out = g_gated * act
    gz_o[...] = (g_gated * o * (sig + act * (1.0 - sig))).astype(bf16)
    gb = g_out.astype(bf16)
    gb_o[...] = gb
    n2_o[...] = (unit * gain).astype(bf16)
    misc_o[0:1, :] += jnp.sum(g_n * unit, axis=0, keepdims=True)
    misc_o[1:2, :] += jnp.sum(g_out * v, axis=0, keepdims=True)
    gf = gb.astype(f32)
    carried = nn(c, st[0]) * scale_x
    prod = gf * (o - dskip * v) + (g_out - gf) * carried
    high, low = halves(prod)
    sums_c = nn(jnp.concatenate([high, low], axis=1), f_sum[...])
    a_o[...] = jnp.transpose(sums_c)[0:HEAD_ROWS]
    gc = (g_out * scale_x).astype(bf16)
    gc_o[...] = gc
    gs = tn(c, gc)
    gs_o[0] = gs
    through = lanes_of(jnp.exp(cum_v[:, STRETCH - 1 : STRETCH]) * flag, e8[...])
    run[...] = through * run[...] + gs
    start_o[...] = run[...].astype(bf16)


def scan_kernel(
    rows, info, vbc, gb, gc, step, cum, pre, a_sum, st, gs_in, outg, sx, sb, jx, jb, par,
    e_step, e_w, e8, f_all, tril,
    gcat_o, tail_o, head_o, misc_o, dt_o,
    run, ext, gram, acc, prod,
):
    step_id = pl.program_id(0)
    blocks = pl.num_programs(0)
    i = blocks - 1 - step_id
    starts, base, end_start, flag = read_info(rows, info, i)
    inner = gb.shape[1]
    width = inner + jb.shape[1]
    cw, taps = par[4:8, :], TAPS
    rate = jnp.exp(par[8:16, 1:2])
    dskip = lanes_of(par[8:16, 2:3], e8[...])

    @pl.when(step_id == 0)
    def _():
        run[...] = outg[...].astype(f32)
        ext[...] = jnp.zeros((8, width), f32)
        misc_o[...] = jnp.zeros_like(misc_o)
        dt_o[...] = jnp.zeros_like(dt_o)

    cum_v = cum[...]
    step_v = step[...]
    cum_e = cum_v[:, STRETCH - 1 : STRETCH]
    after = run[...]
    low_after = after.astype(bf16)
    state = st[0]
    through = lanes_of(jnp.exp(cum_e) * flag, e8[...])
    g_through = jnp.sum(after * state.astype(f32), axis=0, keepdims=True) * through
    end_more = jnp.sum(e8[...] * g_through, axis=1, keepdims=True)
    run[...] = through * after + gs_in[0]

    where_s = base + iota((1, STRETCH), 1)
    row_first = segment_start(where_s, starts)
    end_decay = jnp.exp(cum_e - cum_v) * jnp.where(where_s >= end_start, 1.0, 0.0).astype(f32)
    weight = end_decay * step_v
    cum2 = cum_v * LOG2E
    ok_rows = [
        jnp.where(joined_ok(where_s, d, starts), 1.0, 0.0).astype(f32)
        for d in range(taps - 1, 0, -1)
    ]
    cols, both = columns_of([cum2, step_v, weight] + ok_rows)
    b = vbc[:, inner : inner + 128]
    c = vbc[:, inner + 128 : inner + 256]
    half = STRETCH // 2
    low, high = slice(0, half), slice(half, STRETCH)
    s_at = iota((half, STRETCH), 0)
    t_at = iota((half, STRETCH), 1)
    mask_a = (s_at <= t_at) & (s_at + base >= row_first)
    mask_b = (s_at <= t_at)[:, low] & ((s_at + (base + half)) >= row_first)[:, high]
    gram[low, :] = jnp.where(mask_a, nt(b[low], c), 0.0)
    gram[high, low] = jnp.where(mask_b, nt(b[high], c[high]), 0.0)
    acc[...] = jnp.zeros_like(acc)
    lane = iota((STRETCH, 128), 1)
    ok = [
        jnp.broadcast_to(cols[:, 3 * HEAD_ROWS + k : 3 * HEAD_ROWS + k + 1], (STRETCH, 128))
        for k in range(taps - 1)
    ]

    def convolve(at, own, j_f):
        following = ext[:, at]
        joint = jnp.concatenate([own, following], axis=0)
        ext[:, at] = own[0:8]
        misc_o[taps : taps + 1, at] += jnp.sum(own, axis=0, keepdims=True)
        misc_o[taps - 1 : taps, at] += jnp.sum(own * j_f, axis=0, keepdims=True)
        total = own * cw[taps - 1 : taps, at]
        for k in range(taps - 1):
            d = taps - 1 - k
            term = pltpu.roll(joint, STRETCH + 8 - d, axis=0)[:STRETCH] * ok[k]
            misc_o[k : k + 1, at] += jnp.sum(term * j_f, axis=0, keepdims=True)
            total = total + term * cw[k : k + 1, at]
        gcat_o[:, at] = total.astype(bf16)
        tail_o[:, at] = jnp.where(step_id == 0, total[STRETCH - 8 :], tail_o[:, at])

    g_b = jnp.zeros((STRETCH, 128), f32)
    g_c = jnp.zeros((STRETCH, 128), f32)
    for p in range(inner // 128):
        at = slice(128 * p, 128 * (p + 1))
        step_x = nn(both, e_step[:, at])
        v = vbc[:, at].astype(f32)
        sv = (v * step_x).astype(bf16)
        g_pair = gb[:, at]
        u_low = jnp.zeros((half, 128), f32)
        u_high = jnp.zeros((half, 128), f32)
        for j in range(2):
            h = 2 * p + j
            side = (lane < 64) if j == 0 else (lane >= 64)
            g_side = jnp.where(side, g_pair, jnp.zeros_like(g_pair))
            sv_side = jnp.where(side, sv, jnp.zeros_like(sv))
            row = cum2[h : h + 1, :]
            first_gap = row[:, low] - cols[low, h : h + 1]
            cross_gap = row[:, high] - cols[low, h : h + 1]
            last_gap = row[:, high] - cols[high, h : h + 1]
            decay_a = jnp.concatenate(
                [jnp.exp2(jnp.minimum(first_gap, 0.0)), jnp.exp2(cross_gap)], axis=1
            )
            decay_b = jnp.exp2(jnp.minimum(last_gap, 0.0))
            u_low = u_low + nn((gram[low, :] * decay_a).astype(bf16), g_side)
            u_high = u_high + nn((gram[high, low] * decay_b).astype(bf16), g_side[high])
            acc[low, :] += nt(sv_side[low], g_pair) * decay_a
            acc[high, low] += nt(sv_side[high], g_pair[high]) * decay_b
        u = jnp.concatenate([u_low, u_high], axis=0)
        w_x = nn(both, e_w[:, at])
        y = nn(b, low_after[:, at])
        h1, l1 = halves(sv.astype(f32) * u)
        prod[:, at] = h1
        prod[:, inner + 128 * p : inner + 128 * (p + 1)] = l1
        prod[:, 2 * inner + 128 * p : 2 * inner + 128 * (p + 1)] = (v * y).astype(bf16)
        g_b = g_b + nt((v * w_x).astype(bf16), low_after[:, at])
        g_c = g_c + nt(gc[:, at], state[:, at])
        gv = dskip[:, at] * g_pair.astype(f32) + step_x * u + w_x * y
        convolve(at, gv * sx[:, at].astype(f32), jx[:, at].astype(f32))

    gg_a = jnp.where(mask_a, acc[low, :], 0.0).astype(bf16)
    gg_b = jnp.where(mask_b, acc[high, low], 0.0).astype(bf16)
    g_b = g_b + jnp.concatenate([nn(gg_a, c), nn(gg_b, c[high])], axis=0)
    g_c = g_c + tn(gg_a, b[low])
    g_c = g_c + jnp.concatenate([jnp.zeros((half, 128), f32), tn(gg_b, b[high])], axis=0)
    for k, part in enumerate((g_b, g_c)):
        here = slice(128 * k, 128 * (k + 1))
        convolve(
            slice(inner + 128 * k, inner + 128 * (k + 1)),
            part * sb[:, here],
            jb[:, here].astype(f32),
        )

    sums_r = jnp.transpose(nn(prod[...], f_all[...]))
    g_mixed = sums_r[0:HEAD_ROWS]
    g_end = sums_r[HEAD_ROWS : 2 * HEAD_ROWS]
    ends = g_end * weight
    g_cum = a_sum[...] - g_mixed - ends
    end_add = jnp.sum(ends, axis=1, keepdims=True) + end_more
    g_log = exact_rows(g_cum, tril[...]) + end_add
    slope_dt = jax.nn.sigmoid(pre[...])
    ratio = jnp.where(step_v > 0.0, slope_dt / step_v, 1.0)
    g_pre_dt = (g_end * end_decay - g_log * rate) * slope_dt + g_mixed * ratio
    dt_o[0:HEAD_ROWS, :] += g_log * (-step_v * rate)
    dt_o[HEAD_ROWS:, :] += g_pre_dt
    pad = jnp.zeros((128 - HEAD_ROWS, STRETCH), f32)
    gcat_o[:, width:] = jnp.transpose(jnp.concatenate([g_pre_dt, pad], axis=0)).astype(bf16)

    head_o[...] = ext[...]


def exit_kernel(
    rows, blocks, rim_side, info, tok, gout, mine, gz, gcat, par, wz_out, wj, *rest
):
    step_id = pl.program_id(0)
    i = blocks - 1 - step_id
    starts, base, _end_start, _flag = read_info(rows, info, i)
    inner = gz.shape[1]
    if rim_side:
        tail, nxt, last_j, gr_o, gain_o, rim_o, rim_w_o, fix = rest
        taps, width = TAPS, tail.shape[1]
        cw = par[4:8, :width]
    else:
        gr_o, gain_o = rest
    gain = par[0:1, :]

    g_normed = nt(gz[...], wz_out[:, :inner]) + nt(gcat[...], wj[...])

    def finish(g_normed):
        unit, inverse = norm_rows(tok[...])
        scaled = g_normed * gain
        mean = jnp.mean(scaled * unit, axis=1, keepdims=True)
        own = gout[...].astype(f32) * mine[...]
        gr_o[...] = jnp.transpose(own + inverse * (scaled - unit * mean)).astype(bf16)
        gain_o[...] += jnp.sum(g_normed * unit, axis=0, keepdims=True)

    @pl.when(step_id == 0)
    def _():
        gain_o[...] = jnp.zeros_like(gain_o)

    if not rim_side:
        finish(g_normed)
        return

    @pl.when(step_id == 0)
    def _():
        fix[0:8, :] = jnp.zeros((8, width), f32)
        fix[8:16, :] = nxt[...]
        places = base + STRETCH - 8 + iota((8, 128), 0)
        wide = last_j[8:16, :].astype(f32)
        total = tail[...]
        for k in range(taps - 1):
            d = taps - 1 - k
            ok = jnp.where(joined_ok(places, d, starts), 1.0, 0.0).astype(f32)
            inside = jnp.where(iota((8, width), 0) >= 8 - d, fix[d : d + 8, :], 0.0)
            term = inside * jnp.concatenate([ok] * (width // 128), axis=1)
            total = total + term * cw[k : k + 1, :]
            rim_w_o[k : k + 1, :] = jnp.sum(term * wide, axis=0, keepdims=True)
        rim_w_o[taps - 1 : 8, :] = jnp.zeros((9 - taps, width), f32)
        fix[0:8, :] = jnp.zeros((8, width), f32)
        fix[8:16, :] = total.astype(bf16).astype(f32) - tail[...].astype(bf16).astype(f32)
        rim_o[...] = fix[...].astype(bf16)

    @pl.when(step_id == 0)
    def _():
        more = nt(rim_o[...], wj[:, :width])
        finish(g_normed + jnp.concatenate([jnp.zeros((STRETCH - 16, more.shape[1]), f32), more]))

    @pl.when(step_id > 0)
    def _():
        finish(g_normed)


def finish_kernel(parts, place, part, base, sums, out):
    wide = part[...].astype(f32) * lax.rsqrt(sums[0:1, :] / INNER + epsilon)
    size = out.shape[0]
    for k in range(parts):

        @pl.when(place[0] == k)
        def _():
            add = jnp.transpose(base[:, size * k : size * (k + 1)].astype(f32))
            out[...] = (wide + add).astype(bf16)


def gather_kernel(
    n, chain, x, bc, dt_t, par, tok, out, halo, nrm, dt, dts, sent, came, passed, relayed, own, hop
):
    f = lax.axis_index("fsdp")
    parity, twin = twin_of(lax.axis_index("ctx"))
    half = x.shape[0] // 2
    here = lax.axis_index("ctx")
    following = turned(here, 1, chain)
    sides = [{"ctx": twin}] if chain == 2 else [{"ctx": following}, {"ctx": turned(here, -1, chain)}]
    start_together([{"fsdp": turned(f, d, n)} for d in range(1, n)] + sides)
    heads, rows = dt_t.shape
    wide = -(-rows // 128) * 128
    flat = jnp.concatenate(
        [dt_t[...].astype(f32), jnp.zeros((heads, wide - rows), f32)], axis=1
    )
    flat = jnp.concatenate([flat, jnp.zeros((HEAD_ROWS - heads, wide), f32)], axis=0)
    dt[...] = flat.astype(bf16)
    dts[pl.ds(f, 1)] = dt[...][None]
    tiny = []
    for d in range(1, n):
        copy = remote(
            dt, dts.at[f], sent.at[d - 1, 2], came.at[d - 1, 2], {"fsdp": turned(f, d, n)}
        )
        copy.start()
        tiny.append(copy)
    pieces = []
    at = 0
    for ref in (x, bc):
        pieces.append((ref, slice(at, at + ref.shape[1])))
        at += ref.shape[1]

    def place(source, side):
        return pl.ds(pl.multiple_of(source * rows + side * half, 16), half)

    mine = pl.ds(pl.multiple_of(parity * half, 16), half)
    copies = []
    for d in range(1, n):
        for p, (ref, cols) in enumerate(pieces):
            copy = remote(
                ref.at[mine, :], out.at[place(f, parity), cols],
                sent.at[d - 1, p], came.at[d - 1, p], {"fsdp": turned(f, d, n)},
            )
            copy.start()
            copies.append(copy)
    edge = halo.shape[0]
    copy = remote(
        tok.at[pl.ds(tok.shape[0] - edge, edge), :], halo, hop.at[0], hop.at[1], {"ctx": following}
    )
    copy.start()
    locals_ = [copy]
    for p, (ref, cols) in enumerate(pieces):
        copy = pltpu.make_async_copy(
            ref, out.at[pl.ds(pl.multiple_of(f * rows, 16), rows), cols], own.at[p]
        )
        copy.start()
        locals_.append(copy)
    gain = par[...][None, :]

    def norm_block(tok_block, nrm_block):
        unit, _inverse = norm_rows(tok_block[...])
        nrm_block[...] = (unit * gain).astype(bf16)

    steps = tok.shape[0] // (2 * STRETCH)

    def normalise(first, count):
        block = pl.BlockSpec((2 * STRETCH, tok.shape[1]), lambda i: (i + first, 0))
        pltpu.emit_pipeline(norm_block, grid=(count,), in_specs=[block], out_specs=[block])(
            tok, nrm
        )

    relays = []

    def relay(d):
        source = turned(f, -d, n)
        for p, (ref, cols) in enumerate(pieces):
            copies[(d - 1) * len(pieces) + p].wait_recv()
            piece = out.at[place(source, parity), cols]
            copy = remote(piece, piece, passed.at[d - 1, p], relayed.at[d - 1, p], {"ctx": twin})
            copy.start()
            relays.append(copy)

    normalise(0, steps)
    for d in range(1, n):
        relay(d)
    for copy in tiny:
        copy.wait()
    joint = jnp.concatenate([dts[q].astype(f32)[:, :rows] for q in range(n)], axis=1)
    joint = jnp.concatenate([joint, jnp.zeros((128 - HEAD_ROWS, n * rows), f32)], axis=0)
    out[:, at:] = jnp.transpose(joint).astype(bf16)
    for copy in copies:
        copy.wait_send()
    for copy in locals_:
        copy.wait()
    for copy in relays:
        copy.wait()


def gathered(x, bc, dt_t, par, tok):
    n = lax.axis_size("fsdp")
    pieces = (n - 1, 3)
    width = x.shape[1] + bc.shape[1] + 128
    return pl.pallas_call(
        functools.partial(gather_kernel, n, lax.axis_size("ctx")),
        out_shape=[
            jax.ShapeDtypeStruct((n * x.shape[0], width), bf16),
            jax.ShapeDtypeStruct((16, tok.shape[1]), bf16),
            jax.ShapeDtypeStruct(tok.shape, bf16),
        ],
        in_specs=[pl.BlockSpec(memory_space=pltpu.VMEM)] * 4 + [pl.BlockSpec(memory_space=pl.ANY)],
        out_specs=[pl.BlockSpec(memory_space=pltpu.VMEM)] * 2
        + [pl.BlockSpec(memory_space=pl.ANY)],
        scratch_shapes=[
            pltpu.VMEM((HEAD_ROWS, -(-x.shape[0] // 128) * 128), bf16),
            pltpu.VMEM((n, HEAD_ROWS, -(-x.shape[0] // 128) * 128), bf16),
        ]
        + [pltpu.SemaphoreType.DMA(pieces)] * 4
        + [pltpu.SemaphoreType.DMA((3,)), pltpu.SemaphoreType.DMA((2,))],
        compiler_params=pltpu.CompilerParams(collective_id=1, has_side_effects=True),
    )(x, bc, dt_t, par, tok)


def total_kernel(n, part, out, slots, sent, came):
    me = lax.axis_index("tp")
    start_together([{"tp": turned(me, d, n)} for d in range(1, n)])
    copies = []
    for d in range(1, n):
        copy = remote(
            part, slots.at[d - 1], sent.at[d - 1], came.at[d - 1], {"tp": turned(me, d, n)}
        )
        copy.start()
        copies.append(copy)
    total = part[...]
    for d in range(1, n):
        copies[d - 1].wait_recv()
        total = total + slots[d - 1]
    out[...] = total
    for copy in copies:
        copy.wait_send()


def total_over_tp(part):
    n = lax.axis_size("tp")
    return pl.pallas_call(
        functools.partial(total_kernel, n),
        out_shape=jax.ShapeDtypeStruct(part.shape, f32),
        in_specs=[pl.BlockSpec(memory_space=pltpu.VMEM)],
        out_specs=pl.BlockSpec(memory_space=pltpu.VMEM),
        scratch_shapes=[
            pltpu.VMEM((n - 1,) + part.shape, f32),
            pltpu.SemaphoreType.DMA((n - 1,)),
            pltpu.SemaphoreType.DMA((n - 1,)),
        ],
        compiler_params=pltpu.CompilerParams(collective_id=2, has_side_effects=True),
    )(part)


def share_over_tp(m, t, shares, sent, came):
    copies = []
    for p, (buf, own) in enumerate(shares):
        buf[pl.ds(t, 1)] = own[None]
    for d in range(1, m):
        for p, (buf, _own) in enumerate(shares):
            k = 3 * (d - 1) + p
            copy = remote(buf.at[t], buf.at[t], sent.at[k], came.at[k], {"tp": turned(t, d, m)})
            copy.start()
            copies.append(copy)
    for copy in copies:
        copy.wait()
    totals = []
    for buf, _own in shares:
        total = buf[0].astype(f32)
        for q in range(1, m):
            total = total + buf[q].astype(f32)
        totals.append(total)
    return totals


def fold_over_tp(m, t, shares, sent, came):
    at_edge = (t == 0) | (t == 3)
    in_middle = jnp.logical_not(at_edge)
    inward = jnp.where(t == 0, 1, 2)
    outward = jnp.where(t == 1, 0, 3)
    across = 3 - t

    def copy_of(phase, p, src, dst, peer):
        buf = shares[p][0]
        k = 3 * phase + p
        return remote(buf.at[src], buf.at[dst], sent.at[k], came.at[k], {"tp": peer})

    every = range(len(shares))
    for buf, own in shares:
        buf[0] = own

    @pl.when(at_edge)
    def _():
        for p in every:
            copy_of(0, p, 0, 1, inward).start()
        for p in every:
            copy_of(0, p, 0, 1, inward).wait_send()
        for p in every:
            copy_of(2, p, 4, 4, inward).wait_recv()

    @pl.when(in_middle)
    def _():
        for p in every:
            buf = shares[p][0]
            copy_of(0, p, 0, 1, outward).wait_recv()
            buf[2] = (buf[0].astype(f32) + buf[1].astype(f32)).astype(buf.dtype)
            copy_of(1, p, 2, 3, across).start()
        for p in every:
            buf = shares[p][0]
            copy_of(1, p, 2, 3, across).wait()
            buf[4] = (buf[2].astype(f32) + buf[3].astype(f32)).astype(buf.dtype)
            copy_of(2, p, 4, 4, outward).start()
        for p in every:
            copy_of(2, p, 4, 4, outward).wait_send()

    return [buf[4].astype(f32) for buf, _own in shares]


def reduce_kernel(
    n, m, bc_cols, conv_bc,
    p_out, p_z, p_cat, m_scan, m_rim, m_gate, m_dt, m_gain,
    o_all, o_small, o_wide,
    give, take, mid, slots, final, bc_slots, small, small_slots, wide_slots, gain_slots,
    s1, r1, s2, r2, s3, r3, s4, r4,
):
    f = lax.axis_index("fsdp")
    t = lax.axis_index("tp")
    parity, twin = twin_of(lax.axis_index("ctx"))
    start_together(
        [{"ctx": twin}]
        + [{"fsdp": turned(f, d, n)} for d in range(1, n)]
        + [{"tp": turned(t, d, m)} for d in range(1, m)]
    )
    inner = p_out.shape[1]
    rows = p_out.shape[0] // n
    half = rows // 2

    def piece(q, side):
        at = pl.ds(pl.multiple_of(q * rows + side * half, 16), half)
        return jnp.concatenate([p_out[at, :], p_z[at, :], p_cat[at, :]], axis=1)

    copies = []
    for q in range(n):
        give[q] = piece(q, 1 - parity).astype(bf16)
        copy = remote(give.at[q], take.at[q], s1.at[q], r1.at[q], {"ctx": twin})
        copy.start()
        copies.append(copy)
    w_scan = m_scan.shape[1]
    w_gate = m_gate.shape[1]
    w_dt = m_dt.shape[1]
    small[...] = jnp.zeros_like(small)
    small[:, 0:w_scan] = m_scan[...] + m_rim[...]
    at = w_scan
    small[:, at : at + w_gate] = m_gate[...]
    at += w_gate
    small[:, at : at + w_dt] = m_dt[0:8, :]
    small[:, at + w_dt : at + 2 * w_dt] = m_dt[8:16, :]
    at += 2 * w_dt
    small[0:1, at:] = m_gain[...]
    small_slots[0, pl.ds(parity, 1)] = small[...][None]
    copy = remote(
        small, small_slots.at[0, parity], s1.at[n], r1.at[n], {"ctx": twin}
    )
    copy.start()
    copies.append(copy)

    copies[n].wait()
    small_slots[1, pl.ds(f, 1)] = (small_slots[0, 0] + small_slots[0, 1])[None]
    seconds = []
    for d in range(1, n):
        copy = remote(
            small_slots.at[1, f], small_slots.at[1, f], s2.at[n - 1 + d - 1], r2.at[n - 1 + d - 1],
            {"fsdp": turned(f, d, n)},
        )
        copy.start()
        seconds.append(copy)
    for q in range(n):
        copies[q].wait()
        mid[q] = (piece(q, parity) + take[q].astype(f32)).astype(bf16)
    slots[pl.ds(f, 1)] = mid[pl.ds(f, 1)]
    for d in range(1, n):
        peer = turned(f, d, n)
        copy = remote(
            mid.at[peer], slots.at[f], s2.at[d - 1], r2.at[d - 1], {"fsdp": peer}
        )
        copy.start()
        seconds.append(copy)
    for copy in seconds:
        copy.wait()
    small_sum = small_slots[1, 0]
    whole = slots[0].astype(f32)
    for q in range(1, n):
        small_sum = small_sum + small_slots[1, q]
        whole = whole + slots[q].astype(f32)
    final[...] = whole
    bc_at = slice(3 * inner, 3 * inner + bc_cols)
    o_small[...] = small_sum[:, :at]
    shares = (
        (bc_slots, whole[:, bc_at].astype(bf16)),
        (wide_slots, small_sum[:, conv_bc:w_scan]),
        (gain_slots, small_sum[0:1, at:]),
    )
    bc_sum, wide_sum, gain_sum = (fold_over_tp if m == 4 else share_over_tp)(m, t, shares, s3, r3)
    o_wide[:, :bc_cols] = wide_sum
    o_wide[:, bc_cols:] = jnp.broadcast_to(gain_sum, (8, gain_sum.shape[1]))
    final[:, bc_at] = bc_sum
    here = pl.ds(pl.multiple_of(parity * half, 8), half)
    o_all[here, :] = final[...]
    copy = remote(final, o_all.at[here, :], s4.at[0], r4.at[0], {"ctx": twin})
    copy.start()
    copy.wait()


def reduced(parts, miscs, bc_cols):
    n, m = lax.axis_size("fsdp"), lax.axis_size("tp")
    p_out, _p_z, p_cat = parts
    rows = p_out.shape[0] // n
    half = rows // 2
    inner = p_out.shape[1]
    wide = 2 * inner + p_cat.shape[1]
    m_scan, _m_rim, m_gate, m_dt, m_gain = miscs
    kept = m_scan.shape[1] + m_gate.shape[1] + 2 * m_dt.shape[1]
    small = kept + m_gain.shape[1]
    crossing = m_scan.shape[1] - inner + m_gain.shape[1]
    dma = pltpu.SemaphoreType.DMA

    def shape(*dims):
        return jax.ShapeDtypeStruct(dims, f32)

    return pl.pallas_call(
        functools.partial(reduce_kernel, n, m, bc_cols, inner),
        out_shape=[
            shape(rows, wide), shape(8, kept), shape(8, crossing),
        ],
        in_specs=[pl.BlockSpec(memory_space=pltpu.VMEM)] * 8,
        out_specs=[pl.BlockSpec(memory_space=pltpu.VMEM)] * 3,
        scratch_shapes=[
            pltpu.VMEM((n, half, wide), bf16),
            pltpu.VMEM((n, half, wide), bf16),
            pltpu.VMEM((n, half, wide), bf16),
            pltpu.VMEM((n, half, wide), bf16),
            pltpu.VMEM((half, wide), f32),
            pltpu.VMEM((max(m, 5), half, bc_cols), bf16),
            pltpu.VMEM((8, small), f32),
            pltpu.VMEM((2, max(n, 2), 8, small), f32),
            pltpu.VMEM((max(m, 5), 8, bc_cols), f32),
            pltpu.VMEM((max(m, 5), 1, m_gain.shape[1]), f32),
            dma((n + 1,)), dma((n + 1,)), dma((2 * n - 2,)), dma((2 * n - 2,)),
            dma((3 * m,)), dma((3 * m,)), dma((1,)), dma((1,)),
        ],
        compiler_params=pltpu.CompilerParams(
            collective_id=3, has_side_effects=True, vmem_limit_bytes=48 * 1024 * 1024
        ),
    )(*parts, *miscs)


def constants(inner, heads):
    lane_head = np.arange(inner) // (inner // heads)
    e8 = (np.arange(HEAD_ROWS)[:, None] == lane_head[None, :]).astype(np.float32)

    def spread(kind):
        m = np.zeros((128, inner), np.float32)
        m[HEAD_ROWS * kind : HEAD_ROWS * (kind + 1)] = e8
        return jnp.asarray(np.concatenate([m, m], axis=0), bf16)

    def gather(kind):
        m = np.zeros((inner, 128), np.float32)
        m[:, HEAD_ROWS * kind : HEAD_ROWS * (kind + 1)] = e8.T
        return jnp.asarray(np.concatenate([m, m], axis=0), bf16)

    at = np.arange(STRETCH)
    upper = jnp.asarray((at[:, None] <= at[None, :]).astype(np.float32), bf16)
    lower = jnp.asarray((at[:, None] >= at[None, :]).astype(np.float32), bf16)
    return jnp.asarray(e8), spread, gather, upper, lower


def passed_along(block, axis, distance):
    devices = range(lax.axis_size(axis))
    route = [(i - distance, i) for i in devices if i - distance in devices]
    return lax.ppermute(block, axis, route)


def entering(decay, state, axis, reverse):
    size = lax.axis_size(axis)
    if size == 2:
        return passed_along(state, axis, -1 if reverse else 1)
    index = lax.axis_index(axis)
    decays = lax.all_gather(decay.astype(bf16), axis)
    states = lax.all_gather(state, axis)

    def lap(k, before):
        at = size - 1 - k if reverse else k
        reached = at > index if reverse else at < index
        new = decays[at].astype(f32) * before + states[at].astype(f32)
        return jnp.where(reached, new, before)

    return lax.fori_loop(0, size, lap, jnp.zeros(state.shape, f32)).astype(bf16)


def fill_params(raw, par):
    gain, gate, x_w, bc_w, x_b, bc_b, bias, rate, skip = raw
    inner = x_w.shape[1]
    width = inner + bc_w.shape[1]
    heads = bias.shape[0]

    @pl.when(pl.program_id(0) == 0)
    def _():
        par[0:1, :] = gain[...][None, :]
        par[1:2, :inner] = x_b[...][None, :]
        par[1:2, inner:width] = bc_b[...][None, :]
        par[2:3, :inner] = gate[...][None, :]
        par[4:8, :inner] = x_w[...]
        par[4:8, inner:width] = bc_w[...]
        row, lane = iota((HEAD_ROWS, 128), 0), iota((HEAD_ROWS, 128), 1)
        table = jnp.zeros((HEAD_ROWS, 128), f32)
        for h in range(heads):
            for k, ref in enumerate((bias, rate, skip)):
                table = jnp.where((row == h) & (lane == k), ref[h], table)
        par[8:16, 0:128] = table


def call(kernel, blocks, ins, outs, scratch, remote_id=None, raw=None):
    def spec(shape, how):
        if how == "smem":
            return pl.BlockSpec(memory_space=pltpu.SMEM)
        if how == "any":
            return pl.BlockSpec(memory_space=pl.ANY)
        return pl.BlockSpec(shape, how)

    places = [k for k, (_a, _s, how) in enumerate(ins) if how == "par"]
    ins = [entry for entry in ins if entry[2] != "par"]
    body = kernel
    if places:
        count = len(raw)
        model = raw[0].shape[0]
        scratch = list(scratch) + [pltpu.VMEM((16, model), f32)]

        def body(*refs):
            par = refs[-1]
            fill_params(refs[:count], par)
            rest = list(refs[count:-1])
            rest.insert(places[0], par)
            kernel(*rest)

        def fixed_at(x):
            if x.ndim == 1 and x.shape[0] < 128:
                return (x, None, "smem")
            return (x, x.shape, lambda i: (0,) * x.ndim)

        ins = [fixed_at(x) for x in raw] + ins

    return pl.pallas_call(
        body,
        grid=(blocks,),
        in_specs=[spec(shape, how) for _a, shape, how in ins],
        out_specs=[spec(shape, how) for _s, shape, how in outs],
        out_shape=[s for s, _sh, _h in outs],
        scratch_shapes=scratch,
        compiler_params=pltpu.CompilerParams(
            dimension_semantics=("arbitrary",),
            vmem_limit_bytes=56 * 1024 * 1024,
            collective_id=remote_id,
            has_side_effects=remote_id is not None,
        ),
    )(*[a for a, _s, _h in ins])


def local(
    tokens, grad_out, lengths, norm_gain, w_z, w_x, w_bc, w_dt, conv_x_w, conv_x_b,
    conv_bc_w, conv_bc_b, dt_bias, a_log, d_skip, gate_gain, w_out,
):
    rows, model = tokens.shape
    inner = w_z.shape[1]
    heads = dt_bias.shape[0]
    states = w_bc.shape[1] // 2
    taps = conv_x_w.shape[0]
    blocks = rows // STRETCH
    width = inner + 2 * states
    tp_size = lax.axis_size("tp")
    slice_width = model // tp_size
    tp_index = lax.axis_index("tp")
    ctx_index = lax.axis_index("ctx")
    e8, spread, gather, upper, lower = constants(inner, heads)

    per_head = inner // heads

    w_joined, halo, normed = gathered(
        w_x, w_bc, w_dt.T, norm_gain, tokens
    )
    n = lax.axis_size("fsdp")
    chain = lax.axis_size("ctx")

    def shape(dims, kind):
        return jax.ShapeDtypeStruct(dims, kind)

    def whole(x):
        return (x, x.shape, lambda i: (0,) * x.ndim)

    def by_rows(x, flip=False):
        if flip:
            return (x, (STRETCH, x.shape[1]), lambda i: (blocks - 1 - i, 0))
        return (x, (STRETCH, x.shape[1]), lambda i: (i, 0))

    def by_lanes(x, flip=False):
        if flip:
            return (x, (x.shape[0], STRETCH), lambda i: (0, blocks - 1 - i))
        return (x, (x.shape[0], STRETCH), lambda i: (0, i))

    def by_block(x, flip=False):
        if flip:
            return (x, (1,) + x.shape[1:], lambda i: (blocks - 1 - i, 0, 0))
        return (x, (1,) + x.shape[1:], lambda i: (i, 0, 0))

    def fixed(x):
        return (x, x.shape, lambda i: (0,) * len(x.shape))

    info_in = (lengths, None, "smem")
    params_in = (None, None, "par")
    raw = (
        norm_gain, gate_gain, conv_x_w, conv_bc_w, conv_x_b, conv_bc_b, dt_bias, a_log, d_skip
    )
    run = functools.partial(call, raw=raw)
    state_dims = (blocks, states, inner)
    subs = 2 if blocks % 2 == 0 else 1

    def several(entries, kinds):
        scales = {"r": (subs, 1), "l": (1, subs), "b": (subs, 1, 1)}
        grown = []
        for entry, kind in zip(entries, kinds):
            if kind == "w":
                grown.append(entry)
                continue
            dims = tuple(d * k for d, k in zip(entry[1], scales[kind]))
            grown.append((entry[0], dims, entry[2]))
        return grown

    dma = pltpu.SemaphoreType.DMA
    entry_in, entry_out = "wrwwwwwwww", "rrrrrlllbwwww"
    (
        joined_x, joined_bc, vbc, slope_x, slope_bc, pre, step, cum, s_part, end_state, decay,
        incoming, wz_out,
    ) = run(
        in_turn(
            functools.partial(entry_kernel, rows, n, chain), 1, entry_in + entry_out + "w" * 9
        ),
        blocks,
        list([
            info_in, by_rows(normed), whole(halo), params_in, whole(w_joined), whole(upper),
            whole(spread(0)), whole(e8), (w_z, None, "any"), (w_out.T, None, "any"),
        ]),
        list([
            by_rows(shape((rows, inner), bf16)),
            by_rows(shape((rows, 2 * states), bf16)),
            by_rows(shape((rows, width), bf16)),
            by_rows(shape((rows, inner), bf16)),
            by_rows(shape((rows, 2 * states), f32)),
            by_lanes(shape((HEAD_ROWS, rows), f32)),
            by_lanes(shape((HEAD_ROWS, rows), f32)),
            by_lanes(shape((HEAD_ROWS, rows), f32)),
            by_block(shape(state_dims, f32)),
            fixed(shape((states, inner), bf16)),
            fixed(shape((1, inner), f32)),
            fixed(shape((states, inner), bf16)),
            (shape((model, 2 * inner), bf16), None, "any"),
        ]),
        [
            pltpu.VMEM((8, width), f32),
            pltpu.VMEM((states, inner), f32),
            pltpu.VMEM((1, inner), f32),
            pltpu.VMEM(((taps - 1) * STRETCH, STRETCH), bf16),
            pltpu.VMEM((states, inner), bf16),
            dma((n - 1, 2)),
            dma((n - 1, 2)),
            dma((2,)),
            dma((2,)),
        ],
        remote_id=4,
    )
    if chain > 2:
        incoming = entering(decay, end_state, "ctx", False)
    mix_in, mix_out = "wrllbwrrwwwww", "rrrlbl"
    z_part, out, gn, sums, state_in, branch = run(
        in_turn(functools.partial(mix_kernel, rows), subs, mix_in + mix_out + "wr"),
        blocks // subs,
        several(
            [
                info_in, by_rows(vbc), by_lanes(step), by_lanes(cum), by_block(s_part),
                whole(incoming), by_rows(normed), by_rows(grad_out), whole(wz_out), params_in,
                whole(spread(1)), whole(spread(2)), whole(e8),
            ],
            mix_in,
        ),
        several(
            [
                by_rows(shape((rows, inner), f32)),
                by_rows(shape((rows, inner), f32)),
                by_rows(shape((rows, inner), f32)),
                by_lanes(shape((2, rows), f32)),
                by_block(shape(state_dims, bf16)),
                by_lanes(shape((model, rows), bf16)),
            ],
            mix_out,
        ),
        [pltpu.VMEM((states, inner), f32), pltpu.VMEM((subs * STRETCH, STRETCH), f32)],
    )
    branch = lax.psum_scatter(branch, "tp", scatter_dimension=0, tiled=True)
    sums = total_over_tp(sums)
    g_z, g_b, g_c, normed_two, a_sum, gs_part, start_state, misc_gate = run(
        functools.partial(gate_kernel, rows),
        blocks,
        [
            info_in, by_lanes(sums, True), by_lanes(cum, True), by_rows(out, True),
            by_rows(z_part, True), by_rows(gn, True), by_rows(vbc, True), by_block(state_in, True),
            params_in, whole(spread(2)), whole(e8), whole(gather(0)),
        ],
        [
            by_rows(shape((rows, inner), bf16), True),
            by_rows(shape((rows, inner), bf16), True),
            by_rows(shape((rows, inner), bf16), True),
            by_rows(shape((rows, inner), bf16), True),
            by_lanes(shape((HEAD_ROWS, rows), f32), True),
            by_block(shape(state_dims, f32), True),
            fixed(shape((states, inner), bf16)),
            fixed(shape((8, inner), f32)),
        ],
        [pltpu.VMEM((states, inner), f32)],
    )
    sum_all = jnp.concatenate([gather(0), gather(1)[:inner]], axis=0)
    outgoing = entering(decay, start_state, "ctx", True)
    g_cat, tail, head, misc_scan, misc_dt = run(
        functools.partial(scan_kernel, rows),
        blocks,
        [
            info_in, by_rows(vbc, True), by_rows(g_b, True), by_rows(g_c, True),
            by_lanes(step, True), by_lanes(cum, True), by_lanes(pre, True), by_lanes(a_sum, True),
            by_block(state_in, True), by_block(gs_part, True), whole(outgoing),
            by_rows(slope_x, True), by_rows(slope_bc, True), by_rows(joined_x, True),
            by_rows(joined_bc, True), params_in, whole(spread(1)),
            whole(spread(2)), whole(e8), whole(sum_all), whole(lower),
        ],
        [
            by_rows(shape((rows, width + 128), bf16), True),
            fixed(shape((8, width), f32)),
            fixed(shape((8, width), f32)),
            fixed(shape((8, width), f32)),
            fixed(shape((2 * HEAD_ROWS, STRETCH), f32)),
        ],
        [
            pltpu.VMEM((states, inner), f32),
            pltpu.VMEM((8, width), f32),
            pltpu.VMEM((STRETCH, STRETCH), f32),
            pltpu.VMEM((STRETCH, STRETCH), f32),
            pltpu.VMEM((STRETCH, 3 * inner), bf16),
        ],
    )
    next_rows = passed_along(head, "ctx", -1)
    feature = jnp.arange(model, dtype=jnp.int32) // slice_width
    mine = (feature == tp_index).astype(f32)[None, :]
    last_joined = jnp.concatenate([joined_x[rows - 16 :], joined_bc[rows - 16 :]], axis=1)
    def exit_call(first, extra_in, extra_out, scratch):
        top = count = blocks

        def flipped(x):
            return (x, (STRETCH, x.shape[1]), lambda i: (top - 1 - i, 0))

        return run(
            functools.partial(exit_kernel, rows, top, first),
            count,
            [
                info_in, flipped(tokens), flipped(grad_out), whole(mine), flipped(g_z),
                flipped(g_cat), params_in, whole(wz_out), whole(w_joined),
            ]
            + extra_in,
            [
                (
                    shape((model, count * STRETCH), bf16),
                    (model, STRETCH),
                    lambda i: (0, count - 1 - i),
                ),
                fixed(shape((1, model), f32)),
            ]
            + extra_out,
            scratch,
        )

    g_resid, gain_part, rim, rim_w = exit_call(
        True,
        [whole(tail), whole(next_rows), whole(last_joined)],
        [fixed(shape((16, width), bf16)), fixed(shape((8, width), f32))],
        [pltpu.VMEM((16, width), f32)],
    )
    g_resid = lax.psum_scatter(g_resid, "tp", scatter_dimension=0, tiled=True)

    part_out = tn(grad_out, normed_two)
    part_z = tn(normed, g_z)
    part_cat = tn(normed, g_cat)
    part_rim = tn(normed[rows - 16 :], rim)
    part_cat = part_cat + jnp.pad(part_rim, ((0, 0), (0, 128)))
    s_all, s_small, s_wide = reduced(
        (part_out, part_z, part_cat),
        (misc_scan, rim_w, misc_gate, misc_dt, gain_part),
        2 * states,
    )
    if lax.axis_size("ctx") > 2:
        s_all, s_small, s_wide = jax.tree.map(
            lambda part: lax.psum(0.5 * part, "ctx"), (s_all, s_small, s_wide)
        )
    grad_w_out = s_all[:, :inner].T
    grad_w_z = s_all[:, inner : 2 * inner]
    s_cat = s_all[:, 2 * inner :]
    grad_w_x = s_cat[:, :inner]
    grad_w_bc = s_cat[:, inner : inner + 2 * states]
    grad_w_dt = s_cat[:, inner + 2 * states : inner + 2 * states + heads]
    grad_conv_x_w = s_small[:taps, :inner]
    grad_conv_x_b = s_small[taps, :inner]
    grad_gate_gain = s_small[0, width : width + inner]
    grad_d_skip = jnp.sum(s_small[1, width : width + inner].reshape(heads, per_head), axis=1)
    dt_at = width + inner
    grad_a_log = jnp.sum(s_small[:heads, dt_at : dt_at + STRETCH], axis=1)
    grad_dt_bias = jnp.sum(s_small[:heads, dt_at + STRETCH : dt_at + 2 * STRETCH], axis=1)
    grad_conv_bc_w = s_wide[:taps, : 2 * states]
    grad_conv_bc_b = s_wide[taps, : 2 * states]
    here = tp_index * slice_width
    grad_norm_gain = lax.dynamic_slice_in_dim(s_wide[0, 2 * states :], here, slice_width, 0)
    place = tp_index.astype(jnp.int32)[None]

    wide = 2 * STRETCH
    layer_out = run(
        functools.partial(finish_kernel, tp_size),
        blocks // 2,
        [
            (place, None, "smem"),
            (branch, (slice_width, wide), lambda i: (0, i)),
            (tokens, (wide, model), lambda i: (i, 0)),
            (sums, (2, wide), lambda i: (0, i)),
        ],
        [(shape((slice_width, rows), bf16), (slice_width, wide), lambda i: (0, i))],
        [],
    )[0].T
    grad_tokens = g_resid.T
    return (
        layer_out, grad_tokens, grad_norm_gain, grad_w_z, grad_w_x, grad_w_bc, grad_w_dt,
        grad_conv_x_w, grad_conv_x_b, grad_conv_bc_w, grad_conv_bc_b, grad_dt_bias, grad_a_log,
        grad_d_skip, grad_gate_gain, grad_w_out,
    )


def solution(mesh):
    both = ("fsdp", "ctx")
    in_specs = (
        P(both, None), P(both, None), P("fsdp", None), P(), P("fsdp", "tp"), P("fsdp", "tp"),
        P("fsdp", None), P("fsdp", "tp"), P(None, "tp"), P("tp"), P(), P(), P("tp"), P("tp"),
        P("tp"), P("tp"), P("tp", "fsdp"),
    )
    out_specs = (
        P(both, "tp"), P(both, "tp"), P("tp"), P("fsdp", "tp"), P("fsdp", "tp"), P("fsdp", None),
        P("fsdp", "tp"), P(None, "tp"), P("tp"), P(), P(), P("tp"), P("tp"), P("tp"), P("tp"),
        P("tp", "fsdp"),
    )
    return jax.shard_map(local, mesh=mesh, in_specs=in_specs, out_specs=out_specs, check_vma=False)
```

```python
import functools

import jax
import jax.numpy as jnp
import numpy as np
from jax import lax
from jax.experimental import pallas as pl
from jax.experimental.pallas import tpu as pltpu
from jax.sharding import PartitionSpec as P

STRETCH = 256
TAPS = 4
INNER = 1536
HEAD_ROWS = 8
LOG2E = 1.4426950408889634

epsilon = 1e-05
f32 = jnp.float32
bf16 = jnp.bfloat16


def nn(left, right):
    return lax.dot_general(left, right, (((1,), (0,)), ((), ())), preferred_element_type=f32)


def nt(left, right):
    return lax.dot_general(left, right, (((1,), (1,)), ((), ())), preferred_element_type=f32)


def tn(left, right):
    return lax.dot_general(left, right, (((0,), (0,)), ((), ())), preferred_element_type=f32)


def halves(x):
    high = x.astype(bf16)
    return high, (x - high.astype(f32)).astype(bf16)


def thirds(x):
    high = x.astype(bf16)
    rest = x - high.astype(f32)
    mid = rest.astype(bf16)
    return high, mid, (rest - mid.astype(f32)).astype(bf16)


def exact_rows(x, ones_matrix):
    high, mid, low = thirds(x)
    r = HEAD_ROWS
    out = nn(jnp.concatenate([high, mid, low, jnp.zeros_like(low)], axis=0), ones_matrix)
    return out[:r] + out[r : 2 * r] + out[2 * r : 3 * r]


def columns_of(rows):
    have = sum(r.shape[0] for r in rows)
    pad = jnp.zeros((128 - have, rows[0].shape[1]), f32)
    cols = jnp.transpose(jnp.concatenate(list(rows) + [pad], axis=0))
    high, low = halves(cols)
    return cols, jnp.concatenate([high, low], axis=1)


def segment_start(pos, starts):
    found = jnp.zeros_like(pos)
    for s in starts:
        found = jnp.where(pos >= s, s, found)
    return found


def joined_ok(u, distance, starts):
    ok = jnp.ones(u.shape, jnp.bool_)
    for s in starts[1:]:
        ok = ok & jnp.logical_not((u < s) & (u + distance >= s))
    return ok


def iota(shape, axis):
    return lax.broadcasted_iota(jnp.int32, shape, axis)


def read_info(rows, lengths, block):
    first = lax.axis_index("ctx") * rows
    starts = [jnp.int32(0)]
    for k in range(lengths.shape[1] - 1):
        starts.append(starts[-1] + lengths[0, k])
    base = first + block * STRETCH
    end_start = segment_start(base + STRETCH - 1, starts)
    flag = jnp.where(end_start < base, 1.0, 0.0).astype(f32)
    return starts, base, end_start, flag


def norm_rows(tok):
    x = tok.astype(f32)
    inverse = lax.rsqrt(jnp.mean(x * x, axis=1, keepdims=True) + epsilon)
    return x * inverse, inverse


def lanes_of(column, e8):
    return jnp.sum(column * e8, axis=0, keepdims=True)


MESH = pl.DeviceIdType.MESH


def start_together(peers):
    barrier = pltpu.get_barrier_semaphore()
    for peer in peers:
        pl.semaphore_signal(barrier, inc=1, device_id=peer, device_id_type=MESH)
    pl.semaphore_wait(barrier, len(peers))


def remote(src, dst, sent, came, peer):
    return pltpu.make_async_remote_copy(
        src_ref=src, dst_ref=dst, send_sem=sent, recv_sem=came, device_id=peer, device_id_type=MESH
    )


def turned(index, distance, size):
    return lax.rem(index + distance + size, size)


def twin_of(index):
    parity = lax.rem(index, 2)
    return parity, index + 1 - 2 * parity


def entry_kernel(
    rows, n, chain, sub, subs, info, nrm, halo, par, wj, tri, ew, e8, w_z, w_out_t,
    jx_o, jb_o, vbc_o, sx_o, sb_o, pre_o, step_o, cum_o, s_o, end_o, dec_o, inc_o, wz_o,
    ext, run, dec, shifts, got, sent, came, own, hop,
):
    i = pl.program_id(0) * subs + sub
    f = lax.axis_index("fsdp")
    here = lax.axis_index("ctx")
    _parity, twin = twin_of(here)
    peers = [{"fsdp": turned(f, d, n)} for d in range(1, n)] + [{"ctx": twin}]
    barrier = pltpu.get_barrier_semaphore()
    slab = w_z.shape[0]

    def at_first(body):
        if sub == 0:
            pl.when(pl.program_id(0) == 0)(body)

    def at_last(body):
        if sub == subs - 1:
            pl.when(pl.program_id(0) == pl.num_programs(0) - 1)(body)

    @at_first
    def _():
        for peer in peers:
            pl.semaphore_signal(barrier, inc=1, device_id=peer, device_id_type=MESH)

    def weight_copies():
        at = pl.ds(pl.multiple_of(f * slab, 16), slab)
        for p, ref in enumerate((w_z, w_out_t)):
            cols = slice(p * ref.shape[1], (p + 1) * ref.shape[1])
            target = wz_o.at[at, cols]
            yield pltpu.make_async_copy(ref, target, own.at[p])
            for d in range(1, n):
                yield remote(
                    ref, target, sent.at[d - 1, p], came.at[d - 1, p], {"fsdp": turned(f, d, n)}
                )

    starts, base, end_start, flag = read_info(rows, info, i)
    inner = jx_o.shape[1]
    width = inner + jb_o.shape[1]
    gain, cb, cw, taps = par[0:1, :], par[1:2, :], par[4:8, :], TAPS

    @at_first
    def _():
        unit, _inv = norm_rows(halo[...])
        before = nn((unit * gain).astype(bf16), wj[:, :width])
        ext[0:8, :] = before.astype(bf16).astype(f32)[8:16]
        run[...] = jnp.zeros_like(run)
        dec[...] = jnp.ones_like(dec)
        gap = iota((STRETCH, STRETCH), 0) - iota((STRETCH, STRETCH), 1)
        for k in range(taps - 1):
            moves = jnp.where(gap == taps - 1 - k, 1.0, 0.0).astype(bf16)
            shifts[STRETCH * k : STRETCH * (k + 1), :] = moves

    normed = nrm[...]
    product = nn(normed, wj[...])
    joined = product[:, :width].astype(bf16)
    jx_o[...] = joined[:, :inner]
    jb_o[...] = joined[:, inner:]
    pos = base + iota((STRETCH, 128), 0)
    first_of = segment_start(pos, starts)
    valid = [
        jnp.where(pos - (taps - 1 - k) >= first_of, 1.0, 0.0).astype(f32) for k in range(taps - 1)
    ]
    row_at = iota((8, 128), 0)
    masked = jnp.concatenate(
        [
            shifts[STRETCH * k : STRETCH * (k + 1), :]
            * jnp.concatenate([ok.astype(bf16)] * (STRETCH // 128), axis=1)
            for k, ok in enumerate(valid)
        ],
        axis=0,
    )
    for g in range(width // 128):
        at = slice(128 * g, 128 * (g + 1))
        if g % 2 == 0:
            tile = nn(masked, joined[:, 128 * g : min(128 * (g + 2), width)])
        fresh = joined[:, at].astype(f32)
        before = ext[:, at]
        ext[:, at] = fresh[STRETCH - 8 :]
        acc = cb[:, at] + cw[taps - 1 : taps, at] * fresh
        part = slice(128 * (g % 2), 128 * (g % 2 + 1))
        for k in range(taps - 1):
            d = taps - 1 - k
            moved = tile[STRETCH * k : STRETCH * (k + 1), part]
            edge = jnp.where(row_at < d, pltpu.roll(before, d, axis=0), 0.0) * valid[k][0:8]
            moved = jnp.concatenate([moved[0:8] + edge, moved[8:]], axis=0)
            acc = acc + cw[k : k + 1, at] * moved
        sig = jax.nn.sigmoid(acc)
        act = acc * sig
        vbc_o[:, at] = act.astype(bf16)
        slope = sig + act * (1.0 - sig)
        if 128 * g < inner:
            sx_o[:, at] = slope.astype(bf16)
        else:
            sb_o[:, 128 * g - inner : 128 * (g + 1) - inner] = slope
    pre = jnp.transpose(product[:, width:])[:HEAD_ROWS] + par[8:16, 0:1]
    step = jax.nn.softplus(pre)
    logd = -step * jnp.exp(par[8:16, 1:2])
    cum = exact_rows(logd, tri[...])
    pre_o[...] = pre
    step_o[...] = step
    cum_o[...] = cum
    cum_e = cum[:, STRETCH - 1 : STRETCH]
    where_s = base + iota((1, STRETCH), 1)
    keep = jnp.where(where_s >= end_start, 1.0, 0.0).astype(f32)
    weight = jnp.exp(cum_e - cum) * step * keep
    _cols, both = columns_of([weight])
    spread = nn(both, ew[...])
    v = vbc_o[:, :inner].astype(f32)
    b = vbc_o[:, inner : inner + 128]
    state = tn(b, (v * spread).astype(bf16))
    s_o[0] = state
    through = lanes_of(jnp.exp(cum_e) * flag, e8[...])
    run[...] = through * run[...] + state
    dec[...] = dec[...] * through
    end_o[...] = run[...].astype(bf16)
    dec_o[...] = dec[...]

    @at_first
    def _():
        pl.semaphore_wait(barrier, len(peers))
        for copy in weight_copies():
            copy.start()

    @at_last
    def _():
        if chain == 2:
            copy = remote(end_o, got, hop.at[0], hop.at[1], {"ctx": twin})
            copy.start()
            copy.wait()
            inc_o[...] = jnp.where(here > 0, got[...], jnp.zeros_like(got))
        else:
            inc_o[...] = jnp.zeros_like(inc_o)
        for copy in weight_copies():
            copy.wait()


def view(ref, kind, sub):
    if kind == "r":
        return ref.at[pl.ds(STRETCH * sub, STRETCH), :]
    if kind == "l":
        return ref.at[:, pl.ds(STRETCH * sub, STRETCH)]
    if kind == "b":
        return ref.at[pl.ds(sub, 1)]
    return ref


def in_turn(kernel, subs, kinds):
    def body(*refs):
        for sub in range(subs):
            kernel(sub, subs, *[view(ref, kind, sub) for ref, kind in zip(refs, kinds)])

    return body


def mix_kernel(
    rows, sub, subs, info, vbc, step, cum, s_in, inc, normed, gout, wz_out, par, e_step, e_scale, e8,
    z_o, out_o, gn_o, sum_o, st_o, br_o,
    run, gram,
):
    i = pl.program_id(0) * subs + sub
    starts, base, _end_start, flag = read_info(rows, info, i)
    inner = out_o.shape[1]
    gain = par[2:3, :inner]
    dskip = lanes_of(par[8:16, 2:3], e8[...])

    if sub == 0:

        @pl.when(i == 0)
        def _():
            run[...] = inc[...].astype(f32)

    st = run[...].astype(bf16)
    st_o[0] = st
    cum_v = cum[...]
    cum_e = cum_v[:, STRETCH - 1 : STRETCH]
    through = lanes_of(jnp.exp(cum_e) * flag, e8[...])
    run[...] = through * run[...] + s_in[0]

    row_first = segment_start(base + iota((1, STRETCH), 1), starts)
    scale = jnp.exp(cum_v) * jnp.where(row_first < base, 1.0, 0.0).astype(f32)
    cum2 = cum_v * LOG2E
    cols, both = columns_of([cum2, step[...], scale])
    step_x = nn(both, e_step[...])
    scale_x = nn(both, e_scale[...])
    b = vbc[:, inner : inner + 128]
    c = vbc[:, inner + 128 : inner + 256]
    carried = nn(c, st) * scale_x
    half = STRETCH // 2
    low, high = slice(0, half), slice(half, STRETCH)
    t_at = iota((half, STRETCH), 0)
    s_at = iota((half, STRETCH), 1)
    causal = (s_at <= t_at)[:, low]
    first_low = segment_start(iota((half, half), 0) + base, starts)
    first_high = segment_start(t_at + (base + half), starts)
    mask_a = causal & ((s_at + base)[:, low] >= first_low)
    mask_b = (s_at <= t_at + half) & (s_at + base >= first_high)
    gram[low, low] = jnp.where(mask_a, nt(c[low], b[low]), 0.0)
    gram[high, :] = jnp.where(mask_b, nt(c[high], b), 0.0)
    lane = iota((STRETCH, 128), 1)
    pieces = []
    for p in range(inner // 128):
        at = slice(128 * p, 128 * (p + 1))
        v = vbc[:, at].astype(f32)
        sv = (v * step_x[:, at]).astype(bf16)
        rest = carried[:, at] + dskip[:, at] * v
        acc_low, acc_high = rest[low], rest[high]
        for j in range(2):
            h = 2 * p + j
            side = (lane < 64) if j == 0 else (lane >= 64)
            part = jnp.where(side, sv, jnp.zeros_like(sv))
            row = cum2[h : h + 1, :]
            first_gap = cols[low, h : h + 1] - row[:, low]
            cross_gap = cols[high, h : h + 1] - row[:, low]
            last_gap = cols[high, h : h + 1] - row[:, high]
            decay_b = jnp.concatenate(
                [jnp.exp2(cross_gap), jnp.exp2(jnp.minimum(last_gap, 0.0))], axis=1
            )
            decay_a = jnp.exp2(jnp.minimum(first_gap, 0.0))
            acc_low = acc_low + nn((gram[low, low] * decay_a).astype(bf16), part[low])
            acc_high = acc_high + nn((gram[high, :] * decay_b).astype(bf16), part)
        pieces.append(jnp.concatenate([acc_low, acc_high], axis=0))
    out = jnp.concatenate(pieces, axis=1)
    out_o[...] = out
    zf = nn(normed[...], wz_out[:, :inner])
    z_o[...] = zf
    gated = out * (zf * jax.nn.sigmoid(zf))
    gn = nn(gout[...], wz_out[:, inner:])
    gn_o[...] = gn
    gg = gated * gain
    br_o[...] = nt(wz_out[:, inner:], gg.astype(bf16)).astype(bf16)
    ss = jnp.sum(gated * gated, axis=1, keepdims=True)
    dq = jnp.sum(gn * gg, axis=1, keepdims=True)
    sum_o[...] = jnp.transpose(jnp.where(lane == 0, ss, dq))[0:2]


def gate_kernel(
    rows, info, sums, cum, out, z, gn, vc, st, par, e_scale, e8, f_sum,
    gz_o, gb_o, gc_o, n2_o, a_o, gs_o, start_o, misc_o,
    run,
):
    step_id = pl.program_id(0)
    blocks = pl.num_programs(0)
    i = blocks - 1 - step_id
    starts, base, _end_start, flag = read_info(rows, info, i)
    inner = z.shape[1]
    gain = par[2:3, :inner]
    dskip = lanes_of(par[8:16, 2:3], e8[...])

    @pl.when(step_id == 0)
    def _():
        run[...] = jnp.zeros_like(run)
        misc_o[...] = jnp.zeros_like(misc_o)

    alpha = lax.rsqrt(sums[0:1, :] / INNER + epsilon)
    beta = alpha * alpha * alpha * sums[1:2, :] / INNER
    cum_v = cum[...]
    row_first = segment_start(base + iota((1, STRETCH), 1), starts)
    scale = jnp.exp(cum_v) * jnp.where(row_first < base, 1.0, 0.0).astype(f32)
    cols, both = columns_of([alpha, beta, jnp.zeros((14, STRETCH), f32), scale])
    alpha_c = cols[:, 0:1]
    beta_c = cols[:, 1:2]
    scale_x = nn(both, e_scale[...])
    v = vc[:, :inner].astype(f32)
    c = vc[:, inner + 128 : inner + 256]
    zf = z[...]
    sig = jax.nn.sigmoid(zf)
    act = zf * sig
    o = out[...]
    gated = o * act
    g_n = gn[...]
    unit = gated * alpha_c
    g_gated = alpha_c * (g_n * gain) - beta_c * gated
    g_out = g_gated * act
    gz_o[...] = (g_gated * o * (sig + act * (1.0 - sig))).astype(bf16)
    gb = g_out.astype(bf16)
    gb_o[...] = gb
    n2_o[...] = (unit * gain).astype(bf16)
    misc_o[0:1, :] += jnp.sum(g_n * unit, axis=0, keepdims=True)
    misc_o[1:2, :] += jnp.sum(g_out * v, axis=0, keepdims=True)
    gf = gb.astype(f32)
    carried = nn(c, st[0]) * scale_x
    prod = gf * (o - dskip * v) + (g_out - gf) * carried
    high, low = halves(prod)
    sums_c = nn(jnp.concatenate([high, low], axis=1), f_sum[...])
    a_o[...] = jnp.transpose(sums_c)[0:HEAD_ROWS]
    gc = (g_out * scale_x).astype(bf16)
    gc_o[...] = gc
    gs = tn(c, gc)
    gs_o[0] = gs
    through = lanes_of(jnp.exp(cum_v[:, STRETCH - 1 : STRETCH]) * flag, e8[...])
    run[...] = through * run[...] + gs
    start_o[...] = run[...].astype(bf16)


def scan_kernel(
    rows, info, vbc, gb, gc, step, cum, pre, a_sum, st, gs_in, outg, sx, sb, jx, jb, par,
    e_step, e_w, e8, f_all, tril,
    gcat_o, tail_o, head_o, misc_o, dt_o,
    run, ext, gram, acc, prod,
):
    step_id = pl.program_id(0)
    blocks = pl.num_programs(0)
    i = blocks - 1 - step_id
    starts, base, end_start, flag = read_info(rows, info, i)
    inner = gb.shape[1]
    width = inner + jb.shape[1]
    cw, taps = par[4:8, :], TAPS
    rate = jnp.exp(par[8:16, 1:2])
    dskip = lanes_of(par[8:16, 2:3], e8[...])

    @pl.when(step_id == 0)
    def _():
        run[...] = outg[...].astype(f32)
        ext[...] = jnp.zeros((8, width), f32)
        misc_o[...] = jnp.zeros_like(misc_o)
        dt_o[...] = jnp.zeros_like(dt_o)

    cum_v = cum[...]
    step_v = step[...]
    cum_e = cum_v[:, STRETCH - 1 : STRETCH]
    after = run[...]
    low_after = after.astype(bf16)
    state = st[0]
    through = lanes_of(jnp.exp(cum_e) * flag, e8[...])
    g_through = jnp.sum(after * state.astype(f32), axis=0, keepdims=True) * through
    end_more = jnp.sum(e8[...] * g_through, axis=1, keepdims=True)
    run[...] = through * after + gs_in[0]

    where_s = base + iota((1, STRETCH), 1)
    row_first = segment_start(where_s, starts)
    end_decay = jnp.exp(cum_e - cum_v) * jnp.where(where_s >= end_start, 1.0, 0.0).astype(f32)
    weight = end_decay * step_v
    cum2 = cum_v * LOG2E
    ok_rows = [
        jnp.where(joined_ok(where_s, d, starts), 1.0, 0.0).astype(f32)
        for d in range(taps - 1, 0, -1)
    ]
    cols, both = columns_of([cum2, step_v, weight] + ok_rows)
    b = vbc[:, inner : inner + 128]
    c = vbc[:, inner + 128 : inner + 256]
    half = STRETCH // 2
    low, high = slice(0, half), slice(half, STRETCH)
    s_at = iota((half, STRETCH), 0)
    t_at = iota((half, STRETCH), 1)
    mask_a = (s_at <= t_at) & (s_at + base >= row_first)
    mask_b = (s_at <= t_at)[:, low] & ((s_at + (base + half)) >= row_first)[:, high]
    gram[low, :] = jnp.where(mask_a, nt(b[low], c), 0.0)
    gram[high, low] = jnp.where(mask_b, nt(b[high], c[high]), 0.0)
    acc[...] = jnp.zeros_like(acc)
    lane = iota((STRETCH, 128), 1)
    ok = [
        jnp.broadcast_to(cols[:, 3 * HEAD_ROWS + k : 3 * HEAD_ROWS + k + 1], (STRETCH, 128))
        for k in range(taps - 1)
    ]

    def convolve(at, own, j_f):
        following = ext[:, at]
        joint = jnp.concatenate([own, following], axis=0)
        ext[:, at] = own[0:8]
        misc_o[taps : taps + 1, at] += jnp.sum(own, axis=0, keepdims=True)
        misc_o[taps - 1 : taps, at] += jnp.sum(own * j_f, axis=0, keepdims=True)
        total = own * cw[taps - 1 : taps, at]
        for k in range(taps - 1):
            d = taps - 1 - k
            term = pltpu.roll(joint, STRETCH + 8 - d, axis=0)[:STRETCH] * ok[k]
            misc_o[k : k + 1, at] += jnp.sum(term * j_f, axis=0, keepdims=True)
            total = total + term * cw[k : k + 1, at]
        gcat_o[:, at] = total.astype(bf16)
        tail_o[:, at] = jnp.where(step_id == 0, total[STRETCH - 8 :], tail_o[:, at])

    g_b = jnp.zeros((STRETCH, 128), f32)
    g_c = jnp.zeros((STRETCH, 128), f32)
    for p in range(inner // 128):
        at = slice(128 * p, 128 * (p + 1))
        step_x = nn(both, e_step[:, at])
        v = vbc[:, at].astype(f32)
        sv = (v * step_x).astype(bf16)
        g_pair = gb[:, at]
        u_low = jnp.zeros((half, 128), f32)
        u_high = jnp.zeros((half, 128), f32)
        for j in range(2):
            h = 2 * p + j
            side = (lane < 64) if j == 0 else (lane >= 64)
            g_side = jnp.where(side, g_pair, jnp.zeros_like(g_pair))
            sv_side = jnp.where(side, sv, jnp.zeros_like(sv))
            row = cum2[h : h + 1, :]
            first_gap = row[:, low] - cols[low, h : h + 1]
            cross_gap = row[:, high] - cols[low, h : h + 1]
            last_gap = row[:, high] - cols[high, h : h + 1]
            decay_a = jnp.concatenate(
                [jnp.exp2(jnp.minimum(first_gap, 0.0)), jnp.exp2(cross_gap)], axis=1
            )
            decay_b = jnp.exp2(jnp.minimum(last_gap, 0.0))
            u_low = u_low + nn((gram[low, :] * decay_a).astype(bf16), g_side)
            u_high = u_high + nn((gram[high, low] * decay_b).astype(bf16), g_side[high])
            acc[low, :] += nt(sv_side[low], g_pair) * decay_a
            acc[high, low] += nt(sv_side[high], g_pair[high]) * decay_b
        u = jnp.concatenate([u_low, u_high], axis=0)
        w_x = nn(both, e_w[:, at])
        y = nn(b, low_after[:, at])
        h1, l1 = halves(sv.astype(f32) * u)
        prod[:, at] = h1
        prod[:, inner + 128 * p : inner + 128 * (p + 1)] = l1
        prod[:, 2 * inner + 128 * p : 2 * inner + 128 * (p + 1)] = (v * y).astype(bf16)
        g_b = g_b + nt((v * w_x).astype(bf16), low_after[:, at])
        g_c = g_c + nt(gc[:, at], state[:, at])
        gv = dskip[:, at] * g_pair.astype(f32) + step_x * u + w_x * y
        convolve(at, gv * sx[:, at].astype(f32), jx[:, at].astype(f32))

    gg_a = jnp.where(mask_a, acc[low, :], 0.0).astype(bf16)
    gg_b = jnp.where(mask_b, acc[high, low], 0.0).astype(bf16)
    g_b = g_b + jnp.concatenate([nn(gg_a, c), nn(gg_b, c[high])], axis=0)
    g_c = g_c + tn(gg_a, b[low])
    g_c = g_c + jnp.concatenate([jnp.zeros((half, 128), f32), tn(gg_b, b[high])], axis=0)
    for k, part in enumerate((g_b, g_c)):
        here = slice(128 * k, 128 * (k + 1))
        convolve(
            slice(inner + 128 * k, inner + 128 * (k + 1)),
            part * sb[:, here],
            jb[:, here].astype(f32),
        )

    sums_r = jnp.transpose(nn(prod[...], f_all[...]))
    g_mixed = sums_r[0:HEAD_ROWS]
    g_end = sums_r[HEAD_ROWS : 2 * HEAD_ROWS]
    ends = g_end * weight
    g_cum = a_sum[...] - g_mixed - ends
    end_add = jnp.sum(ends, axis=1, keepdims=True) + end_more
    g_log = exact_rows(g_cum, tril[...]) + end_add
    slope_dt = jax.nn.sigmoid(pre[...])
    ratio = jnp.where(step_v > 0.0, slope_dt / step_v, 1.0)
    g_pre_dt = (g_end * end_decay - g_log * rate) * slope_dt + g_mixed * ratio
    dt_o[0:HEAD_ROWS, :] += g_log * (-step_v * rate)
    dt_o[HEAD_ROWS:, :] += g_pre_dt
    pad = jnp.zeros((128 - HEAD_ROWS, STRETCH), f32)
    gcat_o[:, width:] = jnp.transpose(jnp.concatenate([g_pre_dt, pad], axis=0)).astype(bf16)

    head_o[...] = ext[...]


def exit_kernel(
    rows, blocks, rim_side, info, tok, gout, mine, gz, gcat, par, wz_out, wj, *rest
):
    step_id = pl.program_id(0)
    i = blocks - 1 - step_id
    starts, base, _end_start, _flag = read_info(rows, info, i)
    inner = gz.shape[1]
    if rim_side:
        tail, nxt, last_j, gr_o, gain_o, rim_o, rim_w_o, fix = rest
        taps, width = TAPS, tail.shape[1]
        cw = par[4:8, :width]
    else:
        gr_o, gain_o = rest
    gain = par[0:1, :]

    g_normed = nt(gz[...], wz_out[:, :inner]) + nt(gcat[...], wj[...])

    def finish(g_normed):
        unit, inverse = norm_rows(tok[...])
        scaled = g_normed * gain
        mean = jnp.mean(scaled * unit, axis=1, keepdims=True)
        own = gout[...].astype(f32) * mine[...]
        gr_o[...] = jnp.transpose((own + inverse * (scaled - unit * mean)).astype(bf16))
        gain_o[...] += jnp.sum(g_normed * unit, axis=0, keepdims=True)

    @pl.when(step_id == 0)
    def _():
        gain_o[...] = jnp.zeros_like(gain_o)

    if not rim_side:
        finish(g_normed)
        return

    @pl.when(step_id == 0)
    def _():
        fix[0:8, :] = jnp.zeros((8, width), f32)
        fix[8:16, :] = nxt[...]
        places = base + STRETCH - 8 + iota((8, 128), 0)
        wide = last_j[8:16, :].astype(f32)
        total = tail[...]
        for k in range(taps - 1):
            d = taps - 1 - k
            ok = jnp.where(joined_ok(places, d, starts), 1.0, 0.0).astype(f32)
            inside = jnp.where(iota((8, width), 0) >= 8 - d, fix[d : d + 8, :], 0.0)
            term = inside * jnp.concatenate([ok] * (width // 128), axis=1)
            total = total + term * cw[k : k + 1, :]
            rim_w_o[k : k + 1, :] = jnp.sum(term * wide, axis=0, keepdims=True)
        rim_w_o[taps - 1 : 8, :] = jnp.zeros((9 - taps, width), f32)
        fix[0:8, :] = jnp.zeros((8, width), f32)
        fix[8:16, :] = total.astype(bf16).astype(f32) - tail[...].astype(bf16).astype(f32)
        rim_o[...] = fix[...].astype(bf16)

    @pl.when(step_id == 0)
    def _():
        more = nt(rim_o[...], wj[:, :width])
        finish(g_normed + jnp.concatenate([jnp.zeros((STRETCH - 16, more.shape[1]), f32), more]))

    @pl.when(step_id > 0)
    def _():
        finish(g_normed)


def finish_kernel(parts, place, part, base, sums, out):
    wide = part[...].astype(f32) * lax.rsqrt(sums[0:1, :] / INNER + epsilon)
    size = out.shape[0]
    for k in range(parts):

        @pl.when(place[0] == k)
        def _():
            add = jnp.transpose(base[:, size * k : size * (k + 1)].astype(f32))
            out[...] = (wide + add).astype(bf16)


def gather_kernel(
    n, chain, x, bc, dt_t, par, tok, out, halo, nrm, dt, dts, sent, came, passed, relayed, own, hop
):
    f = lax.axis_index("fsdp")
    parity, twin = twin_of(lax.axis_index("ctx"))
    half = x.shape[0] // 2
    here = lax.axis_index("ctx")
    following = turned(here, 1, chain)
    sides = [{"ctx": twin}] if chain == 2 else [{"ctx": following}, {"ctx": turned(here, -1, chain)}]
    start_together([{"fsdp": turned(f, d, n)} for d in range(1, n)] + sides)
    heads, rows = dt_t.shape
    wide = -(-rows // 128) * 128
    flat = jnp.concatenate(
        [dt_t[...].astype(f32), jnp.zeros((heads, wide - rows), f32)], axis=1
    )
    flat = jnp.concatenate([flat, jnp.zeros((HEAD_ROWS - heads, wide), f32)], axis=0)
    dt[...] = flat.astype(bf16)
    dts[pl.ds(f, 1)] = dt[...][None]
    tiny = []
    for d in range(1, n):
        copy = remote(
            dt, dts.at[f], sent.at[d - 1, 2], came.at[d - 1, 2], {"fsdp": turned(f, d, n)}
        )
        copy.start()
        tiny.append(copy)
    pieces = []
    at = 0
    for ref in (x, bc):
        pieces.append((ref, slice(at, at + ref.shape[1])))
        at += ref.shape[1]

    def place(source, side):
        return pl.ds(pl.multiple_of(source * rows + side * half, 16), half)

    mine = pl.ds(pl.multiple_of(parity * half, 16), half)
    copies = []
    for d in range(1, n):
        for p, (ref, cols) in enumerate(pieces):
            copy = remote(
                ref.at[mine, :], out.at[place(f, parity), cols],
                sent.at[d - 1, p], came.at[d - 1, p], {"fsdp": turned(f, d, n)},
            )
            copy.start()
            copies.append(copy)
    edge = halo.shape[0]
    copy = remote(
        tok.at[pl.ds(tok.shape[0] - edge, edge), :], halo, hop.at[0], hop.at[1], {"ctx": following}
    )
    copy.start()
    locals_ = [copy]
    for p, (ref, cols) in enumerate(pieces):
        copy = pltpu.make_async_copy(
            ref, out.at[pl.ds(pl.multiple_of(f * rows, 16), rows), cols], own.at[p]
        )
        copy.start()
        locals_.append(copy)
    gain = par[...][None, :]

    def norm_block(tok_block, nrm_block):
        unit, _inverse = norm_rows(tok_block[...])
        nrm_block[...] = (unit * gain).astype(bf16)

    steps = tok.shape[0] // (2 * STRETCH)

    def normalise(first, count):
        block = pl.BlockSpec((2 * STRETCH, tok.shape[1]), lambda i: (i + first, 0))
        pltpu.emit_pipeline(norm_block, grid=(count,), in_specs=[block], out_specs=[block])(
            tok, nrm
        )

    relays = []

    def relay(d):
        source = turned(f, -d, n)
        for p, (ref, cols) in enumerate(pieces):
            copies[(d - 1) * len(pieces) + p].wait_recv()
            piece = out.at[place(source, parity), cols]
            copy = remote(piece, piece, passed.at[d - 1, p], relayed.at[d - 1, p], {"ctx": twin})
            copy.start()
            relays.append(copy)

    normalise(0, steps)
    for d in range(1, n):
        relay(d)
    for copy in tiny:
        copy.wait()
    joint = jnp.concatenate([dts[q].astype(f32)[:, :rows] for q in range(n)], axis=1)
    joint = jnp.concatenate([joint, jnp.zeros((128 - HEAD_ROWS, n * rows), f32)], axis=0)
    out[:, at:] = jnp.transpose(joint).astype(bf16)
    for copy in copies:
        copy.wait_send()
    for copy in locals_:
        copy.wait()
    for copy in relays:
        copy.wait()


def gathered(x, bc, dt_t, par, tok):
    n = lax.axis_size("fsdp")
    pieces = (n - 1, 3)
    width = x.shape[1] + bc.shape[1] + 128
    return pl.pallas_call(
        functools.partial(gather_kernel, n, lax.axis_size("ctx")),
        out_shape=[
            jax.ShapeDtypeStruct((n * x.shape[0], width), bf16),
            jax.ShapeDtypeStruct((16, tok.shape[1]), bf16),
            jax.ShapeDtypeStruct(tok.shape, bf16),
        ],
        in_specs=[pl.BlockSpec(memory_space=pltpu.VMEM)] * 4 + [pl.BlockSpec(memory_space=pl.ANY)],
        out_specs=[pl.BlockSpec(memory_space=pltpu.VMEM)] * 2
        + [pl.BlockSpec(memory_space=pl.ANY)],
        scratch_shapes=[
            pltpu.VMEM((HEAD_ROWS, -(-x.shape[0] // 128) * 128), bf16),
            pltpu.VMEM((n, HEAD_ROWS, -(-x.shape[0] // 128) * 128), bf16),
        ]
        + [pltpu.SemaphoreType.DMA(pieces)] * 4
        + [pltpu.SemaphoreType.DMA((3,)), pltpu.SemaphoreType.DMA((2,))],
        compiler_params=pltpu.CompilerParams(collective_id=1, has_side_effects=True),
    )(x, bc, dt_t, par, tok)


def total_kernel(n, part, out, slots, sent, came):
    me = lax.axis_index("tp")
    start_together([{"tp": turned(me, d, n)} for d in range(1, n)])
    copies = []
    for d in range(1, n):
        copy = remote(
            part, slots.at[d - 1], sent.at[d - 1], came.at[d - 1], {"tp": turned(me, d, n)}
        )
        copy.start()
        copies.append(copy)
    total = part[...]
    for d in range(1, n):
        copies[d - 1].wait_recv()
        total = total + slots[d - 1]
    out[...] = total
    for copy in copies:
        copy.wait_send()


def total_over_tp(part):
    n = lax.axis_size("tp")
    return pl.pallas_call(
        functools.partial(total_kernel, n),
        out_shape=jax.ShapeDtypeStruct(part.shape, f32),
        in_specs=[pl.BlockSpec(memory_space=pltpu.VMEM)],
        out_specs=pl.BlockSpec(memory_space=pltpu.VMEM),
        scratch_shapes=[
            pltpu.VMEM((n - 1,) + part.shape, f32),
            pltpu.SemaphoreType.DMA((n - 1,)),
            pltpu.SemaphoreType.DMA((n - 1,)),
        ],
        compiler_params=pltpu.CompilerParams(collective_id=2, has_side_effects=True),
    )(part)


def share_over_tp(m, t, shares, sent, came):
    copies = []
    for p, (buf, own) in enumerate(shares):
        buf[pl.ds(t, 1)] = own[None]
    for d in range(1, m):
        for p, (buf, _own) in enumerate(shares):
            k = 3 * (d - 1) + p
            copy = remote(buf.at[t], buf.at[t], sent.at[k], came.at[k], {"tp": turned(t, d, m)})
            copy.start()
            copies.append(copy)
    for copy in copies:
        copy.wait()
    totals = []
    for buf, _own in shares:
        total = buf[0].astype(f32)
        for q in range(1, m):
            total = total + buf[q].astype(f32)
        totals.append(total)
    return totals


def fold_over_tp(m, t, shares, sent, came):
    at_edge = (t == 0) | (t == 3)
    in_middle = jnp.logical_not(at_edge)
    inward = jnp.where(t == 0, 1, 2)
    outward = jnp.where(t == 1, 0, 3)
    across = 3 - t

    def copy_of(phase, p, src, dst, peer):
        buf = shares[p][0]
        k = 3 * phase + p
        return remote(buf.at[src], buf.at[dst], sent.at[k], came.at[k], {"tp": peer})

    every = range(len(shares))
    for buf, own in shares:
        buf[0] = own

    @pl.when(at_edge)
    def _():
        for p in every:
            copy_of(0, p, 0, 1, inward).start()
        for p in every:
            copy_of(0, p, 0, 1, inward).wait_send()
        for p in every:
            copy_of(2, p, 4, 4, inward).wait_recv()

    @pl.when(in_middle)
    def _():
        for p in every:
            buf = shares[p][0]
            copy_of(0, p, 0, 1, outward).wait_recv()
            buf[2] = (buf[0].astype(f32) + buf[1].astype(f32)).astype(buf.dtype)
            copy_of(1, p, 2, 3, across).start()
        for p in every:
            buf = shares[p][0]
            copy_of(1, p, 2, 3, across).wait()
            buf[4] = (buf[2].astype(f32) + buf[3].astype(f32)).astype(buf.dtype)
            copy_of(2, p, 4, 4, outward).start()
        for p in every:
            copy_of(2, p, 4, 4, outward).wait_send()

    return [buf[4].astype(f32) for buf, _own in shares]


def reduce_kernel(
    n, m, bc_cols, conv_bc,
    p_out, p_z, p_cat, m_scan, m_rim, m_gate, m_dt, m_gain,
    o_all, o_small, o_wide,
    give, take, mid, slots, final, bc_slots, small, small_slots, wide_slots, gain_slots,
    s1, r1, s2, r2, s3, r3, s4, r4,
):
    f = lax.axis_index("fsdp")
    t = lax.axis_index("tp")
    parity, twin = twin_of(lax.axis_index("ctx"))
    start_together(
        [{"ctx": twin}]
        + [{"fsdp": turned(f, d, n)} for d in range(1, n)]
        + [{"tp": turned(t, d, m)} for d in range(1, m)]
    )
    inner = p_out.shape[1]
    rows = p_out.shape[0] // n
    half = rows // 2

    def piece(q, side):
        at = pl.ds(pl.multiple_of(q * rows + side * half, 16), half)
        return jnp.concatenate([p_out[at, :], p_z[at, :], p_cat[at, :]], axis=1)

    copies = []
    for q in range(n):
        give[q] = piece(q, 1 - parity).astype(bf16)
        copy = remote(give.at[q], take.at[q], s1.at[q], r1.at[q], {"ctx": twin})
        copy.start()
        copies.append(copy)
    w_scan = m_scan.shape[1]
    w_gate = m_gate.shape[1]
    w_dt = m_dt.shape[1]
    small[...] = jnp.zeros_like(small)
    small[:, 0:w_scan] = m_scan[...] + m_rim[...]
    at = w_scan
    small[:, at : at + w_gate] = m_gate[...]
    at += w_gate
    small[:, at : at + w_dt] = m_dt[0:8, :]
    small[:, at + w_dt : at + 2 * w_dt] = m_dt[8:16, :]
    at += 2 * w_dt
    small[0:1, at:] = m_gain[...]
    small_slots[0, pl.ds(parity, 1)] = small[...][None]
    copy = remote(
        small, small_slots.at[0, parity], s1.at[n], r1.at[n], {"ctx": twin}
    )
    copy.start()
    copies.append(copy)

    copies[n].wait()
    small_slots[1, pl.ds(f, 1)] = (small_slots[0, 0] + small_slots[0, 1])[None]
    seconds = []
    for d in range(1, n):
        copy = remote(
            small_slots.at[1, f], small_slots.at[1, f], s2.at[n - 1 + d - 1], r2.at[n - 1 + d - 1],
            {"fsdp": turned(f, d, n)},
        )
        copy.start()
        seconds.append(copy)
    for q in range(n):
        copies[q].wait()
        mid[q] = (piece(q, parity) + take[q].astype(f32)).astype(bf16)
    slots[pl.ds(f, 1)] = mid[pl.ds(f, 1)]
    for d in range(1, n):
        peer = turned(f, d, n)
        copy = remote(
            mid.at[peer], slots.at[f], s2.at[d - 1], r2.at[d - 1], {"fsdp": peer}
        )
        copy.start()
        seconds.append(copy)
    for copy in seconds:
        copy.wait()
    small_sum = small_slots[1, 0]
    whole = slots[0].astype(f32)
    for q in range(1, n):
        small_sum = small_sum + small_slots[1, q]
        whole = whole + slots[q].astype(f32)
    final[...] = whole
    bc_at = slice(3 * inner, 3 * inner + bc_cols)
    o_small[...] = small_sum[:, :at]
    shares = (
        (bc_slots, whole[:, bc_at].astype(bf16)),
        (wide_slots, small_sum[:, conv_bc:w_scan]),
        (gain_slots, small_sum[0:1, at:]),
    )
    bc_sum, wide_sum, gain_sum = (fold_over_tp if m == 4 else share_over_tp)(m, t, shares, s3, r3)
    o_wide[:, :bc_cols] = wide_sum
    o_wide[:, bc_cols:] = jnp.broadcast_to(gain_sum, (8, gain_sum.shape[1]))
    final[:, bc_at] = bc_sum
    here = pl.ds(pl.multiple_of(parity * half, 8), half)
    o_all[here, :] = final[...]
    copy = remote(final, o_all.at[here, :], s4.at[0], r4.at[0], {"ctx": twin})
    copy.start()
    copy.wait()


def reduced(parts, miscs, bc_cols):
    n, m = lax.axis_size("fsdp"), lax.axis_size("tp")
    p_out, _p_z, p_cat = parts
    rows = p_out.shape[0] // n
    half = rows // 2
    inner = p_out.shape[1]
    wide = 2 * inner + p_cat.shape[1]
    m_scan, _m_rim, m_gate, m_dt, m_gain = miscs
    kept = m_scan.shape[1] + m_gate.shape[1] + 2 * m_dt.shape[1]
    small = kept + m_gain.shape[1]
    crossing = m_scan.shape[1] - inner + m_gain.shape[1]
    dma = pltpu.SemaphoreType.DMA

    def shape(*dims):
        return jax.ShapeDtypeStruct(dims, f32)

    return pl.pallas_call(
        functools.partial(reduce_kernel, n, m, bc_cols, inner),
        out_shape=[
            shape(rows, wide), shape(8, kept), shape(8, crossing),
        ],
        in_specs=[pl.BlockSpec(memory_space=pltpu.VMEM)] * 8,
        out_specs=[pl.BlockSpec(memory_space=pltpu.VMEM)] * 3,
        scratch_shapes=[
            pltpu.VMEM((n, half, wide), bf16),
            pltpu.VMEM((n, half, wide), bf16),
            pltpu.VMEM((n, half, wide), bf16),
            pltpu.VMEM((n, half, wide), bf16),
            pltpu.VMEM((half, wide), f32),
            pltpu.VMEM((max(m, 5), half, bc_cols), bf16),
            pltpu.VMEM((8, small), f32),
            pltpu.VMEM((2, max(n, 2), 8, small), f32),
            pltpu.VMEM((max(m, 5), 8, bc_cols), f32),
            pltpu.VMEM((max(m, 5), 1, m_gain.shape[1]), f32),
            dma((n + 1,)), dma((n + 1,)), dma((2 * n - 2,)), dma((2 * n - 2,)),
            dma((3 * m,)), dma((3 * m,)), dma((1,)), dma((1,)),
        ],
        compiler_params=pltpu.CompilerParams(
            collective_id=3, has_side_effects=True, vmem_limit_bytes=48 * 1024 * 1024
        ),
    )(*parts, *miscs)


def constants(inner, heads):
    lane_head = np.arange(inner) // (inner // heads)
    e8 = (np.arange(HEAD_ROWS)[:, None] == lane_head[None, :]).astype(np.float32)

    def spread(kind):
        m = np.zeros((128, inner), np.float32)
        m[HEAD_ROWS * kind : HEAD_ROWS * (kind + 1)] = e8
        return jnp.asarray(np.concatenate([m, m], axis=0), bf16)

    def gather(kind):
        m = np.zeros((inner, 128), np.float32)
        m[:, HEAD_ROWS * kind : HEAD_ROWS * (kind + 1)] = e8.T
        return jnp.asarray(np.concatenate([m, m], axis=0), bf16)

    at = np.arange(STRETCH)
    upper = jnp.asarray((at[:, None] <= at[None, :]).astype(np.float32), bf16)
    lower = jnp.asarray((at[:, None] >= at[None, :]).astype(np.float32), bf16)
    return jnp.asarray(e8), spread, gather, upper, lower


def passed_along(block, axis, distance):
    devices = range(lax.axis_size(axis))
    route = [(i - distance, i) for i in devices if i - distance in devices]
    return lax.ppermute(block, axis, route)


def entering(decay, state, axis, reverse):
    size = lax.axis_size(axis)
    if size == 2:
        return passed_along(state, axis, -1 if reverse else 1)
    index = lax.axis_index(axis)
    decays = lax.all_gather(decay.astype(bf16), axis)
    states = lax.all_gather(state, axis)

    def lap(k, before):
        at = size - 1 - k if reverse else k
        reached = at > index if reverse else at < index
        new = decays[at].astype(f32) * before + states[at].astype(f32)
        return jnp.where(reached, new, before)

    return lax.fori_loop(0, size, lap, jnp.zeros(state.shape, f32)).astype(bf16)


def fill_params(raw, par):
    gain, gate, x_w, bc_w, x_b, bc_b, bias, rate, skip = raw
    inner = x_w.shape[1]
    width = inner + bc_w.shape[1]
    heads = bias.shape[0]

    @pl.when(pl.program_id(0) == 0)
    def _():
        par[0:1, :] = gain[...][None, :]
        par[1:2, :inner] = x_b[...][None, :]
        par[1:2, inner:width] = bc_b[...][None, :]
        par[2:3, :inner] = gate[...][None, :]
        par[4:8, :inner] = x_w[...]
        par[4:8, inner:width] = bc_w[...]
        row, lane = iota((HEAD_ROWS, 128), 0), iota((HEAD_ROWS, 128), 1)
        table = jnp.zeros((HEAD_ROWS, 128), f32)
        for h in range(heads):
            for k, ref in enumerate((bias, rate, skip)):
                table = jnp.where((row == h) & (lane == k), ref[h], table)
        par[8:16, 0:128] = table


def call(kernel, blocks, ins, outs, scratch, remote_id=None, raw=None):
    def spec(shape, how):
        if how == "smem":
            return pl.BlockSpec(memory_space=pltpu.SMEM)
        if how == "any":
            return pl.BlockSpec(memory_space=pl.ANY)
        return pl.BlockSpec(shape, how)

    places = [k for k, (_a, _s, how) in enumerate(ins) if how == "par"]
    ins = [entry for entry in ins if entry[2] != "par"]
    body = kernel
    if places:
        count = len(raw)
        model = raw[0].shape[0]
        scratch = list(scratch) + [pltpu.VMEM((16, model), f32)]

        def body(*refs):
            par = refs[-1]
            fill_params(refs[:count], par)
            rest = list(refs[count:-1])
            rest.insert(places[0], par)
            kernel(*rest)

        def fixed_at(x):
            if x.ndim == 1 and x.shape[0] < 128:
                return (x, None, "smem")
            return (x, x.shape, lambda i: (0,) * x.ndim)

        ins = [fixed_at(x) for x in raw] + ins

    return pl.pallas_call(
        body,
        grid=(blocks,),
        in_specs=[spec(shape, how) for _a, shape, how in ins],
        out_specs=[spec(shape, how) for _s, shape, how in outs],
        out_shape=[s for s, _sh, _h in outs],
        scratch_shapes=scratch,
        compiler_params=pltpu.CompilerParams(
            dimension_semantics=("arbitrary",),
            vmem_limit_bytes=56 * 1024 * 1024,
            collective_id=remote_id,
            has_side_effects=remote_id is not None,
        ),
    )(*[a for a, _s, _h in ins])


def local(
    tokens, grad_out, lengths, norm_gain, w_z, w_x, w_bc, w_dt, conv_x_w, conv_x_b,
    conv_bc_w, conv_bc_b, dt_bias, a_log, d_skip, gate_gain, w_out,
):
    rows, model = tokens.shape
    inner = w_z.shape[1]
    heads = dt_bias.shape[0]
    states = w_bc.shape[1] // 2
    taps = conv_x_w.shape[0]
    blocks = rows // STRETCH
    width = inner + 2 * states
    tp_size = lax.axis_size("tp")
    slice_width = model // tp_size
    tp_index = lax.axis_index("tp")
    ctx_index = lax.axis_index("ctx")
    e8, spread, gather, upper, lower = constants(inner, heads)

    per_head = inner // heads

    w_joined, halo, normed = gathered(
        w_x, w_bc, w_dt.T, norm_gain, tokens
    )
    n = lax.axis_size("fsdp")
    chain = lax.axis_size("ctx")

    def shape(dims, kind):
        return jax.ShapeDtypeStruct(dims, kind)

    def whole(x):
        return (x, x.shape, lambda i: (0,) * x.ndim)

    def by_rows(x, flip=False):
        if flip:
            return (x, (STRETCH, x.shape[1]), lambda i: (blocks - 1 - i, 0))
        return (x, (STRETCH, x.shape[1]), lambda i: (i, 0))

    def by_lanes(x, flip=False):
        if flip:
            return (x, (x.shape[0], STRETCH), lambda i: (0, blocks - 1 - i))
        return (x, (x.shape[0], STRETCH), lambda i: (0, i))

    def by_block(x, flip=False):
        if flip:
            return (x, (1,) + x.shape[1:], lambda i: (blocks - 1 - i, 0, 0))
        return (x, (1,) + x.shape[1:], lambda i: (i, 0, 0))

    def fixed(x):
        return (x, x.shape, lambda i: (0,) * len(x.shape))

    info_in = (lengths, None, "smem")
    params_in = (None, None, "par")
    raw = (
        norm_gain, gate_gain, conv_x_w, conv_bc_w, conv_x_b, conv_bc_b, dt_bias, a_log, d_skip
    )
    run = functools.partial(call, raw=raw)
    state_dims = (blocks, states, inner)
    subs = 2 if blocks % 2 == 0 else 1

    def several(entries, kinds):
        scales = {"r": (subs, 1), "l": (1, subs), "b": (subs, 1, 1)}
        grown = []
        for entry, kind in zip(entries, kinds):
            if kind == "w":
                grown.append(entry)
                continue
            dims = tuple(d * k for d, k in zip(entry[1], scales[kind]))
            grown.append((entry[0], dims, entry[2]))
        return grown

    dma = pltpu.SemaphoreType.DMA
    entry_in, entry_out = "wrwwwwwwww", "rrrrrlllbwwww"
    (
        joined_x, joined_bc, vbc, slope_x, slope_bc, pre, step, cum, s_part, end_state, decay,
        incoming, wz_out,
    ) = run(
        in_turn(
            functools.partial(entry_kernel, rows, n, chain), 1, entry_in + entry_out + "w" * 9
        ),
        blocks,
        list([
            info_in, by_rows(normed), whole(halo), params_in, whole(w_joined), whole(upper),
            whole(spread(0)), whole(e8), (w_z, None, "any"), (w_out.T, None, "any"),
        ]),
        list([
            by_rows(shape((rows, inner), bf16)),
            by_rows(shape((rows, 2 * states), bf16)),
            by_rows(shape((rows, width), bf16)),
            by_rows(shape((rows, inner), bf16)),
            by_rows(shape((rows, 2 * states), f32)),
            by_lanes(shape((HEAD_ROWS, rows), f32)),
            by_lanes(shape((HEAD_ROWS, rows), f32)),
            by_lanes(shape((HEAD_ROWS, rows), f32)),
            by_block(shape(state_dims, f32)),
            fixed(shape((states, inner), bf16)),
            fixed(shape((1, inner), f32)),
            fixed(shape((states, inner), bf16)),
            (shape((model, 2 * inner), bf16), None, "any"),
        ]),
        [
            pltpu.VMEM((8, width), f32),
            pltpu.VMEM((states, inner), f32),
            pltpu.VMEM((1, inner), f32),
            pltpu.VMEM(((taps - 1) * STRETCH, STRETCH), bf16),
            pltpu.VMEM((states, inner), bf16),
            dma((n - 1, 2)),
            dma((n - 1, 2)),
            dma((2,)),
            dma((2,)),
        ],
        remote_id=4,
    )
    if chain > 2:
        incoming = entering(decay, end_state, "ctx", False)
    mix_in, mix_out = "wrllbwrrwwwww", "rrrlbl"
    z_part, out, gn, sums, state_in, branch = run(
        in_turn(functools.partial(mix_kernel, rows), subs, mix_in + mix_out + "wr"),
        blocks // subs,
        several(
            [
                info_in, by_rows(vbc), by_lanes(step), by_lanes(cum), by_block(s_part),
                whole(incoming), by_rows(normed), by_rows(grad_out), whole(wz_out), params_in,
                whole(spread(1)), whole(spread(2)), whole(e8),
            ],
            mix_in,
        ),
        several(
            [
                by_rows(shape((rows, inner), f32)),
                by_rows(shape((rows, inner), f32)),
                by_rows(shape((rows, inner), f32)),
                by_lanes(shape((2, rows), f32)),
                by_block(shape(state_dims, bf16)),
                by_lanes(shape((model, rows), bf16)),
            ],
            mix_out,
        ),
        [pltpu.VMEM((states, inner), f32), pltpu.VMEM((subs * STRETCH, STRETCH), f32)],
    )
    branch = lax.psum_scatter(branch, "tp", scatter_dimension=0, tiled=True)
    sums = total_over_tp(sums)
    g_z, g_b, g_c, normed_two, a_sum, gs_part, start_state, misc_gate = run(
        functools.partial(gate_kernel, rows),
        blocks,
        [
            info_in, by_lanes(sums, True), by_lanes(cum, True), by_rows(out, True),
            by_rows(z_part, True), by_rows(gn, True), by_rows(vbc, True), by_block(state_in, True),
            params_in, whole(spread(2)), whole(e8), whole(gather(0)),
        ],
        [
            by_rows(shape((rows, inner), bf16), True),
            by_rows(shape((rows, inner), bf16), True),
            by_rows(shape((rows, inner), bf16), True),
            by_rows(shape((rows, inner), bf16), True),
            by_lanes(shape((HEAD_ROWS, rows), f32), True),
            by_block(shape(state_dims, f32), True),
            fixed(shape((states, inner), bf16)),
            fixed(shape((8, inner), f32)),
        ],
        [pltpu.VMEM((states, inner), f32)],
    )
    sum_all = jnp.concatenate([gather(0), gather(1)[:inner]], axis=0)
    outgoing = entering(decay, start_state, "ctx", True)
    g_cat, tail, head, misc_scan, misc_dt = run(
        functools.partial(scan_kernel, rows),
        blocks,
        [
            info_in, by_rows(vbc, True), by_rows(g_b, True), by_rows(g_c, True),
            by_lanes(step, True), by_lanes(cum, True), by_lanes(pre, True), by_lanes(a_sum, True),
            by_block(state_in, True), by_block(gs_part, True), whole(outgoing),
            by_rows(slope_x, True), by_rows(slope_bc, True), by_rows(joined_x, True),
            by_rows(joined_bc, True), params_in, whole(spread(1)),
            whole(spread(2)), whole(e8), whole(sum_all), whole(lower),
        ],
        [
            by_rows(shape((rows, width + 128), bf16), True),
            fixed(shape((8, width), f32)),
            fixed(shape((8, width), f32)),
            fixed(shape((8, width), f32)),
            fixed(shape((2 * HEAD_ROWS, STRETCH), f32)),
        ],
        [
            pltpu.VMEM((states, inner), f32),
            pltpu.VMEM((8, width), f32),
            pltpu.VMEM((STRETCH, STRETCH), f32),
            pltpu.VMEM((STRETCH, STRETCH), f32),
            pltpu.VMEM((STRETCH, 3 * inner), bf16),
        ],
    )
    next_rows = passed_along(head, "ctx", -1)
    feature = jnp.arange(model, dtype=jnp.int32) // slice_width
    mine = (feature == tp_index).astype(f32)[None, :]
    last_joined = jnp.concatenate([joined_x[rows - 16 :], joined_bc[rows - 16 :]], axis=1)
    def exit_call(first, extra_in, extra_out, scratch):
        top = count = blocks

        def flipped(x):
            return (x, (STRETCH, x.shape[1]), lambda i: (top - 1 - i, 0))

        return run(
            functools.partial(exit_kernel, rows, top, first),
            count,
            [
                info_in, flipped(tokens), flipped(grad_out), whole(mine), flipped(g_z),
                flipped(g_cat), params_in, whole(wz_out), whole(w_joined),
            ]
            + extra_in,
            [
                (
                    shape((model, count * STRETCH), bf16),
                    (model, STRETCH),
                    lambda i: (0, count - 1 - i),
                ),
                fixed(shape((1, model), f32)),
            ]
            + extra_out,
            scratch,
        )

    g_resid, gain_part, rim, rim_w = exit_call(
        True,
        [whole(tail), whole(next_rows), whole(last_joined)],
        [fixed(shape((16, width), bf16)), fixed(shape((8, width), f32))],
        [pltpu.VMEM((16, width), f32)],
    )
    g_resid = lax.psum_scatter(g_resid, "tp", scatter_dimension=0, tiled=True)

    part_out = tn(grad_out, normed_two)
    part_z = tn(normed, g_z)
    part_cat = tn(normed, g_cat)
    part_rim = tn(normed[rows - 16 :], rim)
    part_cat = part_cat + jnp.pad(part_rim, ((0, 0), (0, 128)))
    s_all, s_small, s_wide = reduced(
        (part_out, part_z, part_cat),
        (misc_scan, rim_w, misc_gate, misc_dt, gain_part),
        2 * states,
    )
    if lax.axis_size("ctx") > 2:
        s_all, s_small, s_wide = jax.tree.map(
            lambda part: lax.psum(0.5 * part, "ctx"), (s_all, s_small, s_wide)
        )
    grad_w_out = s_all[:, :inner].T
    grad_w_z = s_all[:, inner : 2 * inner]
    s_cat = s_all[:, 2 * inner :]
    grad_w_x = s_cat[:, :inner]
    grad_w_bc = s_cat[:, inner : inner + 2 * states]
    grad_w_dt = s_cat[:, inner + 2 * states : inner + 2 * states + heads]
    grad_conv_x_w = s_small[:taps, :inner]
    grad_conv_x_b = s_small[taps, :inner]
    grad_gate_gain = s_small[0, width : width + inner]
    grad_d_skip = jnp.sum(s_small[1, width : width + inner].reshape(heads, per_head), axis=1)
    dt_at = width + inner
    grad_a_log = jnp.sum(s_small[:heads, dt_at : dt_at + STRETCH], axis=1)
    grad_dt_bias = jnp.sum(s_small[:heads, dt_at + STRETCH : dt_at + 2 * STRETCH], axis=1)
    grad_conv_bc_w = s_wide[:taps, : 2 * states]
    grad_conv_bc_b = s_wide[taps, : 2 * states]
    here = tp_index * slice_width
    grad_norm_gain = lax.dynamic_slice_in_dim(s_wide[0, 2 * states :], here, slice_width, 0)
    place = tp_index.astype(jnp.int32)[None]

    wide = 2 * STRETCH
    layer_out = run(
        functools.partial(finish_kernel, tp_size),
        blocks // 2,
        [
            (place, None, "smem"),
            (branch, (slice_width, wide), lambda i: (0, i)),
            (tokens, (wide, model), lambda i: (i, 0)),
            (sums, (2, wide), lambda i: (0, i)),
        ],
        [(shape((slice_width, rows), bf16), (slice_width, wide), lambda i: (0, i))],
        [],
    )[0].T
    grad_tokens = g_resid.T
    return (
        layer_out, grad_tokens, grad_norm_gain, grad_w_z, grad_w_x, grad_w_bc, grad_w_dt,
        grad_conv_x_w, grad_conv_x_b, grad_conv_bc_w, grad_conv_bc_b, grad_dt_bias, grad_a_log,
        grad_d_skip, grad_gate_gain, grad_w_out,
    )


def solution(mesh):
    both = ("fsdp", "ctx")
    in_specs = (
        P(both, None), P(both, None), P("fsdp", None), P(), P("fsdp", "tp"), P("fsdp", "tp"),
        P("fsdp", None), P("fsdp", "tp"), P(None, "tp"), P("tp"), P(), P(), P("tp"), P("tp"),
        P("tp"), P("tp"), P("tp", "fsdp"),
    )
    out_specs = (
        P(both, "tp"), P(both, "tp"), P("tp"), P("fsdp", "tp"), P("fsdp", "tp"), P("fsdp", None),
        P("fsdp", "tp"), P(None, "tp"), P("tp"), P(), P(), P("tp"), P("tp"), P("tp"), P("tp"),
        P("tp", "fsdp"),
    )
    return jax.shard_map(local, mesh=mesh, in_specs=in_specs, out_specs=out_specs, check_vma=False)
```
